32 devices in a mesh: fsdp: 32 (over z, y, x, core).
Axes of the slice: x: 2, y: 2, z: 4, core: 2. Of those that a mesh axis runs over, the one named last changes fastest.
Arguments:
- x_in: bfloat16 [32, 1024, 1536], P('fsdp')
- ln1_w: float32 [1536], P('fsdp')
- w_qkv: bfloat16 [1536, 3, 12, 128], P('fsdp')
- w_out: bfloat16 [1536, 1536], P('fsdp')
- ln2_w: float32 [1536], P('fsdp')
- w_up: bfloat16 [1536, 6144], P('fsdp')
- w_down: bfloat16 [6144, 1536], P('fsdp')
- dy_out: bfloat16 [32, 1024, 1536], P('fsdp')
Outputs:
- output 1: bfloat16 [32, 1024, 1536], P('fsdp')
- output 2: bfloat16 [32, 1024, 1536], P('fsdp')
- output 3: float32 [1536], P('fsdp')
- output 4: float32 [1536, 3, 12, 128], P('fsdp')
- output 5: float32 [1536, 1536], P('fsdp')
- output 6: float32 [1536], P('fsdp')
- output 7: float32 [1536, 6144], P('fsdp')
- output 8: float32 [6144, 1536], P('fsdp')
All inputs are finite; a program needn't handle non-finite values.
Results may differ from the reference program's by a relative error of at most 0.018174.
Values are sent between devices in bfloat16 or wider.
A program may use at most 1 GiB of HBM per device.

```python
import math
import jax
import jax.numpy as jnp
from jax import lax

BATCH = 32
SEQ = 1024
D = 1536
HEADS = 12

HEAD = D // HEADS
FF = 4 * D
EPS = 1e-5


def alibi_slopes(n_heads):
    padded = 2 ** math.ceil(math.log2(n_heads))
    base_list = [2.0 ** (-8.0 * (k + 1) / padded) for k in range(padded)]
    ordered = base_list if padded == n_heads else base_list[1::2] + base_list[0::2]
    return jnp.array(ordered[:n_heads], dtype=jnp.float32)


def to_bf16(values):
    return values.astype(jnp.bfloat16).astype(jnp.float32)


def layer_norm(x_rows, ln_gain):
    row_mean = jnp.mean(x_rows, axis=-1, keepdims=True)
    centered = x_rows - row_mean
    row_var = jnp.mean(centered * centered, axis=-1, keepdims=True)
    return centered * lax.rsqrt(row_var + EPS) * ln_gain


def block(x_seq, params):
    ln1_w, w_qkv, w_out, ln2_w, w_up, w_down = params
    h_one = to_bf16(layer_norm(x_seq, ln1_w))
    qkv_rows = to_bf16(jnp.dot(h_one, w_qkv.reshape(D, 3 * D), preferred_element_type=jnp.float32))
    qkv_rows = qkv_rows.reshape(SEQ, 3, HEADS, HEAD)
    q_rows, k_rows, v_rows = qkv_rows[:, 0], qkv_rows[:, 1], qkv_rows[:, 2]
    scores = jnp.einsum('qhe,khe->hqk', q_rows, k_rows) / math.sqrt(HEAD)
    positions = jnp.arange(SEQ)
    rel_pos = (positions[:, None] - positions[None, :]).astype(jnp.float32)
    scores = jnp.where(rel_pos >= 0, scores - alibi_slopes(HEADS)[:, None, None] * rel_pos, -jnp.inf)
    attn_probs = to_bf16(jax.nn.softmax(scores, axis=-1))
    attn_out = to_bf16(jnp.einsum('hqk,khe->qhe', attn_probs, v_rows)).reshape(SEQ, D)
    x_mid = to_bf16(x_seq + jnp.dot(attn_out, w_out, preferred_element_type=jnp.float32))
    h_two = to_bf16(layer_norm(x_mid, ln2_w))
    gelu_out = to_bf16(jax.nn.gelu(jnp.dot(h_two, w_up, preferred_element_type=jnp.float32), approximate=False))
    return to_bf16(x_mid + jnp.dot(gelu_out, w_down, preferred_element_type=jnp.float32))


def setup_inputs(seed: int = 0) -> dict:
    subkeys = jax.random.split(jax.random.key(seed), 8)
    in_scale = 1.0 / math.sqrt(D)
    x_in = jax.random.normal(subkeys[0], (BATCH, SEQ, D), jnp.float32).astype(jnp.bfloat16)
    ln1_w = 1.0 + 0.3 * jax.random.normal(subkeys[1], (D,), jnp.float32)
    w_qkv = (jax.random.normal(subkeys[2], (D, 3, HEADS, HEAD), jnp.float32) * in_scale).astype(jnp.bfloat16)
    w_out = (jax.random.normal(subkeys[3], (D, D), jnp.float32) * in_scale).astype(jnp.bfloat16)
    ln2_w = 1.0 + 0.3 * jax.random.normal(subkeys[4], (D,), jnp.float32)
    w_up = (jax.random.normal(subkeys[5], (D, FF), jnp.float32) * in_scale).astype(jnp.bfloat16)
    w_down = (jax.random.normal(subkeys[6], (FF, D), jnp.float32) / math.sqrt(FF)).astype(jnp.bfloat16)
    dy_out = jax.random.normal(subkeys[7], (BATCH, SEQ, D), jnp.float32).astype(jnp.bfloat16)
    return {'x_in': x_in, 'ln1_w': ln1_w, 'w_qkv': w_qkv, 'w_out': w_out, 'ln2_w': ln2_w, 'w_up': w_up, 'w_down': w_down, 'dy_out': dy_out}


def reference(x_in, ln1_w, w_qkv, w_out, ln2_w, w_up, w_down, dy_out):
    params = (ln1_w, w_qkv.astype(jnp.float32), w_out.astype(jnp.float32), ln2_w, w_up.astype(jnp.float32), w_down.astype(jnp.float32))

    def seq_step(grad_sum, seq_pair):
        x_seq, dy_seq = seq_pair
        y_seq, pull_back = jax.vjp(block, x_seq.astype(jnp.float32), params)
        dx_seq, g_params = pull_back(dy_seq.astype(jnp.float32))
        grad_sum = tuple(a + g for a, g in zip(grad_sum, g_params))
        return grad_sum, (y_seq.astype(jnp.bfloat16), dx_seq.astype(jnp.bfloat16))

    zero_grads = tuple(jnp.zeros_like(p) for p in params)
    grads, outs_seq = lax.scan(seq_step, zero_grads, (x_in, dy_out))
    return (outs_seq[0], outs_seq[1], grads[0], grads[1], grads[2], grads[3], grads[4], grads[5])
```

```python
import functools
import math

import jax
import jax.numpy as jnp
from jax import lax
from jax.experimental import pallas as pl
from jax.experimental.pallas import tpu as pltpu
from jax.sharding import PartitionSpec as P

EPS = 1e-5
SUB = 768
HALF = SUB // 2
RB = 48
F32, BF16 = jnp.float32, jnp.bfloat16
VMEM_LIMIT = 62 * 1024 * 1024
MESH = pl.DeviceIdType.MESH
HBM = pltpu.MemorySpace.HBM


def sds(shape, dtype):
    return jax.ShapeDtypeStruct(shape, dtype)


def dot(a, b, ca=1, cb=0):
    return lax.dot_general(a, b, (((ca,), (cb,)), ((), ())), preferred_element_type=F32)


def clip(t, n):
    return jnp.minimum(jnp.maximum(t, 0), n - 1)


class Phase:
    def __init__(self, n, ins, outs, body, start=None):
        self.n, self.ins, self.outs, self.body, self.start = n, ins, outs, body, start


def coords():
    me = lax.axis_index('fsdp')
    return me, me // 8, (me // 4) % 2, (me // 2) % 2, me % 2


def peers():
    me, z, y, x, c = coords()
    zs = [lax.rem(me + 8 * d, 32) for d in (1, 2, 3)]
    return zs, me + 4 - 8 * y, me + 2 - 4 * x, me + 1 - 2 * c


def remote(src, dst, ssem, rsem, dev):
    return pltpu.make_async_remote_copy(src_ref=src, dst_ref=dst, send_sem=ssem, recv_sem=rsem, device_id=(dev,), device_id_type=MESH)


class Unit:
    def __init__(self, rows, cols):
        self.nc, self.nr = cols // SUB, rows // RB
        self.count = self.nc * self.nr

    def at(self, u, half=None):
        col = pl.multiple_of((u % self.nc) * SUB, HALF)
        width = SUB
        if half is not None:
            col, width = pl.multiple_of(col + half * HALF, HALF), HALF
        rows = slice(None) if self.nr == 1 else pl.ds(pl.multiple_of((u // self.nc) * RB, 16), RB)
        return rows, pl.ds(col, width)


class Gather:
    def __init__(self, shard, off=0):
        rows, cols = shard.shape
        self.unit, self.off = Unit(rows, cols), off
        self.s = self.unit.count
        self.k = off + self.s + 3
        self.ins = [(shard, pl.BlockSpec(memory_space=pltpu.VMEM))]
        self.outs = [(sds((4, 2, 2, 2, rows, cols), BF16), pl.BlockSpec(memory_space=HBM))]
        self.scratch = [pltpu.SemaphoreType.DMA((self.s, 8)), pltpu.SemaphoreType.DMA((self.s, 8)), pltpu.SemaphoreType.DMA]

    def copies(self, stage, u, refs):
        shard, full, ss, rs, _ = refs
        me, z, y, x, c = coords()
        zs, yp, xp, cp = peers()
        at = self.unit.at
        if stage == 0:
            r, q = at(u)
            return [remote(shard.at[r, q], full.at[z, y, x, c, r, q], ss.at[u, d], rs.at[u, d], zs[d]) for d in range(3)]
        if stage == 3:
            r, q = at(u)
            v = full.at[:, :, :, c, r, q]
            return [remote(v, v, ss.at[u, 7], rs.at[u, 7], cp)]
        (ra, qa), (rb, qb) = at(u, 0), at(u, 1)
        if stage == 1:
            va, vb = full.at[:, y, x, c, ra, qa], full.at[:, y, x, c, rb, qb]
            return [remote(va, va, ss.at[u, 3], rs.at[u, 3], yp), remote(vb, vb, ss.at[u, 4], rs.at[u, 4], xp)]
        va, vb = full.at[:, :, x, c, ra, qa], full.at[:, y, :, c, rb, qb]
        return [remote(va, va, ss.at[u, 5], rs.at[u, 5], xp), remote(vb, vb, ss.at[u, 6], rs.at[u, 6], yp)]

    def step(self, k, fire, refs):
        shard, full, ss, rs, ls = refs
        me, z, y, x, c = coords()
        s = self.s

        @pl.when(fire & (k == 0))
        def _():
            own = pltpu.make_async_copy(shard, full.at[z, y, x, c], ls)
            own.start()

            @pl.loop(0, s)
            def _(u):
                for cp in self.copies(0, u, refs):
                    cp.start()

            own.wait()

        for stage in (1, 2, 3):
            u = k - self.off - (stage - 1)

            @pl.when(fire & (u >= 0) & (u < s))
            def _(stage=stage, u=u):
                for cp in self.copies(stage - 1, u, refs):
                    cp.wait_recv()
                for cp in self.copies(stage, u, refs):
                    cp.start()

        @pl.when(fire & (k == self.off + s + 2))
        def _():
            @pl.loop(0, s)
            def _(u):
                for cp in self.copies(3, u, refs):
                    cp.wait_recv()
                for stage in range(4):
                    for cp in self.copies(stage, u, refs):
                        cp.wait_send()


class GatherSmall:
    def __init__(self, tile):
        self.k = 5
        self.ins = [(tile, pl.BlockSpec(memory_space=pltpu.VMEM))]
        self.outs = [(sds((4, 2, 2, 2) + tile.shape, F32), pl.BlockSpec(memory_space=HBM))]
        self.scratch = [pltpu.SemaphoreType.DMA((6,)), pltpu.SemaphoreType.DMA((6,)), pltpu.SemaphoreType.DMA]

    def copies(self, stage, refs):
        tile, full, ss, rs, _ = refs
        me, z, y, x, c = coords()
        zs, yp, xp, cp = peers()
        if stage == 0:
            return [remote(tile, full.at[z, y, x, c], ss.at[d], rs.at[d], zs[d]) for d in range(3)]
        v, dev = ((full.at[:, y, x, c], yp), (full.at[:, :, x, c], xp), (full.at[:, :, :, c], cp))[stage - 1]
        return [remote(v, v, ss.at[2 + stage], rs.at[2 + stage], dev)]

    def step(self, k, fire, refs):
        tile, full, ss, rs, ls = refs
        me, z, y, x, c = coords()
        for stage in range(5):
            @pl.when(fire & (k == stage))
            def _(stage=stage):
                if stage == 0:
                    own = pltpu.make_async_copy(tile, full.at[z, y, x, c], ls)
                    own.start()
                else:
                    for cp in self.copies(stage - 1, refs):
                        cp.wait_recv()
                if stage < 4:
                    for cp in self.copies(stage, refs):
                        cp.start()
                else:
                    for st in range(4):
                        for cp in self.copies(st, refs):
                            cp.wait_send()
                if stage == 0:
                    own.wait()


class Scatter:
    def __init__(self, grad, u0, s, off=0):
        rows, cols = grad.shape[-2:]
        self.unit, self.u0, self.s, self.off = Unit(rows, cols), u0, s, off
        self.k = off + s + 3
        nc = self.unit.nc
        self.ins = [(grad, pl.BlockSpec(memory_space=HBM))]
        nblk = s // nc if self.unit.nr > 1 else 1
        ncol = nc if self.unit.nr > 1 else s
        self.out_shape = sds((nblk * RB, ncol * SUB), F32)
        self.ncol = ncol
        self.scratch = [
            pltpu.VMEM((s, 4, 2, 2, RB, SUB), BF16),
            pltpu.VMEM((2, 4, 2, 2, RB, SUB), BF16),
            pltpu.VMEM((2, s, 4, 2, RB, HALF), BF16),
            pltpu.VMEM((s, 4, RB, SUB), BF16),
            pltpu.VMEM((s, 3, RB, SUB), BF16),
            pltpu.SemaphoreType.DMA((s, 8)), pltpu.SemaphoreType.DMA((s, 8)), pltpu.SemaphoreType.DMA((2,))]

    def out_spec(self, kmap):
        ncol = self.ncol

        def index(t):
            u = clip(kmap(t) - self.off - 3, self.s)
            return u // ncol, u % ncol

        self.outs = [(self.out_shape, pl.BlockSpec((RB, SUB), index))]

    def local(self, u, refs):
        grad, _, _, own, _, _, _, _, _, ls = refs
        me, z, y, x, c = coords()
        r, q = self.unit.at(self.u0 + u)
        slot = u % 2
        return pltpu.make_async_copy(grad.at[:, :, :, c, r, q], own.at[slot], ls.at[slot])

    def copies(self, stage, u, refs):
        grad, _, got, own, two, three, four, ss, rs, ls = refs
        me, z, y, x, c = coords()
        zs, yp, xp, cp = peers()
        a, b = pl.ds(0, HALF), pl.ds(HALF, HALF)
        if stage == 0:
            r, q = self.unit.at(self.u0 + u)
            return [remote(grad.at[:, :, :, 1 - c, r, q], got.at[u], ss.at[u, 0], rs.at[u, 0], cp)]
        if stage == 1:
            return [remote(got.at[u, :, 1 - y, :, :, a], two.at[0, u], ss.at[u, 1], rs.at[u, 1], yp),
                    remote(got.at[u, :, :, 1 - x, :, b], two.at[1, u], ss.at[u, 2], rs.at[u, 2], xp)]
        if stage == 2:
            return [remote(two.at[0, u, :, 1 - x], three.at[u, :, :, a], ss.at[u, 3], rs.at[u, 3], xp),
                    remote(two.at[1, u, :, 1 - y], three.at[u, :, :, b], ss.at[u, 4], rs.at[u, 4], yp)]
        return [remote(three.at[u, lax.rem(z + d + 1, 4)], four.at[u, d], ss.at[u, 5 + d], rs.at[u, 5 + d], zs[d]) for d in range(3)]

    def add(self, stage, u, refs):
        grad, out, got, own, two, three, four, ss, rs, ls = refs
        me, z, y, x, c = coords()
        a, b = pl.ds(0, HALF), pl.ds(HALF, HALF)
        if stage == 1:
            slot = u % 2
            for zz in range(4):
                for yy in range(2):
                    for xx in range(2):
                        got[u, zz, yy, xx] = got[u, zz, yy, xx] + own[slot, zz, yy, xx]
        elif stage == 2:
            for zz in range(4):
                for i in range(2):
                    two[0, u, zz, i] = two[0, u, zz, i] + got[u, zz, y, i, :, a]
                    two[1, u, zz, i] = two[1, u, zz, i] + got[u, zz, i, x, :, b]
        elif stage == 3:
            for zz in range(4):
                three[u, zz, :, a] = three[u, zz, :, a] + two[0, u, zz, x]
                three[u, zz, :, b] = three[u, zz, :, b] + two[1, u, zz, y]
        else:
            total = three[u, z].astype(F32)
            for d in range(3):
                total = total + four[u, d].astype(F32)
            out[...] = total

    def step(self, k, fire, refs):
        s = self.s

        @pl.when(fire & (k == 0))
        def _():
            @pl.loop(0, s)
            def _(u):
                for cp in self.copies(0, u, refs):
                    cp.start()

            for u in range(min(2, s)):
                self.local(u, refs).start()

        for stage in (1, 2, 3, 4):
            u = k - self.off - (stage - 1)

            @pl.when(fire & (u >= 0) & (u < s))
            def _(stage=stage, u=u):
                for cp in self.copies(stage - 1, u, refs):
                    cp.wait_recv()
                if stage == 1:
                    self.local(u, refs).wait()
                self.add(stage, u, refs)
                if stage < 4:
                    for cp in self.copies(stage, u, refs):
                        cp.start()
                if stage == 1:
                    @pl.when(u + 2 < s)
                    def _():
                        self.local(u + 2, refs).start()

        @pl.when(fire & (k == self.off + s + 2))
        def _():
            @pl.loop(0, s)
            def _(u):
                for stage in range(4):
                    for cp in self.copies(stage, u, refs):
                        cp.wait_send()


def host(name, cid, phases, comms=(), shared=(), steps=None, cost=None):
    k_all = max([c.k for c in comms], default=1)
    at = 0
    for p in phases:
        p.at = at if p.start is None else p.start
        at = p.at + p.n
    total = max(at, k_all, steps or 0)
    kmap = (lambda t: t) if total == k_all else (lambda t: (t * k_all) // total)
    ins, in_specs, outs, out_specs, scratch = [], [], [], [], []
    for p in phases:
        for arr, block, index in p.ins:
            ins.append(arr)
            if block == 'smem':
                in_specs.append(pl.BlockSpec(memory_space=pltpu.SMEM))
            elif index is None:
                in_specs.append(pl.BlockSpec(block, functools.partial(lambda n, t: (0,) * n, len(block)), pipeline_mode=pl.Buffered(1)))
            else:
                in_specs.append(pl.BlockSpec(block, functools.partial(lambda p, f, t: f(clip(t - p.at, p.n)), p, index)))
        for shape, block, index in p.outs:
            outs.append(shape)
            out_specs.append(pl.BlockSpec(block, functools.partial(lambda p, f, t: f(clip(t - p.at, p.n)), p, index)))
    for c in comms:
        if isinstance(c, Scatter):
            c.out_spec(kmap)
        for arr, spec in c.ins:
            ins.append(arr)
            in_specs.append(spec)
        for shape, spec in c.outs:
            outs.append(shape)
            out_specs.append(spec)
        scratch += c.scratch
    scratch += list(shared)

    def kernel(*refs):
        refs = list(refs)
        rin, rout, rscr = refs[:len(ins)], refs[len(ins):len(ins) + len(outs)], refs[len(ins) + len(outs):]
        t = pl.program_id(0)
        if comms:
            @pl.when(t == 0)
            def _():
                zs, yp, xp, cp = peers()
                bar = pltpu.get_barrier_semaphore()
                for dev in (*zs, yp, xp, cp):
                    pl.semaphore_signal(bar, inc=1, device_id=(dev,), device_id_type=MESH)
                pl.semaphore_wait(bar, 6)
        i, o, s = sum(len(p.ins) for p in phases), sum(len(p.outs) for p in phases), 0
        k = kmap(t)
        fire = (t == 0) | (k != kmap(jnp.maximum(t - 1, 0)))
        for c in comms:
            ni, no, ns = len(c.ins), len(c.outs), len(c.scratch)
            c.step(k, fire, rin[i:i + ni] + rout[o:o + no] + rscr[s:s + ns])
            i, o, s = i + ni, o + no, s + ns
        extra = rscr[s:]
        i = o = 0
        for p in phases:
            pi, po = rin[i:i + len(p.ins)], rout[o:o + len(p.outs)]
            i, o = i + len(p.ins), o + len(p.outs)

            @pl.when((t >= p.at) & (t < p.at + p.n))
            def _(p=p, pi=pi, po=po):
                p.body(t - p.at, pi, po, extra)

    params = dict(dimension_semantics=("arbitrary",), vmem_limit_bytes=VMEM_LIMIT)
    if comms:
        params.update(collective_id=cid, has_side_effects=True)
    got = pl.pallas_call(kernel, grid=(total,), in_specs=in_specs, out_specs=out_specs, out_shape=outs, scratch_shapes=scratch,
                         compiler_params=pltpu.CompilerParams(**params), name=name,
                         cost_estimate=pl.CostEstimate(flops=int(cost or 2e10), bytes_accessed=int(3e7), transcendentals=0))(*ins)
    return list(got)


def norm_parts(t):
    mean = jnp.mean(t, axis=-1, keepdims=True)
    cen = t - mean
    rstd = lax.rsqrt(jnp.mean(cen * cen, axis=-1, keepdims=True) + EPS)
    return cen * rstd, rstd


def norm_back(d, t, w):
    xhat, rstd = norm_parts(t)
    dh = d * w
    m1 = jnp.mean(dh, axis=-1, keepdims=True)
    m2 = jnp.mean(dh * xhat, axis=-1, keepdims=True)
    return rstd * (dh - m1 - xhat * m2), jnp.sum(d * xhat, axis=0, keepdims=True)


def alibi_slopes(n_heads):
    padded = 2 ** math.ceil(math.log2(n_heads))
    base = [2.0 ** (-8.0 * (k + 1) / padded) for k in range(padded)]
    ordered = base if padded == n_heads else base[1::2] + base[0::2]
    return jnp.array(ordered[:n_heads], dtype=F32)


def causal(i, tq, slope):
    row = lax.broadcasted_iota(jnp.int32, (tq, tq), 0)
    col = lax.broadcasted_iota(jnp.int32, (tq, tq), 1)
    rel = (row - col).astype(F32)
    diag = slope * rel
    past = None
    if i:
        r = lax.broadcasted_iota(jnp.int32, (tq, i * tq), 0) + i * tq
        q = lax.broadcasted_iota(jnp.int32, (tq, i * tq), 1)
        past = slope * (r - q).astype(F32)
    return past, diag, row >= col


def attn_fwd(q_ref, k_ref, v_ref, o_ref, l_ref, slope, scale, tq):
    n = q_ref.shape[0] // tq
    for i in range(n):
        q = q_ref[i * tq:(i + 1) * tq, :]
        past, diag, keep = causal(i, tq, slope)
        sd = jnp.where(keep, dot(q, k_ref[i * tq:(i + 1) * tq, :], 1, 1) * scale - diag, -jnp.inf)
        m = jnp.max(sd, axis=-1, keepdims=True)
        if i:
            sp = dot(q, k_ref[:i * tq, :], 1, 1) * scale - past
            m = jnp.maximum(m, jnp.max(sp, axis=-1, keepdims=True))
            ep = jnp.exp(sp - m)
        ed = jnp.exp(sd - m)
        l = jnp.sum(ed, axis=-1, keepdims=True)
        if i:
            l = l + jnp.sum(ep, axis=-1, keepdims=True)
        inv = 1.0 / l
        o = dot((ed * inv).astype(BF16), v_ref[i * tq:(i + 1) * tq, :])
        if i:
            o = o + dot((ep * inv).astype(BF16), v_ref[:i * tq, :])
        o_ref[i * tq:(i + 1) * tq, :] = o.astype(BF16)
        l_ref[i * tq:(i + 1) * tq, :] = m + jnp.log(l)


def attn_bwd(q_ref, k_ref, v_ref, a_ref, da_ref, l_ref, dq_ref, dk_ref, dv_ref, dk_s, dv_s, slope, scale, tq):
    n = q_ref.shape[0] // tq
    dk_s[...] = jnp.zeros_like(dk_s)
    dv_s[...] = jnp.zeros_like(dv_s)
    for i in range(n):
        rows = slice(i * tq, (i + 1) * tq)
        q, da = q_ref[rows, :], da_ref[rows, :]
        lse = l_ref[rows, :]
        delta = jnp.sum(da.astype(F32) * a_ref[rows, :].astype(F32), axis=-1, keepdims=True)
        past, diag, keep = causal(i, tq, slope)
        dq = None
        for own in ((True,) if i == 0 else (True, False)):
            keys = rows if own else slice(0, i * tq)
            kk, vv = k_ref[keys, :], v_ref[keys, :]
            s = dot(q, kk, 1, 1) * scale - (diag if own else past)
            p = jnp.exp(s - lse)
            if own:
                p = jnp.where(keep, p, 0.0)
            ds = (p * (dot(da, vv, 1, 1) - delta) * scale).astype(BF16)
            dv_s[keys, :] += dot(p.astype(BF16), da, 0, 0)
            dk_s[keys, :] += dot(ds, q, 0, 0)
            part = dot(ds, kk)
            dq = part if dq is None else dq + part
        dq_ref[rows, :] = dq.astype(BF16)
    dk_ref[...] = dk_s[...].astype(BF16)
    dv_ref[...] = dv_s[...].astype(BF16)


def small_sum(cid, vec):
    shape = vec.shape

    def kernel(v_ref, o_ref, acc, got, ss, rs):
        zs, yp, xp, cp = peers()
        bar = pltpu.get_barrier_semaphore()
        for dev in (*zs, yp, xp, cp):
            pl.semaphore_signal(bar, inc=1, device_id=(dev,), device_id_type=MESH)
        pl.semaphore_wait(bar, 6)
        sends = []
        for i, dev in enumerate((cp, xp, yp)):
            cur = v_ref if i == 0 else acc.at[i - 1]
            sends.append(remote(cur, got.at[i], ss.at[i], rs.at[i], dev))
            sends[-1].start()
            sends[-1].wait_recv()
            acc[i] = cur[...] + got[i]
        last = [remote(acc.at[2], got.at[3 + d], ss.at[3 + d], rs.at[3 + d], zs[d]) for d in range(3)]
        for s in last:
            s.start()
        total = acc[2]
        for d, s in enumerate(last):
            s.wait_recv()
            total = total + got[3 + d]
        o_ref[...] = total
        for s in sends + last:
            s.wait_send()

    vm = pl.BlockSpec(memory_space=pltpu.VMEM)
    return pl.pallas_call(kernel, in_specs=[vm], out_specs=vm, out_shape=sds(shape, F32),
                          scratch_shapes=[pltpu.VMEM((3,) + shape, F32), pltpu.VMEM((6,) + shape, F32),
                                          pltpu.SemaphoreType.DMA((6,)), pltpu.SemaphoreType.DMA((6,))],
                          compiler_params=pltpu.CompilerParams(collective_id=cid, has_side_effects=True), name='small_sum')(vec)


def row_map(i):
    return i, 0


def col_map(i):
    return 0, i


def rows_of(a, n):
    return a, (n, a.shape[1]), row_map


def cols_of(a, n):
    return a, (a.shape[0], n), col_map


def heads_of(a, n, off=0):
    return a, (n,) + a.shape[1:], lambda i: (i + off, 0, 0)


def whole(a):
    return a, a.shape, None


def put(ref, i, part):
    @pl.when(i == 0)
    def _():
        ref[...] = part

    @pl.when(i > 0)
    def _():
        ref[...] += part


def side_by_side(ref, n):
    return jnp.concatenate([ref[j] for j in range(n)], axis=1)


def local_step(x, ln1, wq, wo, ln2, wu, wd, dy, comm=True):
    seq, d = x.shape
    heads, hd, ft = 12, 128, 512
    ff, nq, per = wu.shape[1], 3 * d, SUB // hd
    scale = 1 / math.sqrt(hd)
    tm = tq = min(256, seq)
    nm, nf = seq // tm, ff // ft
    slopes = (alibi_slopes(heads), 'smem', None)
    b16 = lambda *shape: sds(shape, BF16)
    f32 = lambda *shape: sds(shape, F32)
    vm16 = lambda *shape: pltpu.VMEM(shape, BF16)
    vm32 = lambda *shape: pltpu.VMEM(shape, F32)
    act, wide, vec = b16(seq, d), b16(seq, ff), f32(1, d)
    one_vec = (vec, vec.shape, lambda i: (0, 0))
    band = lambda i: pl.ds(pl.multiple_of(i * tm, tm), tm)
    G = (lambda *w: [Gather(s, off) for s, off in w]) if comm else (lambda *w: [])
    flat = lambda full: full.reshape(-1, full.shape[-1])

    def S(*parts):
        if not comm:
            return []
        return [Scatter(a.reshape(4, 2, 2, 2, -1, a.shape[-1]), u0, n, off) for a, u0, n, off in parts]

    if comm:
        tile = jnp.pad(jnp.stack([ln1, ln2]), ((0, 6), (0, 128 - ln1.shape[0])))
        fq, lns = host('ag_qkv', 1, [], G((wq, 0)) + [GatherSmall(tile)])
        fq = flat(fq)
        w1, w2 = lns.reshape(-1, 8, 128)[:, :2, :ln1.shape[0]].transpose(1, 0, 2).reshape(2, 1, d)
    else:
        fq, w1, w2 = wq, ln1.reshape(1, d), ln2.reshape(1, d)

    def ln1_body(i, ins, outs, ext):
        (xr, lw), (ht,), (_, h1) = ins, outs, ext
        xhat, _ = norm_parts(xr[...].astype(F32))
        h = (xhat * lw[...]).astype(BF16)
        h1[band(i), :] = h
        ht[...] = h.T

    def qkv_body(i, ins, outs, ext):
        (w,), (o,), (qkv, h1) = ins, outs, ext
        r = dot(h1[...], w[...]).astype(BF16)
        for j in range(per):
            qkv[i * per + j] = r[:, j * hd:(j + 1) * hd]
            o[j] = r[:, j * hd:(j + 1) * hd]

    def attn_body(i, ins, outs, ext):
        (sl,), (o, l), (qkv, _) = ins, outs, ext
        attn_fwd(qkv.at[i], qkv.at[heads + i], qkv.at[2 * heads + i], o, l.at[0], sl[i], scale, tq)

    pb = [Phase(nm, [rows_of(x, tm), whole(w1)], [cols_of(b16(d, seq), tm)], ln1_body),
          Phase(nq // SUB, [cols_of(fq, SUB)], [heads_of(b16(3 * heads, seq, hd), per)], qkv_body),
          Phase(heads, [slopes], [cols_of(act, hd), heads_of(f32(heads, seq, 1), 1)], attn_body)]
    h1t, qkv, attn, lse, *full = host('attn_fwd', 2, pb, G((wo, 0), (wu, 2)), shared=[vm16(3 * heads, seq, hd), vm16(seq, d)])
    fo, fu = map(flat, full) if comm else (wo, wu)

    def out_body(i, ins, outs, ext):
        (xs, a, w, lw), (o, ht), (h2,) = ins, outs, ext
        x1 = (xs[...].astype(F32) + dot(a[...], w[...])).astype(BF16)
        o[...] = x1
        xhat, _ = norm_parts(x1.astype(F32))
        h = (xhat * lw[...]).astype(BF16)
        h2[band(i), :] = h
        ht[...] = h.T

    def up_body(i, ins, outs, ext):
        (w, dyr), (go, gpo, gd), (h2,) = ins, outs, ext
        u = dot(h2[...], w[...])
        cdf = 0.5 * (1.0 + lax.erf(u * math.sqrt(0.5)))
        g = (u * cdf).astype(BF16)
        go[...] = g
        gpo[...] = cdf + u * (jnp.exp(-0.5 * u * u) * math.sqrt(0.5 / math.pi))
        gd[...] = dot(g, dyr[...], 0, 0).astype(BF16)

    pc = [Phase(nm, [rows_of(x, tm), rows_of(attn, tm), whole(fo), whole(w2)], [rows_of(act, tm), cols_of(b16(d, seq), tm)], out_body),
          Phase(nf, [cols_of(fu, ft), whole(dy)], [cols_of(wide, ft), cols_of(f32(seq, ff), ft), rows_of(b16(ff, d), ft)], up_body)]
    x1, h2t, g, gp, g_down, *full = host('up', 3, pc, G((wd, 0)), shared=[vm16(seq, d)])
    fd, = map(flat, full) if comm else (wd,)

    def dup_body(i, ins, outs, ext):
        (dyr, w, gr, gpr, ht), (duo, gu), (acc,) = ins, outs, ext
        du = (dot(dyr[...], w[...], 1, 1) * gpr[...]).astype(BF16)
        duo[...] = du
        gu[...] = dot(ht[...], du).astype(BF16)
        put(acc, i, dot(gr[...], w[...]))

    def y_body(i, ins, outs, ext):
        (xr,), (o,), (acc,) = ins, outs, ext
        o[...] = (xr[...].astype(F32) + acc[band(i), :]).astype(BF16)

    pd = [Phase(nf, [whole(dy), rows_of(fd, ft), cols_of(g, ft), cols_of(gp, ft), whole(h2t)], [cols_of(wide, ft), cols_of(b16(d, ff), ft)], dup_body),
          Phase(nm, [rows_of(x1, tm)], [rows_of(act, tm)], y_body)]
    d_up, g_up, y, *r_down = host('dup', 4, pd, S((g_down, 0, 8, 0)), shared=[vm32(seq, d)])

    def dh2_body(i, ins, outs, ext):
        (du, w), (acc, _) = ins, ext
        put(acc, i, dot(du[...], w[...], 1, 1))

    def ln2b_body(i, ins, outs, ext):
        (xr, dyr, lw), (dmo, gwo), (acc, dmb) = ins, outs, ext
        dx, gw = norm_back(acc[band(i), :], xr[...].astype(F32), lw[...])
        dm = dyr[...].astype(F32) + dx
        dmo[...] = dm
        dmb[band(i), :] = dm.astype(BF16)
        put(gwo, i, gw)

    def dattn_body(i, ins, outs, ext):
        (w, a), (da, go), (_, dmb) = ins, outs, ext
        da[...] = dot(dmb[...], w[...], 1, 1).astype(BF16)
        go[...] = dot(a[...], dmb[...], 0, 0).astype(BF16)

    pe = [Phase(nf, [cols_of(d_up, ft), cols_of(fu, ft)], [], dh2_body),
          Phase(nm, [rows_of(x1, tm), rows_of(dy, tm), whole(w2)], [rows_of(f32(seq, d), tm), one_vec], ln2b_body),
          Phase(d // ft, [rows_of(fo, ft), cols_of(attn, ft)], [cols_of(act, ft), rows_of(b16(d, d), ft)], dattn_body)]
    d_mid, g_ln2, d_attn, g_out, *r_up0 = host('dh2', 5, pe, S((g_up, 0, 4, 0)), shared=[vm32(seq, d), vm16(seq, d)])

    def battn_body(i, ins, outs, ext):
        (q, k, v, a, da, l, sl), (o,), (dk, dv) = ins, outs, ext
        attn_bwd(q.at[0], k.at[0], v.at[0], a, da, l.at[0], *(o.at[j, 0] for j in range(3)), dk, dv, sl[i], scale, tq)

    pf = [Phase(heads, [*(heads_of(qkv, 1, j * heads) for j in range(3)), cols_of(attn, hd), cols_of(d_attn, hd), heads_of(lse, 1), slopes],
                [(b16(3, heads, seq, hd), (3, 1, seq, hd), lambda i: (0, i, 0, 0))], battn_body)]
    d_qkv, *r_up1 = host('attn_bwd', 6, pf, S((g_up, 4, 4, 0)), shared=[vm32(seq, hd), vm32(seq, hd)])
    d_qkv = d_qkv.reshape(3 * heads, seq, hd)

    def gqkv_body(i, ins, outs, ext):
        (ht, dq), (o,) = ins, outs
        o[...] = dot(ht[...], side_by_side(dq, per)).astype(BF16)

    g_qkv, = host('gqkv', 0, [Phase(nq // SUB, [whole(h1t), heads_of(d_qkv, per)], [cols_of(b16(d, nq), SUB)], gqkv_body)])

    def dh1_body(i, ins, outs, ext):
        (dq, w), (acc,) = ins, ext
        put(acc, i, dot(side_by_side(dq, per // 2), w[...], 1, 1))

    def ln1b_body(i, ins, outs, ext):
        (xr, dm, lw), (o, gwo), (acc,) = ins, outs, ext
        dx, gw = norm_back(acc[band(i), :], xr[...].astype(F32), lw[...])
        o[...] = (dm[...] + dx).astype(BF16)
        put(gwo, i, gw)

    ph = [Phase(nq // HALF, [heads_of(d_qkv, per // 2), cols_of(fq, HALF)], [], dh1_body),
          Phase(nm, [rows_of(x, tm), rows_of(d_mid, tm), whole(w1)], [rows_of(act, tm), one_vec], ln1b_body)]
    dx, g_ln1, *r_last = host('dh1', 7, ph, S((g_out, 0, 2, 0), (g_qkv, 0, 6, 2)), shared=[vm32(seq, d)])
    if comm:
        (g_down,), (g_out, g_qkv), g_up = r_down, r_last, jnp.concatenate(r_up0 + r_up1, axis=1)
    return y, dx, g_ln1, g_qkv, g_out, g_ln2, g_up, g_down


def solution(mesh):
    row_spec = P('fsdp')

    def step(x_in, ln1_w, w_qkv, w_out, ln2_w, w_up, w_down, dy_out):
        rows, _, heads, hd = w_qkv.shape
        d = x_in.shape[-1]
        y, dx, g_ln1, g_qkv, g_out, g_ln2, g_up, g_down = local_step(
            x_in[0], ln1_w, w_qkv.reshape(rows, -1), w_out, ln2_w, w_up, w_down, dy_out[0])
        sums = small_sum(8, jnp.concatenate([g_ln1, g_ln2, jnp.zeros((6, d), F32)], axis=0))
        mine = lax.dynamic_slice_in_dim(sums, lax.axis_index('fsdp') * rows, rows, axis=1)
        return (y[None], dx[None], mine[0], g_qkv.reshape(rows, 3, heads, hd), g_out, mine[1], g_up, g_down)

    return jax.shard_map(step, mesh=mesh, in_specs=(row_spec,) * 8, out_specs=(row_spec,) * 8, check_vma=False)
```

```python
import functools
import math

import jax
import jax.numpy as jnp
from jax import lax
from jax.experimental import pallas as pl
from jax.experimental.pallas import tpu as pltpu
from jax.sharding import PartitionSpec as P

EPS = 1e-5
SUB = 512
HALF = SUB // 2
LEAD = 3
RB = 48
F32, BF16 = jnp.float32, jnp.bfloat16
VMEM_LIMIT = 62 * 1024 * 1024
MESH = pl.DeviceIdType.MESH
HBM = pltpu.MemorySpace.HBM
CHIPS = (4, 2, 2)


def sds(shape, dtype):
    return jax.ShapeDtypeStruct(shape, dtype)


def dot(a, b, ca=1, cb=0):
    return lax.dot_general(a, b, (((ca,), (cb,)), ((), ())), preferred_element_type=F32)


def dot_t(a, b):
    return dot(a, b, 1, 1)


def t_dot(a, b):
    return dot(a, b, 0, 0)


def over_rows(f):
    return functools.partial(f, axis=-1, keepdims=True)


row_sum, row_max, row_mean = map(over_rows, (jnp.sum, jnp.max, jnp.mean))


def clip(t, n):
    return jnp.minimum(jnp.maximum(t, 0), n - 1)


class Phase:
    def __init__(self, n, ins, outs, body):
        self.n, self.ins, self.outs, self.body = n, ins, outs, body


def quot(a, b):
    return a // b if isinstance(a, int) else lax.div(a, b)


def rest(a, b):
    return a % b if isinstance(a, int) else lax.rem(a, b)


HERE = {}


def locate():
    me = lax.axis_index('fsdp')
    z, y, x, c = quot(me, 8), rest(quot(me, 4), 2), rest(quot(me, 2), 2), rest(me, 2)
    HERE.update(coords=(me, z, y, x, c), peers=([rest(me + 8 * d, 32) for d in (1, 2, 3)], me + 4 - 8 * y, me + 2 - 4 * x, me + 1 - 2 * c),
                zs=[rest(z + d, 4) for d in (1, 2, 3)])


def coords():
    return HERE['coords']


def peers():
    return HERE['peers']


def remote(src, dst, ssem, rsem, dev):
    return pltpu.make_async_remote_copy(src_ref=src, dst_ref=dst, send_sem=ssem, recv_sem=rsem, device_id=(dev,), device_id_type=MESH)


class Unit:
    def __init__(self, rows, cols):
        self.nc, self.nr = cols // SUB, rows // RB
        self.count = self.nc * self.nr

    def at(self, u, half=None):
        col = pl.multiple_of(rest(u, self.nc) * SUB, HALF)
        width = SUB
        if half is not None:
            col, width = pl.multiple_of(col + half * HALF, HALF), HALF
        rows = slice(None) if self.nr == 1 else pl.ds(pl.multiple_of(quot(u, self.nc) * RB, 16), RB)
        return rows, pl.ds(col, width)


class Gather:
    def __init__(self, weights, k0, k1):
        self.k0, self.k1 = k0, k1
        self.k = k1 - k0 + 1
        self.z0 = k0 + LEAD if k0 else 0
        self.z1 = k1 + LEAD
        self.w, self.ins, self.outs, self.alias = [], [], [], []
        for shard, full, first in weights:
            unit = Unit(*shard.shape)
            self.w.append((len(self.ins), unit, first, first + unit.count, full is None))
            self.ins.append((shard, pl.BlockSpec(memory_space=pltpu.VMEM)))
            if full is not None:
                self.alias.append((len(self.ins), len(self.outs)))
                self.ins.append((full, pl.BlockSpec(memory_space=HBM)))
            self.outs.append((sds(CHIPS + (2,) + shard.shape, BF16), pl.BlockSpec(memory_space=HBM)))
        self.base = max(k0 - 2, 0)
        n = self.z1 - self.base
        self.scratch = [pltpu.SemaphoreType.DMA((n, 8)), pltpu.SemaphoreType.DMA((n, 8)), pltpu.SemaphoreType.DMA((len(weights),))]

    def copies(self, stage, w, u, refs):
        i, unit, first, _, _ = self.w[w]
        shard, full = refs[i], refs[len(self.ins) + w]
        sems = lambda i: (refs[-3].at[u - self.base, i], refs[-2].at[u - self.base, i])
        me, z, y, x, c = coords()
        zs, yp, xp, cp = peers()
        r, q = unit.at(u - first)
        if stage == 0:
            return [remote(shard.at[r, q], full.at[z, y, x, c, r, q], *sems(d), zs[d]) for d in range(3)]
        if stage == 3:
            v = full.at[:, :, :, c, r, q]
            return [remote(v, v, *sems(7), cp)]
        out = []
        for half in range(2):
            r, q = unit.at(u - first, half)
            j = 2 * stage + 1 + half
            if stage == 1:
                v = full.at[:, y, x, c, r, q]
            else:
                v = full.at[:, y, :, c, r, q] if half else full.at[:, :, x, c, r, q]
            out.append(remote(v, v, *sems(j), xp if half == stage % 2 else yp))
        return out

    def each(self, lo, hi, u, fn):
        for w, (_, _, first, last, _) in enumerate(self.w):
            a, b = max(lo, first), min(hi, last)
            if a < b:
                if u is None:
                    pl.loop(a, b)(functools.partial(fn, w))
                else:
                    pl.when((u >= a) & (u < b))(functools.partial(fn, w, u))

    def go(self, stage, w, u, refs):
        for cp in self.copies(stage, w, u, refs):
            cp.start()

    def arrive(self, stage, w, u, refs):
        for cp in self.copies(stage, w, u, refs):
            cp.wait_recv()

    def left(self, stage, w, u, refs):
        for cp in self.copies(stage, w, u, refs):
            cp.wait_send()

    def step(self, k, fire, refs):
        me, z, y, x, c = coords()
        k0, k1, k = self.k0, self.k1, k + self.k0
        span = [(self.z0, self.z1), (k0, k1), (max(k0 - 1, 0), k1 - 1), (max(k0 - 2, 0), k1 - 2)]

        @pl.when(fire & (k == k0))
        def _():
            own = [pltpu.make_async_copy(refs[i], refs[len(self.ins) + w].at[z, y, x, c], refs[-1].at[w])
                   for w, (i, _, _, _, fresh) in enumerate(self.w) if fresh]
            for cp in own:
                cp.start()
            if k0 == 0:
                self.each(0, LEAD, None, lambda w, u: self.go(0, w, u, refs))
            for cp in own:
                cp.wait()

        @pl.when(fire & (k < k1))
        def _():
            self.each(*span[0], k + LEAD, lambda w, u: self.go(0, w, u, refs))
            for stage in (1, 2, 3):
                u = k + 1 - stage
                lo, hi = span[stage - 1]
                self.each(lo, hi, u, lambda w, u: self.arrive(stage - 1, w, u, refs))
                self.each(*span[stage], u, lambda w, u: self.go(stage, w, u, refs))

        @pl.when(fire & (k == k1))
        def _():
            for stage in range(4):
                lo, hi = span[stage]
                self.each(max(lo, k1 - stage) if stage < 3 else lo, hi, None, lambda w, u: self.arrive(stage, w, u, refs))
                self.each(lo, hi, None, lambda w, u: self.left(stage, w, u, refs))


class GatherSmall:
    def __init__(self, tile):
        self.k, self.alias = 5, []
        self.ins = [(tile, pl.BlockSpec(memory_space=pltpu.VMEM))]
        self.outs = [(sds(CHIPS + (2,) + tile.shape, F32), pl.BlockSpec(memory_space=HBM))]
        self.scratch = [pltpu.SemaphoreType.DMA((6,)), pltpu.SemaphoreType.DMA((6,)), pltpu.SemaphoreType.DMA]

    def copies(self, stage, refs):
        tile, full, ss, rs, _ = refs
        me, z, y, x, c = coords()
        zs, yp, xp, cp = peers()
        if stage == 0:
            return [remote(tile, full.at[z, y, x, c], ss.at[d], rs.at[d], zs[d]) for d in range(3)]
        v, dev = ((full.at[:, y, x, c], yp), (full.at[:, :, x, c], xp), (full.at[:, :, :, c], cp))[stage - 1]
        return [remote(v, v, ss.at[2 + stage], rs.at[2 + stage], dev)]

    def step(self, k, fire, refs):
        tile, full, ss, rs, ls = refs
        me, z, y, x, c = coords()
        for stage in range(5):
            @pl.when(fire & (k == stage))
            def _(stage=stage):
                if stage == 0:
                    own = pltpu.make_async_copy(tile, full.at[z, y, x, c], ls)
                    own.start()
                else:
                    for cp in self.copies(stage - 1, refs):
                        cp.wait_recv()
                if stage < 4:
                    for cp in self.copies(stage, refs):
                        cp.start()
                else:
                    for st in range(4):
                        for cp in self.copies(st, refs):
                            cp.wait_send()
                if stage == 0:
                    own.wait()


class Scatter:
    def __init__(self, grads, carry=None, last=False):
        self.last, self.carried = last, carry is not None
        self.parts, self.ins, n = [], [], 0
        for g, u0, m in grads:
            self.parts.append((n, n + m, u0, Unit(*g.shape[-2:])))
            self.ins.append((g, pl.BlockSpec(memory_space=HBM)))
            n += m
        self.n = n
        self.first = 0 if self.carried else 2
        self.done = n + (2 if last else 0)
        self.k = n + (3 if last else 1)
        self.two_shape, self.three_shape = (2, 4, 2, RB, HALF), (4, RB, SUB)
        if self.carried:
            self.ins += [(a, pl.BlockSpec(memory_space=pltpu.VMEM)) for a in carry]
        self.scratch = [
            pltpu.VMEM((n, *CHIPS, RB, SUB), BF16),
            pltpu.VMEM((2, *CHIPS, RB, SUB), BF16),
            pltpu.VMEM((n + 2,) + self.two_shape, BF16),
            pltpu.VMEM((n + 2,) + self.three_shape, BF16),
            pltpu.VMEM((n + 2, 3, RB, SUB), BF16),
            pltpu.SemaphoreType.DMA((n + 2, 8)), pltpu.SemaphoreType.DMA((n + 2, 8)), pltpu.SemaphoreType.DMA((2,))]
        self.alias = []

    def out_spec(self, kmap):
        lo, count = self.first, self.done - self.first
        self.outs = [(sds((count, RB, SUB), F32), pl.BlockSpec((1, RB, SUB), lambda t: (clip(kmap(t) - 1 - lo, count), 0, 0)))]
        if not self.last:
            self.outs += [(sds(shape, BF16), pl.BlockSpec(memory_space=pltpu.VMEM)) for shape in (self.two_shape, self.three_shape)]

    def source(self, j, refs, fn):
        for i, (a, b, u0, unit) in enumerate(self.parts):
            if len(self.parts) == 1:
                fn(refs[i], *unit.at(u0 + j - 2))
            else:
                pl.when((j - 2 >= a) & (j - 2 < b))(lambda: fn(refs[i], *unit.at(u0 + j - 2 - a)))

    def bufs(self, refs):
        return refs[len(self.ins) + len(self.outs):]

    def local(self, j, refs, act):
        me, z, y, x, c = coords()
        own, ls = self.bufs(refs)[1], self.bufs(refs)[-1]
        slot = rest(j, 2)
        self.source(j, refs, lambda g, r, q: act(pltpu.make_async_copy(g.at[:, :, :, c, r, q], own.at[slot], ls.at[slot])))

    def swap(self, j, refs, act):
        me, z, y, x, c = coords()
        got, ss, rs = self.bufs(refs)[0], *self.bufs(refs)[-3:-1]
        cp = peers()[-1]
        self.source(j, refs, lambda g, r, q: act(remote(g.at[:, :, :, 1 - c, r, q], got.at[j - 2], ss.at[j, 0], rs.at[j, 0], cp)))

    def copies(self, stage, j, refs):
        got, own, two, three, four, ss, rs, ls = self.bufs(refs)
        me, z, y, x, c = coords()
        zs, yp, xp, cp = peers()
        a, b = pl.ds(0, HALF), pl.ds(HALF, HALF)
        if stage == 1:
            pairs = [(got.at[j - 2, :, 1 - y, :, :, a], two.at[j, 0], yp), (got.at[j - 2, :, :, 1 - x, :, b], two.at[j, 1], xp)]
        elif stage == 2:
            pairs = [(two.at[j, 0, :, 1 - x], three.at[j, :, :, a], xp), (two.at[j, 1, :, 1 - y], three.at[j, :, :, b], yp)]
        else:
            pairs = [(three.at[j, HERE['zs'][d]], four.at[j, d], zs[d]) for d in range(3)]
        return [remote(src, dst, ss.at[j, 2 * stage + i - 1], rs.at[j, 2 * stage + i - 1], dev) for i, (src, dst, dev) in enumerate(pairs)]

    def add(self, stage, j, refs):
        got, own, two, three, four, ss, rs, ls = self.bufs(refs)
        me, z, y, x, c = coords()
        a, b = pl.ds(0, HALF), pl.ds(HALF, HALF)
        slot = rest(j, 2)
        if stage == 1:
            @pl.loop(0, 4)
            def _(zz):
                for yy in range(2):
                    for xx in range(2):
                        got[j - 2, zz, yy, xx] += own[slot, zz, yy, xx]
        elif stage == 2:
            @pl.loop(0, 4)
            def _(zz):
                for i in range(2):
                    two[j, 0, zz, i] += got[j - 2, zz, y, i, :, a]
                    two[j, 1, zz, i] += got[j - 2, zz, i, x, :, b]
        elif stage == 3:
            for zz in range(4):
                three[j, zz, :, a] += two[j, 0, zz, x]
                three[j, zz, :, b] += two[j, 1, zz, y]
        else:
            total = three[j, z].astype(F32)
            for d in range(3):
                total += four[j, d].astype(F32)
            refs[len(self.ins)][0] = total

    def step(self, k, fire, refs):
        n, last = self.n, self.last
        got, own, two, three, four, ss, rs, ls = self.bufs(refs)
        start = lambda cp: cp.start()

        def go(stage, j):
            for cp in self.copies(stage, j, refs):
                cp.start()

        @pl.when(fire & (k == 0))
        def _():
            if self.carried:
                two[1] = refs[len(self.ins) - 2][...]
                three[0] = refs[len(self.ins) - 1][...]
                go(2, 1)
                go(3, 0)

            @pl.loop(2, n + 2)
            def _(j):
                self.swap(j, refs, start)

            for j in range(2, min(4, n + 2)):
                self.local(j, refs, start)

        for stage in (1, 2, 3, 4):
            j = k + 3 - stage
            low = (2, 2, 1, 0)[stage - 1] if self.carried else 2

            @pl.when(fire & (j >= low) & (j < n + 2))
            def _(stage=stage, j=j):
                if stage == 1:
                    self.swap(j, refs, lambda cp: cp.wait_recv())
                    self.local(j, refs, lambda cp: cp.wait())
                else:
                    for cp in self.copies(stage - 1, j, refs):
                        cp.wait_recv()
                self.add(stage, j, refs)
                if stage < 4:
                    if last or stage == 1:
                        go(stage, j)
                    else:
                        pl.when(k < n)(lambda: go(stage, j))
                if stage == 1:
                    pl.when(j < n)(lambda: self.local(j + 2, refs, start))

        @pl.when(fire & (k == self.k - 1))
        def _():
            for stage in (1, 2, 3):
                low = (2, 1, 0)[stage - 1] if self.carried else 2
                high = n + 2 if last else n + 3 - stage

                @pl.loop(low, high)
                def _(j):
                    for cp in self.copies(stage, j, refs):
                        cp.wait_send()

            @pl.loop(2, n + 2)
            def _(j):
                self.swap(j, refs, lambda cp: cp.wait_send())

            if not last:
                refs[len(self.ins) + 1][...] = two[n + 1]
                refs[len(self.ins) + 2][...] = three[n]


class SmallSum:
    def __init__(self, row, t0, d):
        self.t0, self.k = t0, 1
        self.ins = [(row, pl.BlockSpec(memory_space=pltpu.VMEM))]
        self.outs = [(sds((8, d), F32), pl.BlockSpec(memory_space=pltpu.VMEM))]
        self.alias = []
        self.scratch = [pltpu.VMEM((4, 8, d), F32), pltpu.VMEM((6, 8, d), F32), pltpu.SemaphoreType.DMA((6,)), pltpu.SemaphoreType.DMA((6,))]

    def run(self, t, mine, refs):
        row, out, acc, got, ss, rs = refs
        zs, yp, xp, cp = peers()
        near = (cp, xp, yp, *zs)
        n = len(near) - len(zs)
        copies = [remote(acc.at[min(i, n)], got.at[i], ss.at[i], rs.at[i], dev) for i, dev in enumerate(near)]

        for i in range(n + 2):
            @pl.when(t == self.t0 + i)
            def _(i=i):
                if not i:
                    acc[i] = jnp.zeros_like(acc[i])
                    acc[i, pl.ds(0, 1)] = mine[...]
                    acc[i, pl.ds(1, 1)] = row[...]
                elif i <= n:
                    copies[i - 1].wait_recv()
                    acc[i] = acc[i - 1] + got[i - 1]
                else:
                    total = acc[n]
                    for j in range(n, len(near)):
                        copies[j].wait_recv()
                        total += got[j]
                    out[...] = total
                    for copy in copies:
                        copy.wait_send()
                for copy in copies[i:i + 1] if i < n else copies[n:] if i == n else ():
                    copy.start()


def host(name, cid, phases, comms=(), shared=(), cost=None):
    k_all = max([c.k for c in comms], default=1)
    at = 0
    for p in phases:
        p.at = at
        at = at + p.n
    small = [c for c in comms if isinstance(c, SmallSum)]
    total = max(at + 5 * len(small), k_all)
    kmap = lambda t: t if total == k_all else quot(t * (k_all - 1), total - 1)
    ins, in_specs, outs, out_specs, scratch, alias, resident = [], [], [], [], [], {}, []
    for p in phases:
        for arr, block, index in p.ins:
            if block == 'smem':
                in_specs.append(pl.BlockSpec(memory_space=pltpu.SMEM))
            elif index is None:
                resident.append((len(ins), p.at))
                in_specs.append(pl.BlockSpec(memory_space=HBM))
            else:
                in_specs.append(pl.BlockSpec(block, functools.partial(lambda p, f, t: f(clip(t - p.at, p.n)), p, index)))
            ins.append(arr)
        for shape, block, index in p.outs:
            outs.append(shape)
            out_specs.append(pl.BlockSpec(block, functools.partial(lambda p, f, t: f(clip(t - p.at, p.n)), p, index)))
    for c in comms:
        if isinstance(c, Scatter):
            c.out_spec(kmap)
        alias.update({len(ins) + i: len(outs) + o for i, o in c.alias})
        for arr, spec in c.ins:
            ins.append(arr)
            in_specs.append(spec)
        for shape, spec in c.outs:
            outs.append(shape)
            out_specs.append(spec)
        scratch += c.scratch
    scratch += [pltpu.VMEM(ins[i].shape, ins[i].dtype) for i, _ in resident] + [pltpu.SemaphoreType.DMA((max(len(resident), 1),))]
    scratch += list(shared)

    def kernel(*refs):
        refs = list(refs)
        rin, rout, rscr = refs[:len(ins)], refs[len(ins):len(ins) + len(outs)], refs[len(ins) + len(outs):]
        t = pl.program_id(0)
        if comms:
            locate()

            @pl.when(t == 0)
            def _():
                zs, yp, xp, cp = peers()
                near = (*zs, yp, xp, cp)
                bar = pltpu.get_barrier_semaphore()
                for dev in near:
                    pl.semaphore_signal(bar, inc=1, device_id=(dev,), device_id_type=MESH)
                pl.semaphore_wait(bar, len(near))
        i, o, s = sum(len(p.ins) for p in phases), sum(len(p.outs) for p in phases), 0
        k = kmap(t)
        fire = (t == 0) | (k != kmap(jnp.maximum(t - 1, 0)))
        for c in comms:
            ni, no, ns = len(c.ins), len(c.outs), len(c.scratch)
            crefs = rin[i:i + ni] + rout[o:o + no] + rscr[s:s + ns]
            if c in small:
                small_refs = crefs
            else:
                c.step(k, fire, crefs)
            i, o, s = i + ni, o + no, s + ns
        held, rsem, extra = rscr[s:s + len(resident)], rscr[s + len(resident)], rscr[s + len(resident) + 1:]
        loads = [(pltpu.make_async_copy(rin[i], h, rsem.at[n]), at) for n, ((i, at), h) in enumerate(zip(resident, held))]
        if loads:
            @pl.when(t == 0)
            def _():
                for cp, _ in loads:
                    cp.start()
        for cp, at in loads:
            pl.when(t == at)(cp.wait)
        for (i, _), h in zip(resident, held):
            rin[i] = h
        i = o = 0
        for p in phases:
            pi, po = rin[i:i + len(p.ins)], rout[o:o + len(p.outs)]
            i, o = i + len(p.ins), o + len(p.outs)

            @pl.when((t >= p.at) & (t < p.at + p.n))
            def _(p=p, pi=pi, po=po):
                p.body(t - p.at, pi, po, extra)

        for c in small:
            c.run(t, rout[o - 1], small_refs)

    params = dict(dimension_semantics=("arbitrary",), vmem_limit_bytes=VMEM_LIMIT)
    if comms:
        params.update(collective_id=cid, has_side_effects=True)
    got = pl.pallas_call(kernel, grid=(total,), in_specs=in_specs, out_specs=out_specs, out_shape=outs, scratch_shapes=scratch,
                         input_output_aliases=alias, compiler_params=pltpu.CompilerParams(**params), name=name,
                         cost_estimate=pl.CostEstimate(flops=2 ** 34, bytes_accessed=2 ** 25, transcendentals=0))(*ins)
    return list(got)


def norm_parts(t):
    mean = row_mean(t)
    cen = t - mean
    rstd = lax.rsqrt(row_mean(cen * cen) + EPS)
    return cen * rstd, rstd


def norm_back(d, t, w):
    xhat, rstd = norm_parts(t)
    dh = d * w
    m1 = row_mean(dh)
    m2 = row_mean(dh * xhat)
    return rstd * (dh - m1 - xhat * m2), jnp.sum(d * xhat, axis=0, keepdims=True)


def alibi_slopes(n_heads):
    padded = 2 ** math.ceil(math.log2(n_heads))
    base = [2.0 ** (-8.0 * (k + 1) / padded) for k in range(padded)]
    ordered = base if padded == n_heads else base[1::2] + base[0::2]
    return jnp.array(ordered[:n_heads], dtype=F32)


def causal(i, tq, slope):
    row = lax.broadcasted_iota(jnp.int32, (tq, tq), 0)
    col = lax.broadcasted_iota(jnp.int32, (tq, tq), 1)
    rel = (row - col).astype(F32)
    diag = slope * rel
    past = None
    if i:
        r = lax.broadcasted_iota(jnp.int32, (tq, i * tq), 0) + i * tq
        q = lax.broadcasted_iota(jnp.int32, (tq, i * tq), 1)
        past = slope * (r - q).astype(F32)
    return past, diag, row >= col


def attn_fwd(q_ref, k_ref, v_ref, o_ref, l_ref, slope, scale, tq):
    n = q_ref.shape[0] // tq
    for i in range(n):
        rows, before = pl.ds(i * tq, tq), pl.ds(0, i * tq)
        q = q_ref[rows]
        past, diag, keep = causal(i, tq, slope)
        sd = jnp.where(keep, dot_t(q, k_ref[rows]) * scale - diag, -jnp.inf)
        m = row_max(sd)
        if i:
            sp = dot_t(q, k_ref[before]) * scale - past
            m = jnp.maximum(m, row_max(sp))
            ep = jnp.exp(sp - m)
        ed = jnp.exp(sd - m)
        l = row_sum(ed)
        if i:
            l = l + row_sum(ep)
        inv = 1.0 / l
        o = dot((ed * inv).astype(BF16), v_ref[rows])
        if i:
            o = o + dot((ep * inv).astype(BF16), v_ref[before])
        o_ref[rows] = o.astype(BF16)
        l_ref[rows] = m + jnp.log(l)


def attn_bwd(q_ref, k_ref, v_ref, a_ref, da_ref, l_ref, dq_ref, dk_ref, dv_ref, dk_s, dv_s, slope, scale, tq):
    n = q_ref.shape[0] // tq
    dk_s[...] = jnp.zeros_like(dk_s)
    dv_s[...] = jnp.zeros_like(dv_s)
    for i in range(n):
        rows, before = pl.ds(i * tq, tq), pl.ds(0, i * tq)
        q, da = q_ref[rows], da_ref[rows]
        lse = l_ref[rows]
        delta = row_sum(da.astype(F32) * a_ref[rows].astype(F32))
        past, diag, keep = causal(i, tq, slope)
        dq = None
        for own in ((True,) if i == 0 else (True, False)):
            keys = rows if own else before
            kk, vv = k_ref[keys], v_ref[keys]
            s = dot_t(q, kk) * scale - (diag if own else past)
            p = jnp.exp(s - lse)
            if own:
                p = jnp.where(keep, p, 0.0)
            ds = (p * (dot_t(da, vv) - delta) * scale).astype(BF16)
            dv_s[keys] += t_dot(p.astype(BF16), da)
            dk_s[keys] += t_dot(ds, q)
            part = dot(ds, kk)
            dq = part if dq is None else dq + part
        dq_ref[rows] = dq.astype(BF16)
    dk_ref[...] = dk_s[...].astype(BF16)
    dv_ref[...] = dv_s[...].astype(BF16)


def row_map(i):
    return i, 0


def col_map(i):
    return 0, i


def rows_of(a, n):
    return a, (n, a.shape[1]), row_map


def cols_of(a, n):
    return a, (a.shape[0], n), col_map


def heads_of(a, n, off=0):
    return a, (n,) + a.shape[1:], lambda i: (i + off, 0, 0)


def whole(a):
    return a, a.shape, None


def put(ref, i, part):
    @pl.when(i == 0)
    def _():
        ref[...] = part

    @pl.when(i > 0)
    def _():
        ref[...] += part


def side_by_side(ref, n):
    return jnp.concatenate([ref[j] for j in range(n)], axis=1)


def local_step(x, ln1, wq, wo, ln2, wu, wd, dy, comm=True):
    seq, d = x.shape
    heads, hd, ft = 12, 128, 512
    ff, nq, per = wu.shape[1], 3 * d, SUB // hd
    scale = 1 / math.sqrt(hd)
    tq = min(256, seq)
    tm = tq // 2
    nm, nf = seq // tm, ff // ft
    slopes = (alibi_slopes(heads), 'smem', None)
    b16 = lambda *shape: sds(shape, BF16)
    f32 = lambda *shape: sds(shape, F32)
    vm16 = lambda *shape: pltpu.VMEM(shape, BF16)
    vm32 = lambda *shape: pltpu.VMEM(shape, F32)
    act, wide, vec = b16(seq, d), b16(seq, ff), f32(1, d)
    one_vec = (vec, vec.shape, lambda i: (0, 0))
    band = lambda i: pl.ds(pl.multiple_of(i * tm, tm), tm)
    flat = lambda full: full.reshape(-1, full.shape[-1])
    order = [Unit(*w.shape).count for w in (wq, wo, wu, wd)]
    qs, os, us, ds = (sum(order[:i]) for i in range(4))
    ends = [os + 2, ds + 2, sum(order) + 2]

    def G(*window):
        return [Gather(*window)] if comm else []

    def S(parts, **kw):
        return [Scatter([(a.reshape(*CHIPS, 2, -1, a.shape[-1]), u0, n) for a, u0, n in parts], **kw)] if comm else []

    if comm:
        tile = jnp.pad(jnp.stack([ln1, ln2]), ((0, 6), (0, 128 - ln1.shape[0])))
        fq, fo, fu, lns = host('ag_qkv', 1, [], G([(wq, None, qs), (wo, None, os), (wu, None, us)], 0, ends[0]) + [GatherSmall(tile)])
        fq = flat(fq)
        w1, w2 = lns.reshape(-1, 8, 128)[:, :2, :ln1.shape[0]].transpose(1, 0, 2).reshape(2, 1, d)
    else:
        fq, fo, fu, w1, w2 = wq, wo, wu, ln1.reshape(1, d), ln2.reshape(1, d)

    def ln1_body(i, ins, outs, ext):
        (xr, lw), (ht,), (_, h1) = ins, outs, ext
        xhat, _ = norm_parts(xr[...].astype(F32))
        h = (xhat * lw[...]).astype(BF16)
        h1[band(i)] = h
        ht[...] = h.T

    def qkv_body(i, ins, outs, ext):
        (w,), (o,), (qkv, h1) = ins, outs, ext
        r = dot(h1[...], w[...]).astype(BF16)
        for j in range(per):
            qkv[i * per + j] = r[:, j * hd:(j + 1) * hd]
            o[j] = r[:, j * hd:(j + 1) * hd]

    def attn_body(i, ins, outs, ext):
        (sl,), (o, l), (qkv, _) = ins, outs, ext
        attn_fwd(qkv.at[i], qkv.at[heads + i], qkv.at[2 * heads + i], o, l.at[0], sl[i], scale, tq)

    pb = [Phase(nm, [rows_of(x, tm), whole(w1)], [cols_of(b16(d, seq), tm)], ln1_body),
          Phase(nq // SUB, [cols_of(fq, SUB)], [heads_of(b16(3 * heads, seq, hd), per)], qkv_body),
          Phase(heads, [slopes], [cols_of(act, hd), heads_of(f32(heads, seq, 1), 1)], attn_body)]
    h1t, qkv, attn, lse, *full = host('attn_fwd', 2, pb, G([(wo, fo, os), (wu, fu, us), (wd, None, ds)], ends[0], ends[1]),
                                      shared=[vm16(3 * heads, seq, hd), vm16(seq, d)])
    if comm:
        fo, fu, fd = full
        fo, fu = flat(fo), flat(fu)

    def out_body(i, ins, outs, ext):
        (xs, a, w, lw), (o, ht), (h2,) = ins, outs, ext
        x1 = (xs[...].astype(F32) + dot(a[...], w[...])).astype(BF16)
        o[...] = x1
        xhat, _ = norm_parts(x1.astype(F32))
        h = (xhat * lw[...]).astype(BF16)
        h2[band(i)] = h
        ht[...] = h.T

    def up_body(i, ins, outs, ext):
        (w, dyr), (go, gpo, gd), (h2,) = ins, outs, ext
        u = dot(h2[...], w[...])
        cdf = 0.5 * (1.0 + lax.erf(u * math.sqrt(0.5)))
        g = (u * cdf).astype(BF16)
        go[...] = g
        gpo[...] = cdf + u * (jnp.exp(-0.5 * u * u) * math.sqrt(0.5 / math.pi))
        gd[...] = t_dot(g, dyr[...]).astype(BF16)

    pc = [Phase(nm, [rows_of(x, tm), rows_of(attn, tm), whole(fo), whole(w2)], [rows_of(act, tm), cols_of(b16(d, seq), tm)], out_body),
          Phase(nf, [cols_of(fu, ft), whole(dy)], [cols_of(wide, ft), cols_of(f32(seq, ff), ft), rows_of(b16(ff, d), ft)], up_body)]
    x1, h2t, g, gp, g_down, *full = host('up', 3, pc, G([(wd, fd, ds)], ends[1], ends[2]) if comm else [], shared=[vm16(seq, d)])
    fd, = map(flat, full) if comm else (wd,)

    def dup_body(i, ins, outs, ext):
        (dyr, w, gr, gpr, ht), (duo, gu), (acc,) = ins, outs, ext
        du = (dot_t(dyr[...], w[...]) * gpr[...]).astype(BF16)
        duo[...] = du
        gu[...] = dot(ht[...], du).astype(BF16)
        put(acc, i, dot(gr[...], w[...]))

    def y_body(i, ins, outs, ext):
        (xr,), (o,), (acc,) = ins, outs, ext
        o[...] = (xr[...].astype(F32) + acc[band(i)]).astype(BF16)

    pd = [Phase(nf, [whole(dy), rows_of(fd, ft), cols_of(g, ft), cols_of(gp, ft), whole(h2t)], [cols_of(wide, ft), cols_of(b16(d, ff), ft)], dup_body),
          Phase(nm, [rows_of(x1, tm)], [rows_of(act, tm)], y_body)]
    n_down = Unit(ff // 32, d).count
    d_up, g_up, y, *r1 = host('dup', 4, pd, S([(g_down, 0, n_down)]), shared=[vm32(seq, d)])

    def dh2_body(i, ins, outs, ext):
        (du, w), (acc, _) = ins, ext
        put(acc, i, dot_t(du[...], w[...]))

    def ln2b_body(i, ins, outs, ext):
        (xr, dyr, lw), (dmo, gwo), (acc, dmb) = ins, outs, ext
        dx, gw = norm_back(acc[band(i)], xr[...].astype(F32), lw[...])
        dm = dyr[...].astype(F32) + dx
        dmo[...] = dm
        dmb[band(i)] = dm.astype(BF16)
        put(gwo, i, gw)

    def dattn_body(i, ins, outs, ext):
        (w, a), (da, go), (_, dmb) = ins, outs, ext
        da[...] = dot_t(dmb[...], w[...]).astype(BF16)
        go[...] = t_dot(a[...], dmb[...]).astype(BF16)

    pe = [Phase(nf, [cols_of(d_up, ft), cols_of(fu, ft)], [], dh2_body),
          Phase(nm, [rows_of(x1, tm), rows_of(dy, tm), whole(w2)], [rows_of(f32(seq, d), tm), one_vec], ln2b_body),
          Phase(d // ft, [rows_of(fo, ft), cols_of(attn, ft)], [cols_of(act, ft), rows_of(b16(d, d), ft)], dattn_body)]
    half = n_down // 2
    d_mid, g_ln2, d_attn, g_out, *r2 = host('dh2', 5, pe, S([(g_up, 0, half)], carry=r1[1:]), shared=[vm32(seq, d), vm16(seq, d)])

    def battn_body(i, ins, outs, ext):
        (q, k, v, a, da, l, sl), (o,), (dk, dv) = ins, outs, ext
        attn_bwd(q.at[0], k.at[0], v.at[0], a, da, l.at[0], *(o.at[j, 0] for j in range(3)), dk, dv, sl[i], scale, tq)

    pf = [Phase(heads, [*(heads_of(qkv, 1, j * heads) for j in range(3)), cols_of(attn, hd), cols_of(d_attn, hd), heads_of(lse, 1), slopes],
                [(b16(3, heads, seq, hd), (3, 1, seq, hd), lambda i: (0, i, 0, 0))], battn_body)]
    d_qkv, *r3 = host('attn_bwd', 6, pf, S([(g_up, half, half)], carry=r2[1:]), shared=[vm32(seq, hd), vm32(seq, hd)])
    d_qkv = d_qkv.reshape(3 * heads, seq, hd)

    def gqkv_body(i, ins, outs, ext):
        (ht, dq), (o,) = ins, outs
        o[...] = dot(ht[...], side_by_side(dq, per)).astype(BF16)

    g_qkv, *r4 = host('gqkv', 7, [Phase(nq // SUB, [whole(h1t), heads_of(d_qkv, per)], [cols_of(b16(d, nq), SUB)], gqkv_body)],
                      S([(g_out, 0, d // SUB)], carry=r3[1:]))

    def dh1_body(i, ins, outs, ext):
        (dq, w), (acc,) = ins, ext
        put(acc, i, dot_t(side_by_side(dq, 3), w[...]))

    def ln1b_body(i, ins, outs, ext):
        (xr, dm, lw), (o, gwo), (acc,) = ins, outs, ext
        dx, gw = norm_back(acc[band(i)], xr[...].astype(F32), lw[...])
        o[...] = (dm[...] + dx).astype(BF16)
        put(gwo, i, gw)

    ph = [Phase(heads, [heads_of(d_qkv, 3), cols_of(fq, 3 * hd)], [], dh1_body),
          Phase(nm, [rows_of(x, tm), rows_of(d_mid, tm), whole(w1)], [rows_of(act, tm), one_vec], ln1b_body)]
    comms = S([(g_qkv, 0, nq // SUB)], carry=r4[1:], last=True) + [SmallSum(g_ln2, heads + nm, d)] if comm else []
    dx, g_ln1, *r5 = host('dh1', 8, ph, comms, shared=[vm32(seq, d)])
    if not comm:
        return y, dx, g_ln1, g_qkv, g_out, g_ln2, g_up, g_down
    units = jnp.concatenate([r[0] for r in (r1, r2, r3, r4, r5)])
    nc = d // SUB
    g_down, g_up, g_out, g_qkv = jnp.split(units, (n_down, 2 * n_down, 2 * n_down + nc))
    flat_rows = lambda u: u.transpose(1, 0, 2).reshape(RB, -1)
    g_down = g_down.reshape(-1, nc, RB, SUB).transpose(0, 2, 1, 3).reshape(-1, d)
    return y, dx, r5[1], flat_rows(g_qkv), flat_rows(g_out), None, flat_rows(g_up), g_down


def solution(mesh):
    row_spec = P('fsdp')

    def step(x_in, ln1_w, w_qkv, w_out, ln2_w, w_up, w_down, dy_out):
        rows, _, heads, hd = w_qkv.shape
        d = x_in.shape[-1]
        y, dx, sums, g_qkv, g_out, _, g_up, g_down = local_step(
            x_in[0], ln1_w, w_qkv.reshape(rows, -1), w_out, ln2_w, w_up, w_down, dy_out[0])
        mine = lax.dynamic_slice_in_dim(sums, lax.axis_index('fsdp') * rows, rows, axis=1)
        return (y[None], dx[None], mine[0], g_qkv.reshape(rows, 3, heads, hd), g_out, mine[1], g_up, g_down)

    return jax.shard_map(step, mesh=mesh, in_specs=(row_spec,) * 8, out_specs=(row_spec,) * 8, check_vma=False)
```

```python
import functools
import math

import jax
import jax.numpy as jnp
from jax import lax
from jax.experimental import pallas as pl
from jax.experimental.pallas import tpu as pltpu
from jax.sharding import PartitionSpec as P

EPS = 1e-5
SUB = 512
HALF = SUB // 2
LAG = 2
CARRY = 2 * LAG
LEAD = 3
RB = 48
F32, BF16 = jnp.float32, jnp.bfloat16
VMEM_LIMIT = 62 * 1024 * 1024
MESH = pl.DeviceIdType.MESH
HBM = pltpu.MemorySpace.HBM
CHIPS = (4, 2, 2)


def sds(shape, dtype):
    return jax.ShapeDtypeStruct(shape, dtype)


def dot(a, b, ca=1, cb=0):
    return lax.dot_general(a, b, (((ca,), (cb,)), ((), ())), preferred_element_type=F32)


def dot_t(a, b):
    return dot(a, b, 1, 1)


def t_dot(a, b):
    return dot(a, b, 0, 0)


def over_rows(f):
    return functools.partial(f, axis=-1, keepdims=True)


row_sum, row_max, row_mean = map(over_rows, (jnp.sum, jnp.max, jnp.mean))


def clip(t, n):
    return jnp.minimum(jnp.maximum(t, 0), n - 1)


class Phase:
    def __init__(self, n, ins, outs, body):
        self.n, self.ins, self.outs, self.body = n, ins, outs, body


def quot(a, b):
    return a // b if isinstance(a, int) else lax.div(a, b)


def rest(a, b):
    return a % b if isinstance(a, int) else lax.rem(a, b)


HERE = {}


def locate():
    me = lax.axis_index('fsdp')
    z, y, x, c = quot(me, 8), rest(quot(me, 4), 2), rest(quot(me, 2), 2), rest(me, 2)
    HERE.update(coords=(me, z, y, x, c), peers=([rest(me + 8 * d, 32) for d in (1, 2, 3)], me + 4 - 8 * y, me + 2 - 4 * x, me + 1 - 2 * c),
                zs=[rest(z + d, 4) for d in (1, 2, 3)])


def coords():
    return HERE['coords']


def peers():
    return HERE['peers']


def remote(src, dst, ssem, rsem, dev):
    return pltpu.make_async_remote_copy(src_ref=src, dst_ref=dst, send_sem=ssem, recv_sem=rsem, device_id=(dev,), device_id_type=MESH)


class Unit:
    def __init__(self, rows, cols):
        self.nc, self.nr = cols // SUB, rows // RB
        self.count = self.nc * self.nr

    def at(self, u, half=None):
        col = pl.multiple_of(rest(u, self.nc) * SUB, HALF)
        width = SUB
        if half is not None:
            col, width = pl.multiple_of(col + half * HALF, HALF), HALF
        rows = slice(None) if self.nr == 1 else pl.ds(pl.multiple_of(quot(u, self.nc) * RB, 16), RB)
        return rows, pl.ds(col, width)


class Gather:
    def __init__(self, weights, k0, k1):
        self.k0, self.k1 = k0, k1
        self.k = k1 - k0 + 1
        self.z0 = k0 + LEAD if k0 else 0
        self.z1 = k1 + LEAD
        self.w, self.ins, self.outs, self.alias = [], [], [], []
        for shard, full, first in weights:
            unit = Unit(*shard.shape)
            self.w.append((len(self.ins), unit, first, first + unit.count, full is None))
            self.ins.append((shard, pl.BlockSpec(memory_space=pltpu.VMEM)))
            if full is not None:
                self.alias.append((len(self.ins), len(self.outs)))
                self.ins.append((full, pl.BlockSpec(memory_space=HBM)))
            self.outs.append((sds(CHIPS + (2,) + shard.shape, BF16), pl.BlockSpec(memory_space=HBM)))
        self.base = max(k0 - 2 * LAG, 0)
        n = self.z1 - self.base
        self.scratch = [pltpu.SemaphoreType.DMA((n, 8)), pltpu.SemaphoreType.DMA((n, 8)), pltpu.SemaphoreType.DMA((len(weights),))]

    def copies(self, stage, w, u, refs):
        i, unit, first, _, _ = self.w[w]
        shard, full = refs[i], refs[len(self.ins) + w]
        sems = lambda i: (refs[-3].at[u - self.base, i], refs[-2].at[u - self.base, i])
        me, z, y, x, c = coords()
        zs, yp, xp, cp = peers()
        r, q = unit.at(u - first)
        if stage == 0:
            return [remote(shard.at[r, q], full.at[z, y, x, c, r, q], *sems(d), zs[d]) for d in range(3)]
        if stage == 3:
            v = full.at[:, :, :, c, r, q]
            return [remote(v, v, *sems(7), cp)]
        out = []
        for half in range(2):
            r, q = unit.at(u - first, half)
            j = 2 * stage + 1 + half
            if stage == 1:
                v = full.at[:, y, x, c, r, q]
            else:
                v = full.at[:, y, :, c, r, q] if half else full.at[:, :, x, c, r, q]
            out.append(remote(v, v, *sems(j), xp if half == stage % 2 else yp))
        return out

    def each(self, lo, hi, u, fn):
        for w, (_, _, first, last, _) in enumerate(self.w):
            a, b = max(lo, first), min(hi, last)
            if a < b:
                if u is None:
                    pl.loop(a, b)(functools.partial(fn, w))
                else:
                    pl.when((u >= a) & (u < b))(functools.partial(fn, w, u))

    def go(self, stage, w, u, refs):
        for cp in self.copies(stage, w, u, refs):
            cp.start()

    def arrive(self, stage, w, u, refs):
        for cp in self.copies(stage, w, u, refs):
            cp.wait_recv()

    def left(self, stage, w, u, refs):
        for cp in self.copies(stage, w, u, refs):
            cp.wait_send()

    def step(self, k, fire, refs):
        me, z, y, x, c = coords()
        k0, k1, k = self.k0, self.k1, k + self.k0
        span = [(self.z0, self.z1)] + [(max(k0 - i * LAG, 0), k1 - i * LAG) for i in range(3)]

        @pl.when(fire & (k == k0))
        def _():
            own = [pltpu.make_async_copy(refs[i], refs[len(self.ins) + w].at[z, y, x, c], refs[-1].at[w])
                   for w, (i, _, _, _, fresh) in enumerate(self.w) if fresh]
            for cp in own:
                cp.start()
            if k0 == 0:
                self.each(0, LEAD, None, lambda w, u: self.go(0, w, u, refs))
            for cp in own:
                cp.wait()

        @pl.when(fire & (k < k1))
        def _():
            self.each(*span[0], k + LEAD, lambda w, u: self.go(0, w, u, refs))
            for stage in (1, 2, 3):
                u = k + LAG * (1 - stage)
                lo, hi = span[stage - 1]
                self.each(lo, hi, u, lambda w, u: self.arrive(stage - 1, w, u, refs))
                self.each(*span[stage], u, lambda w, u: self.go(stage, w, u, refs))

        @pl.when(fire & (k == k1))
        def _():
            for stage in range(4):
                lo, hi = span[stage]
                self.each(max(lo, k1 - stage * LAG) if stage < 3 else lo, hi, None, lambda w, u: self.arrive(stage, w, u, refs))
                self.each(lo, hi, None, lambda w, u: self.left(stage, w, u, refs))


class GatherSmall:
    def __init__(self, tile):
        self.k, self.alias = 5, []
        self.ins = [(tile, pl.BlockSpec(memory_space=pltpu.VMEM))]
        self.outs = [(sds(CHIPS + (2,) + tile.shape, F32), pl.BlockSpec(memory_space=HBM))]
        self.scratch = [pltpu.SemaphoreType.DMA((6,)), pltpu.SemaphoreType.DMA((6,)), pltpu.SemaphoreType.DMA]

    def copies(self, stage, refs):
        tile, full, ss, rs, _ = refs
        me, z, y, x, c = coords()
        zs, yp, xp, cp = peers()
        if stage == 0:
            return [remote(tile, full.at[z, y, x, c], ss.at[d], rs.at[d], zs[d]) for d in range(3)]
        v, dev = ((full.at[:, y, x, c], yp), (full.at[:, :, x, c], xp), (full.at[:, :, :, c], cp))[stage - 1]
        return [remote(v, v, ss.at[2 + stage], rs.at[2 + stage], dev)]

    def step(self, k, fire, refs):
        tile, full, ss, rs, ls = refs
        me, z, y, x, c = coords()
        for stage in range(5):
            @pl.when(fire & (k == stage))
            def _(stage=stage):
                if stage == 0:
                    own = pltpu.make_async_copy(tile, full.at[z, y, x, c], ls)
                    own.start()
                else:
                    for cp in self.copies(stage - 1, refs):
                        cp.wait_recv()
                if stage < 4:
                    for cp in self.copies(stage, refs):
                        cp.start()
                else:
                    for st in range(4):
                        for cp in self.copies(st, refs):
                            cp.wait_send()
                if stage == 0:
                    own.wait()


class Scatter:
    def __init__(self, grads, carry=None, last=False):
        self.last, self.carried = last, carry is not None
        self.parts, self.ins, n = [], [], 0
        for g, u0, m in grads:
            self.parts.append((n, n + m, u0, Unit(*g.shape[-2:])))
            self.ins.append((g, pl.BlockSpec(memory_space=HBM)))
            n += m
        self.n = n
        self.first = 0 if self.carried else CARRY
        self.end = n + CARRY
        self.done = self.end if last else n
        self.k = n + (3 * LAG if last else 1)
        self.two_shape, self.three_shape = (2, 4, 2, RB, HALF), (4, RB, SUB)
        if self.carried:
            self.ins += [(a, pl.BlockSpec(memory_space=pltpu.VMEM)) for a in carry]
        self.scratch = [
            pltpu.VMEM((n, *CHIPS, RB, SUB), BF16),
            pltpu.VMEM((2, *CHIPS, RB, SUB), BF16),
            pltpu.VMEM((self.end, *self.two_shape), BF16),
            pltpu.VMEM((self.end, *self.three_shape), BF16),
            pltpu.VMEM((self.end, 3, RB, SUB), BF16),
            pltpu.SemaphoreType.DMA((self.end, 8)), pltpu.SemaphoreType.DMA((self.end, 8)), pltpu.SemaphoreType.DMA((2,))]
        outs = [sds((self.done - self.first, RB, SUB), F32)]
        if not last:
            outs += [sds((LAG, *shape), BF16) for shape in (self.two_shape, self.three_shape)]
        self.outs = [(o, pl.BlockSpec(memory_space=pltpu.VMEM)) for o in outs]
        self.alias = []

    def source(self, j, refs, fn):
        for i, (a, b, u0, unit) in enumerate(self.parts):
            if len(self.parts) == 1:
                fn(refs[i], *unit.at(u0 + j - CARRY))
            else:
                pl.when((j - CARRY >= a) & (j - CARRY < b))(lambda: fn(refs[i], *unit.at(u0 + j - CARRY - a)))

    def bufs(self, refs):
        return refs[len(self.ins) + len(self.outs):]

    def local(self, j, refs, act):
        me, z, y, x, c = coords()
        own, ls = self.bufs(refs)[1], self.bufs(refs)[-1]
        slot = rest(j, 2)
        self.source(j, refs, lambda g, r, q: act(pltpu.make_async_copy(g.at[:, :, :, c, r, q], own.at[slot], ls.at[slot])))

    def swap(self, j, refs, act):
        me, z, y, x, c = coords()
        got, ss, rs = self.bufs(refs)[0], *self.bufs(refs)[-3:-1]
        cp = peers()[-1]
        self.source(j, refs, lambda g, r, q: act(remote(g.at[:, :, :, 1 - c, r, q], got.at[j - CARRY], ss.at[j, 0], rs.at[j, 0], cp)))

    def copies(self, stage, j, refs):
        got, own, two, three, four, ss, rs, ls = self.bufs(refs)
        me, z, y, x, c = coords()
        zs, yp, xp, cp = peers()
        a, b = pl.ds(0, HALF), pl.ds(HALF, HALF)
        if stage == 1:
            pairs = [(got.at[j - CARRY, :, 1 - y, :, :, a], two.at[j, 0], yp), (got.at[j - CARRY, :, :, 1 - x, :, b], two.at[j, 1], xp)]
        elif stage == 2:
            pairs = [(two.at[j, 0, :, 1 - x], three.at[j, :, :, a], xp), (two.at[j, 1, :, 1 - y], three.at[j, :, :, b], yp)]
        else:
            pairs = [(three.at[j, HERE['zs'][d]], four.at[j, d], zs[d]) for d in range(3)]
        return [remote(src, dst, ss.at[j, 2 * stage + i - 1], rs.at[j, 2 * stage + i - 1], dev) for i, (src, dst, dev) in enumerate(pairs)]

    def add(self, stage, j, refs):
        got, own, two, three, four, ss, rs, ls = self.bufs(refs)
        me, z, y, x, c = coords()
        a, b = pl.ds(0, HALF), pl.ds(HALF, HALF)
        slot = rest(j, 2)
        if stage == 1:
            @pl.loop(0, 4)
            def _(zz):
                for yy in range(2):
                    for xx in range(2):
                        got[j - CARRY, zz, yy, xx] += own[slot, zz, yy, xx]
        elif stage == 2:
            @pl.loop(0, 4)
            def _(zz):
                for i in range(2):
                    two[j, 0, zz, i] += got[j - CARRY, zz, y, i, :, a]
                    two[j, 1, zz, i] += got[j - CARRY, zz, i, x, :, b]
        elif stage == 3:
            for zz in range(4):
                three[j, zz, :, a] += two[j, 0, zz, x]
                three[j, zz, :, b] += two[j, 1, zz, y]
        else:
            total = three[j, z].astype(F32)
            for d in range(3):
                total += four[j, d].astype(F32)
            refs[len(self.ins)][j - self.first] = total

    def step(self, k, fire, refs):
        n, end, last = self.n, self.end, self.last
        got, own, two, three, four, ss, rs, ls = self.bufs(refs)
        start = lambda cp: cp.start()

        def go(stage, j):
            for cp in self.copies(stage, j, refs):
                cp.start()

        def take(stage, j):
            for cp in self.copies(stage - 1, j, refs):
                cp.wait_recv()
            self.add(stage, j, refs)

        @pl.when(fire & (k == 0))
        def _():
            @pl.loop(CARRY, end)
            def _(j):
                self.swap(j, refs, start)

            for j in range(CARRY, min(CARRY + 2, end)):
                self.local(j, refs, start)
            if self.carried:
                for i in range(LAG):
                    two[LAG + i] = refs[len(self.ins) - 2][i]
                    three[i] = refs[len(self.ins) - 1][i]
                    go(2, LAG + i)
                    go(3, i)

        @pl.when(fire & (k < n))
        def _():
            j = k + CARRY
            self.swap(j, refs, lambda cp: cp.wait_recv())
            self.local(j, refs, lambda cp: cp.wait())
            self.add(1, j, refs)
            go(1, j)
            pl.when(j + 2 < end)(lambda: self.local(j + 2, refs, start))

        lows = [CARRY, LAG, 0] if self.carried else [CARRY] * 3
        for stage, low in zip((2, 3, 4), lows):
            j = k + (3 - stage) * LAG

            @pl.when(fire & (j >= low) & (j < end) & ((k < n) | last))
            def _(stage=stage, j=j):
                take(stage, j)
                if stage < 4:
                    go(stage, j)

        @pl.when(fire & (k == self.k - 1))
        def _():
            for stage, low in zip((2, 3, 4), lows):
                a = n + (3 - stage) * LAG
                if not last:
                    pl.loop(max(a, low), a + LAG)(functools.partial(take, stage))

                @pl.loop(CARRY if stage == 2 else low, end if last else a + LAG)
                def _(j):
                    for cp in self.copies(stage - 1, j, refs):
                        cp.wait_send()

            @pl.loop(CARRY, end)
            def _(j):
                self.swap(j, refs, lambda cp: cp.wait_send())

            if not last:
                for i in range(LAG):
                    refs[len(self.ins) + 1][i] = two[n + LAG + i]
                    refs[len(self.ins) + 2][i] = three[n + i]


class SmallSum:
    def __init__(self, row, t0, d):
        self.t0, self.k = t0, 1
        self.ins = [(row, pl.BlockSpec(memory_space=pltpu.VMEM))]
        self.outs = [(sds((8, d), F32), pl.BlockSpec(memory_space=pltpu.VMEM))]
        self.alias = []
        self.scratch = [pltpu.VMEM((4, 8, d), F32), pltpu.VMEM((6, 8, d), F32), pltpu.SemaphoreType.DMA((6,)), pltpu.SemaphoreType.DMA((6,))]

    def run(self, t, mine, refs):
        row, out, acc, got, ss, rs = refs
        zs, yp, xp, cp = peers()
        near = (cp, xp, yp, *zs)
        n = len(near) - len(zs)
        copies = [remote(acc.at[min(i, n)], got.at[i], ss.at[i], rs.at[i], dev) for i, dev in enumerate(near)]

        for i in range(n + 2):
            @pl.when(t == self.t0 + i)
            def _(i=i):
                if not i:
                    acc[i] = jnp.zeros_like(acc[i])
                    acc[i, pl.ds(0, 1)] = mine[...]
                    acc[i, pl.ds(1, 1)] = row[...]
                elif i <= n:
                    copies[i - 1].wait_recv()
                    acc[i] = acc[i - 1] + got[i - 1]
                else:
                    total = acc[n]
                    for j in range(n, len(near)):
                        copies[j].wait_recv()
                        total += got[j]
                    out[...] = total
                    for copy in copies:
                        copy.wait_send()
                for copy in copies[i:i + 1] if i < n else copies[n:] if i == n else ():
                    copy.start()


def host(name, cid, phases, comms=(), shared=(), cost=None):
    k_all = max([c.k for c in comms], default=1)
    at = 0
    for p in phases:
        p.at = at
        at = at + p.n
    small = [c for c in comms if isinstance(c, SmallSum)]
    total = max(at + 5 * len(small), k_all)
    kmap = lambda t: t if total == k_all else quot(t * (k_all - 1), total - 1)
    ins, in_specs, outs, out_specs, scratch, alias, resident = [], [], [], [], [], {}, []
    for p in phases:
        for arr, block, index in p.ins:
            if block == 'smem':
                in_specs.append(pl.BlockSpec(memory_space=pltpu.SMEM))
            elif index is None:
                resident.append((len(ins), p.at))
                in_specs.append(pl.BlockSpec(memory_space=HBM))
            else:
                in_specs.append(pl.BlockSpec(block, functools.partial(lambda p, f, t: f(clip(t - p.at, p.n)), p, index)))
            ins.append(arr)
        for shape, block, index in p.outs:
            outs.append(shape)
            out_specs.append(pl.BlockSpec(block, functools.partial(lambda p, f, t: f(clip(t - p.at, p.n)), p, index)))
    for c in comms:
        alias.update({len(ins) + i: len(outs) + o for i, o in c.alias})
        for arr, spec in c.ins:
            ins.append(arr)
            in_specs.append(spec)
        for shape, spec in c.outs:
            outs.append(shape)
            out_specs.append(spec)
        scratch += c.scratch
    scratch += [pltpu.VMEM(ins[i].shape, ins[i].dtype) for i, _ in resident] + [pltpu.SemaphoreType.DMA((max(len(resident), 1),))]
    scratch += list(shared)

    def kernel(*refs):
        refs = list(refs)
        rin, rout, rscr = refs[:len(ins)], refs[len(ins):len(ins) + len(outs)], refs[len(ins) + len(outs):]
        t = pl.program_id(0)
        if comms:
            locate()

            @pl.when(t == 0)
            def _():
                zs, yp, xp, cp = peers()
                near = (*zs, yp, xp, cp)
                bar = pltpu.get_barrier_semaphore()
                for dev in near:
                    pl.semaphore_signal(bar, inc=1, device_id=(dev,), device_id_type=MESH)
                pl.semaphore_wait(bar, len(near))
        i, o, s = sum(len(p.ins) for p in phases), sum(len(p.outs) for p in phases), 0
        k = kmap(t)
        fire = (t == 0) | (k != kmap(jnp.maximum(t - 1, 0)))
        for c in comms:
            ni, no, ns = len(c.ins), len(c.outs), len(c.scratch)
            crefs = rin[i:i + ni] + rout[o:o + no] + rscr[s:s + ns]
            if c in small:
                small_refs = crefs
            else:
                c.step(k, fire, crefs)
            i, o, s = i + ni, o + no, s + ns
        held, rsem, extra = rscr[s:s + len(resident)], rscr[s + len(resident)], rscr[s + len(resident) + 1:]
        loads = [(pltpu.make_async_copy(rin[i], h, rsem.at[n]), at) for n, ((i, at), h) in enumerate(zip(resident, held))]
        if loads:
            @pl.when(t == 0)
            def _():
                for cp, _ in loads:
                    cp.start()
        for cp, at in loads:
            pl.when(t == at)(cp.wait)
        for (i, _), h in zip(resident, held):
            rin[i] = h
        i = o = 0
        for p in phases:
            pi, po = rin[i:i + len(p.ins)], rout[o:o + len(p.outs)]
            i, o = i + len(p.ins), o + len(p.outs)

            @pl.when((t >= p.at) & (t < p.at + p.n))
            def _(p=p, pi=pi, po=po):
                p.body(t - p.at, pi, po, extra)

        for c in small:
            c.run(t, rout[o - 1], small_refs)

    params = dict(dimension_semantics=("arbitrary",), vmem_limit_bytes=VMEM_LIMIT)
    if comms:
        params.update(collective_id=cid, has_side_effects=True)
    got = pl.pallas_call(kernel, grid=(total,), in_specs=in_specs, out_specs=out_specs, out_shape=outs, scratch_shapes=scratch,
                         input_output_aliases=alias, compiler_params=pltpu.CompilerParams(**params), name=name,
                         cost_estimate=pl.CostEstimate(flops=2 ** 34, bytes_accessed=2 ** 25, transcendentals=0))(*ins)
    return list(got)


def norm_parts(t):
    mean = row_mean(t)
    cen = t - mean
    rstd = lax.rsqrt(row_mean(cen * cen) + EPS)
    return cen * rstd, rstd


def norm_back(d, t, w):
    xhat, rstd = norm_parts(t)
    dh = d * w
    m1 = row_mean(dh)
    m2 = row_mean(dh * xhat)
    return rstd * (dh - m1 - xhat * m2), jnp.sum(d * xhat, axis=0, keepdims=True)


def alibi_slopes(n_heads):
    padded = 2 ** math.ceil(math.log2(n_heads))
    base = [2.0 ** (-8.0 * (k + 1) / padded) for k in range(padded)]
    ordered = base if padded == n_heads else base[1::2] + base[0::2]
    return jnp.array(ordered[:n_heads], dtype=F32)


def causal(i, tq, slope):
    row = lax.broadcasted_iota(jnp.int32, (tq, tq), 0)
    col = lax.broadcasted_iota(jnp.int32, (tq, tq), 1)
    rel = (row - col).astype(F32)
    diag = slope * rel
    past = None
    if i:
        r = lax.broadcasted_iota(jnp.int32, (tq, i * tq), 0) + i * tq
        q = lax.broadcasted_iota(jnp.int32, (tq, i * tq), 1)
        past = slope * (r - q).astype(F32)
    return past, diag, row >= col


def attn_fwd(q_ref, k_ref, v_ref, o_ref, l_ref, slope, scale, tq):
    n = q_ref.shape[0] // tq
    for i in range(n):
        rows, before = pl.ds(i * tq, tq), pl.ds(0, i * tq)
        q = q_ref[rows]
        past, diag, keep = causal(i, tq, slope)
        sd = jnp.where(keep, dot_t(q, k_ref[rows]) * scale - diag, -jnp.inf)
        m = row_max(sd)
        if i:
            sp = dot_t(q, k_ref[before]) * scale - past
            m = jnp.maximum(m, row_max(sp))
            ep = jnp.exp(sp - m)
        ed = jnp.exp(sd - m)
        l = row_sum(ed)
        if i:
            l = l + row_sum(ep)
        inv = 1.0 / l
        o = dot((ed * inv).astype(BF16), v_ref[rows])
        if i:
            o = o + dot((ep * inv).astype(BF16), v_ref[before])
        o_ref[rows] = o.astype(BF16)
        l_ref[rows] = m + jnp.log(l)


def attn_bwd(q_ref, k_ref, v_ref, a_ref, da_ref, l_ref, dq_ref, dk_ref, dv_ref, dk_s, dv_s, slope, scale, tq):
    n = q_ref.shape[0] // tq
    dk_s[...] = jnp.zeros_like(dk_s)
    dv_s[...] = jnp.zeros_like(dv_s)
    for i in range(n):
        rows, before = pl.ds(i * tq, tq), pl.ds(0, i * tq)
        q, da = q_ref[rows], da_ref[rows]
        lse = l_ref[rows]
        delta = row_sum(da.astype(F32) * a_ref[rows].astype(F32))
        past, diag, keep = causal(i, tq, slope)
        dq = None
        for own in ((True,) if i == 0 else (True, False)):
            keys = rows if own else before
            kk, vv = k_ref[keys], v_ref[keys]
            s = dot_t(q, kk) * scale - (diag if own else past)
            p = jnp.exp(s - lse)
            if own:
                p = jnp.where(keep, p, 0.0)
            ds = (p * (dot_t(da, vv) - delta) * scale).astype(BF16)
            dv_s[keys] += t_dot(p.astype(BF16), da)
            dk_s[keys] += t_dot(ds, q)
            part = dot(ds, kk)
            dq = part if dq is None else dq + part
        dq_ref[rows] = dq.astype(BF16)
    dk_ref[...] = dk_s[...].astype(BF16)
    dv_ref[...] = dv_s[...].astype(BF16)


def row_map(i):
    return i, 0


def col_map(i):
    return 0, i


def rows_of(a, n):
    return a, (n, a.shape[1]), row_map


def cols_of(a, n):
    return a, (a.shape[0], n), col_map


def heads_of(a, n, off=0):
    return a, (n,) + a.shape[1:], lambda i: (i + off, 0, 0)


def whole(a):
    return a, a.shape, None


def put(ref, i, part):
    @pl.when(i == 0)
    def _():
        ref[...] = part

    @pl.when(i > 0)
    def _():
        ref[...] += part


def side_by_side(ref, n):
    return jnp.concatenate([ref[j] for j in range(n)], axis=1)


def local_step(x, ln1, wq, wo, ln2, wu, wd, dy, comm=True):
    seq, d = x.shape
    heads, hd, ft = 12, 128, 512
    ff, nq, per = wu.shape[1], 3 * d, SUB // hd
    scale = 1 / math.sqrt(hd)
    tq = min(256, seq)
    tm = tq // 2
    nm, nf = seq // tm, ff // ft
    slopes = (alibi_slopes(heads), 'smem', None)
    b16 = lambda *shape: sds(shape, BF16)
    f32 = lambda *shape: sds(shape, F32)
    vm16 = lambda *shape: pltpu.VMEM(shape, BF16)
    vm32 = lambda *shape: pltpu.VMEM(shape, F32)
    act, wide, vec = b16(seq, d), b16(seq, ff), f32(1, d)
    one_vec = (vec, vec.shape, lambda i: (0, 0))
    band = lambda i: pl.ds(pl.multiple_of(i * tm, tm), tm)
    flat = lambda full: full.reshape(-1, full.shape[-1])
    order = [Unit(*w.shape).count for w in (wq, wo, wu, wd)]
    qs, os, us, ds = (sum(order[:i]) for i in range(4))
    ends = [i + 2 * LAG for i in (os, ds, sum(order))]

    def G(*window):
        return [Gather(*window)] if comm else []

    def S(parts, **kw):
        return [Scatter([(a.reshape(*CHIPS, 2, -1, a.shape[-1]), u0, n) for a, u0, n in parts], **kw)] if comm else []

    if comm:
        tile = jnp.pad(jnp.stack([ln1, ln2]), ((0, 6), (0, 128 - ln1.shape[0])))
        fq, fo, fu, lns = host('ag_qkv', 1, [], G([(wq, None, qs), (wo, None, os), (wu, None, us)], 0, ends[0]) + [GatherSmall(tile)])
        fq = flat(fq)
        w1, w2 = lns.reshape(-1, 8, 128)[:, :2, :ln1.shape[0]].transpose(1, 0, 2).reshape(2, 1, d)
    else:
        fq, fo, fu, w1, w2 = wq, wo, wu, ln1.reshape(1, d), ln2.reshape(1, d)

    def ln1_body(i, ins, outs, ext):
        (xr, lw), (ht,), (_, h1) = ins, outs, ext
        xhat, _ = norm_parts(xr[...].astype(F32))
        h = (xhat * lw[...]).astype(BF16)
        h1[band(i)] = h
        ht[...] = h.T

    def qkv_body(i, ins, outs, ext):
        (w,), (o,), (qkv, h1) = ins, outs, ext
        r = dot(h1[...], w[...]).astype(BF16)
        for j in range(per):
            qkv[i * per + j] = r[:, j * hd:(j + 1) * hd]
            o[j] = r[:, j * hd:(j + 1) * hd]

    def attn_body(i, ins, outs, ext):
        (sl,), (o, l), (qkv, _) = ins, outs, ext
        attn_fwd(qkv.at[i], qkv.at[heads + i], qkv.at[2 * heads + i], o, l.at[0], sl[i], scale, tq)

    pb = [Phase(nm, [rows_of(x, tm), whole(w1)], [cols_of(b16(d, seq), tm)], ln1_body),
          Phase(nq // SUB, [cols_of(fq, SUB)], [heads_of(b16(3 * heads, seq, hd), per)], qkv_body),
          Phase(heads, [slopes], [cols_of(act, hd), heads_of(f32(heads, seq, 1), 1)], attn_body)]
    h1t, qkv, attn, lse, *full = host('attn_fwd', 2, pb, G([(wo, fo, os), (wu, fu, us), (wd, None, ds)], ends[0], ends[1]),
                                      shared=[vm16(3 * heads, seq, hd), vm16(seq, d)])
    if comm:
        fo, fu, fd = full
        fo, fu = flat(fo), flat(fu)

    def out_body(i, ins, outs, ext):
        (xs, a, w, lw), (o, ht), (h2,) = ins, outs, ext
        x1 = (xs[...].astype(F32) + dot(a[...], w[...])).astype(BF16)
        o[...] = x1
        xhat, _ = norm_parts(x1.astype(F32))
        h = (xhat * lw[...]).astype(BF16)
        h2[band(i)] = h
        ht[...] = h.T

    def up_body(i, ins, outs, ext):
        (w, dyr), (go, gpo, gd), (h2,) = ins, outs, ext
        u = dot(h2[...], w[...])
        cdf = 0.5 * (1.0 + lax.erf(u * math.sqrt(0.5)))
        g = (u * cdf).astype(BF16)
        go[...] = g
        gpo[...] = cdf + u * (jnp.exp(-0.5 * u * u) * math.sqrt(0.5 / math.pi))
        gd[...] = t_dot(g, dyr[...]).astype(BF16)

    pc = [Phase(nm, [rows_of(x, tm), rows_of(attn, tm), whole(fo), whole(w2)], [rows_of(act, tm), cols_of(b16(d, seq), tm)], out_body),
          Phase(nf, [cols_of(fu, ft), whole(dy)], [cols_of(wide, ft), cols_of(f32(seq, ff), ft), rows_of(b16(ff, d), ft)], up_body)]
    x1, h2t, g, gp, g_down, *full = host('up', 3, pc, G([(wd, fd, ds)], ends[1], ends[2]) if comm else [], shared=[vm16(seq, d)])
    fd, = map(flat, full) if comm else (wd,)

    def dup_body(i, ins, outs, ext):
        (dyr, w, gr, gpr, ht), (duo, gu), (acc,) = ins, outs, ext
        du = (dot_t(dyr[...], w[...]) * gpr[...]).astype(BF16)
        duo[...] = du
        gu[...] = dot(ht[...], du).astype(BF16)
        put(acc, i, dot(gr[...], w[...]))

    def y_body(i, ins, outs, ext):
        (xr,), (o,), (acc,) = ins, outs, ext
        o[...] = (xr[...].astype(F32) + acc[band(i)]).astype(BF16)

    pd = [Phase(nf, [whole(dy), rows_of(fd, ft), cols_of(g, ft), cols_of(gp, ft), whole(h2t)], [cols_of(wide, ft), cols_of(b16(d, ff), ft)], dup_body),
          Phase(nm, [rows_of(x1, tm)], [rows_of(act, tm)], y_body)]
    n_down = Unit(ff // 32, d).count
    d_up, g_up, y, *r1 = host('dup', 4, pd, S([(g_down, 0, n_down)]), shared=[vm32(seq, d)])

    def dh2_body(i, ins, outs, ext):
        (du, w), (acc, _) = ins, ext
        put(acc, i, dot_t(du[...], w[...]))

    def ln2b_body(i, ins, outs, ext):
        (xr, dyr, lw), (dmo, gwo), (acc, dmb) = ins, outs, ext
        dx, gw = norm_back(acc[band(i)], xr[...].astype(F32), lw[...])
        dm = dyr[...].astype(F32) + dx
        dmo[...] = dm
        dmb[band(i)] = dm.astype(BF16)
        put(gwo, i, gw)

    def dattn_body(i, ins, outs, ext):
        (w, a), (da, go), (_, dmb) = ins, outs, ext
        da[...] = dot_t(dmb[...], w[...]).astype(BF16)
        go[...] = t_dot(a[...], dmb[...]).astype(BF16)

    pe = [Phase(nf, [cols_of(d_up, ft), cols_of(fu, ft)], [], dh2_body),
          Phase(nm, [rows_of(x1, tm), rows_of(dy, tm), whole(w2)], [rows_of(f32(seq, d), tm), one_vec], ln2b_body),
          Phase(d // ft, [rows_of(fo, ft), cols_of(attn, ft)], [cols_of(act, ft), rows_of(b16(d, d), ft)], dattn_body)]
    half = n_down // 2
    d_mid, g_ln2, d_attn, g_out, *r2 = host('dh2', 5, pe, S([(g_up, 0, half)], carry=r1[1:]), shared=[vm32(seq, d), vm16(seq, d)])

    def battn_body(i, ins, outs, ext):
        (q, k, v, a, da, l, sl), (o,), (dk, dv) = ins, outs, ext
        attn_bwd(q.at[0], k.at[0], v.at[0], a, da, l.at[0], *(o.at[j, 0] for j in range(3)), dk, dv, sl[i], scale, tq)

    pf = [Phase(heads, [*(heads_of(qkv, 1, j * heads) for j in range(3)), cols_of(attn, hd), cols_of(d_attn, hd), heads_of(lse, 1), slopes],
                [(b16(3, heads, seq, hd), (3, 1, seq, hd), lambda i: (0, i, 0, 0))], battn_body)]
    d_qkv, *r3 = host('attn_bwd', 6, pf, S([(g_up, half, half)], carry=r2[1:]), shared=[vm32(seq, hd), vm32(seq, hd)])
    d_qkv = d_qkv.reshape(3 * heads, seq, hd)

    def gqkv_body(i, ins, outs, ext):
        (ht, dq), (o,) = ins, outs
        o[...] = dot(ht[...], side_by_side(dq, per)).astype(BF16)

    g_qkv, *r4 = host('gqkv', 7, [Phase(nq // SUB, [whole(h1t), heads_of(d_qkv, per)], [cols_of(b16(d, nq), SUB)], gqkv_body)],
                      S([(g_out, 0, d // SUB)], carry=r3[1:]))

    def dh1_body(i, ins, outs, ext):
        (dq, w), (acc,) = ins, ext
        put(acc, i, dot_t(side_by_side(dq, 3), w[...]))

    def ln1b_body(i, ins, outs, ext):
        (xr, dm, lw), (o, gwo), (acc,) = ins, outs, ext
        dx, gw = norm_back(acc[band(i)], xr[...].astype(F32), lw[...])
        o[...] = (dm[...] + dx).astype(BF16)
        put(gwo, i, gw)

    ph = [Phase(heads, [heads_of(d_qkv, 3), cols_of(fq, 3 * hd)], [], dh1_body),
          Phase(nm, [rows_of(x, tm), rows_of(d_mid, tm), whole(w1)], [rows_of(act, tm), one_vec], ln1b_body)]
    comms = S([(g_qkv, 0, nq // SUB)], carry=r4[1:], last=True) + [SmallSum(g_ln2, heads + nm, d)] if comm else []
    dx, g_ln1, *r5 = host('dh1', 8, ph, comms, shared=[vm32(seq, d)])
    if not comm:
        return y, dx, g_ln1, g_qkv, g_out, g_ln2, g_up, g_down
    units = jnp.concatenate([r[0] for r in (r1, r2, r3, r4, r5)])
    nc = d // SUB
    g_down, g_up, g_out, g_qkv = jnp.split(units, (n_down, 2 * n_down, 2 * n_down + nc))
    flat_rows = lambda u: u.transpose(1, 0, 2).reshape(RB, -1)
    g_down = g_down.reshape(-1, nc, RB, SUB).transpose(0, 2, 1, 3).reshape(-1, d)
    return y, dx, r5[1], flat_rows(g_qkv), flat_rows(g_out), None, flat_rows(g_up), g_down


def solution(mesh):
    row_spec = P('fsdp')

    def step(x_in, ln1_w, w_qkv, w_out, ln2_w, w_up, w_down, dy_out):
        rows, _, heads, hd = w_qkv.shape
        d = x_in.shape[-1]
        y, dx, sums, g_qkv, g_out, _, g_up, g_down = local_step(
            x_in[0], ln1_w, w_qkv.reshape(rows, -1), w_out, ln2_w, w_up, w_down, dy_out[0])
        mine = lax.dynamic_slice_in_dim(sums, lax.axis_index('fsdp') * rows, rows, axis=1)
        return (y[None], dx[None], mine[0], g_qkv.reshape(rows, 3, heads, hd), g_out, mine[1], g_up, g_down)

    return jax.shard_map(step, mesh=mesh, in_specs=(row_spec,) * 8, out_specs=(row_spec,) * 8, check_vma=False)
```

```python
import functools
import math

import jax
import jax.numpy as jnp
from jax import lax
from jax.experimental import pallas as pl
from jax.experimental.pallas import tpu as pltpu
from jax.sharding import PartitionSpec as P

EPS = 1e-5
SUB = 512
HALF = SUB // 2
LAG = 2
CARRY = 2 * LAG
LEAD = 3
RB = 48
F32, BF16 = jnp.float32, jnp.bfloat16
VMEM_LIMIT = 67_000_000
MESH = pl.DeviceIdType.MESH
HBM = pltpu.MemorySpace.HBM
CHIPS = (4, 2, 2)


def sds(shape, dtype):
    return jax.ShapeDtypeStruct(shape, dtype)


def dot(a, b, ca=1, cb=0):
    return lax.dot_general(a, b, (((ca,), (cb,)), ((), ())), preferred_element_type=F32)


def dot_t(a, b):
    return dot(a, b, 1, 1)


def t_dot(a, b):
    return dot(a, b, 0, 0)


def over_rows(f):
    return functools.partial(f, axis=-1, keepdims=True)


row_sum, row_max, row_mean = map(over_rows, (jnp.sum, jnp.max, jnp.mean))


def clip(t, n):
    return jnp.minimum(jnp.maximum(t, 0), n - 1)


class Phase:
    def __init__(self, n, ins, outs, body, at=None, stride=1):
        self.n, self.ins, self.outs, self.body, self.at, self.stride = n, ins, outs, body, at, stride

    def own(self, t):
        return quot(t - self.at, self.stride)

    def on(self, t):
        here = (t >= self.at) & (t < self.end())
        return here if self.stride == 1 else here & (rest(t - self.at, self.stride) == 0)

    def end(self):
        return self.at + (self.n - 1) * self.stride + 1

    def index(self, f):
        return lambda t: f(clip(self.own(jnp.maximum(t, self.at)), self.n))


def quot(a, b):
    return a // b if isinstance(a, int) else lax.div(a, b)


def rest(a, b):
    return a % b if isinstance(a, int) else lax.rem(a, b)


HERE = {}


def locate():
    me = lax.axis_index('fsdp')
    z, y, x, c = quot(me, 8), rest(quot(me, 4), 2), rest(quot(me, 2), 2), rest(me, 2)
    HERE.update(coords=(me, z, y, x, c), peers=([rest(me + 8 * d, 32) for d in (1, 2, 3)], me + 4 - 8 * y, me + 2 - 4 * x, me + 1 - 2 * c),
                zs=[rest(z + d, 4) for d in (1, 2, 3)])


def coords():
    return HERE['coords']


def peers():
    return HERE['peers']


def remote(src, dst, ssem, rsem, dev):
    return pltpu.make_async_remote_copy(src_ref=src, dst_ref=dst, send_sem=ssem, recv_sem=rsem, device_id=(dev,), device_id_type=MESH)


class Unit:
    def __init__(self, rows, cols):
        self.nc, self.nr = cols // SUB, rows // RB
        self.count = self.nc * self.nr

    def at(self, u, half=None):
        col = pl.multiple_of(rest(u, self.nc) * SUB, HALF)
        width = SUB
        if half is not None:
            col, width = pl.multiple_of(col + half * HALF, HALF), HALF
        rows = slice(None) if self.nr == 1 else pl.ds(pl.multiple_of(quot(u, self.nc) * RB, 16), RB)
        return rows, pl.ds(col, width)


class Gather:
    def __init__(self, weights, k0, k1):
        self.k0, self.k1 = k0, k1
        self.k = k1 - k0 + 1
        self.z0 = k0 + LEAD if k0 else 0
        self.z1 = k1 + LEAD
        self.w, self.ins, self.outs, self.alias = [], [], [], []
        for shard, full, first in weights:
            unit = Unit(*shard.shape)
            self.w.append((len(self.ins), unit, first, first + unit.count, full is None))
            self.ins.append((shard, pl.BlockSpec(memory_space=pltpu.VMEM)))
            if full is not None:
                self.alias.append((len(self.ins), len(self.outs)))
                self.ins.append((full, pl.BlockSpec(memory_space=HBM)))
            self.outs.append((sds(CHIPS + (2,) + shard.shape, BF16), pl.BlockSpec(memory_space=HBM)))
        self.base = max(k0 - 2 * LAG, 0)
        n = self.z1 - self.base
        self.scratch = [pltpu.SemaphoreType.DMA((n, 8)), pltpu.SemaphoreType.DMA((n, 8)), pltpu.SemaphoreType.DMA((len(weights),))]

    def copies(self, stage, w, u, refs):
        i, unit, first, _, _ = self.w[w]
        shard, full = refs[i], refs[len(self.ins) + w]
        sems = lambda i: (refs[-3].at[u - self.base, i], refs[-2].at[u - self.base, i])
        me, z, y, x, c = coords()
        zs, yp, xp, cp = peers()
        r, q = unit.at(u - first)
        if stage == 0:
            return [remote(shard.at[r, q], full.at[z, y, x, c, r, q], *sems(d), zs[d]) for d in range(3)]
        if stage == 3:
            v = full.at[:, :, :, c, r, q]
            return [remote(v, v, *sems(7), cp)]
        out = []
        for half in range(2):
            r, q = unit.at(u - first, half)
            j = 2 * stage + 1 + half
            if stage == 1:
                v = full.at[:, y, x, c, r, q]
            else:
                v = full.at[:, y, :, c, r, q] if half else full.at[:, :, x, c, r, q]
            out.append(remote(v, v, *sems(j), xp if half == stage % 2 else yp))
        return out

    def each(self, lo, hi, u, fn):
        for w, (_, _, first, last, _) in enumerate(self.w):
            a, b = max(lo, first), min(hi, last)
            if a < b:
                if u is None:
                    pl.loop(a, b)(functools.partial(fn, w))
                else:
                    pl.when((u >= a) & (u < b))(functools.partial(fn, w, u))

    def go(self, stage, w, u, refs):
        for cp in self.copies(stage, w, u, refs):
            cp.start()

    def arrive(self, stage, w, u, refs):
        for cp in self.copies(stage, w, u, refs):
            cp.wait_recv()

    def left(self, stage, w, u, refs):
        for cp in self.copies(stage, w, u, refs):
            cp.wait_send()

    def step(self, k, fire, refs):
        me, z, y, x, c = coords()
        k0, k1, k = self.k0, self.k1, k + self.k0
        span = [(self.z0, self.z1)] + [(max(k0 - i * LAG, 0), k1 - i * LAG) for i in range(3)]

        @pl.when(fire & (k == k0))
        def _():
            own = [pltpu.make_async_copy(refs[i], refs[len(self.ins) + w].at[z, y, x, c], refs[-1].at[w])
                   for w, (i, _, _, _, fresh) in enumerate(self.w) if fresh]
            for cp in own:
                cp.start()
            if k0 == 0:
                self.each(0, LEAD, None, lambda w, u: self.go(0, w, u, refs))
            for cp in own:
                cp.wait()

        @pl.when(fire & (k < k1))
        def _():
            self.each(*span[0], k + LEAD, lambda w, u: self.go(0, w, u, refs))
            for stage in (1, 2, 3):
                u = k + LAG * (1 - stage)
                lo, hi = span[stage - 1]
                self.each(lo, hi, u, lambda w, u: self.arrive(stage - 1, w, u, refs))
                self.each(*span[stage], u, lambda w, u: self.go(stage, w, u, refs))

        @pl.when(fire & (k == k1))
        def _():
            for stage in range(4):
                lo, hi = span[stage]
                self.each(max(lo, k1 - stage * LAG) if stage < 3 else lo, hi, None, lambda w, u: self.arrive(stage, w, u, refs))
                self.each(lo, hi, None, lambda w, u: self.left(stage, w, u, refs))


class GatherSmall:
    def __init__(self, tile):
        self.k, self.alias = 5, []
        self.ins = [(tile, pl.BlockSpec(memory_space=pltpu.VMEM))]
        self.outs = [(sds(CHIPS + (2,) + tile.shape, F32), pl.BlockSpec(memory_space=HBM))]
        self.scratch = [pltpu.SemaphoreType.DMA((6,)), pltpu.SemaphoreType.DMA((6,)), pltpu.SemaphoreType.DMA]

    def copies(self, stage, refs):
        tile, full, ss, rs, _ = refs
        me, z, y, x, c = coords()
        zs, yp, xp, cp = peers()
        if stage == 0:
            return [remote(tile, full.at[z, y, x, c], ss.at[d], rs.at[d], zs[d]) for d in range(3)]
        v, dev = ((full.at[:, y, x, c], yp), (full.at[:, :, x, c], xp), (full.at[:, :, :, c], cp))[stage - 1]
        return [remote(v, v, ss.at[2 + stage], rs.at[2 + stage], dev)]

    def step(self, k, fire, refs):
        tile, full, ss, rs, ls = refs
        me, z, y, x, c = coords()
        for stage in range(5):
            @pl.when(fire & (k == stage))
            def _(stage=stage):
                if stage == 0:
                    own = pltpu.make_async_copy(tile, full.at[z, y, x, c], ls)
                    own.start()
                else:
                    for cp in self.copies(stage - 1, refs):
                        cp.wait_recv()
                if stage < 4:
                    for cp in self.copies(stage, refs):
                        cp.start()
                else:
                    for st in range(4):
                        for cp in self.copies(st, refs):
                            cp.wait_send()
                if stage == 0:
                    own.wait()


class Scatter:
    def __init__(self, grads, carry=None, last=False):
        self.last, self.carried = last, carry is not None
        self.parts, self.ins, n = [], [], 0
        self.late = None
        for g, u0, m in grads:
            self.parts.append((n, n + m, u0, Unit(*g.shape[-2:])))
            if isinstance(g, jax.ShapeDtypeStruct):
                self.late = g
            else:
                self.ins.append((g, pl.BlockSpec(memory_space=HBM)))
            n += m
        self.known = n - m if self.late else n
        self.n = n
        self.first = 0 if self.carried else CARRY
        self.end = n + CARRY
        self.done = self.end if last else n
        self.k = n + (3 * LAG if last else 1)
        self.two_shape, self.three_shape = (2, 4, 2, RB, HALF), (4, RB, SUB)
        if self.carried:
            self.ins += [(a, pl.BlockSpec(memory_space=pltpu.VMEM)) for a in carry]
        self.scratch = [
            pltpu.VMEM((n, *CHIPS, RB, SUB), BF16),
            pltpu.VMEM((2, *CHIPS, RB, SUB), BF16),
            pltpu.VMEM((self.end, *self.two_shape), BF16),
            pltpu.VMEM((self.end, *self.three_shape), BF16),
            pltpu.VMEM((self.end, 3, RB, SUB), BF16),
            pltpu.SemaphoreType.DMA((self.end, 8)), pltpu.SemaphoreType.DMA((self.end, 8)), pltpu.SemaphoreType.DMA((2,))]
        outs = [sds((self.done - self.first, RB, SUB), F32)]
        if not last:
            outs += [sds((LAG, *shape), BF16) for shape in (self.two_shape, self.three_shape)]
        self.outs = [(o, pl.BlockSpec(memory_space=pltpu.VMEM)) for o in outs]
        if self.late:
            self.outs.append((self.late, pl.BlockSpec(memory_space=HBM)))
        self.alias = []

    def source(self, j, refs, fn):
        for i, (a, b, u0, unit) in enumerate(self.parts):
            ref = self.written() if self.late and a == self.known else refs[i]
            u = j - CARRY
            if len(self.parts) == 1:
                fn(ref, *unit.at(u0 + u))
            else:
                pl.when((u >= a) & (u < b))(functools.partial(lambda ref, unit, u: fn(ref, *unit.at(u)), ref, unit, u0 + u - a))

    def written(self):
        return self.refs[len(self.ins) + len(self.outs) - 1]

    def ship(self, u):
        self.swap(CARRY + self.known + u, self.refs, lambda cp: cp.start())

    def bufs(self, refs):
        return refs[len(self.ins) + len(self.outs):]

    def local(self, j, refs, act):
        me, z, y, x, c = coords()
        own, ls = self.bufs(refs)[1], self.bufs(refs)[-1]
        slot = rest(j, 2)
        self.source(j, refs, lambda g, r, q: act(pltpu.make_async_copy(g.at[:, :, :, c, r, q], own.at[slot], ls.at[slot])))

    def swap(self, j, refs, act):
        me, z, y, x, c = coords()
        got, ss, rs = self.bufs(refs)[0], *self.bufs(refs)[-3:-1]
        cp = peers()[-1]
        self.source(j, refs, lambda g, r, q: act(remote(g.at[:, :, :, 1 - c, r, q], got.at[j - CARRY], ss.at[j, 0], rs.at[j, 0], cp)))

    def copies(self, stage, j, refs):
        got, own, two, three, four, ss, rs, ls = self.bufs(refs)
        me, z, y, x, c = coords()
        zs, yp, xp, cp = peers()
        a, b = pl.ds(0, HALF), pl.ds(HALF, HALF)
        if stage == 1:
            pairs = [(got.at[j - CARRY, :, 1 - y, :, :, a], two.at[j, 0], yp), (got.at[j - CARRY, :, :, 1 - x, :, b], two.at[j, 1], xp)]
        elif stage == 2:
            pairs = [(two.at[j, 0, :, 1 - x], three.at[j, :, :, a], xp), (two.at[j, 1, :, 1 - y], three.at[j, :, :, b], yp)]
        else:
            pairs = [(three.at[j, HERE['zs'][d]], four.at[j, d], zs[d]) for d in range(3)]
        return [remote(src, dst, ss.at[j, 2 * stage + i - 1], rs.at[j, 2 * stage + i - 1], dev) for i, (src, dst, dev) in enumerate(pairs)]

    def add(self, stage, j, refs):
        got, own, two, three, four, ss, rs, ls = self.bufs(refs)
        me, z, y, x, c = coords()
        a, b = pl.ds(0, HALF), pl.ds(HALF, HALF)
        slot = rest(j, 2)
        if stage == 1:
            @pl.loop(0, 4)
            def _(zz):
                for yy in range(2):
                    for xx in range(2):
                        got[j - CARRY, zz, yy, xx] += own[slot, zz, yy, xx]
        elif stage == 2:
            @pl.loop(0, 4)
            def _(zz):
                for i in range(2):
                    two[j, 0, zz, i] += got[j - CARRY, zz, y, i, :, a]
                    two[j, 1, zz, i] += got[j - CARRY, zz, i, x, :, b]
        elif stage == 3:
            for zz in range(4):
                three[j, zz, :, a] += two[j, 0, zz, x]
                three[j, zz, :, b] += two[j, 1, zz, y]
        else:
            total = three[j, z].astype(F32)
            for d in range(3):
                total += four[j, d].astype(F32)
            refs[len(self.ins)][j - self.first] = total

    def step(self, k, fire, refs):
        n, end, last = self.n, self.end, self.last
        got, own, two, three, four, ss, rs, ls = self.bufs(refs)
        start = lambda cp: cp.start()

        def go(stage, j):
            for cp in self.copies(stage, j, refs):
                cp.start()

        def take(stage, j):
            for cp in self.copies(stage - 1, j, refs):
                cp.wait_recv()
            self.add(stage, j, refs)

        @pl.when(fire & (k == 0))
        def _():
            @pl.loop(CARRY, CARRY + self.known)
            def _(j):
                self.swap(j, refs, start)

            for j in range(CARRY, min(CARRY + 2, end)):
                self.local(j, refs, start)
            if self.carried:
                for i in range(LAG):
                    two[LAG + i] = refs[len(self.ins) - 2][i]
                    three[i] = refs[len(self.ins) - 1][i]
                    go(2, LAG + i)
                    go(3, i)

        @pl.when(fire & (k < n))
        def _():
            j = k + CARRY
            self.swap(j, refs, lambda cp: cp.wait_recv())
            self.local(j, refs, lambda cp: cp.wait())
            self.add(1, j, refs)
            go(1, j)
            pl.when(j + 2 < end)(lambda: self.local(j + 2, refs, start))

        lows = [CARRY, LAG, 0] if self.carried else [CARRY] * 3
        for stage, low in zip((2, 3, 4), lows):
            j = k + (3 - stage) * LAG

            @pl.when(fire & (j >= low) & (j < end) & ((k < n) | last))
            def _(stage=stage, j=j):
                take(stage, j)
                if stage < 4:
                    go(stage, j)

        @pl.when(fire & (k == self.k - 1))
        def _():
            for stage, low in zip((2, 3, 4), lows):
                a = n + (3 - stage) * LAG
                if not last:
                    pl.loop(max(a, low), a + LAG)(functools.partial(take, stage))

                @pl.loop(CARRY if stage == 2 else low, end if last else a + LAG)
                def _(j):
                    for cp in self.copies(stage - 1, j, refs):
                        cp.wait_send()

            @pl.loop(CARRY, end)
            def _(j):
                self.swap(j, refs, lambda cp: cp.wait_send())

            if not last:
                for i in range(LAG):
                    refs[len(self.ins) + 1][i] = two[n + LAG + i]
                    refs[len(self.ins) + 2][i] = three[n + i]


class SmallSum:
    def __init__(self, row, at, t0, d):
        self.at, self.t0, self.k = at, t0, 1
        self.ins = [(row, pl.BlockSpec(memory_space=pltpu.VMEM))]
        self.outs = [(sds((8, d), F32), pl.BlockSpec(memory_space=pltpu.VMEM))]
        self.alias = []
        self.scratch = [pltpu.VMEM((4, 8, d), F32), pltpu.VMEM((6, 8, d), F32), pltpu.SemaphoreType.DMA((6,)), pltpu.SemaphoreType.DMA((6,))]

    def run(self, t, mine, refs):
        row, out, acc, got, ss, rs = refs
        zs, yp, xp, cp = peers()
        near = (cp, xp, yp, *zs)
        n = len(near) - len(zs)
        copies = [remote(acc.at[min(i, n)], got.at[i], ss.at[i], rs.at[i], dev) for i, dev in enumerate(near)]

        for i in range(n + 2):
            @pl.when(t == self.t0 + i)
            def _(i=i):
                if not i:
                    acc[i] = jnp.zeros_like(acc[i])
                    acc[i, pl.ds(0, 1)] = mine[...]
                    acc[i, pl.ds(1, 1)] = row[...]
                elif i <= n:
                    copies[i - 1].wait_recv()
                    acc[i] = acc[i - 1] + got[i - 1]
                else:
                    total = acc[n]
                    for j in range(n, len(near)):
                        copies[j].wait_recv()
                        total += got[j]
                    out[...] = total
                    for copy in copies:
                        copy.wait_send()
                for copy in copies[i:i + 1] if i < n else copies[n:] if i == n else ():
                    copy.start()


def host(name, cid, phases, comms=(), shared=(), cost=None):
    k_all = max([c.k for c in comms], default=1)
    at = 0
    for p in phases:
        if p.at is None:
            p.at = at
        at = max(at, p.end())
    small = [c for c in comms if isinstance(c, SmallSum)]
    total = max([at, k_all] + [c.t0 + 5 for c in small])
    kmap = lambda t: t if total == k_all else quot(t * (k_all - 1), total - 1)
    ins, in_specs, outs, out_specs, scratch, alias, resident = [], [], [], [], [], {}, []
    for p in phases:
        for arr, block, index in p.ins:
            if block == 'smem':
                in_specs.append(pl.BlockSpec(memory_space=pltpu.SMEM))
            elif index is None:
                resident.append((len(ins), p.at))
                in_specs.append(pl.BlockSpec(memory_space=HBM))
            else:
                in_specs.append(pl.BlockSpec(block, p.index(index)))
            ins.append(arr)
        for shape, block, index in p.outs:
            outs.append(shape)
            out_specs.append(pl.BlockSpec(block, p.index(index)))
    for c in comms:
        alias.update({len(ins) + i: len(outs) + o for i, o in c.alias})
        for arr, spec in c.ins:
            ins.append(arr)
            in_specs.append(spec)
        for shape, spec in c.outs:
            outs.append(shape)
            out_specs.append(spec)
        scratch += c.scratch
    scratch += [pltpu.VMEM(ins[i].shape, ins[i].dtype) for i, _ in resident] + [pltpu.SemaphoreType.DMA((max(len(resident), 1),))]
    scratch += list(shared)

    def kernel(*refs):
        refs = list(refs)
        rin, rout, rscr = refs[:len(ins)], refs[len(ins):len(ins) + len(outs)], refs[len(ins) + len(outs):]
        t = pl.program_id(0)
        if comms:
            locate()

            @pl.when(t == 0)
            def _():
                zs, yp, xp, cp = peers()
                near = (*zs, yp, xp, cp)
                bar = pltpu.get_barrier_semaphore()
                for dev in near:
                    pl.semaphore_signal(bar, inc=1, device_id=(dev,), device_id_type=MESH)
                pl.semaphore_wait(bar, len(near))
        i, o, s = sum(len(p.ins) for p in phases), sum(len(p.outs) for p in phases), 0
        k = kmap(t)
        fire = (t == 0) | (k != kmap(jnp.maximum(t - 1, 0)))
        for c in comms:
            ni, no, ns = len(c.ins), len(c.outs), len(c.scratch)
            crefs = rin[i:i + ni] + rout[o:o + no] + rscr[s:s + ns]
            c.refs = crefs
            if c not in small:
                c.step(k, fire, crefs)
            i, o, s = i + ni, o + no, s + ns
        held, rsem, extra = rscr[s:s + len(resident)], rscr[s + len(resident)], rscr[s + len(resident) + 1:]
        loads = [(pltpu.make_async_copy(rin[i], h, rsem.at[n]), at) for n, ((i, at), h) in enumerate(zip(resident, held))]
        if loads:
            @pl.when(t == 0)
            def _():
                for cp, _ in loads:
                    cp.start()
        for cp, at in loads:
            pl.when(t == at)(cp.wait)
        for (i, _), h in zip(resident, held):
            rin[i] = h
        i = o = 0
        for p in phases:
            pi, po = rin[i:i + len(p.ins)], rout[o:o + len(p.outs)]
            i, o = i + len(p.ins), o + len(p.outs)

            @pl.when(p.on(t))
            def _(p=p, pi=pi, po=po):
                p.body(p.own(t), pi, po, extra)

        for c in small:
            c.run(t, rout[c.at], c.refs)

    params = dict(dimension_semantics=("arbitrary",), vmem_limit_bytes=VMEM_LIMIT)
    if comms:
        params.update(collective_id=cid, has_side_effects=True)
    got = pl.pallas_call(kernel, grid=(total,), in_specs=in_specs, out_specs=out_specs, out_shape=outs, scratch_shapes=scratch,
                         input_output_aliases=alias, compiler_params=pltpu.CompilerParams(**params), name=name,
                         cost_estimate=pl.CostEstimate(flops=2 ** 34, bytes_accessed=2 ** 25, transcendentals=0))(*ins)
    return list(got)


def norm_parts(t):
    mean = row_mean(t)
    cen = t - mean
    rstd = lax.rsqrt(row_mean(cen * cen) + EPS)
    return cen * rstd, rstd


def norm_back(d, t, w):
    xhat, rstd = norm_parts(t)
    dh = d * w
    m1 = row_mean(dh)
    m2 = row_mean(dh * xhat)
    return rstd * (dh - m1 - xhat * m2), jnp.sum(d * xhat, axis=0, keepdims=True)


def alibi_slopes(n_heads):
    padded = 2 ** math.ceil(math.log2(n_heads))
    base = [2.0 ** (-8.0 * (k + 1) / padded) for k in range(padded)]
    ordered = base if padded == n_heads else base[1::2] + base[0::2]
    return jnp.array(ordered[:n_heads], dtype=F32)


def causal(i, tq, slope):
    row = lax.broadcasted_iota(jnp.int32, (tq, tq), 0)
    col = lax.broadcasted_iota(jnp.int32, (tq, tq), 1)
    rel = (row - col).astype(F32)
    diag = slope * rel
    past = None
    if i:
        r = lax.broadcasted_iota(jnp.int32, (tq, i * tq), 0) + i * tq
        q = lax.broadcasted_iota(jnp.int32, (tq, i * tq), 1)
        past = slope * (r - q).astype(F32)
    return past, diag, row >= col


def attn_fwd(q_ref, k_ref, v_ref, o_ref, l_ref, slope, scale, tq):
    n = q_ref.shape[0] // tq
    for i in range(n):
        rows, before = pl.ds(i * tq, tq), pl.ds(0, i * tq)
        q = q_ref[rows]
        past, diag, keep = causal(i, tq, slope)
        sd = jnp.where(keep, dot_t(q, k_ref[rows]) * scale - diag, -jnp.inf)
        m = row_max(sd)
        if i:
            sp = dot_t(q, k_ref[before]) * scale - past
            m = jnp.maximum(m, row_max(sp))
            ep = jnp.exp(sp - m)
        ed = jnp.exp(sd - m)
        l = row_sum(ed)
        if i:
            l = l + row_sum(ep)
        inv = 1.0 / l
        o = dot((ed * inv).astype(BF16), v_ref[rows])
        if i:
            o = o + dot((ep * inv).astype(BF16), v_ref[before])
        o_ref[rows] = o.astype(BF16)
        l_ref[rows] = m + jnp.log(l)


def attn_bwd(q_ref, k_ref, v_ref, a_ref, da_ref, l_ref, dq_ref, dk_ref, dv_ref, dk_s, dv_s, slope, scale, tq):
    n = q_ref.shape[0] // tq
    dk_s[...] = jnp.zeros_like(dk_s)
    dv_s[...] = jnp.zeros_like(dv_s)
    for i in range(n):
        rows, before = pl.ds(i * tq, tq), pl.ds(0, i * tq)
        q, da = q_ref[rows], da_ref[rows]
        lse = l_ref[rows]
        delta = row_sum(da.astype(F32) * a_ref[rows].astype(F32))
        past, diag, keep = causal(i, tq, slope)
        dq = None
        for own in ((True,) if i == 0 else (True, False)):
            keys = rows if own else before
            kk, vv = k_ref[keys], v_ref[keys]
            s = dot_t(q, kk) * scale - (diag if own else past)
            p = jnp.exp(s - lse)
            if own:
                p = jnp.where(keep, p, 0.0)
            ds = (p * (dot_t(da, vv) - delta) * scale).astype(BF16)
            dv_s[keys] += t_dot(p.astype(BF16), da)
            dk_s[keys] += t_dot(ds, q)
            part = dot(ds, kk)
            dq = part if dq is None else dq + part
        dq_ref[rows] = dq.astype(BF16)
    dk_ref[...] = dk_s[...].astype(BF16)
    dv_ref[...] = dv_s[...].astype(BF16)


def row_map(i):
    return i, 0


def col_map(i):
    return 0, i


def rows_of(a, n):
    return a, (n, a.shape[1]), row_map


def cols_of(a, n):
    return a, (a.shape[0], n), col_map


def heads_of(a, n, off=0):
    return a, (n,) + a.shape[1:], lambda i: (i + off, 0, 0)


def whole(a):
    return a, a.shape, None


def put(ref, i, part):
    @pl.when(i == 0)
    def _():
        ref[...] = part

    @pl.when(i > 0)
    def _():
        ref[...] += part


def side_by_side(ref, n):
    return jnp.concatenate([ref[j] for j in range(n)], axis=1)


def local_step(x, ln1, wq, wo, ln2, wu, wd, dy, comm=True):
    seq, d = x.shape
    heads, hd, ft = 12, 128, 512
    ff, nq, per = wu.shape[1], 3 * d, SUB // hd
    scale = 1 / math.sqrt(hd)
    tq = min(256, seq)
    tm = tq // 2
    nm, nf = seq // tm, ff // ft
    slopes = (alibi_slopes(heads), 'smem', None)
    b16 = lambda *shape: sds(shape, BF16)
    f32 = lambda *shape: sds(shape, F32)
    vm16 = lambda *shape: pltpu.VMEM(shape, BF16)
    vm32 = lambda *shape: pltpu.VMEM(shape, F32)
    act, wide, vec = b16(seq, d), b16(seq, ff), f32(1, d)
    one_vec = (vec, vec.shape, lambda i: (0, 0))
    band = lambda i: pl.ds(pl.multiple_of(i * tm, tm), tm)
    flat = lambda full: full.reshape(-1, full.shape[-1])
    order = [Unit(*w.shape).count for w in (wq, wo, wu, wd)]
    qs, os, us, ds = (sum(order[:i]) for i in range(4))
    ends = [i + 2 * LAG for i in (os, ds, sum(order))]

    nu = nq // SUB
    pack = sds((*CHIPS, 2, RB, nq), BF16)

    def G(*window):
        return [Gather(*window)] if comm else []

    def S(parts, **kw):
        return [Scatter([(a if a is pack else a.reshape(*CHIPS, 2, -1, a.shape[-1]), u0, n) for a, u0, n in parts], **kw)] if comm else []

    if comm:
        tile = jnp.pad(jnp.stack([ln1, ln2]), ((0, 6), (0, 128 - ln1.shape[0])))
        fq, fo, fu, lns = host('ag_qkv', 1, [], G([(wq, None, qs), (wo, None, os), (wu, None, us)], 0, ends[0]) + [GatherSmall(tile)])
        fq = flat(fq)
        w1, w2 = lns.reshape(-1, 8, 128)[:, :2, :ln1.shape[0]].transpose(1, 0, 2).reshape(2, 1, d)
    else:
        fq, fo, fu, w1, w2 = wq, wo, wu, ln1.reshape(1, d), ln2.reshape(1, d)

    def ln1_body(i, ins, outs, ext):
        (xr, lw), (ht,), (_, h1) = ins, outs, ext
        xhat, _ = norm_parts(xr[...].astype(F32))
        h = (xhat * lw[...]).astype(BF16)
        h1[band(i)] = h
        ht[...] = h.T

    def qkv_body(i, ins, outs, ext):
        (w,), (o,), (qkv, h1) = ins, outs, ext
        r = dot(h1[...], w[...]).astype(BF16)
        for j in range(per):
            qkv[i * per + j] = r[:, j * hd:(j + 1) * hd]
            o[j] = r[:, j * hd:(j + 1) * hd]

    def attn_body(i, ins, outs, ext):
        (sl,), (o, l), (qkv, _) = ins, outs, ext
        attn_fwd(qkv.at[i], qkv.at[heads + i], qkv.at[2 * heads + i], o, l.at[0], sl[i], scale, tq)

    pb = [Phase(nm, [rows_of(x, tm), whole(w1)], [cols_of(b16(d, seq), tm)], ln1_body),
          Phase(nq // SUB, [cols_of(fq, SUB)], [heads_of(b16(3 * heads, seq, hd), per)], qkv_body),
          Phase(heads, [slopes], [cols_of(act, hd), heads_of(f32(heads, seq, 1), 1)], attn_body)]
    h1t, qkv, attn, lse, *full = host('attn_fwd', 2, pb, G([(wo, fo, os), (wu, fu, us), (wd, None, ds)], ends[0], ends[1]),
                                      shared=[vm16(3 * heads, seq, hd), vm16(seq, d)])
    if comm:
        fo, fu, fd = full
        fo, fu = flat(fo), flat(fu)

    def out_body(i, ins, outs, ext):
        (xs, a, w, lw), (o, ht), (h2,) = ins, outs, ext
        x1 = (xs[...].astype(F32) + dot(a[...], w[...])).astype(BF16)
        o[...] = x1
        xhat, _ = norm_parts(x1.astype(F32))
        h = (xhat * lw[...]).astype(BF16)
        h2[band(i)] = h
        ht[...] = h.T

    def up_body(i, ins, outs, ext):
        (w, dyr), (go, gpo, gd), (h2,) = ins, outs, ext
        u = dot(h2[...], w[...])
        cdf = 0.5 * (1.0 + lax.erf(u * math.sqrt(0.5)))
        g = (u * cdf).astype(BF16)
        go[...] = g
        gpo[...] = cdf + u * (jnp.exp(-0.5 * u * u) * math.sqrt(0.5 / math.pi))
        gd[...] = t_dot(g, dyr[...]).astype(BF16)

    pc = [Phase(nm, [rows_of(x, tm), rows_of(attn, tm), whole(fo), whole(w2)], [rows_of(act, tm), cols_of(b16(d, seq), tm)], out_body),
          Phase(nf, [cols_of(fu, ft), whole(dy)], [cols_of(wide, ft), cols_of(f32(seq, ff), ft), rows_of(b16(ff, d), ft)], up_body)]
    x1, h2t, g, gp, g_down, *full = host('up', 3, pc, G([(wd, fd, ds)], ends[1], ends[2]) if comm else [], shared=[vm16(seq, d)])
    fd, = map(flat, full) if comm else (wd,)

    def dup_body(i, ins, outs, ext):
        (dyr, w, gpr, ht), (duo, gu) = ins, outs
        du = (dot_t(dyr[...], w[...]) * gpr[...]).astype(BF16)
        duo[...] = du
        gu[...] = dot(ht[...], du).astype(BF16)

    pd = [Phase(nf, [whole(dy), rows_of(fd, ft), cols_of(gp, ft), whole(h2t)], [cols_of(wide, ft), cols_of(b16(d, ff), ft)], dup_body)]
    n_down = Unit(ff // 32, d).count
    d_up, g_up, *r1 = host('dup', 4, pd, S([(g_down, 0, n_down)]))

    def dh2_body(i, ins, outs, ext):
        (du, w), acc = ins, ext[0]
        put(acc, i, dot_t(du[...], w[...]))

    def ln2b_body(i, ins, outs, ext):
        (xr, dyr, lw), (dmo, gwo), (acc, dmb, *_) = ins, outs, ext
        dx, gw = norm_back(acc[band(i)], xr[...].astype(F32), lw[...])
        dm = dyr[...].astype(F32) + dx
        dmo[...] = dm
        dmb[band(i)] = dm.astype(BF16)
        put(gwo, i, gw)

    def dattn_body(i, ins, outs, ext):
        (w,), (_, dmb, da, *_) = ins, ext
        r = dot_t(dmb[...], w[...]).astype(BF16)
        for j in range(ft // hd):
            da[i * (ft // hd) + j] = r[:, j * hd:(j + 1) * hd]

    def battn_body(i, ins, outs, ext):
        (q, k, v, a, l, sl), (o,), (acc, _, da) = ins, outs, ext
        dk, dv = (acc.at[:, pl.ds(j * hd, hd)] for j in range(2))
        attn_bwd(q.at[0], k.at[0], v.at[0], a, da.at[i], l.at[0], *(o.at[j, 0] for j in range(3)), dk, dv, sl[i], scale, tq)

    def gout_body(i, ins, outs, ext):
        (a,), (o,), (_, dmb, *_) = ins, outs, ext
        o[...] = t_dot(a[...], dmb[...]).astype(BF16)

    pe = [Phase(nf, [cols_of(d_up, ft), cols_of(fu, ft)], [], dh2_body),
          Phase(nm, [rows_of(x1, tm), rows_of(dy, tm), whole(w2)], [rows_of(f32(seq, d), tm), one_vec], ln2b_body),
          Phase(d // ft, [rows_of(fo, ft)], [], dattn_body),
          Phase(heads, [*(heads_of(qkv, 1, j * heads) for j in range(3)), cols_of(attn, hd), heads_of(lse, 1), slopes],
                [(b16(3, heads, seq, hd), (3, 1, seq, hd), lambda i: (0, i, 0, 0))], battn_body),
          Phase(d // ft, [cols_of(attn, ft)], [rows_of(b16(d, d), ft)], gout_body)]
    d_mid, g_ln2, d_qkv, g_out, *r2 = host('dh2', 5, pe, S([(g_up, 0, n_down)], carry=r1[1:]),
                                          shared=[vm32(seq, d), vm16(seq, d), vm16(heads, seq, hd)])
    d_qkv = d_qkv.reshape(3 * heads, seq, hd)

    scat = S([(g_out, 0, d // SUB), (pack, 0, nu)], carry=r2[1:], last=True)

    def tile_copy(i, ext):
        at = Unit(RB, nq).at(i)
        return pltpu.make_async_copy(ext[2].at[rest(i, 2)], scat[0].written().at[:, :, :, :, at[0], at[1]], ext[3].at[rest(i, 2)])

    def macro_body(i, ins, outs, ext):
        (ht, dq, w), acc = ins, ext[0]
        tile = side_by_side(dq, per)
        r = dot(ht[...], tile).astype(BF16)
        if comm:
            ext[2][rest(i, 2)] = r.reshape(*CHIPS, 2, RB, SUB)
            tile_copy(i, ext).start()
        else:
            outs[0][...] = r
        put(acc, i, dot_t(tile, w[...]))

    def ship_body(i, ins, outs, ext):
        tile_copy(i, ext).wait()
        scat[0].ship(i)

    def ln1b_body(i, ins, outs, ext):
        (xr, dm, lw), (o, gwo) = ins, outs
        dx, gw = norm_back(ext[0][band(i)], xr[...].astype(F32), lw[...])
        o[...] = (dm[...] + dx).astype(BF16)
        put(gwo, i, gw)

    def ydot_body(i, ins, outs, ext):
        (gr, w) = ins
        put(ext[1], i, dot(gr[...], w[...]))

    def y_body(i, ins, outs, ext):
        (xr,), (o,) = ins, outs
        o[...] = (xr[...].astype(F32) + ext[1][band(i)]).astype(BF16)

    first = [] if comm else [cols_of(b16(d, nq), SUB)]
    pf = [Phase(nu, [whole(h1t), heads_of(d_qkv, per), cols_of(fq, SUB)], first, macro_body, 0, 2),
          Phase(nm, [rows_of(x, tm), rows_of(d_mid, tm), whole(w1)], [rows_of(act, tm), one_vec], ln1b_body, 2 * nu, 2),
          Phase(nf, [cols_of(g, ft), rows_of(fd, ft)], [], ydot_body, 1, 2),
          Phase(nm, [rows_of(x1, tm)], [rows_of(act, tm)], y_body, 2 * nf + 1, 2)]
    if comm:
        pf.append(Phase(nu, [], [], ship_body, 1, 2))
        scat.append(SmallSum(g_ln2, 1, pf[1].end(), d))
    shared = [vm32(seq, d), vm32(seq, d), vm16(2, *CHIPS, 2, RB, SUB), pltpu.SemaphoreType.DMA((2,))]
    got = host('last', 6, pf, scat, shared=shared)
    if not comm:
        g_qkv, dx, g_ln1, y = got
        return y, dx, g_ln1, g_qkv, g_out, g_ln2, g_up, g_down
    dx, _, y, r3, _, sums = got
    units = jnp.concatenate([r1[0], r2[0], r3])
    nc = d // SUB
    g_down, g_up, g_out, g_qkv = jnp.split(units, (n_down, 2 * n_down, 2 * n_down + nc))
    flat_rows = lambda u: u.transpose(1, 0, 2).reshape(RB, -1)
    g_down = g_down.reshape(-1, nc, RB, SUB).transpose(0, 2, 1, 3).reshape(-1, d)
    return y, dx, sums, flat_rows(g_qkv), flat_rows(g_out), None, flat_rows(g_up), g_down


def solution(mesh):
    row_spec = P('fsdp')

    def step(x_in, ln1_w, w_qkv, w_out, ln2_w, w_up, w_down, dy_out):
        rows, _, heads, hd = w_qkv.shape
        d = x_in.shape[-1]
        y, dx, sums, g_qkv, g_out, _, g_up, g_down = local_step(
            x_in[0], ln1_w, w_qkv.reshape(rows, -1), w_out, ln2_w, w_up, w_down, dy_out[0])
        mine = lax.dynamic_slice_in_dim(sums, lax.axis_index('fsdp') * rows, rows, axis=1)
        return (y[None], dx[None], mine[0], g_qkv.reshape(rows, 3, heads, hd), g_out, mine[1], g_up, g_down)

    return jax.shard_map(step, mesh=mesh, in_specs=(row_spec,) * 8, out_specs=(row_spec,) * 8, check_vma=False)
```

```python
import functools
import math

import jax
import jax.numpy as jnp
from jax import lax
from jax.experimental import pallas as pl
from jax.experimental.pallas import tpu as pltpu
from jax.sharding import PartitionSpec as P

EPS = 1e-5
SUB = 512
WIDE = 768
HALF = SUB // 2
LAG = 2
GLAG = 1
CARRY = 2 * LAG
LEAD = 3
RB = 48
F32, BF16 = jnp.float32, jnp.bfloat16
VMEM_LIMIT = 67_000_000
MESH = pl.DeviceIdType.MESH
HBM = pltpu.MemorySpace.HBM
CHIPS = (4, 2, 2)


def sds(shape, dtype):
    return jax.ShapeDtypeStruct(shape, dtype)


def dot(a, b, ca=1, cb=0):
    return lax.dot_general(a, b, (((ca,), (cb,)), ((), ())), preferred_element_type=F32)


def dot_t(a, b):
    return dot(a, b, 1, 1)


def t_dot(a, b):
    return dot(a, b, 0, 0)


def over_rows(f):
    return functools.partial(f, axis=-1, keepdims=True)


row_sum, row_max, row_mean = map(over_rows, (jnp.sum, jnp.max, jnp.mean))


def clip(t, n):
    return jnp.minimum(jnp.maximum(t, 0), n - 1)


class Phase:
    def __init__(self, n, cost, ins, outs, body, at=None, stride=1):
        self.n, self.cost, self.ins, self.outs, self.body, self.at, self.stride = n, cost, ins, outs, body, at, stride

    def own(self, t):
        return quot(t - self.at, self.stride)

    def on(self, t):
        here = (t >= self.at) & (t < self.end())
        return here if self.stride == 1 else here & (rest(t - self.at, self.stride) == 0)

    def end(self):
        return self.at + (self.n - 1) * self.stride + 1

    def index(self, f):
        return lambda t: f(clip(self.own(jnp.maximum(t, self.at)), self.n))


def quot(a, b):
    return a // b if isinstance(a, int) else lax.div(a, b)


def rest(a, b):
    return a % b if isinstance(a, int) else lax.rem(a, b)


HERE = {}


def locate():
    me = lax.axis_index('fsdp')
    left, place = me, []
    for n in (2, *reversed(CHIPS)):
        place.append(rest(left, n))
        left = quot(left, n)
    c, x, y, z = place
    n, step, ways = CHIPS[0], 8, (1, 2, 3)
    cp, xp, yp = (me + s - 2 * s * b for s, b in zip((1, 2, 4), place))
    HERE.update(coords=(me, z, y, x, c), peers=([rest(me + step * d, step * n) for d in ways], yp, xp, cp), zs=[rest(z + d, n) for d in ways])


def coords():
    return HERE['coords']


def peers():
    return HERE['peers']


def remote(src, dst, ssem, rsem, dev):
    return pltpu.make_async_remote_copy(src_ref=src, dst_ref=dst, send_sem=ssem, recv_sem=rsem, device_id=(dev,), device_id_type=MESH)


class Unit:
    def __init__(self, rows, cols, width=SUB):
        self.width, self.nc, self.nr = width, cols // width, rows // RB
        self.count = self.nc * self.nr

    def at(self, u, half=None):
        lanes, col = self.width, rest(u, self.nc) * self.width
        if half is not None:
            lanes //= 2
            col = col + half * lanes
        rows = slice(None) if self.nr == 1 else pl.ds(pl.multiple_of(quot(u, self.nc) * RB, 16), RB)
        return rows, pl.ds(pl.multiple_of(col, 128), lanes)


class Gather:
    def __init__(self, weights, k0, k1):
        self.k0, self.k1 = k0, k1
        self.k, self.tail = k1 - k0 + 1, 0
        self.z0 = k0 + LEAD if k0 else 0
        self.z1 = k1 + LEAD
        self.w, self.ins, self.outs, self.alias = [], [], [], []
        for shard, full, first in weights:
            unit = Unit(*shard.shape, WIDE)
            self.w.append((len(self.ins), unit, first, first + unit.count, full is None))
            self.ins.append((shard, pl.BlockSpec(memory_space=pltpu.VMEM)))
            if full is not None:
                self.alias.append((len(self.ins), len(self.outs)))
                self.ins.append((full, pl.BlockSpec(memory_space=HBM)))
            self.outs.append((sds(CHIPS + (2,) + shard.shape, BF16), pl.BlockSpec(memory_space=HBM)))
        self.base = max(k0 - 2 * GLAG, 0)
        n = self.z1 - self.base
        self.scratch = [pltpu.SemaphoreType.DMA((n, 8)), pltpu.SemaphoreType.DMA((n, 8)), pltpu.SemaphoreType.DMA((len(weights),))]

    def copies(self, stage, w, u, refs):
        i, unit, first, _, _ = self.w[w]
        shard, full = refs[i], refs[len(self.ins) + w]
        sems = lambda i: (refs[-3].at[u - self.base, i], refs[-2].at[u - self.base, i])
        me, z, y, x, c = coords()
        zs, yp, xp, cp = peers()
        r, q = unit.at(u - first)
        if stage == 0:
            return [remote(shard.at[r, q], full.at[z, y, x, c, r, q], *sems(d), zs[d]) for d in range(3)]
        if stage == 3:
            v = full.at[:, :, :, c, r, q]
            return [remote(v, v, *sems(7), cp)]
        out = []
        for half in range(2):
            r, q = unit.at(u - first, half)
            j = 2 * stage + 1 + half
            if stage == 1:
                v = full.at[:, y, x, c, r, q]
            else:
                v = full.at[:, y, :, c, r, q] if half else full.at[:, :, x, c, r, q]
            out.append(remote(v, v, *sems(j), xp if half == stage % 2 else yp))
        return out

    def each(self, lo, hi, u, fn):
        for w, (_, _, first, last, _) in enumerate(self.w):
            a, b = max(lo, first), min(hi, last)
            if a < b:
                if u is None:
                    pl.loop(a, b)(functools.partial(fn, w))
                else:
                    pl.when((u >= a) & (u < b))(functools.partial(fn, w, u))

    def go(self, stage, w, u, refs):
        for cp in self.copies(stage, w, u, refs):
            cp.start()

    def arrive(self, stage, w, u, refs):
        for cp in self.copies(stage, w, u, refs):
            cp.wait_recv()

    def left(self, stage, w, u, refs):
        for cp in self.copies(stage, w, u, refs):
            cp.wait_send()

    def step(self, k, fire, refs):
        me, z, y, x, c = coords()
        k0, k1, k = self.k0, self.k1, k + self.k0
        span = [(self.z0, self.z1)] + [(max(k0 - i * GLAG, 0), k1 - i * GLAG) for i in range(3)]

        @pl.when(fire & (k == k0))
        def _():
            own = [pltpu.make_async_copy(refs[i], refs[len(self.ins) + w].at[z, y, x, c], refs[-1].at[w])
                   for w, (i, _, _, _, fresh) in enumerate(self.w) if fresh]
            for cp in own:
                cp.start()
            if k0 == 0:
                self.each(0, LEAD, None, lambda w, u: self.go(0, w, u, refs))
            for cp in own:
                cp.wait()

        @pl.when(fire & (k < k1))
        def _():
            self.each(*span[0], k + LEAD, lambda w, u: self.go(0, w, u, refs))
            for stage in (1, 2, 3):
                u = k + GLAG * (1 - stage)
                lo, hi = span[stage - 1]
                self.each(lo, hi, u, lambda w, u: self.arrive(stage - 1, w, u, refs))
                self.each(*span[stage], u, lambda w, u: self.go(stage, w, u, refs))

        @pl.when(fire & (k == k1))
        def _():
            for stage in range(4):
                lo, hi = span[stage]
                self.each(max(lo, k1 - stage * GLAG) if stage < 3 else lo, hi, None, lambda w, u: self.arrive(stage, w, u, refs))
                self.each(lo, hi, None, lambda w, u: self.left(stage, w, u, refs))


class GatherSmall:
    def __init__(self, tile):
        self.k, self.alias, self.tail = 5, [], 0
        self.ins = [(tile, pl.BlockSpec(memory_space=pltpu.VMEM))]
        self.outs = [(sds(CHIPS + (2,) + tile.shape, F32), pl.BlockSpec(memory_space=HBM))]
        self.scratch = [pltpu.SemaphoreType.DMA((6,)), pltpu.SemaphoreType.DMA((6,)), pltpu.SemaphoreType.DMA]

    def copies(self, stage, refs):
        tile, full, ss, rs, _ = refs
        me, z, y, x, c = coords()
        zs, yp, xp, cp = peers()
        if stage == 0:
            return [remote(tile, full.at[z, y, x, c], ss.at[d], rs.at[d], zs[d]) for d in range(3)]
        v, dev = ((full.at[:, y, x, c], yp), (full.at[:, :, x, c], xp), (full.at[:, :, :, c], cp))[stage - 1]
        return [remote(v, v, ss.at[2 + stage], rs.at[2 + stage], dev)]

    def step(self, k, fire, refs):
        tile, full, ss, rs, ls = refs
        me, z, y, x, c = coords()
        for stage in range(5):
            @pl.when(fire & (k == stage))
            def _(stage=stage):
                if stage == 0:
                    own = pltpu.make_async_copy(tile, full.at[z, y, x, c], ls)
                    own.start()
                else:
                    for cp in self.copies(stage - 1, refs):
                        cp.wait_recv()
                if stage < 4:
                    for cp in self.copies(stage, refs):
                        cp.start()
                else:
                    for st in range(4):
                        for cp in self.copies(st, refs):
                            cp.wait_send()
                if stage == 0:
                    own.wait()


class Scatter:
    def __init__(self, grads, carry=None, last=False):
        self.last, self.carried = last, carry is not None
        self.parts, self.ins, n = [], [], 0
        self.late = None
        for g, u0, m in grads:
            self.parts.append((n, n + m, u0, Unit(*g.shape[-2:])))
            if isinstance(g, jax.ShapeDtypeStruct):
                self.late = g
            else:
                self.ins.append((g, pl.BlockSpec(memory_space=HBM)))
            n += m
        self.known = n - m if self.late else n
        self.n = n
        self.first = 0 if self.carried else CARRY
        self.end = n + CARRY
        self.done = self.end if last else n
        self.k = n + (3 * LAG if last else 1)
        self.tail = 3 * LAG - 1 if last else 0
        self.two_shape, self.three_shape = (2, 4, 2, RB, HALF), (4, RB, SUB)
        if self.carried:
            self.ins += [(a, pl.BlockSpec(memory_space=pltpu.VMEM)) for a in carry]
        self.scratch = [
            pltpu.VMEM((n, *CHIPS, RB, SUB), BF16),
            pltpu.VMEM((2, *CHIPS, RB, SUB), BF16),
            pltpu.VMEM((self.end, *self.two_shape), BF16),
            pltpu.VMEM((self.end, *self.three_shape), BF16),
            pltpu.VMEM((self.end, 3, RB, SUB), BF16),
            pltpu.SemaphoreType.DMA((self.end, 8)), pltpu.SemaphoreType.DMA((self.end, 8)), pltpu.SemaphoreType.DMA((2,))]
        outs = [sds((self.done - self.first, RB, SUB), F32)]
        if not last:
            outs += [sds((LAG, *shape), BF16) for shape in (self.two_shape, self.three_shape)]
        self.outs = [(o, pl.BlockSpec(memory_space=pltpu.VMEM)) for o in outs]
        if self.late:
            self.outs.append((self.late, pl.BlockSpec(memory_space=HBM)))
        self.alias = []

    def source(self, j, refs, fn):
        for i, (a, b, u0, unit) in enumerate(self.parts):
            ref = self.written() if self.late and a == self.known else refs[i]
            u = j - CARRY
            if len(self.parts) == 1:
                fn(ref, *unit.at(u0 + u))
            else:
                pl.when((u >= a) & (u < b))(functools.partial(lambda ref, unit, u: fn(ref, *unit.at(u)), ref, unit, u0 + u - a))

    def written(self):
        return self.refs[len(self.ins) + len(self.outs) - 1]

    def ship(self, u):
        self.swap(CARRY + self.known + u, self.refs, lambda cp: cp.start())

    def bufs(self, refs):
        return refs[len(self.ins) + len(self.outs):]

    def local(self, j, refs, act):
        me, z, y, x, c = coords()
        own, ls = self.bufs(refs)[1], self.bufs(refs)[-1]
        slot = rest(j, 2)
        self.source(j, refs, lambda g, r, q: act(pltpu.make_async_copy(g.at[:, :, :, c, r, q], own.at[slot], ls.at[slot])))

    def swap(self, j, refs, act):
        me, z, y, x, c = coords()
        got, ss, rs = self.bufs(refs)[0], *self.bufs(refs)[-3:-1]
        cp = peers()[-1]
        self.source(j, refs, lambda g, r, q: act(remote(g.at[:, :, :, 1 - c, r, q], got.at[j - CARRY], ss.at[j, 0], rs.at[j, 0], cp)))

    def copies(self, stage, j, refs):
        got, own, two, three, four, ss, rs, ls = self.bufs(refs)
        me, z, y, x, c = coords()
        zs, yp, xp, cp = peers()
        a, b = pl.ds(0, HALF), pl.ds(HALF, HALF)
        if stage == 1:
            pairs = [(got.at[j - CARRY, :, 1 - y, :, :, a], two.at[j, 0], yp), (got.at[j - CARRY, :, :, 1 - x, :, b], two.at[j, 1], xp)]
        elif stage == 2:
            pairs = [(two.at[j, 0, :, 1 - x], three.at[j, :, :, a], xp), (two.at[j, 1, :, 1 - y], three.at[j, :, :, b], yp)]
        else:
            pairs = [(three.at[j, HERE['zs'][d]], four.at[j, d], zs[d]) for d in range(3)]
        return [remote(src, dst, ss.at[j, 2 * stage + i - 1], rs.at[j, 2 * stage + i - 1], dev) for i, (src, dst, dev) in enumerate(pairs)]

    def add(self, stage, j, refs):
        got, own, two, three, four, ss, rs, ls = self.bufs(refs)
        me, z, y, x, c = coords()
        a, b = pl.ds(0, HALF), pl.ds(HALF, HALF)
        slot = rest(j, 2)
        if stage == 1:
            @pl.loop(0, 4)
            def _(zz):
                for yy in range(2):
                    for xx in range(2):
                        got[j - CARRY, zz, yy, xx] += own[slot, zz, yy, xx]
        elif stage == 2:
            @pl.loop(0, 4)
            def _(zz):
                for i in range(2):
                    two[j, 0, zz, i] += got[j - CARRY, zz, y, i, :, a]
                    two[j, 1, zz, i] += got[j - CARRY, zz, i, x, :, b]
        elif stage == 3:
            for zz in range(4):
                three[j, zz, :, a] += two[j, 0, zz, x]
                three[j, zz, :, b] += two[j, 1, zz, y]
        else:
            total = three[j, z].astype(F32)
            for d in range(3):
                total += four[j, d].astype(F32)
            refs[len(self.ins)][j - self.first] = total

    def step(self, k, fire, refs):
        n, end, last = self.n, self.end, self.last
        got, own, two, three, four, ss, rs, ls = self.bufs(refs)
        start = lambda cp: cp.start()

        def go(stage, j):
            for cp in self.copies(stage, j, refs):
                cp.start()

        def take(stage, j):
            for cp in self.copies(stage - 1, j, refs):
                cp.wait_recv()
            self.add(stage, j, refs)

        @pl.when(fire & (k == 0))
        def _():
            @pl.loop(CARRY, CARRY + self.known)
            def _(j):
                self.swap(j, refs, start)

            self.local(CARRY, refs, start)
            if self.carried:
                for i in range(LAG):
                    two[LAG + i] = refs[len(self.ins) - 2][i]
                    three[i] = refs[len(self.ins) - 1][i]
                    go(2, LAG + i)
                    go(3, i)

        @pl.when(fire & (k < n))
        def _():
            j = k + CARRY
            pl.when(j + 1 < end)(lambda: self.local(j + 1, refs, start))
            self.swap(j, refs, lambda cp: cp.wait_recv())
            self.local(j, refs, lambda cp: cp.wait())
            self.add(1, j, refs)
            go(1, j)

        lows = [CARRY, LAG, 0] if self.carried else [CARRY] * 3
        for stage, low in zip((2, 3, 4), lows):
            j = k + (3 - stage) * LAG

            @pl.when(fire & (j >= low) & (j < end) & ((k < n) | last))
            def _(stage=stage, j=j):
                take(stage, j)
                if stage < 4:
                    go(stage, j)

        @pl.when(fire & (k == self.k - 1))
        def _():
            for stage, low in zip((2, 3, 4), lows):
                a = n + (3 - stage) * LAG
                if not last:
                    pl.loop(max(a, low), a + LAG)(functools.partial(take, stage))

                @pl.loop(CARRY if stage == 2 else low, end if last else a + LAG)
                def _(j):
                    for cp in self.copies(stage - 1, j, refs):
                        cp.wait_send()

            @pl.loop(CARRY, end)
            def _(j):
                self.swap(j, refs, lambda cp: cp.wait_send())

            if not last:
                for i in range(LAG):
                    refs[len(self.ins) + 1][i] = two[n + LAG + i]
                    refs[len(self.ins) + 2][i] = three[n + i]


class SmallSum:
    def __init__(self, row, at, t0, d):
        self.at, self.t0, self.k, self.tail = at, t0, 1, 0
        self.ins = [(row, pl.BlockSpec(memory_space=pltpu.VMEM))]
        self.outs = [(sds((8, d), F32), pl.BlockSpec(memory_space=pltpu.VMEM))]
        self.alias = []
        self.scratch = [pltpu.VMEM((4, 8, d), F32), pltpu.VMEM((6, 8, d), F32), pltpu.SemaphoreType.DMA((6,)), pltpu.SemaphoreType.DMA((6,))]

    def run(self, t, mine, refs):
        row, out, acc, got, ss, rs = refs
        zs, yp, xp, cp = peers()
        near = (cp, xp, yp, *zs)
        n = len(near) - len(zs)
        copies = [remote(acc.at[min(i, n)], got.at[i], ss.at[i], rs.at[i], dev) for i, dev in enumerate(near)]

        for i in range(n + 2):
            @pl.when(t == self.t0 + i)
            def _(i=i):
                if not i:
                    acc[i] = jnp.zeros_like(acc[i])
                    acc[i, pl.ds(0, 1)] = mine[...]
                    acc[i, pl.ds(1, 1)] = row[...]
                elif i <= n:
                    copies[i - 1].wait_recv()
                    acc[i] = acc[i - 1] + got[i - 1]
                else:
                    total = acc[n]
                    for j in range(n, len(near)):
                        copies[j].wait_recv()
                        total += got[j]
                    out[...] = total
                    for copy in copies:
                        copy.wait_send()
                for copy in copies[i:i + 1] if i < n else copies[n:] if i == n else ():
                    copy.start()


KERNELS = ['gather', 'attention', 'up', 'down', 'back', 'last']


def host(name, phases, comms=(), shared=(), pace=1):
    k_all = max([c.k for c in comms], default=1)
    at = 0
    for p in phases:
        if p.at is None:
            p.at = at
        at = max(at, p.end())
    small = [c for c in comms if isinstance(c, SmallSum)]
    tail = max([c.tail for c in comms], default=0)
    spread, clock, fires = k_all - 1 - tail, [0.0], [0]
    for t in range(at):
        clock.append(clock[-1] + sum(p.cost for p in phases if p.at <= t < p.end() and (t - p.at) % p.stride == 0))
    for k in range(1, k_all):
        t = at if k >= spread else min(t for t in range(at + 1) if clock[t] * spread >= clock[at] * k)
        fires.append(max(t, fires[-1] + 1, pace * k))
    total = max([at, fires[-1] + 1] + [c.t0 + 5 for c in small])
    ins, in_specs, outs, out_specs, scratch, alias, resident = [], [], [], [], [], {}, []
    for p in phases:
        for arr, block, index in p.ins:
            if block == 'smem':
                in_specs.append(pl.BlockSpec(memory_space=pltpu.SMEM))
            elif index is None:
                resident.append((len(ins), p.at))
                in_specs.append(pl.BlockSpec(memory_space=HBM))
            else:
                in_specs.append(pl.BlockSpec(block, p.index(index)))
            ins.append(arr)
        for shape, block, index in p.outs:
            outs.append(shape)
            out_specs.append(pl.BlockSpec(block, p.index(index)))
    for c in comms:
        alias.update({len(ins) + i: len(outs) + o for i, o in c.alias})
        for arr, spec in c.ins:
            ins.append(arr)
            in_specs.append(spec)
        for shape, spec in c.outs:
            outs.append(shape)
            out_specs.append(spec)
        scratch += c.scratch
    scratch += [pltpu.VMEM(ins[i].shape, ins[i].dtype) for i, _ in resident] + [pltpu.SemaphoreType.DMA((max(len(resident), 1),))]
    scratch += list(shared)

    def kernel(*refs):
        refs = list(refs)
        rin, rout, rscr = refs[:len(ins)], refs[len(ins):len(ins) + len(outs)], refs[len(ins) + len(outs):]
        t = pl.program_id(0)
        if comms:
            locate()

            @pl.when(t == 0)
            def _():
                zs, yp, xp, cp = peers()
                near = (*zs, yp, xp, cp)
                bar = pltpu.get_barrier_semaphore()
                for dev in near:
                    pl.semaphore_signal(bar, inc=1, device_id=(dev,), device_id_type=MESH)
                pl.semaphore_wait(bar, len(near))
        i, o, s = sum(len(p.ins) for p in phases), sum(len(p.outs) for p in phases), 0
        k = sum([(t >= f).astype(jnp.int32) for f in fires[1:]], 0 * t)
        fire = functools.reduce(jnp.logical_or, [t == f for f in fires])
        for c in comms:
            ni, no, ns = len(c.ins), len(c.outs), len(c.scratch)
            crefs = rin[i:i + ni] + rout[o:o + no] + rscr[s:s + ns]
            c.refs = crefs
            if c not in small:
                c.step(k, fire, crefs)
            i, o, s = i + ni, o + no, s + ns
        held, rsem, extra = rscr[s:s + len(resident)], rscr[s + len(resident)], rscr[s + len(resident) + 1:]
        loads = [(pltpu.make_async_copy(rin[i], h, rsem.at[n]), at) for n, ((i, at), h) in enumerate(zip(resident, held))]
        if loads:
            @pl.when(t == 0)
            def _():
                for cp, _ in loads:
                    cp.start()
        for cp, at in loads:
            pl.when(t == at)(cp.wait)
        for (i, _), h in zip(resident, held):
            rin[i] = h
        i = o = 0
        for p in phases:
            pi, po = rin[i:i + len(p.ins)], rout[o:o + len(p.outs)]
            i, o = i + len(p.ins), o + len(p.outs)

            @pl.when(p.on(t))
            def _(p=p, pi=pi, po=po):
                p.body(p.own(t), pi, po, extra)

        for c in small:
            c.run(t, rout[c.at], c.refs)

    params = dict(dimension_semantics=("arbitrary",), vmem_limit_bytes=VMEM_LIMIT)
    if comms:
        params.update(collective_id=KERNELS.index(name), has_side_effects=True)
    got = pl.pallas_call(kernel, grid=(total,), in_specs=in_specs, out_specs=out_specs, out_shape=outs, scratch_shapes=scratch,
                         input_output_aliases=alias, compiler_params=pltpu.CompilerParams(**params), name=name,
                         cost_estimate=pl.CostEstimate(flops=2 ** 34, bytes_accessed=2 ** 25, transcendentals=0))(*ins)
    return list(got)


def norm_parts(t):
    mean = row_mean(t)
    cen = t - mean
    rstd = lax.rsqrt(row_mean(cen * cen) + EPS)
    return cen * rstd, rstd


def norm_back(d, t, w):
    xhat, rstd = norm_parts(t)
    dh = d * w
    m1 = row_mean(dh)
    m2 = row_mean(dh * xhat)
    return rstd * (dh - m1 - xhat * m2), jnp.sum(d * xhat, axis=0, keepdims=True)


def alibi_slopes(n_heads):
    padded = 2 ** math.ceil(math.log2(n_heads))
    base = [2.0 ** (-8.0 * (k + 1) / padded) for k in range(padded)]
    ordered = base if padded == n_heads else base[1::2] + base[0::2]
    return jnp.array(ordered[:n_heads], dtype=F32)


def causal(i, tq, slope):
    row = lax.broadcasted_iota(jnp.int32, (tq, tq), 0)
    col = lax.broadcasted_iota(jnp.int32, (tq, tq), 1)
    rel = (row - col).astype(F32)
    diag = slope * rel
    past = None
    if i:
        r = lax.broadcasted_iota(jnp.int32, (tq, i * tq), 0) + i * tq
        q = lax.broadcasted_iota(jnp.int32, (tq, i * tq), 1)
        past = slope * (r - q).astype(F32)
    return past, diag, row >= col


def attn_fwd(q_ref, k_ref, v_ref, o_ref, l_ref, slope, scale, tq):
    n = q_ref.shape[0] // tq
    for i in range(n):
        rows, before = pl.ds(i * tq, tq), pl.ds(0, i * tq)
        q = q_ref[rows]
        past, diag, keep = causal(i, tq, slope)
        sd = jnp.where(keep, dot_t(q, k_ref[rows]) * scale - diag, -jnp.inf)
        m = row_max(sd)
        if i:
            sp = dot_t(q, k_ref[before]) * scale - past
            m = jnp.maximum(m, row_max(sp))
            ep = jnp.exp(sp - m)
        ed = jnp.exp(sd - m)
        l = row_sum(ed)
        if i:
            l = l + row_sum(ep)
        inv = 1.0 / l
        o = dot((ed * inv).astype(BF16), v_ref[rows])
        if i:
            o = o + dot((ep * inv).astype(BF16), v_ref[before])
        o_ref[rows] = o.astype(BF16)
        l_ref[rows] = m + jnp.log(l)


def attn_bwd(q_ref, k_ref, v_ref, a_ref, da_ref, l_ref, dq_ref, dk_ref, dv_ref, dk_s, dv_s, slope, scale, tq):
    n = q_ref.shape[0] // tq
    dk_s[...] = jnp.zeros_like(dk_s)
    dv_s[...] = jnp.zeros_like(dv_s)
    for i in range(n):
        rows, before = pl.ds(i * tq, tq), pl.ds(0, i * tq)
        q, da = q_ref[rows], da_ref[rows]
        lse = l_ref[rows]
        delta = row_sum(da.astype(F32) * a_ref[rows].astype(F32))
        past, diag, keep = causal(i, tq, slope)
        dq = None
        for own in ((True,) if i == 0 else (True, False)):
            keys = rows if own else before
            kk, vv = k_ref[keys], v_ref[keys]
            s = dot_t(q, kk) * scale - (diag if own else past)
            p = jnp.exp(s - lse)
            if own:
                p = jnp.where(keep, p, 0.0)
            ds = (p * (dot_t(da, vv) - delta) * scale).astype(BF16)
            dv_s[keys] += t_dot(p.astype(BF16), da)
            dk_s[keys] += t_dot(ds, q)
            part = dot(ds, kk)
            dq = part if dq is None else dq + part
        dq_ref[rows] = dq.astype(BF16)
    dk_ref[...] = dk_s[...].astype(BF16)
    dv_ref[...] = dv_s[...].astype(BF16)


def row_map(i):
    return i, 0


def col_map(i):
    return 0, i


def rows_of(a, n):
    return a, (n, a.shape[1]), row_map


def cols_of(a, n):
    return a, (a.shape[0], n), col_map


def heads_of(a, n, off=0):
    return a, (n,) + a.shape[1:], lambda i: (i + off, 0, 0)


def whole(a):
    return a, a.shape, None


def put(ref, i, part):
    @pl.when(i == 0)
    def _():
        ref[...] = part

    @pl.when(i > 0)
    def _():
        ref[...] += part


def side_by_side(ref, n):
    return jnp.concatenate([ref[j] for j in range(n)], axis=1)


def local_step(x, ln1, wq, wo, ln2, wu, wd, dy, comm=True):
    seq, d = x.shape
    heads, hd, ft = 12, 128, 512
    ff, nq, per = wu.shape[1], 3 * d, SUB // hd
    scale = 1 / math.sqrt(hd)
    tq = min(256, seq)
    tm = tq // 2
    nm, nf = seq // tm, ff // ft
    slopes = (alibi_slopes(heads), 'smem', None)
    b16 = lambda *shape: sds(shape, BF16)
    f32 = lambda *shape: sds(shape, F32)
    vm16 = lambda *shape: pltpu.VMEM(shape, BF16)
    vm32 = lambda *shape: pltpu.VMEM(shape, F32)
    act, wide, vec = b16(seq, d), b16(seq, ff), f32(1, d)
    one_vec = (vec, vec.shape, lambda i: (0, 0))
    band = lambda i: pl.ds(pl.multiple_of(i * tm, tm), tm)
    flat = lambda full: full.reshape(-1, full.shape[-1])
    order = [Unit(*w.shape, WIDE).count for w in (wq, wo, wu, wd)]
    qs, os, us, ds = (sum(order[:i]) for i in range(4))
    ends = [i + 2 * GLAG for i in (os, ds, sum(order))]

    nu = nq // SUB
    pack = sds((*CHIPS, 2, RB, nq), BF16)

    def G(*window):
        return [Gather(*window)] if comm else []

    def S(parts, **kw):
        return [Scatter([(a if a is pack else a.reshape(*CHIPS, 2, -1, a.shape[-1]), u0, n) for a, u0, n in parts], **kw)] if comm else []

    if comm:
        tile = jnp.pad(jnp.stack([ln1, ln2]), ((0, 6), (0, 128 - ln1.shape[0])))
        fq, fo, fu, lns = host('gather', [], G([(wq, None, qs), (wo, None, os), (wu, None, us)], 0, ends[0]) + [GatherSmall(tile)])
        fq = flat(fq)
        w1, w2 = lns.reshape(-1, 8, 128)[:, :2, :ln1.shape[0]].transpose(1, 0, 2).reshape(2, 1, d)
    else:
        fq, fo, fu, w1, w2 = wq, wo, wu, ln1.reshape(1, d), ln2.reshape(1, d)

    def ln1_body(i, ins, outs, ext):
        (xr, lw), (ht,), (_, h1) = ins, outs, ext
        xhat, _ = norm_parts(xr[...].astype(F32))
        h = (xhat * lw[...]).astype(BF16)
        h1[band(i)] = h
        ht[...] = h.T

    def qkv_body(i, ins, outs, ext):
        (w,), (o,), (qkv, h1) = ins, outs, ext
        r = dot(h1[...], w[...]).astype(BF16)
        for j in range(per):
            qkv[i * per + j] = r[:, j * hd:(j + 1) * hd]
            o[j] = r[:, j * hd:(j + 1) * hd]

    def attn_body(i, ins, outs, ext):
        (sl,), (o, l), (qkv, _) = ins, outs, ext
        attn_fwd(qkv.at[i], qkv.at[heads + i], qkv.at[2 * heads + i], o, l.at[0], sl[i], scale, tq)

    pb = [Phase(nm, 0.5, [rows_of(x, tm), whole(w1)], [cols_of(b16(d, seq), tm)], ln1_body),
          Phase(nq // SUB, 1.9, [cols_of(fq, SUB)], [heads_of(b16(3 * heads, seq, hd), per)], qkv_body),
          Phase(heads, 1.8, [slopes], [cols_of(act, hd), heads_of(f32(heads, seq, 1), 1)], attn_body)]
    h1t, qkv, attn, lse, *full = host('attention', pb, G([(wo, fo, os), (wu, fu, us), (wd, None, ds)], ends[0], ends[1]),
                                      shared=[vm16(3 * heads, seq, hd), vm16(seq, d)])
    if comm:
        fo, fu, fd = full
        fo, fu = flat(fo), flat(fu)

    def out_body(i, ins, outs, ext):
        (xs, a, w, lw), (o, ht), (h2,) = ins, outs, ext
        x1 = (xs[...].astype(F32) + dot(a[...], w[...])).astype(BF16)
        o[...] = x1
        xhat, _ = norm_parts(x1.astype(F32))
        h = (xhat * lw[...]).astype(BF16)
        h2[band(i)] = h
        ht[...] = h.T

    def up_body(i, ins, outs, ext):
        (w, dyr), (go, gpo, gd), (h2,) = ins, outs, ext
        u = dot(h2[...], w[...])
        cdf = 0.5 * (1.0 + lax.erf(u * math.sqrt(0.5)))
        g = (u * cdf).astype(BF16)
        go[...] = g
        gpo[...] = cdf + u * (jnp.exp(-0.5 * u * u) * math.sqrt(0.5 / math.pi))
        gd[...] = t_dot(g, dyr[...]).astype(BF16)

    pc = [Phase(nm, 1.4, [rows_of(x, tm), rows_of(attn, tm), whole(fo), whole(w2)], [rows_of(act, tm), cols_of(b16(d, seq), tm)], out_body),
          Phase(nf, 4.0, [cols_of(fu, ft), whole(dy)], [cols_of(wide, ft), cols_of(f32(seq, ff), ft), rows_of(b16(ff, d), ft)], up_body)]
    x1, h2t, g, gp, g_down, *full = host('up', pc, G([(wd, fd, ds)], ends[1], ends[2]) if comm else [], shared=[vm16(seq, d)])
    fd, = map(flat, full) if comm else (wd,)

    def dup_body(i, ins, outs, ext):
        (dyr, w, gpr, ht), (duo, gu) = ins, outs
        du = (dot_t(dyr[...], w[...]) * gpr[...]).astype(BF16)
        duo[...] = du
        gu[...] = dot(ht[...], du).astype(BF16)

    pd = [Phase(nf, 3.9, [whole(dy), rows_of(fd, ft), cols_of(gp, ft), whole(h2t)], [cols_of(wide, ft), cols_of(b16(d, ff), ft)], dup_body)]
    n_down = Unit(ff // 32, d).count
    d_up, g_up, *r1 = host('down', pd, S([(g_down, 0, n_down)]))

    def dh2_body(i, ins, outs, ext):
        (du, w), acc = ins, ext[0]
        put(acc, i, dot_t(du[...], w[...]))

    def ln2b_body(i, ins, outs, ext):
        (xr, dyr, lw), (dmo, gwo), (acc, dmb, *_) = ins, outs, ext
        dx, gw = norm_back(acc[band(i)], xr[...].astype(F32), lw[...])
        dm = dyr[...].astype(F32) + dx
        dmo[...] = dm
        dmb[band(i)] = dm.astype(BF16)
        put(gwo, i, gw)

    def dattn_body(i, ins, outs, ext):
        (w,), (_, dmb, da, *_) = ins, ext
        r = dot_t(dmb[...], w[...]).astype(BF16)
        for j in range(ft // hd):
            da[i * (ft // hd) + j] = r[:, j * hd:(j + 1) * hd]

    def battn_body(i, ins, outs, ext):
        (q, k, v, a, l, sl), (o,), (acc, _, da) = ins, outs, ext
        dk, dv = (acc.at[:, pl.ds(j * hd, hd)] for j in range(2))
        attn_bwd(q.at[0], k.at[0], v.at[0], a, da.at[i], l.at[0], *(o.at[j, 0] for j in range(3)), dk, dv, sl[i], scale, tq)

    def gout_body(i, ins, outs, ext):
        (a,), (o,), (_, dmb, *_) = ins, outs, ext
        o[...] = t_dot(a[...], dmb[...]).astype(BF16)

    pe = [Phase(nf, 2.3, [cols_of(d_up, ft), cols_of(fu, ft)], [], dh2_body),
          Phase(nm, 0.7, [rows_of(x1, tm), rows_of(dy, tm), whole(w2)], [rows_of(f32(seq, d), tm), one_vec], ln2b_body),
          Phase(d // ft, 1.9, [rows_of(fo, ft)], [], dattn_body),
          Phase(heads, 2.9, [*(heads_of(qkv, 1, j * heads) for j in range(3)), cols_of(attn, hd), heads_of(lse, 1), slopes],
                [(b16(3, heads, seq, hd), (3, 1, seq, hd), lambda i: (0, i, 0, 0))], battn_body),
          Phase(d // ft, 1.9, [cols_of(attn, ft)], [rows_of(b16(d, d), ft)], gout_body)]
    d_mid, g_ln2, d_qkv, g_out, *r2 = host('back', pe, S([(g_up, 0, n_down)], carry=r1[1:]),
                                          shared=[vm32(seq, d), vm16(seq, d), vm16(heads, seq, hd)])
    d_qkv = d_qkv.reshape(3 * heads, seq, hd)

    scat = S([(g_out, 0, d // SUB), (pack, 0, nu)], carry=r2[1:], last=True)

    def tile_copy(i, ext):
        r, q = Unit(RB, nq).at(i)
        return pltpu.make_async_copy(ext[2], scat[0].written().at[:, :, :, :, r, q], ext[3])

    def macro_body(i, ins, outs, ext):
        (ht, dq, w), acc = ins, ext[0]
        tile = side_by_side(dq, per)
        r = dot(ht[...], tile).astype(BF16)
        if comm:
            ext[2][...] = r.reshape(*CHIPS, 2, RB, SUB)
            tile_copy(i, ext).start()
        else:
            outs[0][...] = r
        put(acc, i, dot_t(tile, w[...]))

    def ship_body(i, ins, outs, ext):
        tile_copy(i, ext).wait()
        scat[0].ship(i)

    def ln1b_body(i, ins, outs, ext):
        (xr, dm, lw), (o, gwo) = ins, outs
        dx, gw = norm_back(ext[0][band(i)], xr[...].astype(F32), lw[...])
        o[...] = (dm[...] + dx).astype(BF16)
        put(gwo, i, gw)

    def ydot_body(i, ins, outs, ext):
        (gr, w) = ins
        put(ext[1], i, dot(gr[...], w[...]))

    def y_body(i, ins, outs, ext):
        (xr,), (o,) = ins, outs
        o[...] = (xr[...].astype(F32) + ext[1][band(i)]).astype(BF16)

    first = [] if comm else [cols_of(b16(d, nq), SUB)]
    pf = [Phase(nu, 3.9, [whole(h1t), heads_of(d_qkv, per), cols_of(fq, SUB)], first, macro_body, 0, 2),
          Phase(nm, 0.7, [rows_of(x, tm), rows_of(d_mid, tm), whole(w1)], [rows_of(act, tm), one_vec], ln1b_body, 2 * nu, 2),
          Phase(nf, 2.3, [cols_of(g, ft), rows_of(fd, ft)], [], ydot_body, 1, 2),
          Phase(nm, 0.4, [rows_of(x1, tm)], [rows_of(act, tm)], y_body, 2 * nf + 1, 2)]
    if comm:
        pf.append(Phase(nu, 0, [], [], ship_body, 1, 2))
        scat.append(SmallSum(g_ln2, 1, pf[1].end(), d))
    shared = [vm32(seq, d), vm32(seq, d), vm16(*CHIPS, 2, RB, SUB), pltpu.SemaphoreType.DMA]
    got = host('last', pf, scat, shared=shared, pace=2)
    if not comm:
        g_qkv, dx, g_ln1, y = got
        return y, dx, g_ln1, g_qkv, g_out, g_ln2, g_up, g_down
    dx, _, y, r3, _, sums = got
    units = jnp.concatenate([r1[0], r2[0], r3])
    nc = d // SUB
    g_down, g_up, g_out, g_qkv = jnp.split(units, (n_down, 2 * n_down, 2 * n_down + nc))
    flat_rows = lambda u: u.transpose(1, 0, 2).reshape(RB, -1)
    g_down = g_down.reshape(-1, nc, RB, SUB).transpose(0, 2, 1, 3).reshape(-1, d)
    return y, dx, sums, flat_rows(g_qkv), flat_rows(g_out), None, flat_rows(g_up), g_down


def solution(mesh):
    row_spec = P('fsdp')

    def step(x_in, ln1_w, w_qkv, w_out, ln2_w, w_up, w_down, dy_out):
        rows, _, heads, hd = w_qkv.shape
        d = x_in.shape[-1]
        y, dx, sums, g_qkv, g_out, _, g_up, g_down = local_step(
            x_in[0], ln1_w, w_qkv.reshape(rows, -1), w_out, ln2_w, w_up, w_down, dy_out[0])
        mine = lax.dynamic_slice_in_dim(sums, lax.axis_index('fsdp') * rows, rows, axis=1)
        return (y[None], dx[None], mine[0], g_qkv.reshape(rows, 3, heads, hd), g_out, mine[1], g_up, g_down)

    return jax.shard_map(step, mesh=mesh, in_specs=(row_spec,) * 8, out_specs=(row_spec,) * 8, check_vma=False)
```

```python
import functools
import math

import jax
import jax.numpy as jnp
from jax import lax
from jax.experimental import pallas as pl
from jax.experimental.pallas import tpu as pltpu
from jax.sharding import PartitionSpec as P

EPS = 1e-5
LOG2E = math.log2(math.e)
SUB = 512
WIDE = 768
HALF = SUB // 2
LAG = 1
CARRY = 2 * LAG
LEAD = 3
RB = 48
F32, BF16 = jnp.float32, jnp.bfloat16
VMEM_LIMIT = 67_000_000
MESH = pl.DeviceIdType.MESH
HBM = pltpu.MemorySpace.HBM
CHIPS = (4, 2, 2)


def sds(shape, dtype):
    return jax.ShapeDtypeStruct(shape, dtype)


def dot(a, b, ca=1, cb=0):
    return lax.dot_general(a, b, (((ca,), (cb,)), ((), ())), preferred_element_type=F32)


def dot_t(a, b):
    return dot(a, b, 1, 1)


def t_dot(a, b):
    return dot(a, b, 0, 0)


def over_rows(f):
    return functools.partial(f, axis=-1, keepdims=True)


row_sum, row_max, row_mean = map(over_rows, (jnp.sum, jnp.max, jnp.mean))


def clip(t, n):
    return jnp.minimum(jnp.maximum(t, 0), n - 1)


class Phase:
    def __init__(self, n, cost, ins, outs, body, at=None):
        self.n, self.cost, self.ins, self.outs, self.body, self.at = n, cost, ins, outs, body, at

    def on(self, t):
        return (t >= self.at) & (t < self.at + self.n)

    def index(self, f):
        return lambda t: f(clip(t - self.at, self.n))


def quot(a, b):
    return a // b if isinstance(a, int) else lax.div(a, b)


def rest(a, b):
    return a % b if isinstance(a, int) else lax.rem(a, b)


HERE = {}


def locate():
    me = lax.axis_index('fsdp')
    left, place = me, []
    for n in (2, *reversed(CHIPS)):
        place.append(rest(left, n))
        left = quot(left, n)
    c, x, y, z = place
    n, step, ways = CHIPS[0], 8, (1, 2, 3)
    cp, xp, yp = (me + s - 2 * s * b for s, b in zip((1, 2, 4), place))
    HERE.update(coords=(me, z, y, x, c), peers=([rest(me + step * d, step * n) for d in ways], yp, xp, cp), zs=[rest(z + d, n) for d in ways])


def coords():
    return HERE['coords']


def peers():
    return HERE['peers']


def remote(src, dst, ssem, rsem, dev):
    return pltpu.make_async_remote_copy(src_ref=src, dst_ref=dst, send_sem=ssem, recv_sem=rsem, device_id=(dev,), device_id_type=MESH)


class Unit:
    def __init__(self, rows, cols, width=SUB):
        self.width, self.nc, self.nr = width, cols // width, rows // RB
        self.count = self.nc * self.nr

    def at(self, u, half=None):
        lanes, col = self.width, rest(u, self.nc) * self.width
        if half is not None:
            lanes //= 2
            col = col + half * lanes
        rows = slice(None) if self.nr == 1 else pl.ds(pl.multiple_of(quot(u, self.nc) * RB, 16), RB)
        return rows, pl.ds(pl.multiple_of(col, 128), lanes)


class Gather:
    def __init__(self, weights, k0, k1):
        self.k0, self.k1 = k0, k1
        self.k, self.tail = k1 - k0 + 1, 0
        self.z0 = k0 + LEAD if k0 else 0
        self.z1 = k1 + LEAD
        self.w, self.ins, self.outs, self.alias = [], [], [], []
        for shard, full, first in weights:
            unit = Unit(*shard.shape, WIDE)
            self.w.append((len(self.ins), unit, first, first + unit.count, full is None))
            self.ins.append((shard, pl.BlockSpec(memory_space=pltpu.VMEM)))
            if full is not None:
                self.alias.append((len(self.ins), len(self.outs)))
                self.ins.append((full, pl.BlockSpec(memory_space=HBM)))
            self.outs.append((sds(CHIPS + (2,) + shard.shape, BF16), pl.BlockSpec(memory_space=HBM)))
        self.base = max(k0 - 2 * LAG, 0)
        n = self.z1 - self.base
        self.scratch = [pltpu.SemaphoreType.DMA((n, 8)), pltpu.SemaphoreType.DMA((n, 8)), pltpu.SemaphoreType.DMA((len(weights),))]

    def copies(self, stage, w, u, refs):
        i, unit, first, _, _ = self.w[w]
        shard, full = refs[i], refs[len(self.ins) + w]
        sems = lambda i: (refs[-3].at[u - self.base, i], refs[-2].at[u - self.base, i])
        me, z, y, x, c = coords()
        zs, yp, xp, cp = peers()
        r, q = unit.at(u - first)
        if stage == 0:
            return [remote(shard.at[r, q], full.at[z, y, x, c, r, q], *sems(d), zs[d]) for d in range(3)]
        if stage == 3:
            v = full.at[:, :, :, c, r, q]
            return [remote(v, v, *sems(7), cp)]
        out = []
        for half in range(2):
            r, q = unit.at(u - first, half)
            j = 2 * stage + 1 + half
            if stage == 1:
                v = full.at[:, y, x, c, r, q]
            else:
                v = full.at[:, y, :, c, r, q] if half else full.at[:, :, x, c, r, q]
            out.append(remote(v, v, *sems(j), xp if half == stage % 2 else yp))
        return out

    def each(self, lo, hi, u, fn):
        for w, (_, _, first, last, _) in enumerate(self.w):
            a, b = max(lo, first), min(hi, last)
            if a < b:
                if u is None:
                    pl.loop(a, b)(functools.partial(fn, w))
                else:
                    pl.when((u >= a) & (u < b))(functools.partial(fn, w, u))

    def go(self, stage, w, u, refs):
        for cp in self.copies(stage, w, u, refs):
            cp.start()

    def arrive(self, stage, w, u, refs):
        for cp in self.copies(stage, w, u, refs):
            cp.wait_recv()

    def left(self, stage, w, u, refs):
        for cp in self.copies(stage, w, u, refs):
            cp.wait_send()

    def step(self, k, fire, refs):
        me, z, y, x, c = coords()
        k0, k1, k = self.k0, self.k1, k + self.k0
        span = [(self.z0, self.z1)] + [(max(k0 - i * LAG, 0), k1 - i * LAG) for i in range(3)]

        @pl.when(fire & (k == k0))
        def _():
            own = [pltpu.make_async_copy(refs[i], refs[len(self.ins) + w].at[z, y, x, c], refs[-1].at[w])
                   for w, (i, _, _, _, fresh) in enumerate(self.w) if fresh]
            for cp in own:
                cp.start()
            if k0 == 0:
                self.each(0, LEAD, None, lambda w, u: self.go(0, w, u, refs))
            for cp in own:
                cp.wait()

        @pl.when(fire & (k < k1))
        def _():
            self.each(*span[0], k + LEAD, lambda w, u: self.go(0, w, u, refs))
            for stage in (1, 2, 3):
                u = k + LAG * (1 - stage)
                lo, hi = span[stage - 1]
                self.each(lo, hi, u, lambda w, u: self.arrive(stage - 1, w, u, refs))
                self.each(*span[stage], u, lambda w, u: self.go(stage, w, u, refs))

        @pl.when(fire & (k == k1))
        def _():
            for stage in range(4):
                lo, hi = span[stage]
                self.each(max(lo, k1 - stage * LAG) if stage < 3 else lo, hi, None, lambda w, u: self.arrive(stage, w, u, refs))
                self.each(lo, hi, None, lambda w, u: self.left(stage, w, u, refs))


class GatherSmall:
    def __init__(self, tile):
        self.k, self.alias, self.tail = 5, [], 0
        self.ins = [(tile, pl.BlockSpec(memory_space=pltpu.VMEM))]
        self.outs = [(sds(CHIPS + (2,) + tile.shape, F32), pl.BlockSpec(memory_space=HBM))]
        self.scratch = [pltpu.SemaphoreType.DMA((6,)), pltpu.SemaphoreType.DMA((6,)), pltpu.SemaphoreType.DMA]

    def copies(self, stage, refs):
        tile, full, ss, rs, _ = refs
        me, z, y, x, c = coords()
        zs, yp, xp, cp = peers()
        if stage == 0:
            return [remote(tile, full.at[z, y, x, c], ss.at[d], rs.at[d], zs[d]) for d in range(3)]
        v, dev = ((full.at[:, y, x, c], yp), (full.at[:, :, x, c], xp), (full.at[:, :, :, c], cp))[stage - 1]
        return [remote(v, v, ss.at[2 + stage], rs.at[2 + stage], dev)]

    def step(self, k, fire, refs):
        tile, full, ss, rs, ls = refs
        me, z, y, x, c = coords()
        for stage in range(5):
            @pl.when(fire & (k == stage))
            def _(stage=stage):
                if stage == 0:
                    own = pltpu.make_async_copy(tile, full.at[z, y, x, c], ls)
                    own.start()
                else:
                    for cp in self.copies(stage - 1, refs):
                        cp.wait_recv()
                if stage < 4:
                    for cp in self.copies(stage, refs):
                        cp.start()
                else:
                    for st in range(4):
                        for cp in self.copies(st, refs):
                            cp.wait_send()
                if stage == 0:
                    own.wait()


class Scatter:
    def __init__(self, grads, carry=None, last=False):
        self.last, self.carried = last, carry is not None
        self.parts, self.ins, n = [], [], 0
        self.late = None
        for g, u0, m in grads:
            self.parts.append((n, n + m, u0, Unit(*g.shape[-2:])))
            if isinstance(g, jax.ShapeDtypeStruct):
                self.late = g
            else:
                self.ins.append((g, pl.BlockSpec(memory_space=HBM)))
            n += m
        self.known = n - m if self.late else n
        self.n = n
        self.first = 0 if self.carried else CARRY
        self.end = n + CARRY
        self.done = self.end if last else n
        self.k = n + (3 * LAG if last else 1)
        self.tail = 3 * LAG - 1 if last else 0
        self.two_shape, self.three_shape = (2, 4, 2, RB, HALF), (4, RB, SUB)
        if self.carried:
            self.ins += [(a, pl.BlockSpec(memory_space=pltpu.VMEM)) for a in carry]
        self.scratch = [
            pltpu.VMEM((n, *CHIPS, RB, SUB), BF16),
            pltpu.VMEM((2, *CHIPS, RB, SUB), BF16),
            pltpu.VMEM((self.end, *self.two_shape), BF16),
            pltpu.VMEM((self.end, *self.three_shape), BF16),
            pltpu.VMEM((self.end, 3, RB, SUB), BF16),
            pltpu.SemaphoreType.DMA((self.end, 8)), pltpu.SemaphoreType.DMA((self.end, 8)), pltpu.SemaphoreType.DMA((2,))]
        outs = [sds((self.done - self.first, RB, SUB), F32)]
        if not last:
            outs += [sds((LAG, *shape), BF16) for shape in (self.two_shape, self.three_shape)]
        self.outs = [(o, pl.BlockSpec(memory_space=pltpu.VMEM)) for o in outs]
        if self.late:
            self.outs.append((self.late, pl.BlockSpec(memory_space=HBM)))
        self.alias = []

    def source(self, j, refs, fn):
        for i, (a, b, u0, unit) in enumerate(self.parts):
            ref = self.written() if self.late and a == self.known else refs[i]
            u = j - CARRY
            if len(self.parts) == 1:
                fn(ref, *unit.at(u0 + u))
            else:
                pl.when((u >= a) & (u < b))(functools.partial(lambda ref, unit, u: fn(ref, *unit.at(u)), ref, unit, u0 + u - a))

    def written(self):
        return self.refs[len(self.ins) + len(self.outs) - 1]

    def ship(self, u):
        self.swap(CARRY + self.known + u, self.refs, lambda cp: cp.start())

    def bufs(self, refs):
        return refs[len(self.ins) + len(self.outs):]

    def local(self, j, refs, act):
        me, z, y, x, c = coords()
        own, ls = self.bufs(refs)[1], self.bufs(refs)[-1]
        slot = rest(j, 2)
        self.source(j, refs, lambda g, r, q: act(pltpu.make_async_copy(g.at[:, :, :, c, r, q], own.at[slot], ls.at[slot])))

    def swap(self, j, refs, act):
        me, z, y, x, c = coords()
        got, ss, rs = self.bufs(refs)[0], *self.bufs(refs)[-3:-1]
        cp = peers()[-1]
        self.source(j, refs, lambda g, r, q: act(remote(g.at[:, :, :, 1 - c, r, q], got.at[j - CARRY], ss.at[j, 0], rs.at[j, 0], cp)))

    def copies(self, stage, j, refs):
        got, own, two, three, four, ss, rs, ls = self.bufs(refs)
        me, z, y, x, c = coords()
        zs, yp, xp, cp = peers()
        a, b = pl.ds(0, HALF), pl.ds(HALF, HALF)
        if stage == 1:
            pairs = [(got.at[j - CARRY, :, 1 - y, :, :, a], two.at[j, 0], yp), (got.at[j - CARRY, :, :, 1 - x, :, b], two.at[j, 1], xp)]
        elif stage == 2:
            pairs = [(two.at[j, 0, :, 1 - x], three.at[j, :, :, a], xp), (two.at[j, 1, :, 1 - y], three.at[j, :, :, b], yp)]
        else:
            pairs = [(three.at[j, HERE['zs'][d]], four.at[j, d], zs[d]) for d in range(3)]
        return [remote(src, dst, ss.at[j, 2 * stage + i - 1], rs.at[j, 2 * stage + i - 1], dev) for i, (src, dst, dev) in enumerate(pairs)]

    def add(self, stage, j, refs):
        got, own, two, three, four, ss, rs, ls = self.bufs(refs)
        me, z, y, x, c = coords()
        a, b = pl.ds(0, HALF), pl.ds(HALF, HALF)
        slot = rest(j, 2)
        if stage == 1:
            @pl.loop(0, 4)
            def _(zz):
                for yy in range(2):
                    for xx in range(2):
                        got[j - CARRY, zz, yy, xx] += own[slot, zz, yy, xx]
        elif stage == 2:
            @pl.loop(0, 4)
            def _(zz):
                for i in range(2):
                    two[j, 0, zz, i] += got[j - CARRY, zz, y, i, :, a]
                    two[j, 1, zz, i] += got[j - CARRY, zz, i, x, :, b]
        elif stage == 3:
            for zz in range(4):
                three[j, zz, :, a] += two[j, 0, zz, x]
                three[j, zz, :, b] += two[j, 1, zz, y]
        else:
            total = three[j, z].astype(F32)
            for d in range(3):
                total += four[j, d].astype(F32)
            refs[len(self.ins)][j - self.first] = total

    def step(self, k, fire, refs):
        n, end, last = self.n, self.end, self.last
        got, own, two, three, four, ss, rs, ls = self.bufs(refs)
        start = lambda cp: cp.start()

        def go(stage, j):
            for cp in self.copies(stage, j, refs):
                cp.start()

        def take(stage, j):
            for cp in self.copies(stage - 1, j, refs):
                cp.wait_recv()
            self.add(stage, j, refs)

        @pl.when(fire & (k == 0))
        def _():
            @pl.loop(CARRY, CARRY + self.known)
            def _(j):
                self.swap(j, refs, start)

            self.local(CARRY, refs, start)
            if self.carried:
                for i in range(LAG):
                    two[LAG + i] = refs[len(self.ins) - 2][i]
                    three[i] = refs[len(self.ins) - 1][i]
                    go(2, LAG + i)
                    go(3, i)

        @pl.when(fire & (k < n))
        def _():
            j = k + CARRY
            pl.when(j + 1 < end)(lambda: self.local(j + 1, refs, start))
            self.swap(j, refs, lambda cp: cp.wait_recv())
            self.local(j, refs, lambda cp: cp.wait())
            self.add(1, j, refs)
            go(1, j)

        lows = [CARRY, LAG, 0] if self.carried else [CARRY] * 3
        for stage, low in zip((2, 3, 4), lows):
            j = k + (3 - stage) * LAG

            @pl.when(fire & (j >= low) & (j < end) & ((k < n) | last))
            def _(stage=stage, j=j):
                take(stage, j)
                if stage < 4:
                    go(stage, j)

        @pl.when(fire & (k == self.k - 1))
        def _():
            for stage, low in zip((2, 3, 4), lows):
                a = n + (3 - stage) * LAG
                if not last:
                    pl.loop(max(a, low), a + LAG)(functools.partial(take, stage))

                @pl.loop(CARRY if stage == 2 else low, end if last else a + LAG)
                def _(j):
                    for cp in self.copies(stage - 1, j, refs):
                        cp.wait_send()

            @pl.loop(CARRY, end)
            def _(j):
                self.swap(j, refs, lambda cp: cp.wait_send())

            if not last:
                for i in range(LAG):
                    refs[len(self.ins) + 1][i] = two[n + LAG + i]
                    refs[len(self.ins) + 2][i] = three[n + i]


class SmallSum:
    def __init__(self, row, at, t0, d):
        self.at, self.t0, self.k, self.tail = at, t0, 1, 0
        self.ins = [(row, pl.BlockSpec(memory_space=pltpu.VMEM))]
        self.outs = [(sds((8, d), F32), pl.BlockSpec(memory_space=pltpu.VMEM))]
        self.alias = []
        self.scratch = [pltpu.VMEM((4, 8, d), F32), pltpu.VMEM((6, 8, d), F32), pltpu.SemaphoreType.DMA((6,)), pltpu.SemaphoreType.DMA((6,))]

    def run(self, t, mine, refs):
        row, out, acc, got, ss, rs = refs
        zs, yp, xp, cp = peers()
        near = (cp, xp, yp, *zs)
        n = len(near) - len(zs)
        copies = [remote(acc.at[min(i, n)], got.at[i], ss.at[i], rs.at[i], dev) for i, dev in enumerate(near)]

        for i in range(n + 2):
            @pl.when(t == self.t0 + i)
            def _(i=i):
                if not i:
                    acc[i] = jnp.zeros_like(acc[i])
                    acc[i, pl.ds(0, 1)] = mine[...]
                    acc[i, pl.ds(1, 1)] = row[...]
                elif i <= n:
                    copies[i - 1].wait_recv()
                    acc[i] = acc[i - 1] + got[i - 1]
                else:
                    total = acc[n]
                    for j in range(n, len(near)):
                        copies[j].wait_recv()
                        total += got[j]
                    out[...] = total
                    for copy in copies:
                        copy.wait_send()
                for copy in copies[i:i + 1] if i < n else copies[n:] if i == n else ():
                    copy.start()


KERNELS = ['gather', 'attention', 'up', 'down', 'back', 'last']


def host(name, phases, comms=(), shared=()):
    k_all = max([c.k for c in comms], default=1)
    at = 0
    for p in phases:
        if p.at is None:
            p.at = at
        at = max(at, p.at + p.n)
    small = [c for c in comms if isinstance(c, SmallSum)]
    tail = max([c.tail for c in comms], default=0)
    spread, clock, fires = k_all - 1 - tail, [0.0], [0]
    for t in range(at):
        clock.append(clock[-1] + sum(p.cost for p in phases if p.at <= t < p.at + p.n))
    for k in range(1, k_all):
        t = at if k >= spread else min(t for t in range(at + 1) if clock[t] * spread >= clock[at] * k)
        fires.append(max(t, fires[-1] + 1))
    total = max([at, fires[-1] + 1] + [c.t0 + 5 for c in small])
    ins, in_specs, outs, out_specs, scratch, alias, resident = [], [], [], [], [], {}, []
    for p in phases:
        for arr, block, index in p.ins:
            if block == 'smem':
                in_specs.append(pl.BlockSpec(memory_space=pltpu.SMEM))
            elif index is None:
                resident.append((len(ins), p.at))
                in_specs.append(pl.BlockSpec(memory_space=HBM))
            else:
                in_specs.append(pl.BlockSpec(block, p.index(index)))
            ins.append(arr)
        for shape, block, index in p.outs:
            outs.append(shape)
            out_specs.append(pl.BlockSpec(block, p.index(index)))
    for c in comms:
        alias.update({len(ins) + i: len(outs) + o for i, o in c.alias})
        for arr, spec in c.ins:
            ins.append(arr)
            in_specs.append(spec)
        for shape, spec in c.outs:
            outs.append(shape)
            out_specs.append(spec)
        scratch += c.scratch
    scratch += [pltpu.VMEM(ins[i].shape, ins[i].dtype) for i, _ in resident] + [pltpu.SemaphoreType.DMA((max(len(resident), 1),))]
    scratch += list(shared)

    def kernel(*refs):
        refs = list(refs)
        rin, rout, rscr = refs[:len(ins)], refs[len(ins):len(ins) + len(outs)], refs[len(ins) + len(outs):]
        t = pl.program_id(0)
        if comms:
            locate()

            @pl.when(t == 0)
            def _():
                zs, yp, xp, cp = peers()
                near = (*zs, yp, xp, cp)
                bar = pltpu.get_barrier_semaphore()
                for dev in near:
                    pl.semaphore_signal(bar, inc=1, device_id=(dev,), device_id_type=MESH)
                pl.semaphore_wait(bar, len(near))
        i, o, s = sum(len(p.ins) for p in phases), sum(len(p.outs) for p in phases), 0
        k = sum([(t >= f).astype(jnp.int32) for f in fires[1:]], 0 * t)
        fire = functools.reduce(jnp.logical_or, [t == f for f in fires])
        for c in comms:
            ni, no, ns = len(c.ins), len(c.outs), len(c.scratch)
            crefs = rin[i:i + ni] + rout[o:o + no] + rscr[s:s + ns]
            c.refs = crefs
            if c not in small:
                c.step(k, fire, crefs)
            i, o, s = i + ni, o + no, s + ns
        held, rsem, extra = rscr[s:s + len(resident)], rscr[s + len(resident)], rscr[s + len(resident) + 1:]
        loads = [(pltpu.make_async_copy(rin[i], h, rsem.at[n]), at) for n, ((i, at), h) in enumerate(zip(resident, held))]
        if loads:
            @pl.when(t == 0)
            def _():
                for cp, _ in loads:
                    cp.start()
        for cp, at in loads:
            pl.when(t == at)(cp.wait)
        for (i, _), h in zip(resident, held):
            rin[i] = h
        i = o = 0
        for p in phases:
            pi, po = rin[i:i + len(p.ins)], rout[o:o + len(p.outs)]
            i, o = i + len(p.ins), o + len(p.outs)

            @pl.when(p.on(t))
            def _(p=p, pi=pi, po=po):
                p.body(t - p.at, pi, po, extra)

        for c in small:
            c.run(t, rout[c.at], c.refs)

    params = dict(dimension_semantics=("arbitrary",), vmem_limit_bytes=VMEM_LIMIT)
    if comms:
        params.update(collective_id=KERNELS.index(name), has_side_effects=True)
    got = pl.pallas_call(kernel, grid=(total,), in_specs=in_specs, out_specs=out_specs, out_shape=outs, scratch_shapes=scratch,
                         input_output_aliases=alias, compiler_params=pltpu.CompilerParams(**params), name=name,
                         cost_estimate=pl.CostEstimate(flops=2 ** 34, bytes_accessed=2 ** 25, transcendentals=0))(*ins)
    return list(got)


def norm_parts(t):
    mean = row_mean(t)
    cen = t - mean
    rstd = lax.rsqrt(row_mean(cen * cen) + EPS)
    return cen * rstd, rstd


def norm_back(d, t, w):
    xhat, rstd = norm_parts(t)
    dh = d * w
    m1 = row_mean(dh)
    m2 = row_mean(dh * xhat)
    return rstd * (dh - m1 - xhat * m2), jnp.sum(d * xhat, axis=0, keepdims=True)


def alibi_slopes(n_heads):
    padded = 2 ** math.ceil(math.log2(n_heads))
    base = [2.0 ** (-8.0 * (k + 1) / padded) for k in range(padded)]
    ordered = base if padded == n_heads else base[1::2] + base[0::2]
    return jnp.array(ordered[:n_heads], dtype=F32)


def bias(i, tq, slope):
    def ahead(n, first):
        return lax.broadcasted_iota(jnp.int32, (1, n), 1).astype(F32) * slope + slope * first

    row, col = (lax.broadcasted_iota(jnp.int32, (tq, tq), a) for a in range(2))
    return ahead(tq, 0.0), ahead(i * tq, -float(i * tq)) if i else None, row >= col


def attn_fwd(q_ref, k_ref, v_ref, o_ref, l_ref, slope, scale, tq):
    slope, scale = slope * LOG2E, scale * LOG2E
    for i in range(q_ref.shape[0] // tq):
        rows, before = pl.ds(i * tq, tq), pl.ds(0, i * tq)
        q = q_ref[rows]
        near, far, keep = bias(i, tq, slope)
        sd = jnp.where(keep, dot_t(q, k_ref[rows]) * scale + near, -jnp.inf)
        m = row_max(sd)
        if i:
            sp = dot_t(q, k_ref[before]) * scale + far
            m = jnp.maximum(m, row_max(sp))
            ep = jnp.exp2(sp - m)
        ed = jnp.exp2(sd - m)
        l = row_sum(ed)
        if i:
            l = l + row_sum(ep)
        inv = 1 / l
        o = dot((ed * inv).astype(BF16), v_ref[rows])
        if i:
            o = o + dot((ep * inv).astype(BF16), v_ref[before])
        o_ref[rows] = o.astype(BF16)
        l_ref[rows] = m + jnp.log2(l)


def attn_bwd(q_ref, k_ref, v_ref, a_ref, da_ref, l_ref, dq_ref, dk_ref, dv_ref, dk_s, dv_s, slope, scale, tq):
    slope2, scale2 = slope * LOG2E, scale * LOG2E
    dk_s[...] = jnp.zeros_like(dk_s)
    dv_s[...] = jnp.zeros_like(dv_s)
    for i in range(q_ref.shape[0] // tq):
        rows, before = pl.ds(i * tq, tq), pl.ds(0, i * tq)
        q, da = q_ref[rows], da_ref[rows]
        lse = l_ref[rows]
        delta = row_sum(da.astype(F32) * a_ref[rows].astype(F32))
        near, far, keep = bias(i, tq, slope2)
        dq = None
        for keys, ahead in ((rows, near), (before, far))[:2 if i else 1]:
            kk, vv = k_ref[keys], v_ref[keys]
            p = jnp.exp2(dot_t(q, kk) * scale2 + ahead - lse)
            if keys is rows:
                p = jnp.where(keep, p, 0)
            ds = (p * (dot_t(da, vv) - delta)).astype(BF16)
            dv_s[keys] += t_dot(p.astype(BF16), da)
            dk_s[keys] += t_dot(ds, q)
            part = dot(ds, kk)
            dq = part if dq is None else dq + part
        dq_ref[rows] = (dq * scale).astype(BF16)
    dk_ref[...] = (dk_s[...] * scale).astype(BF16)
    dv_ref[...] = dv_s[...].astype(BF16)


def row_map(i):
    return i, 0


def col_map(i):
    return 0, i


def rows_of(a, n):
    return a, (n, a.shape[1]), row_map


def cols_of(a, n):
    return a, (a.shape[0], n), col_map


def heads_of(a, n, off=0):
    return a, (n,) + a.shape[1:], lambda i: (i + off, 0, 0)


def whole(a):
    return a, a.shape, None


def put(ref, i, part):
    @pl.when(i == 0)
    def _():
        ref[...] = jnp.zeros_like(ref)

    ref[...] += part()


def side_by_side(ref, n):
    return jnp.concatenate([ref[j] for j in range(n)], axis=1)


def local_step(x, ln1, wq, wo, ln2, wu, wd, dy, comm=True):
    seq, d = x.shape
    heads, hd, ft = 12, 128, 512
    ff, nq, per = wu.shape[1], 3 * d, SUB // hd
    scale = 1 / math.sqrt(hd)
    tq = min(256, seq)
    tm = tq
    nm, nf = seq // tm, ff // ft
    slopes = (alibi_slopes(heads), 'smem', None)
    b16 = lambda *shape: sds(shape, BF16)
    f32 = lambda *shape: sds(shape, F32)
    vm16 = lambda *shape: pltpu.VMEM(shape, BF16)
    vm32 = lambda *shape: pltpu.VMEM(shape, F32)
    act, wide, vec = b16(seq, d), b16(seq, ff), f32(1, d)
    one_vec = (vec, vec.shape, lambda i: (0, 0))
    band = lambda i: pl.ds(pl.multiple_of(i * tm, tm), tm)
    flat = lambda full: full.reshape(-1, full.shape[-1])
    order = [Unit(*w.shape, WIDE).count for w in (wq, wo, wu, wd)]
    qs, os, us, ds = (sum(order[:i]) for i in range(4))
    ends = [i + 2 * LAG for i in (os, ds, sum(order))]

    nu = nq // SUB
    pack = sds((*CHIPS, 2, RB, nq), BF16)

    def G(*window):
        return [Gather(*window)] if comm else []

    def S(parts, **kw):
        return [Scatter([(a if a is pack else a.reshape(*CHIPS, 2, -1, a.shape[-1]), u0, n) for a, u0, n in parts], **kw)] if comm else []

    if comm:
        tile = jnp.pad(jnp.stack([ln1, ln2]), ((0, 6), (0, 128 - ln1.shape[0])))
        fq, fo, fu, lns = host('gather', [], G([(wq, None, qs), (wo, None, os), (wu, None, us)], 0, ends[0]) + [GatherSmall(tile)])
        fq = flat(fq)
        w1, w2 = lns.reshape(-1, 8, 128)[:, :2, :ln1.shape[0]].transpose(1, 0, 2).reshape(2, 1, d)
    else:
        fq, fo, fu, w1, w2 = wq, wo, wu, ln1.reshape(1, d), ln2.reshape(1, d)

    def ln1_body(i, ins, outs, ext):
        (xr, lw), (ht,), (_, h1) = ins, outs, ext
        xhat, _ = norm_parts(xr[...].astype(F32))
        h = (xhat * lw[...]).astype(BF16)
        h1[band(i)] = h
        ht[...] = h.T

    def qkv_body(i, ins, outs, ext):
        (w,), (o,), (qkv, h1) = ins, outs, ext
        r = dot(h1[...], w[...]).astype(BF16)
        for j in range(per):
            qkv[i * per + j] = r[:, j * hd:(j + 1) * hd]
            o[j] = r[:, j * hd:(j + 1) * hd]

    def attn_body(i, ins, outs, ext):
        (sl,), (o, l), (qkv, _) = ins, outs, ext
        attn_fwd(qkv.at[i], qkv.at[heads + i], qkv.at[2 * heads + i], o, l.at[0], sl[i], scale, tq)

    pb = [Phase(nm, 1, [rows_of(x, tm), whole(w1)], [cols_of(b16(d, seq), tm)], ln1_body),
          Phase(nq // SUB, 1.9, [cols_of(fq, SUB)], [heads_of(b16(3 * heads, seq, hd), per)], qkv_body),
          Phase(heads, 2.2, [slopes], [cols_of(act, hd), heads_of(f32(heads, seq, 1), 1)], attn_body)]
    h1t, qkv, attn, lse, *full = host('attention', pb, G([(wo, fo, os), (wu, fu, us), (wd, None, ds)], ends[0], ends[1]),
                                      shared=[vm16(3 * heads, seq, hd), vm16(seq, d)])
    if comm:
        fo, fu, fd = full
        fo, fu = flat(fo), flat(fu)

    def out_body(i, ins, outs, ext):
        (xs, a, w, lw), (o, ht), (h2,) = ins, outs, ext
        x1 = (xs[...].astype(F32) + dot(a[...], w[...])).astype(BF16)
        o[...] = x1
        xhat, _ = norm_parts(x1.astype(F32))
        h = (xhat * lw[...]).astype(BF16)
        h2[band(i)] = h
        ht[...] = h.T

    def up_body(i, ins, outs, ext):
        (w, dyr), (go, gpo, gd), (h2,) = ins, outs, ext
        u = dot(h2[...], w[...])
        cdf = 0.5 * (1.0 + lax.erf(u * math.sqrt(0.5)))
        g = (u * cdf).astype(BF16)
        go[...] = g
        gpo[...] = cdf + u * (jnp.exp(-0.5 * u * u) * math.sqrt(0.5 / math.pi))
        gd[...] = t_dot(g, dyr[...]).astype(BF16)

    pc = [Phase(nm, 3, [rows_of(x, tm), rows_of(attn, tm), whole(fo), whole(w2)], [rows_of(act, tm), cols_of(b16(d, seq), tm)], out_body),
          Phase(nf, 4.0, [cols_of(fu, ft), whole(dy)], [cols_of(wide, ft), cols_of(f32(seq, ff), ft), rows_of(b16(ff, d), ft)], up_body)]
    x1, h2t, g, gp, g_down, *full = host('up', pc, G([(wd, fd, ds)], ends[1], ends[2]) if comm else [], shared=[vm16(seq, d)])
    fd, = map(flat, full) if comm else (wd,)

    def dup_body(i, ins, outs, ext):
        (dyr, w, gr, gpr, ht), (duo, gu), (acc,) = ins, outs, ext
        du = (dot_t(dyr[...], w[...]) * gpr[...]).astype(BF16)
        duo[...] = du
        gu[...] = dot(ht[...], du).astype(BF16)
        put(acc, i, lambda: dot(gr[...], w[...]))

    def y_body(i, ins, outs, ext):
        (xr,), (o,), (acc,) = ins, outs, ext
        o[...] = (xr[...].astype(F32) + acc[band(i)]).astype(BF16)

    pd = [Phase(nf, 6, [whole(dy), rows_of(fd, ft), cols_of(g, ft), cols_of(gp, ft), whole(h2t)], [cols_of(wide, ft), cols_of(b16(d, ff), ft)], dup_body),
          Phase(nm, 1, [rows_of(x1, tm)], [rows_of(act, tm)], y_body)]
    n_down = Unit(ff // 32, d).count
    d_up, g_up, y, *r1 = host('down', pd, S([(g_down, 0, n_down)]), shared=[vm32(seq, d)])

    def dh2_body(i, ins, outs, ext):
        (du, w), acc = ins, ext[0]
        put(acc, i, lambda: dot_t(du[...], w[...]))

    def ln2b_body(i, ins, outs, ext):
        (xr, dyr, lw), (dmo, gwo), (acc, dmb, *_) = ins, outs, ext
        dx, gw = norm_back(acc[band(i)], xr[...].astype(F32), lw[...])
        dm = dyr[...].astype(F32) + dx
        dmo[...] = dm
        dmb[band(i)] = dm.astype(BF16)
        put(gwo, i, lambda: gw)

    def dattn_body(i, ins, outs, ext):
        (w,), (_, dmb, da, *_) = ins, ext
        r = dot_t(dmb[...], w[...]).astype(BF16)
        for j in range(ft // hd):
            da[i * (ft // hd) + j] = r[:, j * hd:(j + 1) * hd]

    def battn_body(i, ins, outs, ext):
        (q, k, v, a, l, sl), (o,), (acc, _, da) = ins, outs, ext
        dk, dv = (acc.at[:, pl.ds(j * hd, hd)] for j in range(2))
        attn_bwd(q.at[0], k.at[0], v.at[0], a, da.at[i], l.at[0], *(o.at[j, 0] for j in range(3)), dk, dv, sl[i], scale, tq)

    def gout_body(i, ins, outs, ext):
        (a,), (o,), (_, dmb, *_) = ins, outs, ext
        o[...] = t_dot(a[...], dmb[...]).astype(BF16)

    pe = [Phase(nf, 2.4, [cols_of(d_up, ft), cols_of(fu, ft)], [], dh2_body),
          Phase(nm, 2, [rows_of(x1, tm), rows_of(dy, tm), whole(w2)], [rows_of(f32(seq, d), tm), one_vec], ln2b_body),
          Phase(d // ft, 1.9, [rows_of(fo, ft)], [], dattn_body),
          Phase(heads, 3.5, [*(heads_of(qkv, 1, j * heads) for j in range(3)), cols_of(attn, hd), heads_of(lse, 1), slopes],
                [(b16(3, heads, seq, hd), (3, 1, seq, hd), lambda i: (0, i, 0, 0))], battn_body),
          Phase(d // ft, 1.9, [cols_of(attn, ft)], [rows_of(b16(d, d), ft)], gout_body)]
    d_mid, g_ln2, d_qkv, g_out, *r2 = host('back', pe, S([(g_up, 0, n_down)], carry=r1[1:]),
                                          shared=[vm32(seq, d), vm16(seq, d), vm16(heads, seq, hd)])
    d_qkv = d_qkv.reshape(3 * heads, seq, hd)

    scat = S([(g_out, 0, d // SUB), (pack, 0, nu)], carry=r2[1:], last=True)

    def tile_copy(i, ext):
        r, q = Unit(RB, nq).at(i)
        return pltpu.make_async_copy(ext[1].at[rest(i, 2)], scat[0].written().at[:, :, :, :, r, q], ext[2].at[rest(i, 2)])

    def macro_body(i, ins, outs, ext):
        (ht, dq, w), acc = ins, ext[0]
        tile = side_by_side(dq, per)
        r = dot(ht[...], tile).astype(BF16)
        if comm:
            ext[1][rest(i, 2)] = r.reshape(*CHIPS, 2, RB, SUB)
            tile_copy(i, ext).start()
        else:
            outs[0][...] = r
        put(acc, i, lambda: dot_t(tile, w[...]))

    def ship_body(i, ins, outs, ext):
        tile_copy(i, ext).wait()
        scat[0].ship(i)

    def ln1b_body(i, ins, outs, ext):
        (xr, dm, lw), (o, gwo) = ins, outs
        dx, gw = norm_back(ext[0][band(i)], xr[...].astype(F32), lw[...])
        o[...] = (dm[...] + dx).astype(BF16)
        put(gwo, i, lambda: gw)

    first = [] if comm else [cols_of(b16(d, nq), SUB)]
    pf = [Phase(nu, 3.9, [whole(h1t), heads_of(d_qkv, per), cols_of(fq, SUB)], first, macro_body),
          Phase(nm, 2, [rows_of(x, tm), rows_of(d_mid, tm), whole(w1)], [rows_of(act, tm), one_vec], ln1b_body)]
    if comm:
        pf.append(Phase(nu, 0, [], [], ship_body, 1))
        scat.append(SmallSum(g_ln2, 1, nu + nm, d))
    shared = [vm32(seq, d), vm16(2, *CHIPS, 2, RB, SUB), pltpu.SemaphoreType.DMA((2,))]
    got = host('last', pf, scat, shared=shared)
    if not comm:
        g_qkv, dx, g_ln1 = got
        return y, dx, g_ln1, g_qkv, g_out, g_ln2, g_up, g_down
    dx, _, r3, _, sums = got
    units = jnp.concatenate([r1[0], r2[0], r3])
    nc = d // SUB
    g_down, g_up, g_out, g_qkv = jnp.split(units, (n_down, 2 * n_down, 2 * n_down + nc))
    flat_rows = lambda u: u.transpose(1, 0, 2).reshape(RB, -1)
    g_down = g_down.reshape(-1, nc, RB, SUB).transpose(0, 2, 1, 3).reshape(-1, d)
    return y, dx, sums, flat_rows(g_qkv), flat_rows(g_out), None, flat_rows(g_up), g_down


def solution(mesh):
    row_spec = P('fsdp')

    def step(x_in, ln1_w, w_qkv, w_out, ln2_w, w_up, w_down, dy_out):
        rows, _, heads, hd = w_qkv.shape
        d = x_in.shape[-1]
        y, dx, sums, g_qkv, g_out, _, g_up, g_down = local_step(
            x_in[0], ln1_w, w_qkv.reshape(rows, -1), w_out, ln2_w, w_up, w_down, dy_out[0])
        mine = lax.dynamic_slice_in_dim(sums, lax.axis_index('fsdp') * rows, rows, axis=1)
        return (y[None], dx[None], mine[0], g_qkv.reshape(rows, 3, heads, hd), g_out, mine[1], g_up, g_down)

    return jax.shard_map(step, mesh=mesh, in_specs=(row_spec,) * 8, out_specs=(row_spec,) * 8, check_vma=False)
```

```python
import functools
import math

import jax
import jax.numpy as jnp
from jax import lax
from jax.experimental import pallas as pl
from jax.experimental.pallas import tpu as pltpu
from jax.sharding import PartitionSpec as P

EPS = 1e-5
LOG2E = math.log2(math.e)
SUB = 512
WIDE = 768
HALF = SUB // 2
LAG = 2
GLAG = 1
THIRD = 3
CARRY = 2 * LAG
LEAD = 3
RB = 48
F32, BF16 = jnp.float32, jnp.bfloat16
VMEM_LIMIT = 67_000_000
MESH = pl.DeviceIdType.MESH
HBM = pltpu.MemorySpace.HBM
CHIPS = (4, 2, 2)


def sds(shape, dtype):
    return jax.ShapeDtypeStruct(shape, dtype)


def dot(a, b, ca=1, cb=0):
    return lax.dot_general(a, b, (((ca,), (cb,)), ((), ())), preferred_element_type=F32)


def dot_t(a, b):
    return dot(a, b, 1, 1)


def t_dot(a, b):
    return dot(a, b, 0, 0)


def over_rows(f):
    return functools.partial(f, axis=-1, keepdims=True)


row_sum, row_max, row_mean = map(over_rows, (jnp.sum, jnp.max, jnp.mean))


def clip(t, n):
    return jnp.minimum(jnp.maximum(t, 0), n - 1)


class Phase:
    def __init__(self, n, cost, ins, outs, body, at=None):
        self.n, self.cost, self.ins, self.outs, self.body, self.at = n, cost, ins, outs, body, at

    def on(self, t):
        return (t >= self.at) & (t < self.at + self.n)

    def index(self, f):
        return lambda t: f(clip(t - self.at, self.n))


def quot(a, b):
    return a // b if isinstance(a, int) else lax.div(a, b)


def rest(a, b):
    return a % b if isinstance(a, int) else lax.rem(a, b)


HERE = {}


def locate():
    me = lax.axis_index('fsdp')
    left, place = me, []
    for n in (2, *reversed(CHIPS)):
        place.append(rest(left, n))
        left = quot(left, n)
    c, x, y, z = place
    n, step, ways = CHIPS[0], 8, (1, 2, 3)
    cp, xp, yp = (me + s - 2 * s * b for s, b in zip((1, 2, 4), place))
    HERE.update(coords=(me, z, y, x, c), peers=([rest(me + step * d, step * n) for d in ways], yp, xp, cp), zs=[rest(z + d, n) for d in ways])


def coords():
    return HERE['coords']


def peers():
    return HERE['peers']


def remote(src, dst, ssem, rsem, dev):
    return pltpu.make_async_remote_copy(src_ref=src, dst_ref=dst, send_sem=ssem, recv_sem=rsem, device_id=(dev,), device_id_type=MESH)


class Unit:
    def __init__(self, rows, cols, width=SUB):
        self.width, self.nc, self.nr = width, cols // width, rows // RB
        self.count = self.nc * self.nr

    def at(self, u, half=None):
        lanes, col = self.width, rest(u, self.nc) * self.width
        if half is not None:
            lanes //= 2
            col = col + half * lanes
        rows = slice(None) if self.nr == 1 else pl.ds(pl.multiple_of(quot(u, self.nc) * RB, 16), RB)
        return rows, pl.ds(pl.multiple_of(col, 128), lanes)


class Gather:
    def __init__(self, weights, k0, k1):
        self.k0, self.k1 = k0, k1
        self.k, self.tail = k1 - k0 + 1, 0
        self.z0 = k0 + LEAD if k0 else 0
        self.z1 = k1 + LEAD
        self.w, self.ins, self.outs, self.alias = [], [], [], []
        for shard, full, first in weights:
            unit = Unit(*shard.shape, WIDE)
            self.w.append((len(self.ins), unit, first, first + unit.count, full is None))
            self.ins.append((shard, pl.BlockSpec(memory_space=pltpu.VMEM)))
            if full is not None:
                self.alias.append((len(self.ins), len(self.outs)))
                self.ins.append((full, pl.BlockSpec(memory_space=HBM)))
            self.outs.append((sds(CHIPS + (2,) + shard.shape, BF16), pl.BlockSpec(memory_space=HBM)))
        self.base = max(k0 - 2 * GLAG, 0)
        n = self.z1 - self.base
        self.scratch = [pltpu.SemaphoreType.DMA((n, 12)), pltpu.SemaphoreType.DMA((n, 12)), pltpu.SemaphoreType.DMA((len(weights),))]

    def copies(self, stage, w, u, turned, refs):
        i, unit, first, _, _ = self.w[w]
        shard, full = refs[i], refs[len(self.ins) + w]
        sems = lambda i: (refs[-3].at[u - self.base, i], refs[-2].at[u - self.base, i])
        me, z, y, x, c = coords()
        zs, yp, xp, cp = peers()
        r, q = unit.at(u - first)
        sides = [unit.at(u - first, half) for half in range(2)]
        if stage == 0 and not turned:
            return [remote(shard.at[r, q], full.at[z, y, x, c, r, q], *sems(d), dev) for d, dev in enumerate(zs)]
        if stage == 0:
            return [remote(shard.at[r, q], full.at[z, y, x, c, r, q], *sems(j), dev) for j, ((r, q), dev) in enumerate(zip(sides, (yp, xp)))]
        if stage == 3:
            v = full.at[:, :, :, c, r, q]
            return [remote(v, v, *sems(11), cp)]
        (ra, qa), (rb, qb) = sides
        if stage == 2:
            views = [(full.at[:, :, x, c, ra, qa], xp), (full.at[:, y, :, c, rb, qb], yp)]
        elif turned:
            views = [(v, dev) for v in (full.at[z, :, x, c, ra, qa], full.at[z, y, :, c, rb, qb]) for dev in zs]
        else:
            views = [(full.at[:, y, x, c, ra, qa], yp), (full.at[:, y, x, c, rb, qb], xp)]
        return [remote(v, v, *sems(6 * stage - 3 + j), dev) for j, (v, dev) in enumerate(views)]

    def act(self, what, stage, w, u, refs):
        def run(turned):
            for cp in self.copies(stage, w, u, turned, refs):
                getattr(cp, what)()

        if stage < 2:
            odd = rest(u, THIRD) == 1
            pl.when(odd)(lambda: run(True))
            pl.when(jnp.logical_not(odd))(lambda: run(False))
        else:
            run(False)

    def each(self, lo, hi, u, fn):
        for w, (_, _, first, last, _) in enumerate(self.w):
            a, b = max(lo, first), min(hi, last)
            if a < b:
                if u is None:
                    pl.loop(a, b)(functools.partial(fn, w))
                else:
                    pl.when((u >= a) & (u < b))(functools.partial(fn, w, u))

    def go(self, *args):
        self.act('start', *args)

    def arrive(self, *args):
        self.act('wait_recv', *args)

    def left(self, *args):
        self.act('wait_send', *args)

    def step(self, k, fire, refs):
        me, z, y, x, c = coords()
        k0, k1, k = self.k0, self.k1, k + self.k0
        span = [(self.z0, self.z1)] + [(max(k0 - i * GLAG, 0), k1 - i * GLAG) for i in range(3)]

        @pl.when(fire & (k == k0))
        def _():
            own = [pltpu.make_async_copy(refs[i], refs[len(self.ins) + w].at[z, y, x, c], refs[-1].at[w])
                   for w, (i, _, _, _, fresh) in enumerate(self.w) if fresh]
            for cp in own:
                cp.start()
            if k0 == 0:
                self.each(0, LEAD, None, lambda w, u: self.go(0, w, u, refs))
            for cp in own:
                cp.wait()

        @pl.when(fire & (k < k1))
        def _():
            self.each(*span[0], k + LEAD, lambda w, u: self.go(0, w, u, refs))
            for stage in (1, 2, 3):
                u = k + GLAG * (1 - stage)
                lo, hi = span[stage - 1]
                self.each(lo, hi, u, lambda w, u: self.arrive(stage - 1, w, u, refs))
                self.each(*span[stage], u, lambda w, u: self.go(stage, w, u, refs))

        @pl.when(fire & (k == k1))
        def _():
            for stage in range(4):
                lo, hi = span[stage]
                self.each(max(lo, k1 - stage * GLAG) if stage < 3 else lo, hi, None, lambda w, u: self.arrive(stage, w, u, refs))
                self.each(lo, hi, None, lambda w, u: self.left(stage, w, u, refs))


class GatherSmall:
    def __init__(self, tile):
        self.k, self.alias, self.tail = 5, [], 0
        self.ins = [(tile, pl.BlockSpec(memory_space=pltpu.VMEM))]
        self.outs = [(sds(CHIPS + (2,) + tile.shape, F32), pl.BlockSpec(memory_space=HBM))]
        self.scratch = [pltpu.SemaphoreType.DMA((6,)), pltpu.SemaphoreType.DMA((6,)), pltpu.SemaphoreType.DMA]

    def copies(self, stage, refs):
        tile, full, ss, rs, _ = refs
        me, z, y, x, c = coords()
        zs, yp, xp, cp = peers()
        if stage == 0:
            return [remote(tile, full.at[z, y, x, c], ss.at[d], rs.at[d], zs[d]) for d in range(3)]
        v, dev = ((full.at[:, y, x, c], yp), (full.at[:, :, x, c], xp), (full.at[:, :, :, c], cp))[stage - 1]
        return [remote(v, v, ss.at[2 + stage], rs.at[2 + stage], dev)]

    def step(self, k, fire, refs):
        tile, full, ss, rs, ls = refs
        me, z, y, x, c = coords()
        for stage in range(5):
            @pl.when(fire & (k == stage))
            def _(stage=stage):
                if stage == 0:
                    own = pltpu.make_async_copy(tile, full.at[z, y, x, c], ls)
                    own.start()
                else:
                    for cp in self.copies(stage - 1, refs):
                        cp.wait_recv()
                if stage < 4:
                    for cp in self.copies(stage, refs):
                        cp.start()
                else:
                    for st in range(4):
                        for cp in self.copies(st, refs):
                            cp.wait_send()
                if stage == 0:
                    own.wait()


class Scatter:
    def __init__(self, grads, carry=None, last=False):
        self.last, self.carried = last, carry is not None
        self.parts, self.ins, n = [], [], 0
        self.late = None
        for g, u0, m in grads:
            self.parts.append((n, n + m, u0, Unit(*g.shape[-2:])))
            if isinstance(g, jax.ShapeDtypeStruct):
                self.late = g
            else:
                self.ins.append((g, pl.BlockSpec(memory_space=HBM)))
            n += m
        self.known = n - m if self.late else n
        self.n = n
        self.first = 0 if self.carried else CARRY
        self.end = n + CARRY
        self.done = self.end if last else n
        self.k = n + (3 * LAG if last else 1)
        self.tail = 3 * LAG - 1 if last else 0
        self.two_shape, self.three_shape = (2, 4, 2, RB, HALF), (4, RB, SUB)
        if self.carried:
            self.ins += [(a, pl.BlockSpec(memory_space=pltpu.VMEM)) for a in carry]
        self.scratch = [
            pltpu.VMEM((n, *CHIPS, RB, SUB), BF16),
            pltpu.VMEM((2, *CHIPS, RB, SUB), BF16),
            pltpu.VMEM((self.end, *self.two_shape), BF16),
            pltpu.VMEM((self.end, *self.three_shape), BF16),
            pltpu.VMEM((self.end, 3, RB, SUB), BF16),
            pltpu.SemaphoreType.DMA((self.end, 8)), pltpu.SemaphoreType.DMA((self.end, 8)), pltpu.SemaphoreType.DMA((2,))]
        outs = [sds((self.done - self.first, RB, SUB), F32)]
        if not last:
            outs += [sds((LAG, *shape), BF16) for shape in (self.two_shape, self.three_shape)]
        self.outs = [(o, pl.BlockSpec(memory_space=pltpu.VMEM)) for o in outs]
        if self.late:
            self.outs.append((self.late, pl.BlockSpec(memory_space=HBM)))
        self.alias = []

    def source(self, j, refs, fn):
        for i, (a, b, u0, unit) in enumerate(self.parts):
            ref = self.written() if self.late and a == self.known else refs[i]
            u = j - CARRY
            if len(self.parts) == 1:
                fn(ref, *unit.at(u0 + u))
            else:
                pl.when((u >= a) & (u < b))(functools.partial(lambda ref, unit, u: fn(ref, *unit.at(u)), ref, unit, u0 + u - a))

    def written(self):
        return self.refs[len(self.ins) + len(self.outs) - 1]

    def ship(self, u):
        self.swap(CARRY + self.known + u, self.refs, lambda cp: cp.start())

    def bufs(self, refs):
        return refs[len(self.ins) + len(self.outs):]

    def local(self, j, refs, act):
        me, z, y, x, c = coords()
        own, ls = self.bufs(refs)[1], self.bufs(refs)[-1]
        slot = rest(j, 2)
        self.source(j, refs, lambda g, r, q: act(pltpu.make_async_copy(g.at[:, :, :, c, r, q], own.at[slot], ls.at[slot])))

    def swap(self, j, refs, act):
        me, z, y, x, c = coords()
        got, ss, rs = self.bufs(refs)[0], *self.bufs(refs)[-3:-1]
        cp = peers()[-1]
        self.source(j, refs, lambda g, r, q: act(remote(g.at[:, :, :, 1 - c, r, q], got.at[j - CARRY], ss.at[j, 0], rs.at[j, 0], cp)))

    def copies(self, stage, j, refs):
        got, own, two, three, four, ss, rs, ls = self.bufs(refs)
        me, z, y, x, c = coords()
        zs, yp, xp, cp = peers()
        a, b = pl.ds(0, HALF), pl.ds(HALF, HALF)
        if stage == 1:
            pairs = [(got.at[j - CARRY, :, 1 - y, :, :, a], two.at[j, 0], yp), (got.at[j - CARRY, :, :, 1 - x, :, b], two.at[j, 1], xp)]
        elif stage == 2:
            pairs = [(two.at[j, 0, :, 1 - x], three.at[j, :, :, a], xp), (two.at[j, 1, :, 1 - y], three.at[j, :, :, b], yp)]
        else:
            pairs = [(three.at[j, HERE['zs'][d]], four.at[j, d], zs[d]) for d in range(3)]
        return [remote(src, dst, ss.at[j, 2 * stage + i - 1], rs.at[j, 2 * stage + i - 1], dev) for i, (src, dst, dev) in enumerate(pairs)]

    def add(self, stage, j, refs):
        got, own, two, three, four, ss, rs, ls = self.bufs(refs)
        me, z, y, x, c = coords()
        a, b = pl.ds(0, HALF), pl.ds(HALF, HALF)
        slot = rest(j, 2)
        if stage == 1:
            @pl.loop(0, 4)
            def _(zz):
                for yy in range(2):
                    for xx in range(2):
                        got[j - CARRY, zz, yy, xx] += own[slot, zz, yy, xx]
        elif stage == 2:
            @pl.loop(0, 4)
            def _(zz):
                for i in range(2):
                    two[j, 0, zz, i] += got[j - CARRY, zz, y, i, :, a]
                    two[j, 1, zz, i] += got[j - CARRY, zz, i, x, :, b]
        elif stage == 3:
            for zz in range(4):
                three[j, zz, :, a] += two[j, 0, zz, x]
                three[j, zz, :, b] += two[j, 1, zz, y]
        else:
            total = three[j, z].astype(F32)
            for d in range(3):
                total += four[j, d].astype(F32)
            refs[len(self.ins)][j - self.first] = total

    def step(self, k, fire, refs):
        n, end, last = self.n, self.end, self.last
        got, own, two, three, four, ss, rs, ls = self.bufs(refs)
        start = lambda cp: cp.start()

        def go(stage, j):
            for cp in self.copies(stage, j, refs):
                cp.start()

        def take(stage, j):
            for cp in self.copies(stage - 1, j, refs):
                cp.wait_recv()
            self.add(stage, j, refs)

        @pl.when(fire & (k == 0))
        def _():
            @pl.loop(CARRY, CARRY + self.known)
            def _(j):
                self.swap(j, refs, start)

            self.local(CARRY, refs, start)
            if self.carried:
                for i in range(LAG):
                    two[LAG + i] = refs[len(self.ins) - 2][i]
                    three[i] = refs[len(self.ins) - 1][i]
                    go(2, LAG + i)
                    go(3, i)

        @pl.when(fire & (k < n))
        def _():
            j = k + CARRY
            pl.when(j + 1 < end)(lambda: self.local(j + 1, refs, start))
            self.swap(j, refs, lambda cp: cp.wait_recv())
            self.local(j, refs, lambda cp: cp.wait())
            self.add(1, j, refs)
            go(1, j)

        lows = [CARRY, LAG, 0] if self.carried else [CARRY] * 3
        for stage, low in zip((2, 3, 4), lows):
            j = k + (3 - stage) * LAG

            @pl.when(fire & (j >= low) & (j < end) & ((k < n) | last))
            def _(stage=stage, j=j):
                take(stage, j)
                if stage < 4:
                    go(stage, j)

        @pl.when(fire & (k == self.k - 1))
        def _():
            for stage, low in zip((2, 3, 4), lows):
                a = n + (3 - stage) * LAG
                if not last:
                    pl.loop(max(a, low), a + LAG)(functools.partial(take, stage))

                @pl.loop(CARRY if stage == 2 else low, end if last else a + LAG)
                def _(j):
                    for cp in self.copies(stage - 1, j, refs):
                        cp.wait_send()

            @pl.loop(CARRY, end)
            def _(j):
                self.swap(j, refs, lambda cp: cp.wait_send())

            if not last:
                for i in range(LAG):
                    refs[len(self.ins) + 1][i] = two[n + LAG + i]
                    refs[len(self.ins) + 2][i] = three[n + i]


class SmallSum:
    def __init__(self, row, at, t0, d):
        self.at, self.t0, self.k, self.tail = at, t0, 1, 0
        self.ins = [(row, pl.BlockSpec(memory_space=pltpu.VMEM))]
        self.outs = [(sds((8, d), F32), pl.BlockSpec(memory_space=pltpu.VMEM))]
        self.alias = []
        self.scratch = [pltpu.VMEM((4, 8, d), F32), pltpu.VMEM((6, 8, d), F32), pltpu.SemaphoreType.DMA((6,)), pltpu.SemaphoreType.DMA((6,))]

    def run(self, t, mine, refs):
        row, out, acc, got, ss, rs = refs
        zs, yp, xp, cp = peers()
        near = (cp, xp, yp, *zs)
        n = len(near) - len(zs)
        copies = [remote(acc.at[min(i, n)], got.at[i], ss.at[i], rs.at[i], dev) for i, dev in enumerate(near)]

        for i in range(n + 2):
            @pl.when(t == self.t0 + i)
            def _(i=i):
                if not i:
                    acc[i] = jnp.zeros_like(acc[i])
                    acc[i, pl.ds(0, 1)] = mine[...]
                    acc[i, pl.ds(1, 1)] = row[...]
                elif i <= n:
                    copies[i - 1].wait_recv()
                    acc[i] = acc[i - 1] + got[i - 1]
                else:
                    total = acc[n]
                    for j in range(n, len(near)):
                        copies[j].wait_recv()
                        total += got[j]
                    out[...] = total
                    for copy in copies:
                        copy.wait_send()
                for copy in copies[i:i + 1] if i < n else copies[n:] if i == n else ():
                    copy.start()


KERNELS = ['gather', 'attention', 'up', 'down', 'back', 'last']


def host(name, phases, comms=(), shared=()):
    k_all = max([c.k for c in comms], default=1)
    at = 0
    for p in phases:
        if p.at is None:
            p.at = at
        at = max(at, p.at + p.n)
    small = [c for c in comms if isinstance(c, SmallSum)]
    tail = max([c.tail for c in comms], default=0)
    spread, clock, fires = k_all - 1 - tail, [0.0], [0]
    for t in range(at):
        clock.append(clock[-1] + sum(p.cost for p in phases if p.at <= t < p.at + p.n))
    for k in range(1, k_all):
        t = at if k >= spread else min(t for t in range(at + 1) if clock[t] * spread >= clock[at] * k)
        fires.append(max(t, fires[-1] + 1))
    total = max([at, fires[-1] + 1] + [c.t0 + 5 for c in small])
    ins, in_specs, outs, out_specs, scratch, alias, resident = [], [], [], [], [], {}, []
    for p in phases:
        for arr, block, index in p.ins:
            if block == 'smem':
                in_specs.append(pl.BlockSpec(memory_space=pltpu.SMEM))
            elif index is None:
                resident.append((len(ins), p.at))
                in_specs.append(pl.BlockSpec(memory_space=HBM))
            else:
                in_specs.append(pl.BlockSpec(block, p.index(index)))
            ins.append(arr)
        for shape, block, index in p.outs:
            outs.append(shape)
            out_specs.append(pl.BlockSpec(block, p.index(index)))
    for c in comms:
        alias.update({len(ins) + i: len(outs) + o for i, o in c.alias})
        for arr, spec in c.ins:
            ins.append(arr)
            in_specs.append(spec)
        for shape, spec in c.outs:
            outs.append(shape)
            out_specs.append(spec)
        scratch += c.scratch
    scratch += [pltpu.VMEM(ins[i].shape, ins[i].dtype) for i, _ in resident] + [pltpu.SemaphoreType.DMA((max(len(resident), 1),))]
    scratch += list(shared)

    def kernel(*refs):
        refs = list(refs)
        rin, rout, rscr = refs[:len(ins)], refs[len(ins):len(ins) + len(outs)], refs[len(ins) + len(outs):]
        t = pl.program_id(0)
        if comms:
            locate()

            @pl.when(t == 0)
            def _():
                zs, yp, xp, cp = peers()
                near = (*zs, yp, xp, cp)
                bar = pltpu.get_barrier_semaphore()
                for dev in near:
                    pl.semaphore_signal(bar, inc=1, device_id=(dev,), device_id_type=MESH)
                pl.semaphore_wait(bar, len(near))
        i, o, s = sum(len(p.ins) for p in phases), sum(len(p.outs) for p in phases), 0
        k = sum([(t >= f).astype(jnp.int32) for f in fires[1:]], 0 * t)
        fire = functools.reduce(jnp.logical_or, [t == f for f in fires])
        for c in comms:
            ni, no, ns = len(c.ins), len(c.outs), len(c.scratch)
            crefs = rin[i:i + ni] + rout[o:o + no] + rscr[s:s + ns]
            c.refs = crefs
            if c not in small:
                c.step(k, fire, crefs)
            i, o, s = i + ni, o + no, s + ns
        held, rsem, extra = rscr[s:s + len(resident)], rscr[s + len(resident)], rscr[s + len(resident) + 1:]
        loads = [(pltpu.make_async_copy(rin[i], h, rsem.at[n]), at) for n, ((i, at), h) in enumerate(zip(resident, held))]
        if loads:
            @pl.when(t == 0)
            def _():
                for cp, _ in loads:
                    cp.start()
        for cp, at in loads:
            pl.when(t == at)(cp.wait)
        for (i, _), h in zip(resident, held):
            rin[i] = h
        i = o = 0
        for p in phases:
            pi, po = rin[i:i + len(p.ins)], rout[o:o + len(p.outs)]
            i, o = i + len(p.ins), o + len(p.outs)

            @pl.when(p.on(t))
            def _(p=p, pi=pi, po=po):
                p.body(t - p.at, pi, po, extra)

        for c in small:
            c.run(t, rout[c.at], c.refs)

    params = dict(dimension_semantics=("arbitrary",), vmem_limit_bytes=VMEM_LIMIT)
    if comms:
        params.update(collective_id=KERNELS.index(name), has_side_effects=True)
    got = pl.pallas_call(kernel, grid=(total,), in_specs=in_specs, out_specs=out_specs, out_shape=outs, scratch_shapes=scratch,
                         input_output_aliases=alias, compiler_params=pltpu.CompilerParams(**params), name=name,
                         cost_estimate=pl.CostEstimate(flops=2 ** 34, bytes_accessed=2 ** 25, transcendentals=0))(*ins)
    return list(got)


def norm_parts(t):
    mean = row_mean(t)
    cen = t - mean
    rstd = lax.rsqrt(row_mean(cen * cen) + EPS)
    return cen * rstd, rstd


def norm_back(d, t, w):
    xhat, rstd = norm_parts(t)
    dh = d * w
    m1 = row_mean(dh)
    m2 = row_mean(dh * xhat)
    return rstd * (dh - m1 - xhat * m2), jnp.sum(d * xhat, axis=0, keepdims=True)


def alibi_slopes(n_heads):
    padded = 2 ** math.ceil(math.log2(n_heads))
    base = [2.0 ** (-8.0 * (k + 1) / padded) for k in range(padded)]
    ordered = base if padded == n_heads else base[1::2] + base[0::2]
    return jnp.array(ordered[:n_heads], dtype=F32)


def bias(i, tq, slope):
    def ahead(n, first):
        return lax.broadcasted_iota(jnp.int32, (1, n), 1).astype(F32) * slope + slope * first

    row, col = (lax.broadcasted_iota(jnp.int32, (tq, tq), a) for a in range(2))
    return ahead(tq, 0.0), ahead(i * tq, -float(i * tq)) if i else None, row >= col


def attn_fwd(q_ref, k_ref, v_ref, o_ref, l_ref, slope, scale, tq):
    slope, scale = slope * LOG2E, scale * LOG2E
    for i in range(q_ref.shape[0] // tq):
        rows, before = pl.ds(i * tq, tq), pl.ds(0, i * tq)
        q = q_ref[rows]
        near, far, keep = bias(i, tq, slope)
        sd = jnp.where(keep, dot_t(q, k_ref[rows]) * scale + near, -jnp.inf)
        m = row_max(sd)
        if i:
            sp = dot_t(q, k_ref[before]) * scale + far
            m = jnp.maximum(m, row_max(sp))
            ep = jnp.exp2(sp - m)
        ed = jnp.exp2(sd - m)
        l = row_sum(ed)
        if i:
            l = l + row_sum(ep)
        inv = 1 / l
        o = dot((ed * inv).astype(BF16), v_ref[rows])
        if i:
            o = o + dot((ep * inv).astype(BF16), v_ref[before])
        o_ref[rows] = o.astype(BF16)
        l_ref[rows] = m + jnp.log2(l)


def attn_bwd(q_ref, k_ref, v_ref, a_ref, da_ref, l_ref, dq_ref, dk_ref, dv_ref, dk_s, dv_s, slope, scale, tq):
    slope2, scale2 = slope * LOG2E, scale * LOG2E
    dk_s[...] = jnp.zeros_like(dk_s)
    dv_s[...] = jnp.zeros_like(dv_s)
    for i in range(q_ref.shape[0] // tq):
        rows, before = pl.ds(i * tq, tq), pl.ds(0, i * tq)
        q, da = q_ref[rows], da_ref[rows].astype(BF16)
        lse = l_ref[rows]
        delta = row_sum(da.astype(F32) * a_ref[rows].astype(F32))
        near, far, keep = bias(i, tq, slope2)
        dq = None
        for keys, ahead in ((rows, near), (before, far))[:2 if i else 1]:
            kk, vv = k_ref[keys], v_ref[keys]
            p = jnp.exp2(dot_t(q, kk) * scale2 + ahead - lse)
            if keys is rows:
                p = jnp.where(keep, p, 0)
            ds = (p * (dot_t(da, vv) - delta)).astype(BF16)
            dv_s[keys] += t_dot(p.astype(BF16), da)
            dk_s[keys] += t_dot(ds, q)
            part = dot(ds, kk)
            dq = part if dq is None else dq + part
        dq_ref[rows] = (dq * scale).astype(BF16)
    dk_ref[...] = (dk_s[...] * scale).astype(BF16)
    dv_ref[...] = dv_s[...].astype(BF16)


def row_map(i):
    return i, 0


def col_map(i):
    return 0, i


def rows_of(a, n):
    return a, (n, a.shape[1]), row_map


def cols_of(a, n):
    return a, (a.shape[0], n), col_map


def heads_of(a, n):
    return a, (n,) + a.shape[1:], lambda i: (i, 0, 0)


def whole(a):
    return a, a.shape, None


def put(ref, i, part):
    @pl.when(i == 0)
    def _():
        ref[...] = jnp.zeros_like(ref)

    ref[...] += part()


def side_by_side(ref, n):
    return jnp.concatenate([ref[j] for j in range(n)], axis=1)


def local_step(x, ln1, wq, wo, ln2, wu, wd, dy, comm=True):
    seq, d = x.shape
    heads, hd, ft = 12, 128, 512
    ff, nq, per = wu.shape[1], 3 * d, SUB // hd
    scale = 1 / math.sqrt(hd)
    tq = min(256, seq)
    tm = tq
    nm, nf = seq // tm, ff // ft
    slopes = (alibi_slopes(heads), 'smem', None)
    b16 = lambda *shape: sds(shape, BF16)
    f32 = lambda *shape: sds(shape, F32)
    vm16 = lambda *shape: pltpu.VMEM(shape, BF16)
    vm32 = lambda *shape: pltpu.VMEM(shape, F32)
    act, wide, vec = b16(seq, d), b16(seq, ff), f32(1, d)
    one_vec = (vec, vec.shape, lambda i: (0, 0))
    band = lambda i: pl.ds(pl.multiple_of(i * tm, tm), tm)
    flat = lambda full: full.reshape(-1, full.shape[-1])
    order = [Unit(*w.shape, WIDE).count for w in (wq, wo, wu, wd)]
    qs, os, us, ds = (sum(order[:i]) for i in range(4))
    ends = [i + 2 * GLAG for i in (os, ds, sum(order))]

    nu = nq // SUB
    pack = sds((*CHIPS, 2, RB, nq), BF16)

    def G(*window):
        return [Gather(*window)] if comm else []

    def S(parts, **kw):
        return [Scatter([(a if a is pack else a.reshape(*CHIPS, 2, -1, a.shape[-1]), u0, n) for a, u0, n in parts], **kw)] if comm else []

    if comm:
        tile = jnp.pad(jnp.stack([ln1, ln2]), ((0, 6), (0, 128 - ln1.shape[0])))
        fq, fo, fu, lns = host('gather', [], G([(wq, None, qs), (wo, None, os), (wu, None, us)], 0, ends[0]) + [GatherSmall(tile)])
        fq = flat(fq)
        w1, w2 = lns.reshape(-1, 8, 128)[:, :2, :ln1.shape[0]].transpose(1, 0, 2).reshape(2, 1, d)
    else:
        fq, fo, fu, w1, w2 = wq, wo, wu, ln1.reshape(1, d), ln2.reshape(1, d)

    def ln1_body(i, ins, outs, ext):
        (xr, lw), (ht,), (_, h1) = ins, outs, ext
        xhat, _ = norm_parts(xr[...].astype(F32))
        h = (xhat * lw[...]).astype(BF16)
        h1[band(i)] = h
        ht[...] = h.T

    def qkv_body(i, ins, outs, ext):
        (w,), (o,), (qkv, h1) = ins, outs, ext
        r = dot(h1[...], w[...]).astype(BF16)
        for j in range(per):
            qkv[i * per + j] = r[:, j * hd:(j + 1) * hd]
            o[j] = r[:, j * hd:(j + 1) * hd]

    def attn_body(i, ins, outs, ext):
        (sl,), (o, l), (qkv, _) = ins, outs, ext
        attn_fwd(qkv.at[i], qkv.at[heads + i], qkv.at[2 * heads + i], o, l.at[0], sl[i], scale, tq)

    pb = [Phase(nm, 1, [rows_of(x, tm), whole(w1)], [cols_of(b16(d, seq), tm)], ln1_body),
          Phase(nq // SUB, 1.9, [cols_of(fq, SUB)], [heads_of(b16(3 * heads, seq, hd), per)], qkv_body),
          Phase(heads, 2.2, [slopes], [cols_of(act, hd), heads_of(f32(heads, seq, 1), 1)], attn_body)]
    h1t, qkv, attn, lse, *full = host('attention', pb, G([(wo, fo, os), (wu, fu, us), (wd, None, ds)], ends[0], ends[1]),
                                      shared=[vm16(3 * heads, seq, hd), vm16(seq, d)])
    if comm:
        fo, fu, fd = full
        fo, fu = flat(fo), flat(fu)

    def out_body(i, ins, outs, ext):
        (xs, a, w, lw), (o, ht), (h2,) = ins, outs, ext
        x1 = (xs[...].astype(F32) + dot(a[...], w[...])).astype(BF16)
        o[...] = x1
        xhat, _ = norm_parts(x1.astype(F32))
        h = (xhat * lw[...]).astype(BF16)
        h2[band(i)] = h
        ht[...] = h.T

    def up_body(i, ins, outs, ext):
        (w, dyr), (go, gpo, gd), (h2,) = ins, outs, ext
        u = dot(h2[...], w[...])
        cdf = 0.5 * (1.0 + lax.erf(u * math.sqrt(0.5)))
        g = (u * cdf).astype(BF16)
        go[...] = g
        gpo[...] = cdf + u * (jnp.exp(-0.5 * u * u) * math.sqrt(0.5 / math.pi))
        gd[...] = t_dot(g, dyr[...]).astype(BF16)

    pc = [Phase(nm, 3, [rows_of(x, tm), rows_of(attn, tm), whole(fo), whole(w2)], [rows_of(act, tm), cols_of(b16(d, seq), tm)], out_body),
          Phase(nf, 4.0, [cols_of(fu, ft), whole(dy)], [cols_of(wide, ft), cols_of(f32(seq, ff), ft), rows_of(b16(ff, d), ft)], up_body)]
    x1, h2t, g, gp, g_down, *full = host('up', pc, G([(wd, fd, ds)], ends[1], ends[2]) if comm else [], shared=[vm16(seq, d)])
    fd, = map(flat, full) if comm else (wd,)

    def dup_body(i, ins, outs, ext):
        (dyr, w, gr, gpr, ht), (duo, gu), (acc,) = ins, outs, ext
        du = (dot_t(dyr[...], w[...]) * gpr[...]).astype(BF16)
        duo[...] = du
        gu[...] = dot(ht[...], du).astype(BF16)
        put(acc, i, lambda: dot(gr[...], w[...]))

    def y_body(i, ins, outs, ext):
        (xr,), (o,), (acc,) = ins, outs, ext
        o[...] = (xr[...].astype(F32) + acc[band(i)]).astype(BF16)

    pd = [Phase(nf, 6, [whole(dy), rows_of(fd, ft), cols_of(g, ft), cols_of(gp, ft), whole(h2t)], [cols_of(wide, ft), cols_of(b16(d, ff), ft)], dup_body),
          Phase(nm, 1, [rows_of(x1, tm)], [rows_of(act, tm)], y_body)]
    n_down = Unit(ff // 32, d).count
    d_up, g_up, y, *r1 = host('down', pd, S([(g_down, 0, n_down)]), shared=[vm32(seq, d)])

    def dh2_body(i, ins, outs, ext):
        (du, w), acc = ins, ext[0]
        put(acc, i, lambda: dot_t(du[...], w[...]))

    def ln2b_body(i, ins, outs, ext):
        (xr, dyr, lw), (dmo, gwo), (acc, dmb, *_) = ins, outs, ext
        dx, gw = norm_back(acc[band(i)], xr[...].astype(F32), lw[...])
        dm = dyr[...].astype(F32) + dx
        dmo[...] = dm
        dmb[band(i)] = dm.astype(BF16)
        put(gwo, i, lambda: gw)

    def dattn_body(i, ins, outs, ext):
        (w,), (acc, dmb, *_) = ins, ext
        acc[:, pl.ds(pl.multiple_of(i * ft, ft), ft)] = dot_t(dmb[...], w[...])

    def battn_body(i, ins, outs, ext):
        (qkv, a, l, sl), (o,), (acc, _, dk, dv) = ins, outs, ext
        da = acc.at[:, pl.ds(pl.multiple_of(i * hd, hd), hd)]
        attn_bwd(*(qkv.at[j, 0] for j in range(3)), a, da, l.at[0], *(o.at[j, 0] for j in range(3)), dk, dv, sl[i], scale, tq)

    def gout_body(i, ins, outs, ext):
        (a,), (o,), (_, dmb, *_) = ins, outs, ext
        o[...] = t_dot(a[...], dmb[...]).astype(BF16)

    triple = lambda a: (a, (3, 1, seq, hd), lambda i: (0, i, 0, 0))
    pe = [Phase(nf, 2.4, [cols_of(d_up, ft), cols_of(fu, ft)], [], dh2_body),
          Phase(nm, 2, [rows_of(x1, tm), rows_of(dy, tm), whole(w2)], [rows_of(f32(seq, d), tm), one_vec], ln2b_body),
          Phase(d // ft, 1.9, [rows_of(fo, ft)], [], dattn_body),
          Phase(heads, 3.5, [triple(qkv.reshape(3, heads, seq, hd)), cols_of(attn, hd), heads_of(lse, 1), slopes],
                [triple(b16(3, heads, seq, hd))], battn_body),
          Phase(d // ft, 1.9, [cols_of(attn, ft)], [rows_of(b16(d, d), ft)], gout_body)]
    d_mid, g_ln2, d_qkv, g_out, *r2 = host('back', pe, S([(g_up, 0, n_down)], carry=r1[1:]),
                                          shared=[vm32(seq, d), vm16(seq, d), vm32(seq, hd), vm32(seq, hd)])
    d_qkv = d_qkv.reshape(3 * heads, seq, hd)

    scat = S([(g_out, 0, d // SUB), (pack, 0, nu)], carry=r2[1:], last=True)

    def tile_copy(i, ext):
        r, q = Unit(RB, nq).at(i)
        return pltpu.make_async_copy(ext[1].at[rest(i, 2)], scat[0].written().at[:, :, :, :, r, q], ext[2].at[rest(i, 2)])

    def macro_body(i, ins, outs, ext):
        (ht, dq, w), acc = ins, ext[0]
        tile = side_by_side(dq, per)
        r = dot(ht[...], tile).astype(BF16)
        if comm:
            ext[1][rest(i, 2)] = r.reshape(*CHIPS, 2, RB, SUB)
            tile_copy(i, ext).start()
        else:
            outs[0][...] = r
        put(acc, i, lambda: dot_t(tile, w[...]))

    def ship_body(i, ins, outs, ext):
        tile_copy(i, ext).wait()
        scat[0].ship(i)

    def ln1b_body(i, ins, outs, ext):
        (xr, dm, lw), (o, gwo) = ins, outs
        dx, gw = norm_back(ext[0][band(i)], xr[...].astype(F32), lw[...])
        o[...] = (dm[...] + dx).astype(BF16)
        put(gwo, i, lambda: gw)

    first = [] if comm else [cols_of(b16(d, nq), SUB)]
    pf = [Phase(nu, 3.9, [whole(h1t), heads_of(d_qkv, per), cols_of(fq, SUB)], first, macro_body),
          Phase(nm, 2, [rows_of(x, tm), rows_of(d_mid, tm), whole(w1)], [rows_of(act, tm), one_vec], ln1b_body)]
    if comm:
        pf.append(Phase(nu, 0, [], [], ship_body, 1))
        scat.append(SmallSum(g_ln2, 1, nu + nm, d))
    shared = [vm32(seq, d), vm16(2, *CHIPS, 2, RB, SUB), pltpu.SemaphoreType.DMA((2,))]
    got = host('last', pf, scat, shared=shared)
    if not comm:
        g_qkv, dx, g_ln1 = got
        return y, dx, g_ln1, g_qkv, g_out, g_ln2, g_up, g_down
    dx, _, r3, _, sums = got
    units = jnp.concatenate([r1[0], r2[0], r3])
    nc = d // SUB
    g_down, g_up, g_out, g_qkv = jnp.split(units, (n_down, 2 * n_down, 2 * n_down + nc))
    flat_rows = lambda u: u.transpose(1, 0, 2).reshape(RB, -1)
    g_down = g_down.reshape(-1, nc, RB, SUB).transpose(0, 2, 1, 3).reshape(-1, d)
    return y, dx, sums, flat_rows(g_qkv), flat_rows(g_out), None, flat_rows(g_up), g_down


def solution(mesh):
    row_spec = P('fsdp')

    def step(x_in, ln1_w, w_qkv, w_out, ln2_w, w_up, w_down, dy_out):
        rows, _, heads, hd = w_qkv.shape
        d = x_in.shape[-1]
        y, dx, sums, g_qkv, g_out, _, g_up, g_down = local_step(
            x_in[0], ln1_w, w_qkv.reshape(rows, -1), w_out, ln2_w, w_up, w_down, dy_out[0])
        mine = lax.dynamic_slice_in_dim(sums, lax.axis_index('fsdp') * rows, rows, axis=1)
        return (y[None], dx[None], mine[0], g_qkv.reshape(rows, 3, heads, hd), g_out, mine[1], g_up, g_down)

    return jax.shard_map(step, mesh=mesh, in_specs=(row_spec,) * 8, out_specs=(row_spec,) * 8, check_vma=False)
```

```python
import functools
import math

import jax
import jax.numpy as jnp
from jax import lax
from jax.experimental import pallas as pl
from jax.experimental.pallas import tpu as pltpu
from jax.sharding import PartitionSpec as P

EPS = 1e-5
LOG2E = math.log2(math.e)
SUB = 512
WIDE = 768
HALF = SUB // 2
LAG = 2
GLAG = 1
CARRY = 2 * LAG
LEAD = 3
RB = 48
F32, BF16 = jnp.float32, jnp.bfloat16
VMEM_LIMIT = 67_000_000
MESH = pl.DeviceIdType.MESH
HBM = pltpu.MemorySpace.HBM
CHIPS = (4, 2, 2)


def sds(shape, dtype):
    return jax.ShapeDtypeStruct(shape, dtype)


def dot(a, b, ca=1, cb=0):
    return lax.dot_general(a, b, (((ca,), (cb,)), ((), ())), preferred_element_type=F32)


def dot_t(a, b):
    return dot(a, b, 1, 1)


def t_dot(a, b):
    return dot(a, b, 0, 0)


def over_rows(f):
    return functools.partial(f, axis=-1, keepdims=True)


row_sum, row_max, row_mean = map(over_rows, (jnp.sum, jnp.max, jnp.mean))


def clip(t, n):
    return jnp.minimum(jnp.maximum(t, 0), n - 1)


class Phase:
    def __init__(self, n, cost, ins, outs, body, at=None):
        self.n, self.cost, self.ins, self.outs, self.body, self.at = n, cost, ins, outs, body, at

    def on(self, t):
        return (t >= self.at) & (t < self.at + self.n)

    def index(self, f):
        return lambda t: f(clip(t - self.at, self.n))


def quot(a, b):
    return a // b if isinstance(a, int) else lax.div(a, b)


def rest(a, b):
    return a % b if isinstance(a, int) else lax.rem(a, b)


HERE = {}


def locate():
    me = lax.axis_index('fsdp')
    left, place = me, []
    for n in (2, *reversed(CHIPS)):
        place.append(rest(left, n))
        left = quot(left, n)
    c, x, y, z = place
    n, step, ways = CHIPS[0], 8, (1, 2, 3)
    cp, xp, yp = (me + s - 2 * s * b for s, b in zip((1, 2, 4), place))
    HERE.update(coords=(me, z, y, x, c), peers=([rest(me + step * d, step * n) for d in ways], yp, xp, cp), zs=[rest(z + d, n) for d in ways])


def coords():
    return HERE['coords']


def peers():
    return HERE['peers']


def remote(src, dst, ssem, rsem, dev):
    return pltpu.make_async_remote_copy(src_ref=src, dst_ref=dst, send_sem=ssem, recv_sem=rsem, device_id=(dev,), device_id_type=MESH)


class Unit:
    def __init__(self, rows, cols, width=SUB):
        self.width, self.nc, self.nr = width, cols // width, rows // RB
        self.count = self.nc * self.nr

    def at(self, u, half=None):
        lanes, col = self.width, rest(u, self.nc) * self.width
        if half is not None:
            lanes //= 2
            col = col + half * lanes
        rows = slice(None) if self.nr == 1 else pl.ds(pl.multiple_of(quot(u, self.nc) * RB, 16), RB)
        return rows, pl.ds(pl.multiple_of(col, 128), lanes)


class Gather:
    def __init__(self, weights, k0, k1):
        self.k0, self.k1 = k0, k1
        self.k, self.tail = k1 - k0 + 1, 0
        self.z0 = k0 + LEAD if k0 else 0
        self.z1 = k1 + LEAD
        self.w, self.ins, self.outs, self.alias = [], [], [], []
        for shard, full, first in weights:
            unit = Unit(*shard.shape, WIDE)
            self.w.append((len(self.ins), unit, first, first + unit.count, full is None))
            self.ins.append((shard, pl.BlockSpec(memory_space=pltpu.VMEM)))
            if full is not None:
                self.alias.append((len(self.ins), len(self.outs)))
                self.ins.append((full, pl.BlockSpec(memory_space=HBM)))
            self.outs.append((sds(CHIPS + (2,) + shard.shape, BF16), pl.BlockSpec(memory_space=HBM)))
        self.base = max(k0 - 2 * GLAG, 0)
        n = self.z1 - self.base
        self.scratch = [pltpu.SemaphoreType.DMA((n, 8)), pltpu.SemaphoreType.DMA((n, 8)), pltpu.SemaphoreType.DMA((len(weights),))]

    def copies(self, stage, w, u, refs):
        i, unit, first, _, _ = self.w[w]
        shard, full = refs[i], refs[len(self.ins) + w]
        sems = lambda i: (refs[-3].at[u - self.base, i], refs[-2].at[u - self.base, i])
        me, z, y, x, c = coords()
        zs, yp, xp, cp = peers()
        r, q = unit.at(u - first)
        if stage == 0:
            return [remote(shard.at[r, q], full.at[z, y, x, c, r, q], *sems(d), zs[d]) for d in range(3)]
        if stage == 3:
            v = full.at[:, :, :, c, r, q]
            return [remote(v, v, *sems(7), cp)]
        out = []
        for half in range(2):
            r, q = unit.at(u - first, half)
            j = 2 * stage + 1 + half
            if stage == 1:
                v = full.at[:, y, x, c, r, q]
            else:
                v = full.at[:, y, :, c, r, q] if half else full.at[:, :, x, c, r, q]
            out.append(remote(v, v, *sems(j), xp if half == stage % 2 else yp))
        return out

    def each(self, lo, hi, u, fn):
        for w, (_, _, first, last, _) in enumerate(self.w):
            a, b = max(lo, first), min(hi, last)
            if a < b:
                if u is None:
                    pl.loop(a, b)(functools.partial(fn, w))
                else:
                    pl.when((u >= a) & (u < b))(functools.partial(fn, w, u))

    def go(self, stage, w, u, refs):
        for cp in self.copies(stage, w, u, refs):
            cp.start()

    def arrive(self, stage, w, u, refs):
        for cp in self.copies(stage, w, u, refs):
            cp.wait_recv()

    def left(self, stage, w, u, refs):
        for cp in self.copies(stage, w, u, refs):
            cp.wait_send()

    def step(self, k, fire, refs):
        me, z, y, x, c = coords()
        k0, k1, k = self.k0, self.k1, k + self.k0
        span = [(self.z0, self.z1)] + [(max(k0 - i * GLAG, 0), k1 - i * GLAG) for i in range(3)]

        @pl.when(fire & (k == k0))
        def _():
            own = [pltpu.make_async_copy(refs[i], refs[len(self.ins) + w].at[z, y, x, c], refs[-1].at[w])
                   for w, (i, _, _, _, fresh) in enumerate(self.w) if fresh]
            for cp in own:
                cp.start()
            if k0 == 0:
                self.each(0, LEAD, None, lambda w, u: self.go(0, w, u, refs))
            for cp in own:
                cp.wait()

        @pl.when(fire & (k < k1))
        def _():
            self.each(*span[0], k + LEAD, lambda w, u: self.go(0, w, u, refs))
            for stage in (1, 2, 3):
                u = k + GLAG * (1 - stage)
                lo, hi = span[stage - 1]
                self.each(lo, hi, u, lambda w, u: self.arrive(stage - 1, w, u, refs))
                self.each(*span[stage], u, lambda w, u: self.go(stage, w, u, refs))
            self.each(*span[3], k - 3 * GLAG, lambda w, u: self.arrive(3, w, u, refs))

        @pl.when(fire & (k == k1))
        def _():
            for stage in range(4):
                lo, hi = span[stage]
                self.each(max(lo, k1 - stage * GLAG), hi, None, lambda w, u: self.arrive(stage, w, u, refs))
                self.each(lo, hi, None, lambda w, u: self.left(stage, w, u, refs))


class Scatter:
    def __init__(self, grads, carry=None, last=False):
        self.last, self.carried = last, carry is not None
        self.parts, self.ins, n = [], [], 0
        self.late = None
        for g, u0, m in grads:
            self.parts.append((n, n + m, u0, Unit(*g.shape[-2:])))
            if isinstance(g, jax.ShapeDtypeStruct):
                self.late = g
            else:
                self.ins.append((g, pl.BlockSpec(memory_space=HBM)))
            n += m
        self.known = n - m if self.late else n
        self.n = n
        self.first = 0 if self.carried else CARRY
        self.end = n + CARRY
        self.done = self.end if last else n
        self.k = n + (3 * LAG if last else 1)
        self.tail = 3 * LAG - 1 if last else 0
        self.two_shape, self.three_shape = (2, 4, 2, RB, HALF), (4, RB, SUB)
        if self.carried:
            self.ins += [(a, pl.BlockSpec(memory_space=pltpu.VMEM)) for a in carry]
        self.scratch = [
            pltpu.VMEM((n, *CHIPS, RB, SUB), BF16),
            pltpu.VMEM((2, *CHIPS, RB, SUB), BF16),
            pltpu.VMEM((self.end, *self.two_shape), BF16),
            pltpu.VMEM((self.end, *self.three_shape), BF16),
            pltpu.VMEM((self.end, 3, RB, SUB), BF16),
            pltpu.SemaphoreType.DMA((self.end, 8)), pltpu.SemaphoreType.DMA((self.end, 8)), pltpu.SemaphoreType.DMA((2,))]
        outs = [sds((self.done - self.first, RB, SUB), F32)]
        if not last:
            outs += [sds((LAG, *shape), BF16) for shape in (self.two_shape, self.three_shape)]
        self.outs = [(o, pl.BlockSpec(memory_space=pltpu.VMEM)) for o in outs]
        if self.late:
            self.outs.append((self.late, pl.BlockSpec(memory_space=HBM)))
        self.alias = []

    def source(self, j, refs, fn):
        for i, (a, b, u0, unit) in enumerate(self.parts):
            ref = self.written() if self.late and a == self.known else refs[i]
            u = j - CARRY
            if len(self.parts) == 1:
                fn(ref, *unit.at(u0 + u))
            else:
                pl.when((u >= a) & (u < b))(functools.partial(lambda ref, unit, u: fn(ref, *unit.at(u)), ref, unit, u0 + u - a))

    def written(self):
        return self.refs[len(self.ins) + len(self.outs) - 1]

    def ship(self, u):
        self.swap(CARRY + self.known + u, self.refs, lambda cp: cp.start())

    def bufs(self, refs):
        return refs[len(self.ins) + len(self.outs):]

    def local(self, j, refs, act):
        me, z, y, x, c = coords()
        own, ls = self.bufs(refs)[1], self.bufs(refs)[-1]
        slot = rest(j, 2)
        self.source(j, refs, lambda g, r, q: act(pltpu.make_async_copy(g.at[:, :, :, c, r, q], own.at[slot], ls.at[slot])))

    def swap(self, j, refs, act):
        me, z, y, x, c = coords()
        got, ss, rs = self.bufs(refs)[0], *self.bufs(refs)[-3:-1]
        cp = peers()[-1]
        self.source(j, refs, lambda g, r, q: act(remote(g.at[:, :, :, 1 - c, r, q], got.at[j - CARRY], ss.at[j, 0], rs.at[j, 0], cp)))

    def copies(self, stage, j, refs):
        got, own, two, three, four, ss, rs, ls = self.bufs(refs)
        me, z, y, x, c = coords()
        zs, yp, xp, cp = peers()
        a, b = pl.ds(0, HALF), pl.ds(HALF, HALF)
        if stage == 1:
            pairs = [(got.at[j - CARRY, :, 1 - y, :, :, a], two.at[j, 0], yp), (got.at[j - CARRY, :, :, 1 - x, :, b], two.at[j, 1], xp)]
        elif stage == 2:
            pairs = [(two.at[j, 0, :, 1 - x], three.at[j, :, :, a], xp), (two.at[j, 1, :, 1 - y], three.at[j, :, :, b], yp)]
        else:
            pairs = [(three.at[j, HERE['zs'][d]], four.at[j, d], zs[d]) for d in range(3)]
        return [remote(src, dst, ss.at[j, 2 * stage + i - 1], rs.at[j, 2 * stage + i - 1], dev) for i, (src, dst, dev) in enumerate(pairs)]

    def add(self, stage, j, refs):
        got, own, two, three, four, ss, rs, ls = self.bufs(refs)
        me, z, y, x, c = coords()
        a, b = pl.ds(0, HALF), pl.ds(HALF, HALF)
        slot = rest(j, 2)
        if stage == 1:
            @pl.loop(0, 4)
            def _(zz):
                for yy in range(2):
                    for xx in range(2):
                        got[j - CARRY, zz, yy, xx] += own[slot, zz, yy, xx]
        elif stage == 2:
            @pl.loop(0, 4)
            def _(zz):
                for i in range(2):
                    two[j, 0, zz, i] += got[j - CARRY, zz, y, i, :, a]
                    two[j, 1, zz, i] += got[j - CARRY, zz, i, x, :, b]
        elif stage == 3:
            for zz in range(4):
                three[j, zz, :, a] += two[j, 0, zz, x]
                three[j, zz, :, b] += two[j, 1, zz, y]
        else:
            total = three[j, z].astype(F32)
            for d in range(3):
                total += four[j, d].astype(F32)
            refs[len(self.ins)][j - self.first] = total

    def step(self, k, fire, refs):
        n, end, last = self.n, self.end, self.last
        got, own, two, three, four, ss, rs, ls = self.bufs(refs)
        start = lambda cp: cp.start()

        def go(stage, j):
            for cp in self.copies(stage, j, refs):
                cp.start()

        def take(stage, j):
            for cp in self.copies(stage - 1, j, refs):
                cp.wait_recv()
            self.add(stage, j, refs)

        @pl.when(fire & (k == 0))
        def _():
            @pl.loop(CARRY, CARRY + self.known)
            def _(j):
                self.swap(j, refs, start)

            self.local(CARRY, refs, start)
            if self.carried:
                for i in range(LAG):
                    two[LAG + i] = refs[len(self.ins) - 2][i]
                    three[i] = refs[len(self.ins) - 1][i]
                    go(2, LAG + i)
                    go(3, i)

        @pl.when(fire & (k < n))
        def _():
            j = k + CARRY
            pl.when(j + 1 < end)(lambda: self.local(j + 1, refs, start))
            self.swap(j, refs, lambda cp: cp.wait_recv())
            self.local(j, refs, lambda cp: cp.wait())
            self.add(1, j, refs)
            go(1, j)

        lows = [CARRY, LAG, 0] if self.carried else [CARRY] * 3
        for stage, low in zip((2, 3, 4), lows):
            j = k + (3 - stage) * LAG

            @pl.when(fire & (j >= low) & (j < end) & ((k < n) | last))
            def _(stage=stage, j=j):
                take(stage, j)
                if stage < 4:
                    go(stage, j)

        @pl.when(fire & (k == self.k - 1))
        def _():
            for stage, low in zip((2, 3, 4), lows):
                a = n + (3 - stage) * LAG
                if not last:
                    pl.loop(max(a, low), a + LAG)(functools.partial(take, stage))

                @pl.loop(CARRY if stage == 2 else low, end if last else a + LAG)
                def _(j):
                    for cp in self.copies(stage - 1, j, refs):
                        cp.wait_send()

            @pl.loop(CARRY, end)
            def _(j):
                self.swap(j, refs, lambda cp: cp.wait_send())

            if not last:
                for i in range(LAG):
                    refs[len(self.ins) + 1][i] = two[n + LAG + i]
                    refs[len(self.ins) + 2][i] = three[n + i]


class SmallSum:
    def __init__(self, rows, t0, at=None):
        d = rows.shape[1]
        self.at, self.t0, self.k, self.tail = at, t0, 1, 0
        self.ins = [(rows, pl.BlockSpec(memory_space=pltpu.VMEM))]
        self.outs = [(sds((8, d), F32), pl.BlockSpec(memory_space=pltpu.VMEM))]
        self.alias = []
        self.scratch = [pltpu.VMEM((4, 8, d), F32), pltpu.VMEM((6, 8, d), F32), pltpu.SemaphoreType.DMA((6,)), pltpu.SemaphoreType.DMA((6,))]

    def run(self, t, outs):
        rows, out, acc, got, ss, rs = self.refs
        zs, yp, xp, cp = peers()
        near = (cp, xp, yp, *zs)
        n = len(near) - len(zs)
        copies = [remote(acc.at[min(i, n)], got.at[i], ss.at[i], rs.at[i], dev) for i, dev in enumerate(near)]

        for i in range(n + 2):
            @pl.when(t == self.t0 + i)
            def _(i=i):
                if not i:
                    acc[i] = rows[...]
                    if self.at is not None:
                        acc[i, pl.ds(self.at, 1)] = outs[self.at][...]
                elif i <= n:
                    copies[i - 1].wait_recv()
                    acc[i] = acc[i - 1] + got[i - 1]
                else:
                    total = acc[n]
                    for j in range(n, len(near)):
                        copies[j].wait_recv()
                        total += got[j]
                    out[...] = total
                    for copy in copies:
                        copy.wait_send()
                for copy in copies[i:i + 1] if i < n else copies[n:] if i == n else ():
                    copy.start()


KERNELS = ['forward', 'down', 'back', 'last']


def host(name, phases, comms=(), shared=(), fires=None):
    k_all = max([c.k for c in comms], default=1)
    at = 0
    for p in phases:
        if p.at is None:
            p.at = at
        at = max(at, p.at + p.n)
    small = [c for c in comms if isinstance(c, SmallSum)]
    tail = max([c.tail for c in comms], default=0)
    if fires is None:
        spread, clock, fires = k_all - 1 - tail, [0.0], [0]
        for t in range(at):
            clock.append(clock[-1] + sum(p.cost for p in phases if p.at <= t < p.at + p.n))
        for k in range(1, k_all):
            t = at if k >= spread else min(t for t in range(at + 1) if clock[t] * spread >= clock[at] * k)
            fires.append(max(t, fires[-1] + 1))
    total = max([at, fires[-1] + 1] + [c.t0 + 5 for c in small])
    ins, in_specs, outs, out_specs, scratch, alias, resident = [], [], [], [], [], {}, []
    for p in phases:
        for arr, block, index in p.ins:
            if isinstance(block, pltpu.MemorySpace):
                in_specs.append(pl.BlockSpec(memory_space=block))
            elif index is None:
                resident.append((len(ins), p.at))
                in_specs.append(pl.BlockSpec(memory_space=HBM))
            else:
                in_specs.append(pl.BlockSpec(block, p.index(index)))
            ins.append(arr)
        for shape, block, index in p.outs:
            outs.append(shape)
            out_specs.append(pl.BlockSpec(block, p.index(index)))
    for c in comms:
        alias.update({len(ins) + i: len(outs) + o for i, o in c.alias})
        for arr, spec in c.ins:
            ins.append(arr)
            in_specs.append(spec)
        for shape, spec in c.outs:
            outs.append(shape)
            out_specs.append(spec)
        scratch += c.scratch
    scratch += [pltpu.VMEM(ins[i].shape, ins[i].dtype) for i, _ in resident] + [pltpu.SemaphoreType.DMA((max(len(resident), 1),))]
    scratch += list(shared)

    def kernel(*refs):
        refs = list(refs)
        rin, rout, rscr = refs[:len(ins)], refs[len(ins):len(ins) + len(outs)], refs[len(ins) + len(outs):]
        t = pl.program_id(0)
        if comms:
            locate()

            @pl.when(t == 0)
            def _():
                zs, yp, xp, cp = peers()
                near = (*zs, yp, xp, cp)
                bar = pltpu.get_barrier_semaphore()
                for dev in near:
                    pl.semaphore_signal(bar, inc=1, device_id=(dev,), device_id_type=MESH)
                pl.semaphore_wait(bar, len(near))
        i, o, s = sum(len(p.ins) for p in phases), sum(len(p.outs) for p in phases), 0
        k = sum([(t >= f).astype(jnp.int32) for f in fires[1:]], 0 * t)
        fire = functools.reduce(jnp.logical_or, [t == f for f in fires])
        for c in comms:
            ni, no, ns = len(c.ins), len(c.outs), len(c.scratch)
            crefs = rin[i:i + ni] + rout[o:o + no] + rscr[s:s + ns]
            c.refs = crefs
            if c not in small:
                c.step(k, fire, crefs)
            elif c.at is None:
                c.run(t, rout)
            i, o, s = i + ni, o + no, s + ns
        held, rsem, extra = rscr[s:s + len(resident)], rscr[s + len(resident)], rscr[s + len(resident) + 1:]
        loads = [(pltpu.make_async_copy(rin[i], h, rsem.at[n]), at) for n, ((i, at), h) in enumerate(zip(resident, held))]
        if loads:
            @pl.when(t == 0)
            def _():
                for cp, _ in loads:
                    cp.start()
        for cp, at in loads:
            pl.when(t == at)(cp.wait)
        for (i, _), h in zip(resident, held):
            rin[i] = h
        i = o = 0
        for p in phases:
            pi, po = rin[i:i + len(p.ins)], rout[o:o + len(p.outs)]
            i, o = i + len(p.ins), o + len(p.outs)

            @pl.when(p.on(t))
            def _(p=p, pi=pi, po=po):
                p.body(t - p.at, pi, po, extra)

        for c in small:
            if c.at is not None:
                c.run(t, rout)

    params = dict(dimension_semantics=("arbitrary",), vmem_limit_bytes=VMEM_LIMIT)
    if comms:
        params.update(collective_id=KERNELS.index(name), has_side_effects=True)
    got = pl.pallas_call(kernel, grid=(total,), in_specs=in_specs, out_specs=out_specs, out_shape=outs, scratch_shapes=scratch,
                         input_output_aliases=alias, compiler_params=pltpu.CompilerParams(**params), name=name,
                         cost_estimate=pl.CostEstimate(flops=2 ** 34, bytes_accessed=2 ** 25, transcendentals=0))(*ins)
    return list(got)


def norm_parts(t):
    mean = row_mean(t)
    cen = t - mean
    rstd = lax.rsqrt(row_mean(cen * cen) + EPS)
    return cen * rstd, rstd


def norm_back(d, t, w):
    xhat, rstd = norm_parts(t)
    dh = d * w
    m1 = row_mean(dh)
    m2 = row_mean(dh * xhat)
    return rstd * (dh - m1 - xhat * m2), jnp.sum(d * xhat, axis=0, keepdims=True)


def alibi_slopes(n_heads):
    padded = 2 ** math.ceil(math.log2(n_heads))
    base = [2.0 ** (-8.0 * (k + 1) / padded) for k in range(padded)]
    ordered = base if padded == n_heads else base[1::2] + base[0::2]
    return jnp.array(ordered[:n_heads], dtype=F32)


def bias(i, tq, slope):
    def ahead(n, first):
        return lax.broadcasted_iota(jnp.int32, (1, n), 1).astype(F32) * slope + slope * first

    row, col = (lax.broadcasted_iota(jnp.int32, (tq, tq), a) for a in range(2))
    return ahead(tq, 0.0), ahead(i * tq, -float(i * tq)) if i else None, row >= col


def attn_fwd(q_ref, k_ref, v_ref, o_ref, l_ref, slope, scale, tq):
    slope, scale = slope * LOG2E, scale * LOG2E
    for i in range(q_ref.shape[0] // tq):
        rows, before = pl.ds(i * tq, tq), pl.ds(0, i * tq)
        q = q_ref[rows]
        near, far, keep = bias(i, tq, slope)
        sd = jnp.where(keep, dot_t(q, k_ref[rows]) * scale + near, -jnp.inf)
        m = row_max(sd)
        if i:
            sp = dot_t(q, k_ref[before]) * scale + far
            m = jnp.maximum(m, row_max(sp))
            ep = jnp.exp2(sp - m)
        ed = jnp.exp2(sd - m)
        l = row_sum(ed)
        if i:
            l = l + row_sum(ep)
        inv = 1 / l
        o = dot((ed * inv).astype(BF16), v_ref[rows])
        if i:
            o = o + dot((ep * inv).astype(BF16), v_ref[before])
        o_ref[rows] = o.astype(BF16)
        l_ref[rows] = m + jnp.log2(l)


def attn_bwd(q_ref, k_ref, v_ref, a_ref, da_ref, l_ref, dq_ref, dk_ref, dv_ref, dk_s, dv_s, slope, scale, tq):
    slope2, scale2 = slope * LOG2E, scale * LOG2E
    dk_s[...] = jnp.zeros_like(dk_s)
    dv_s[...] = jnp.zeros_like(dv_s)
    for i in range(q_ref.shape[0] // tq):
        rows, before = pl.ds(i * tq, tq), pl.ds(0, i * tq)
        q, da = q_ref[rows], da_ref[rows].astype(BF16)
        lse = l_ref[rows]
        delta = row_sum(da.astype(F32) * a_ref[rows].astype(F32))
        near, far, keep = bias(i, tq, slope2)
        dq = None
        for keys, ahead in ((rows, near), (before, far))[:2 if i else 1]:
            kk, vv = k_ref[keys], v_ref[keys]
            p = jnp.exp2(dot_t(q, kk) * scale2 + ahead - lse)
            if keys is rows:
                p = jnp.where(keep, p, 0)
            ds = (p * (dot_t(da, vv) - delta)).astype(BF16)
            dv_s[keys] += t_dot(p.astype(BF16), da)
            dk_s[keys] += t_dot(ds, q)
            part = dot(ds, kk)
            dq = part if dq is None else dq + part
        dq_ref[rows] = (dq * scale).astype(BF16)
    dk_ref[...] = (dk_s[...] * scale).astype(BF16)
    dv_ref[...] = dv_s[...].astype(BF16)


def row_map(i):
    return i, 0


def col_map(i):
    return 0, i


def rows_of(a, n):
    return a, (n, a.shape[1]), row_map


def cols_of(a, n):
    return a, (a.shape[0], n), col_map


def heads_of(a, n):
    return a, (n,) + a.shape[1:], lambda i: (i, 0, 0)


def whole(a):
    return a, a.shape, None


def put(ref, i, part):
    @pl.when(i == 0)
    def _():
        ref[...] = jnp.zeros_like(ref)

    ref[...] += part()


def side_by_side(ref, n):
    return jnp.concatenate([ref[j] for j in range(n)], axis=1)


def local_step(x, lns, wq, wo, wu, wd, dy, comm=True):
    seq, d = x.shape
    heads, hd, ft = 12, 128, 512
    ff, nq, per = wu.shape[1], 3 * d, SUB // hd
    scale = 1 / math.sqrt(hd)
    tq = min(256, seq)
    tm = tq
    nm, nf = seq // tm, ff // ft
    slopes = (alibi_slopes(heads), pltpu.SMEM, None)
    b16 = lambda *shape: sds(shape, BF16)
    f32 = lambda *shape: sds(shape, F32)
    vm16 = lambda *shape: pltpu.VMEM(shape, BF16)
    vm32 = lambda *shape: pltpu.VMEM(shape, F32)
    act, wide_act, vec = b16(seq, d), b16(seq, ff), f32(1, d)
    one_vec = (vec, vec.shape, lambda i: (0, 0))
    band = lambda i, n=tm: pl.ds(pl.multiple_of(i * n, n), n)
    ts = tm // 2
    ns = seq // ts
    order = [Unit(w.shape[0] if comm else w.shape[0] // 32, w.shape[1], WIDE).count for w in (wq, wo, wu, wd)]
    qs, os, us, ds = (sum(order[:i]) for i in range(4))
    nu = nq // SUB
    pack = sds((*CHIPS, 2, RB, nq), BF16)

    def S(parts, **kw):
        return [Scatter([(a if a is pack else a.reshape(*CHIPS, 2, -1, a.shape[-1]), u0, n) for a, u0, n in parts], **kw)] if comm else []

    blocks = lambda w: w.reshape(*CHIPS, 2, -1, w.shape[-1])
    if comm:
        gather = Gather([(wq, None, qs), (wo, None, os), (wu, None, us), (wd, None, ds)], 0, sum(order) + 2 * GLAG)
        lnsum = SmallSum(lns, 0)
    held = {}

    def load(u, ext):
        out = []
        for w, (first, last) in enumerate(((qs, os), (os, us), (us, ds))):
            if first <= u[0] < last:
                full = gather.refs[len(gather.ins) + w] if comm else held['weights'][w]
                r, q = Unit(RB, WIDE * (last - first), WIDE).at(u[1] - first)
                slot = rest(u[1], 2)
                out.append(pltpu.make_async_copy(full.at[:, :, :, :, r, q], ext[3].at[slot], ext[4].at[slot]))
        return out[0]

    def weight(u, ext):
        return ext[3][rest(u, 2)].reshape(d, WIDE)

    def gain(row):
        return (lnsum.refs[1] if comm else held['lns'])[pl.ds(row, 1)]

    def start_body(i, ins, outs, ext):
        load((qs, qs), ext).start()
        load((qs, qs + 1), ext).start()

    def ln1_body(i, ins, outs, ext):
        (xr, *more), (ht,), (_, h, *_) = ins, outs, ext
        if more:
            held.update(weights=more[1:], lns=more[0])
        xhat, _ = norm_parts(xr[...].astype(F32))
        h1 = (xhat * gain(0)).astype(BF16)
        h[band(i, ts)] = h1
        ht[...] = h1.T

    def qkv_body(i, ins, outs, ext):
        (o,), (qkv, h, *_) = outs, ext
        load((qs, i), ext).wait()
        r = dot(h[...], weight(i, ext)).astype(BF16)
        for j in range(wide):
            head = r[:, j * hd:(j + 1) * hd]
            qkv[i * wide + j] = head
            o[j] = head
        pl.when(i + 2 < os)(lambda: load((qs, i + 2), ext).start())
        pl.when(i + 2 >= os)(lambda: load((os, i + 2), ext).start())

    def attn_body(i, ins, outs, ext):
        (sl,), (o, l), (qkv, _, a, *_) = ins, outs, ext
        attn_fwd(qkv.at[i], qkv.at[heads + i], qkv.at[2 * heads + i], o, l.at[0], sl[i], scale, tq)
        a[:, pl.ds(pl.multiple_of(i * hd, hd), hd)] = o[...]

    def out_body(i, ins, outs, ext):
        (xs,), (o, ht), (_, h, a, *_) = ins, outs, ext

        @pl.when(i == 0)
        def _():
            for u in range(os, us):
                load((os, u), ext).wait()

        ar = a[band(i, ts)]
        r = jnp.concatenate([dot(ar, weight(u, ext)) for u in range(os, us)], axis=1)
        x1 = (xs[...].astype(F32) + r).astype(BF16)
        o[...] = x1
        xhat, _ = norm_parts(x1.astype(F32))
        h2 = (xhat * gain(1)).astype(BF16)
        h[band(i, ts)] = h2
        ht[...] = h2.T

        @pl.when(i == ns - 1)
        def _():
            for u in range(us, us + 2):
                load((us, u), ext).start()

    def up_body(i, ins, outs, ext):
        (dyr,), (go, gpo, gd), h = ins, outs, ext[1]
        load((us, us + i), ext).wait()
        u = dot(h[...], weight(us + i, ext))
        cdf = 0.5 * (1.0 + lax.erf(u * math.sqrt(0.5)))
        g = (u * cdf).astype(BF16)
        go[...] = g
        gpo[...] = cdf + u * (jnp.exp(-0.5 * u * u) * math.sqrt(0.5 / math.pi))
        gd[...] = t_dot(g, dyr[...]).astype(BF16)
        pl.when(us + i + 2 < ds)(lambda: load((us, us + i + 2), ext).start())

    wide = WIDE // hd
    more = [] if comm else [(lns, pltpu.VMEM, None)] + [(blocks(w), HBM, None) for w in (wq, wo, wu)]
    pa = [Phase(ns, 1, [rows_of(x, ts), *more], [cols_of(b16(d, seq), ts)], ln1_body, 5),
          Phase(1, 0, [], [], start_body, 4),
          Phase(nq // WIDE, 3, [], [heads_of(b16(3 * heads, seq, hd), wide)], qkv_body, 5 + ns),
          Phase(heads, 2.7, [slopes], [cols_of(act, hd), heads_of(f32(heads, seq, 1), 1)], attn_body, 5 + ns + nq // WIDE),
          Phase(ns, 2, [rows_of(x, ts)], [rows_of(act, ts), cols_of(b16(d, seq), ts)], out_body, 5 + ns + nq // WIDE + heads),
          Phase(ff // WIDE, 6, [whole(dy)], [cols_of(wide_act, WIDE), cols_of(f32(seq, ff), WIDE), rows_of(b16(ff, d), WIDE)], up_body, 5 + 2 * ns + nq // WIDE + heads)]
    shared = [vm16(3 * heads, seq, hd), vm16(seq, d), vm16(seq, d), vm16(2, *CHIPS, 2, RB, WIDE), pltpu.SemaphoreType.DMA((2,))]
    t_qkv, t_attn, t_out, t_up = (p.at for p in pa[2:])
    fires = [*range(6), t_qkv - 4, t_qkv, t_qkv + 2, t_qkv + 4, t_attn - 1, *range(t_attn, t_up, 4), *range(t_up, t_up + ff // WIDE + 3)]
    got = host('forward', pa, [gather, lnsum] if comm else [], shared=shared, fires=fires if comm else None)
    h1t, qkv, attn, lse, x1, h2t, g, gp, g_down, *full = got
    fq, fo, fu, fd = wq, wo, wu, wd
    if comm:
        fq, fo, fu, fd = (f.reshape(-1, f.shape[-1]) for f in full[:4])
        lns = full[4]

    def dup_body(i, ins, outs, ext):
        (dyr, w, gr, gpr, ht), (duo, gu), (acc,) = ins, outs, ext
        du = (dot_t(dyr[...], w[...]) * gpr[...]).astype(BF16)
        duo[...] = du
        gu[...] = dot(ht[...], du).astype(BF16)
        put(acc, i, lambda: dot(gr[...], w[...]))

    def y_body(i, ins, outs, ext):
        (xr,), (o,), (acc,) = ins, outs, ext
        o[...] = (xr[...].astype(F32) + acc[band(i)]).astype(BF16)

    pd = [Phase(nf, 6, [whole(dy), rows_of(fd, ft), cols_of(g, ft), cols_of(gp, ft), whole(h2t)], [cols_of(wide_act, ft), cols_of(b16(d, ff), ft)], dup_body),
          Phase(nm, 1, [rows_of(x1, tm)], [rows_of(act, tm)], y_body)]
    n_down = Unit(ff // 32, d).count
    d_up, g_up, y, *r1 = host('down', pd, S([(g_down, 0, n_down)]), shared=[vm32(seq, d)])

    def dh2_body(i, ins, outs, ext):
        (du, w), acc = ins, ext[0]
        put(acc, i, lambda: dot_t(du[...], w[...]))

    def ln2b_body(i, ins, outs, ext):
        (xr, dyr, lw), (dmo, gwo), (acc, dmb, *_) = ins, outs, ext
        dx, gw = norm_back(acc[band(i)], xr[...].astype(F32), lw[pl.ds(1, 1)])
        dm = dyr[...].astype(F32) + dx
        dmo[...] = dm
        dmb[band(i)] = dm.astype(BF16)
        put(gwo, i, lambda: gw)

    def dattn_body(i, ins, outs, ext):
        (w,), (acc, dmb, *_) = ins, ext
        acc[:, pl.ds(pl.multiple_of(i * ft, ft), ft)] = dot_t(dmb[...], w[...])

    def battn_body(i, ins, outs, ext):
        (qkv, a, l, sl), (o,), (acc, _, dk, dv) = ins, outs, ext
        da = acc.at[:, pl.ds(pl.multiple_of(i * hd, hd), hd)]
        attn_bwd(*(qkv.at[j, 0] for j in range(3)), a, da, l.at[0], *(o.at[j, 0] for j in range(3)), dk, dv, sl[i], scale, tq)

    def gout_body(i, ins, outs, ext):
        (a,), (o,), (_, dmb, *_) = ins, outs, ext
        o[...] = t_dot(a[...], dmb[...]).astype(BF16)

    triple = lambda a: (a, (3, 1, seq, hd), lambda i: (0, i, 0, 0))
    pe = [Phase(nf, 2.4, [cols_of(d_up, ft), cols_of(fu, ft)], [], dh2_body),
          Phase(nm, 2, [rows_of(x1, tm), rows_of(dy, tm), whole(lns)], [rows_of(f32(seq, d), tm), one_vec], ln2b_body),
          Phase(d // ft, 1.9, [rows_of(fo, ft)], [], dattn_body),
          Phase(heads, 3.5, [triple(qkv.reshape(3, heads, seq, hd)), cols_of(attn, hd), heads_of(lse, 1), slopes],
                [triple(b16(3, heads, seq, hd))], battn_body),
          Phase(d // ft, 1.9, [cols_of(attn, ft)], [rows_of(b16(d, d), ft)], gout_body)]
    d_mid, g_ln2, d_qkv, g_out, *r2 = host('back', pe, S([(g_up, 0, n_down)], carry=r1[1:]),
                                          shared=[vm32(seq, d), vm16(seq, d), vm32(seq, hd), vm32(seq, hd)])
    d_qkv = d_qkv.reshape(3 * heads, seq, hd)

    scat = S([(g_out, 0, d // SUB), (pack, 0, nu)], carry=r2[1:], last=True)

    def tile_copy(i, ext):
        r, q = Unit(RB, nq).at(i)
        return pltpu.make_async_copy(ext[1].at[rest(i, 2)], scat[0].written().at[:, :, :, :, r, q], ext[2].at[rest(i, 2)])

    def macro_body(i, ins, outs, ext):
        (ht, dq, w), acc = ins, ext[0]
        tile = side_by_side(dq, per)
        r = dot(ht[...], tile).astype(BF16)
        if comm:
            ext[1][rest(i, 2)] = r.reshape(*CHIPS, 2, RB, SUB)
            tile_copy(i, ext).start()
        else:
            outs[0][...] = r
        put(acc, i, lambda: dot_t(tile, w[...]))

    def ship_body(i, ins, outs, ext):
        tile_copy(i, ext).wait()
        scat[0].ship(i)

    def ln1b_body(i, ins, outs, ext):
        (xr, dm, lw), (o, gwo) = ins, outs
        dx, gw = norm_back(ext[0][band(i)], xr[...].astype(F32), lw[pl.ds(0, 1)])
        o[...] = (dm[...] + dx).astype(BF16)
        put(gwo, i, lambda: gw)

    first = [] if comm else [cols_of(b16(d, nq), SUB)]
    pf = [Phase(nu, 3.9, [whole(h1t), heads_of(d_qkv, per), cols_of(fq, SUB)], first, macro_body),
          Phase(nm, 2, [rows_of(x, tm), rows_of(d_mid, tm), whole(lns)], [rows_of(act, tm), one_vec], ln1b_body)]
    if comm:
        pf.append(Phase(nu, 0, [], [], ship_body, 1))
        scat.append(SmallSum(jnp.pad(g_ln2, ((0, 7), (0, 0))), nu + nm, 1))
    shared = [vm32(seq, d), vm16(2, *CHIPS, 2, RB, SUB), pltpu.SemaphoreType.DMA((2,))]
    got = host('last', pf, scat, shared=shared)
    if not comm:
        g_qkv, dx, g_ln1 = got
        return y, dx, g_ln1, g_qkv, g_out, g_ln2, g_up, g_down
    dx, _, r3, _, sums = got
    parts, done = [r1[0], r2[0], r3], 0
    grads = []
    for count in (n_down, n_down, d // SUB, nu):
        pieces, at = [], 0
        for p in parts:
            a, b = max(done - at, 0), min(done + count - at, p.shape[0])
            if a < b:
                pieces.append(p[a:b])
            at += p.shape[0]
        done += count
        grads.append(jnp.concatenate(pieces))
    g_down, *others = grads
    g_down = g_down.reshape(-1, d // SUB, RB, SUB).transpose(0, 2, 1, 3).reshape(-1, d)
    g_up, g_out, g_qkv = (u.transpose(1, 0, 2).reshape(RB, -1) for u in others)
    return y, dx, sums, g_qkv, g_out, None, g_up, g_down


def solution(mesh):
    row_spec = P('fsdp')

    def step(x_in, ln1_w, w_qkv, w_out, ln2_w, w_up, w_down, dy_out):
        rows, _, heads, hd = w_qkv.shape
        d = x_in.shape[-1]
        lns = lax.dynamic_update_slice(jnp.zeros((8, d), F32), jnp.stack([ln1_w, ln2_w]), (0, lax.axis_index('fsdp') * rows))
        y, dx, sums, g_qkv, g_out, _, g_up, g_down = local_step(
            x_in[0], lns, w_qkv.reshape(rows, -1), w_out, w_up, w_down, dy_out[0])
        mine = lax.dynamic_slice_in_dim(sums, lax.axis_index('fsdp') * rows, rows, axis=1)
        return (y[None], dx[None], mine[1], g_qkv.reshape(rows, 3, heads, hd), g_out, mine[0], g_up, g_down)

    return jax.shard_map(step, mesh=mesh, in_specs=(row_spec,) * 8, out_specs=(row_spec,) * 8, check_vma=False)
```

```python
import functools
import math

import jax
import jax.numpy as jnp
from jax import lax
from jax.experimental import pallas as pl
from jax.experimental.pallas import tpu as pltpu
from jax.sharding import PartitionSpec as P

EPS = 1e-5
LOG2E = math.log2(math.e)
SUB = 512
WIDE = 768
HALF = SUB // 2
LAG = 2
GLAG = 1
CARRY = 2 * LAG
LEAD = 3
SIDE = -4
RB = 48
F32, BF16 = jnp.float32, jnp.bfloat16
VMEM_LIMIT = 67_000_000
MESH = pl.DeviceIdType.MESH
HBM = pltpu.MemorySpace.HBM
CHIPS = (4, 2, 2)


def sds(shape, dtype):
    return jax.ShapeDtypeStruct(shape, dtype)


def dot(a, b, ca=1, cb=0):
    return lax.dot_general(a, b, (((ca,), (cb,)), ((), ())), preferred_element_type=F32)


def dot_t(a, b):
    return dot(a, b, 1, 1)


def t_dot(a, b):
    return dot(a, b, 0, 0)


def over_rows(f):
    return functools.partial(f, axis=-1, keepdims=True)


row_sum, row_max, row_mean = map(over_rows, (jnp.sum, jnp.max, jnp.mean))


def clip(t, n):
    return jnp.minimum(jnp.maximum(t, 0), n - 1)


class Phase:
    def __init__(self, n, cost, ins, outs, body, at=None):
        self.n, self.cost, self.ins, self.outs, self.body, self.at = n, cost, ins, outs, body, at

    def on(self, t):
        return (t >= self.at) & (t < self.at + self.n)

    def index(self, f):
        return lambda t: f(clip(t - self.at, self.n))


def quot(a, b):
    return a // b if isinstance(a, int) else lax.div(a, b)


def rest(a, b):
    return a % b if isinstance(a, int) else lax.rem(a, b)


HERE = {}


def locate():
    me = lax.axis_index('fsdp')
    left, place = me, []
    for n in (2, *reversed(CHIPS)):
        place.append(rest(left, n))
        left = quot(left, n)
    c, x, y, z = place
    n, step, ways = CHIPS[0], 8, (1, 2, 3)
    cp, xp, yp = (me + s - 2 * s * b for s, b in zip((1, 2, 4), place))
    HERE.update(coords=(me, z, y, x, c), peers=([rest(me + step * d, step * n) for d in ways], yp, xp, cp), zs=[rest(z + d, n) for d in ways])


def coords():
    return HERE['coords']


def peers():
    return HERE['peers']


def remote(src, dst, ssem, rsem, dev):
    return pltpu.make_async_remote_copy(src_ref=src, dst_ref=dst, send_sem=ssem, recv_sem=rsem, device_id=(dev,), device_id_type=MESH)


class Unit:
    def __init__(self, rows, cols, width=SUB):
        self.width, self.nc, self.nr = width, cols // width, rows // RB
        self.count = self.nc * self.nr

    def at(self, u, half=None):
        lanes, col = self.width, rest(u, self.nc) * self.width
        if half is not None:
            lanes //= 2
            col = col + half * lanes
        rows = slice(None) if self.nr == 1 else pl.ds(pl.multiple_of(quot(u, self.nc) * RB, 16), RB)
        return rows, pl.ds(pl.multiple_of(col, 128), lanes)


class Gather:
    def __init__(self, weights, k0, k1):
        self.k0, self.k1 = k0, k1
        self.k, self.tail = k1 - k0 + 1, 0
        self.z0 = k0 + LEAD if k0 else 0
        self.z1 = k1 + LEAD
        self.w, self.ins, self.outs, self.alias = [], [], [], []
        for shard, full, first in weights:
            heads, rows = shard.shape[:2] if shard.ndim == 3 else (0, shard.shape[0])
            shape = (rows, shard.size // rows)
            unit = Unit(*shape, WIDE)
            self.w.append((SIDE if heads else len(self.ins), unit, first, first + unit.count, full is None))
            self.ins.append((shard, pl.BlockSpec(memory_space=pltpu.VMEM)))
            if heads:
                self.heads, side = (len(self.ins) - 1, heads), pltpu.VMEM(shape, BF16)
            if full is not None:
                self.alias.append((len(self.ins), len(self.outs)))
                self.ins.append((full, pl.BlockSpec(memory_space=HBM)))
            self.outs.append((sds(CHIPS + (2,) + shape, BF16), pl.BlockSpec(memory_space=HBM)))
        self.base = max(k0 - 2 * GLAG, 0)
        n = self.z1 - self.base
        self.scratch = [side, pltpu.SemaphoreType.DMA((n, 8)), pltpu.SemaphoreType.DMA((n, 8)), pltpu.SemaphoreType.DMA((len(weights),))]

    def copies(self, stage, w, u, refs):
        i, unit, first, _, _ = self.w[w]
        shard, full = refs[i], refs[len(self.ins) + w]
        sems = lambda i: (refs[-3].at[u - self.base, i], refs[-2].at[u - self.base, i])
        me, z, y, x, c = coords()
        zs, yp, xp, cp = peers()
        r, q = unit.at(u - first)
        if stage == 0:
            return [remote(shard.at[r, q], full.at[z, y, x, c, r, q], *sems(d), zs[d]) for d in range(3)]
        if stage == 3:
            v = full.at[:, :, :, c, r, q]
            return [remote(v, v, *sems(7), cp)]
        out = []
        for half in range(2):
            r, q = unit.at(u - first, half)
            j = 2 * stage + 1 + half
            if stage == 1:
                v = full.at[:, y, x, c, r, q]
            else:
                v = full.at[:, y, :, c, r, q] if half else full.at[:, :, x, c, r, q]
            out.append(remote(v, v, *sems(j), xp if half == stage % 2 else yp))
        return out

    def each(self, lo, hi, u, fn):
        for w, (_, _, first, last, _) in enumerate(self.w):
            a, b = max(lo, first), min(hi, last)
            if a < b:
                if u is None:
                    pl.loop(a, b)(functools.partial(fn, w))
                else:
                    pl.when((u >= a) & (u < b))(functools.partial(fn, w, u))

    def go(self, stage, w, u, refs):
        for cp in self.copies(stage, w, u, refs):
            cp.start()

    def arrive(self, stage, w, u, refs):
        for cp in self.copies(stage, w, u, refs):
            cp.wait_recv()

    def left(self, stage, w, u, refs):
        for cp in self.copies(stage, w, u, refs):
            cp.wait_send()

    def step(self, k, fire, begin, refs):
        me, z, y, x, c = coords()
        k0, k1, k = self.k0, self.k1, k + self.k0
        span = [(self.z0, self.z1)] + [(max(k0 - i * GLAG, 0), k1 - i * GLAG) for i in range(3)]

        @pl.when(fire & (k == k0))
        def _():
            i, heads = self.heads
            for h in range(heads):
                refs[SIDE][:, h * 128:(h + 1) * 128] = refs[i][h]
            own = [pltpu.make_async_copy(refs[i], refs[len(self.ins) + w].at[z, y, x, c], refs[-1].at[w])
                   for w, (i, _, _, _, fresh) in enumerate(self.w) if fresh]
            for cp in own:
                cp.start()
            if k0 == 0:
                self.each(0, LEAD, None, lambda w, u: self.go(0, w, u, refs))
            for cp in own:
                cp.wait()

        @pl.when(fire & (k < k1))
        def _():
            self.each(*span[0], k + LEAD, lambda w, u: self.go(0, w, u, refs))
            for stage in (1, 2, 3):
                u = k + GLAG * (1 - stage)
                lo, hi = span[stage - 1]
                self.each(lo, hi, u, lambda w, u: self.arrive(stage - 1, w, u, refs))
                self.each(*span[stage], u, lambda w, u: self.go(stage, w, u, refs))
            self.each(*span[3], k - 3 * GLAG, lambda w, u: self.arrive(3, w, u, refs))

        @pl.when(fire & (k == k1))
        def _():
            for stage in range(4):
                lo, hi = span[stage]
                self.each(max(lo, k1 - stage * GLAG), hi, None, lambda w, u: self.arrive(stage, w, u, refs))
                self.each(lo, hi, None, lambda w, u: self.left(stage, w, u, refs))


class Scatter:
    def __init__(self, grads, layout, carry=None, last=False):
        self.last, self.carried = last, carry is not None
        self.parts, self.ins, n = [], [], 0
        self.late = []
        for g, u0, m in grads:
            self.parts.append((n, n + m, u0, Unit(*g.shape[-2:])))
            if isinstance(g, jax.ShapeDtypeStruct):
                self.late.append(g)
            else:
                self.ins.append((g, pl.BlockSpec(memory_space=HBM)))
            n += m
        self.known = sum(m for g, _, m in grads if not isinstance(g, jax.ShapeDtypeStruct))
        self.n = n
        self.first = 0 if self.carried else CARRY
        self.end = n + CARRY
        self.done = self.end if last else n
        self.k = n + (3 * LAG if last else 1)
        self.tail = 3 * LAG - 1 if last else 0
        self.two_shape, self.three_shape = (2, 4, 2, RB, HALF), (4, RB, SUB)
        if self.carried:
            self.ins += [(a, pl.BlockSpec(memory_space=pltpu.VMEM)) for a in carry]
        self.scratch = [
            pltpu.VMEM((n, *CHIPS, RB, SUB), BF16),
            pltpu.VMEM((2, *CHIPS, RB, SUB), BF16),
            pltpu.VMEM((self.end, *self.two_shape), BF16),
            pltpu.VMEM((self.end, *self.three_shape), BF16),
            pltpu.VMEM((self.end, 3, RB, SUB), BF16),
            pltpu.SemaphoreType.DMA((self.end, 8)), pltpu.SemaphoreType.DMA((self.end, 8)), pltpu.SemaphoreType.DMA((2,))]
        self.layout = layout
        outs = [sds((RB, n * SUB) if n > 0 else (-n * SUB // 128, RB, 128), F32) for n in layout]
        if not last:
            outs += [sds((LAG, *shape), BF16) for shape in (self.two_shape, self.three_shape)]
        self.outs = [(o, pl.BlockSpec(memory_space=pltpu.VMEM)) for o in outs]
        self.outs += [(g, pl.BlockSpec(memory_space=HBM)) for g in self.late]
        self.alias = []

    def source(self, j, refs, fn):
        for i, (a, b, u0, unit) in enumerate(self.parts):
            ref = self.written(i - len(self.parts)) if self.late and a >= self.known else refs[i]
            u = j - CARRY
            if len(self.parts) == 1:
                fn(ref, *unit.at(u0 + u))
            else:
                pl.when((u >= a) & (u < b))(functools.partial(lambda ref, unit, u: fn(ref, *unit.at(u)), ref, unit, u0 + u - a))

    def written(self, i):
        return self.refs[len(self.ins) + len(self.outs) + i]

    def ship(self, u):
        self.swap(CARRY + u, self.refs, lambda cp: cp.start())

    def bufs(self, refs):
        return refs[len(self.ins) + len(self.outs):]

    def local(self, j, refs, act):
        me, z, y, x, c = coords()
        own, ls = self.bufs(refs)[1], self.bufs(refs)[-1]
        slot = rest(j, 2)
        self.source(j, refs, lambda g, r, q: act(pltpu.make_async_copy(g.at[:, :, :, c, r, q], own.at[slot], ls.at[slot])))

    def swap(self, j, refs, act):
        me, z, y, x, c = coords()
        got, ss, rs = self.bufs(refs)[0], *self.bufs(refs)[-3:-1]
        cp = peers()[-1]
        self.source(j, refs, lambda g, r, q: act(remote(g.at[:, :, :, 1 - c, r, q], got.at[j - CARRY], ss.at[j, 0], rs.at[j, 0], cp)))

    def copies(self, stage, j, refs):
        got, own, two, three, four, ss, rs, ls = self.bufs(refs)
        me, z, y, x, c = coords()
        zs, yp, xp, cp = peers()
        a, b = pl.ds(0, HALF), pl.ds(HALF, HALF)
        if stage == 1:
            pairs = [(got.at[j - CARRY, :, 1 - y, :, :, a], two.at[j, 0], yp), (got.at[j - CARRY, :, :, 1 - x, :, b], two.at[j, 1], xp)]
        elif stage == 2:
            pairs = [(two.at[j, 0, :, 1 - x], three.at[j, :, :, a], xp), (two.at[j, 1, :, 1 - y], three.at[j, :, :, b], yp)]
        else:
            pairs = [(three.at[j, HERE['zs'][d]], four.at[j, d], zs[d]) for d in range(3)]
        return [remote(src, dst, ss.at[j, 2 * stage + i - 1], rs.at[j, 2 * stage + i - 1], dev) for i, (src, dst, dev) in enumerate(pairs)]

    def add(self, stage, j, refs):
        got, own, two, three, four, ss, rs, ls = self.bufs(refs)
        me, z, y, x, c = coords()
        a, b = pl.ds(0, HALF), pl.ds(HALF, HALF)
        slot = rest(j, 2)
        if stage == 1:
            @pl.loop(0, 4)
            def _(zz):
                for yy in range(2):
                    for xx in range(2):
                        got[j - CARRY, zz, yy, xx] += own[slot, zz, yy, xx]
        elif stage == 2:
            @pl.loop(0, 4)
            def _(zz):
                for i in range(2):
                    two[j, 0, zz, i] += got[j - CARRY, zz, y, i, :, a]
                    two[j, 1, zz, i] += got[j - CARRY, zz, i, x, :, b]
        elif stage == 3:
            for zz in range(4):
                three[j, zz, :, a] += two[j, 0, zz, x]
                three[j, zz, :, b] += two[j, 1, zz, y]
        else:
            total = three[j, z].astype(F32)
            for d in range(3):
                total += four[j, d].astype(F32)
            a = self.first
            for i, n in enumerate(self.layout):
                b, out = a + abs(n), refs[len(self.ins) + i]

                @pl.when((j >= a) & (j < b))
                def _(out=out, a=a, n=n):
                    if n > 0:
                        out[:, pl.ds(pl.multiple_of((j - a) * SUB, SUB), SUB)] = total
                    else:
                        for h in range(SUB // 128):
                            out[(j - a) * (SUB // 128) + h] = total[:, h * 128:(h + 1) * 128]

                a = b

    def step(self, k, fire, begin, refs):
        n, end, last = self.n, self.end, self.last
        got, own, two, three, four, ss, rs, ls = self.bufs(refs)
        start = lambda cp: cp.start()

        def go(stage, j):
            for cp in self.copies(stage, j, refs):
                cp.start()

        def take(stage, j):
            for cp in self.copies(stage - 1, j, refs):
                cp.wait_recv()
            self.add(stage, j, refs)

        @pl.when(begin)
        def _():
            if self.known:
                pl.loop(CARRY, CARRY + self.known)(lambda j: self.swap(j, refs, start))
                self.local(CARRY, refs, start)
            if self.carried:
                for i in range(LAG):
                    two[LAG + i] = refs[len(self.ins) - 2][i]
                    three[i] = refs[len(self.ins) - 1][i]
                    go(2, LAG + i)
                    go(3, i)

        @pl.when(fire & (k < n))
        def _():
            j = k + CARRY
            if not self.known:
                pl.when(j == CARRY)(lambda: self.local(j, refs, start))
            pl.when(j + 1 < end)(lambda: self.local(j + 1, refs, start))
            self.swap(j, refs, lambda cp: cp.wait_recv())
            self.local(j, refs, lambda cp: cp.wait())
            self.add(1, j, refs)
            go(1, j)

        lows = [CARRY, LAG, 0] if self.carried else [CARRY] * 3
        for stage, low in zip((2, 3, 4), lows):
            j = k + (3 - stage) * LAG

            @pl.when(fire & (j >= low) & (j < end) & ((k < n) | last))
            def _(stage=stage, j=j):
                take(stage, j)
                if stage < 4:
                    go(stage, j)

        @pl.when(fire & (k == self.k - 1))
        def _():
            for stage, low in zip((2, 3, 4), lows):
                a = n + (3 - stage) * LAG
                if not last:
                    pl.loop(max(a, low), a + LAG)(functools.partial(take, stage))

                @pl.loop(CARRY if stage == 2 else low, end if last else a + LAG)
                def _(j):
                    for cp in self.copies(stage - 1, j, refs):
                        cp.wait_send()

            @pl.loop(CARRY, end)
            def _(j):
                self.swap(j, refs, lambda cp: cp.wait_send())

            if not last:
                for i in range(LAG):
                    refs[len(self.ins) + len(self.layout)][i] = two[n + LAG + i]
                    refs[len(self.ins) + len(self.layout) + 1][i] = three[n + i]


class SmallSum:
    def __init__(self, rows, t0, at=None):
        d = rows.shape[1]
        self.at, self.t0, self.k, self.tail = at, t0, 1, 0
        self.ins = [(rows, pl.BlockSpec(memory_space=pltpu.VMEM))]
        self.outs = [(sds((8, d if at is None else 128), F32), pl.BlockSpec(memory_space=pltpu.VMEM))]
        self.alias = []
        self.scratch = [pltpu.VMEM((4, 8, d), F32), pltpu.VMEM((6, 8, d), F32), pltpu.SemaphoreType.DMA((6,)), pltpu.SemaphoreType.DMA((6,))]

    def run(self, t, outs):
        rows, out, acc, got, ss, rs = self.refs
        me = coords()[0]
        zs, yp, xp, cp = peers()
        near = (cp, xp, yp, *zs)
        n = len(near) - len(zs)
        copies = [remote(acc.at[min(i, n)], got.at[i], ss.at[i], rs.at[i], dev) for i, dev in enumerate(near)]

        for i in range(n + 2):
            @pl.when(t == self.t0 + i)
            def _(i=i):
                if not i:
                    if self.at is None:
                        acc[i] = pltpu.roll(rows[:], RB * me, 1)
                    else:
                        acc[i] = jnp.zeros_like(acc[i])
                        acc[i, pl.ds(0, 1)] = rows[:]
                        acc[i, pl.ds(self.at, 1)] = outs[self.at][:]
                elif i <= n:
                    copies[i - 1].wait_recv()
                    acc[i] = acc[i - 1] + got[i - 1]
                else:
                    total = acc[n]
                    for j in range(n, len(near)):
                        copies[j].wait_recv()
                        total += got[j]
                    out[:] = total if self.at is None else pltpu.roll(total, total.shape[1] - RB * me, 1)[:, :128]
                    for copy in copies:
                        copy.wait_send()
                for copy in copies[i:i + 1] if i < n else copies[n:] if i == n else ():
                    copy.start()


KERNELS = ['forward', 'down', 'back', 'last']


def host(name, phases, comms=(), shared=(), fires=None):
    k_all = max([c.k for c in comms], default=1)
    at = 0
    for p in phases:
        if p.at is None:
            p.at = at
        at = max(at, p.at + p.n)
    small = [c for c in comms if isinstance(c, SmallSum)]
    tail = max([c.tail for c in comms], default=0)
    if fires is None:
        spread, clock, fires = k_all - 1 - tail, [0.0], [0]
        for t in range(at):
            clock.append(clock[-1] + sum(p.cost for p in phases if p.at <= t < p.at + p.n))
        for k in range(1, k_all):
            t = at if k >= spread else min(t for t in range(at + 1) if clock[t] * spread >= clock[at] * k)
            fires.append(max(t, fires[-1] + 1))
    total = max([at, fires[-1] + 1] + [c.t0 + 5 for c in small])
    ins, in_specs, outs, out_specs, scratch, alias, resident = [], [], [], [], [], {}, []
    for p in phases:
        for arr, block, index in p.ins:
            if isinstance(block, pltpu.MemorySpace):
                in_specs.append(pl.BlockSpec(memory_space=block))
            elif index is None:
                resident.append((len(ins), p.at))
                in_specs.append(pl.BlockSpec(memory_space=HBM))
            else:
                in_specs.append(pl.BlockSpec(block, p.index(index)))
            ins.append(arr)
        for shape, block, index in p.outs:
            outs.append(shape)
            out_specs.append(pl.BlockSpec(block, p.index(index)))
    for c in comms:
        alias.update({len(ins) + i: len(outs) + o for i, o in c.alias})
        for arr, spec in c.ins:
            ins.append(arr)
            in_specs.append(spec)
        for shape, spec in c.outs:
            outs.append(shape)
            out_specs.append(spec)
        scratch += c.scratch
    scratch += [pltpu.VMEM(ins[i].shape, ins[i].dtype) for i, _ in resident] + [pltpu.SemaphoreType.DMA((max(len(resident), 1),))]
    scratch += list(shared)

    def kernel(*refs):
        refs = list(refs)
        rin, rout, rscr = refs[:len(ins)], refs[len(ins):len(ins) + len(outs)], refs[len(ins) + len(outs):]
        t = pl.program_id(0)
        if comms:
            locate()

            @pl.when(t == 0)
            def _():
                zs, yp, xp, cp = peers()
                near = (*zs, yp, xp, cp)
                bar = pltpu.get_barrier_semaphore()
                for dev in near:
                    pl.semaphore_signal(bar, inc=1, device_id=(dev,), device_id_type=MESH)
                pl.semaphore_wait(bar, len(near))
        i, o, s = sum(len(p.ins) for p in phases), sum(len(p.outs) for p in phases), 0
        k = sum([(t >= f).astype(jnp.int32) for f in fires[1:]], 0 * t)
        fire = functools.reduce(jnp.logical_or, [t == f for f in fires])
        for c in comms:
            ni, no, ns = len(c.ins), len(c.outs), len(c.scratch)
            crefs = rin[i:i + ni] + rout[o:o + no] + rscr[s:s + ns]
            c.refs = crefs
            if c not in small:
                c.step(k, fire, t == 0, crefs)
            elif c.at is None:
                c.run(t, rout)
            i, o, s = i + ni, o + no, s + ns
        held, rsem, extra = rscr[s:s + len(resident)], rscr[s + len(resident)], rscr[s + len(resident) + 1:]
        loads = [(pltpu.make_async_copy(rin[i], h, rsem.at[n]), at) for n, ((i, at), h) in enumerate(zip(resident, held))]
        if loads:
            @pl.when(t == 0)
            def _():
                for cp, _ in loads:
                    cp.start()
        for cp, at in loads:
            pl.when(t == at)(cp.wait)
        for (i, _), h in zip(resident, held):
            rin[i] = h
        i = o = 0
        for p in phases:
            pi, po = rin[i:i + len(p.ins)], rout[o:o + len(p.outs)]
            i, o = i + len(p.ins), o + len(p.outs)

            @pl.when(p.on(t))
            def _(p=p, pi=pi, po=po):
                p.body(t - p.at, pi, po, extra)

        for c in small:
            if c.at is not None:
                c.run(t, rout)

    params = dict(dimension_semantics=("arbitrary",), vmem_limit_bytes=VMEM_LIMIT)
    if comms:
        params.update(collective_id=KERNELS.index(name), has_side_effects=True)
    got = pl.pallas_call(kernel, grid=(total,), in_specs=in_specs, out_specs=out_specs, out_shape=outs, scratch_shapes=scratch,
                         input_output_aliases=alias, compiler_params=pltpu.CompilerParams(**params), name=name,
                         cost_estimate=pl.CostEstimate(flops=2 ** 34, bytes_accessed=2 ** 25, transcendentals=0))(*ins)
    return list(got)


def norm_parts(t):
    mean = row_mean(t)
    cen = t - mean
    rstd = lax.rsqrt(row_mean(cen * cen) + EPS)
    return cen * rstd, rstd


def norm_back(d, t, w):
    xhat, rstd = norm_parts(t)
    dh = d * w
    m1 = row_mean(dh)
    m2 = row_mean(dh * xhat)
    return rstd * (dh - m1 - xhat * m2), jnp.sum(d * xhat, axis=0, keepdims=True)


def alibi_slopes(n_heads):
    padded = 2 ** math.ceil(math.log2(n_heads))
    base = [2.0 ** (-8.0 * (k + 1) / padded) for k in range(padded)]
    ordered = base if padded == n_heads else base[1::2] + base[0::2]
    return jnp.array(ordered[:n_heads], dtype=F32)


def bias(i, tq, slope):
    def ahead(n, first):
        return lax.broadcasted_iota(jnp.int32, (1, n), 1).astype(F32) * slope + slope * first

    row, col = (lax.broadcasted_iota(jnp.int32, (tq, tq), a) for a in range(2))
    return ahead(tq, 0.0), ahead(i * tq, -float(i * tq)) if i else None, row >= col


def attn_fwd(q_ref, k_ref, v_ref, o_ref, l_ref, slope, scale, tq):
    slope, scale = slope * LOG2E, scale * LOG2E
    for i in range(q_ref.shape[0] // tq):
        rows, before = pl.ds(i * tq, tq), pl.ds(0, i * tq)
        q = q_ref[rows]
        near, far, keep = bias(i, tq, slope)
        sd = jnp.where(keep, dot_t(q, k_ref[rows]) * scale + near, -jnp.inf)
        m = row_max(sd)
        if i:
            sp = dot_t(q, k_ref[before]) * scale + far
            m = jnp.maximum(m, row_max(sp))
            ep = jnp.exp2(sp - m)
        ed = jnp.exp2(sd - m)
        l = row_sum(ed)
        if i:
            l = l + row_sum(ep)
        inv = 1 / l
        o = dot((ed * inv).astype(BF16), v_ref[rows])
        if i:
            o = o + dot((ep * inv).astype(BF16), v_ref[before])
        o_ref[rows] = o.astype(BF16)
        l_ref[rows] = m + jnp.log2(l)


def attn_bwd(q_ref, k_ref, v_ref, a_ref, da_ref, l_ref, dq_ref, dk_ref, dv_ref, dk_s, dv_s, slope, scale, tq):
    slope2, scale2 = slope * LOG2E, scale * LOG2E
    dk_s[:] = jnp.zeros_like(dk_s)
    dv_s[:] = jnp.zeros_like(dv_s)
    for i in range(q_ref.shape[0] // tq):
        rows, before = pl.ds(i * tq, tq), pl.ds(0, i * tq)
        q, da = q_ref[rows], da_ref[rows].astype(BF16)
        lse = l_ref[rows]
        delta = row_sum(da.astype(F32) * a_ref[rows].astype(F32))
        near, far, keep = bias(i, tq, slope2)
        dq = None
        for keys, ahead in ((rows, near), (before, far))[:2 if i else 1]:
            kk, vv = k_ref[keys], v_ref[keys]
            p = jnp.exp2(dot_t(q, kk) * scale2 + ahead - lse)
            if keys is rows:
                p = jnp.where(keep, p, 0)
            ds = (p * (dot_t(da, vv) - delta)).astype(BF16)
            dv_s[keys] += t_dot(p.astype(BF16), da)
            dk_s[keys] += t_dot(ds, q)
            part = dot(ds, kk)
            dq = part if dq is None else dq + part
        dq_ref[rows] = (dq * scale).astype(BF16)
    dk_ref[:] = (dk_s[:] * scale).astype(BF16)
    dv_ref[:] = dv_s[:].astype(BF16)


def row_map(i):
    return i, 0


def col_map(i):
    return 0, i


def rows_of(a, n):
    return a, (n, a.shape[1]), row_map


def cols_of(a, n):
    return a, (a.shape[0], n), col_map


def heads_of(a, n):
    return a, (n,) + a.shape[1:], lambda i: (i, 0, 0)


def whole(a):
    return a, a.shape, None


def put(ref, i, part):
    @pl.when(i == 0)
    def _():
        ref[:] = jnp.zeros_like(ref)

    ref[:] += part()


def side_by_side(ref, n):
    return jnp.concatenate([ref[j] for j in range(n)], axis=1)


def local_step(x, lns, wq, wo, wu, wd, dy, comm=True):
    seq, d = x.shape
    heads, hd, ft = 12, 128, 512
    ff, nq, per, slab = wu.shape[1], 3 * d, SUB // hd, d // 4
    scale = 1 / math.sqrt(hd)
    tq = min(256, seq)
    tm = tq
    nm, nf = seq // tm, ff // ft
    slopes = (alibi_slopes(heads), pltpu.SMEM, None)
    b16 = lambda *shape: sds(shape, BF16)
    f32 = lambda *shape: sds(shape, F32)
    vm16 = lambda *shape: pltpu.VMEM(shape, BF16)
    vm32 = lambda *shape: pltpu.VMEM(shape, F32)
    act, wide_act, vec = b16(seq, d), b16(seq, ff), f32(1, d)
    one_vec = (vec, vec.shape, lambda i: (0, 0))
    band = lambda i, n=tm: pl.ds(pl.multiple_of(i * n, n), n)
    ts = tm // 2
    ns = seq // ts
    order = [n // (WIDE * d) for n in (d * nq, d * d, d * ff, d * ff)]
    qs, os, us, ds = (sum(order[:i]) for i in range(4))
    nu = nq // SUB
    packs = [sds((*CHIPS, 2, RB, n), BF16) for n in (d, nq)]

    def S(parts, *args, **kw):
        return [Scatter([(a.reshape(*CHIPS, 2, -1, a.shape[-1]) if isinstance(a, jax.Array) else a, 0, n) for a, n in parts], *args, **kw)] if comm else []

    blocks = lambda w: w.reshape(*CHIPS, 2, -1, w.shape[-1])
    if comm:
        gather = Gather([(wq, None, qs), (wo, None, os), (wu, None, us), (wd, None, ds)], 0, sum(order) + 2 * GLAG)
        lnsum = SmallSum(lns, 0)
    held = {}

    def load(u, ext):
        out = []
        for w, (first, last) in enumerate(((qs, os), (os, us), (us, ds))):
            if first <= u[0] < last:
                full = gather.refs[len(gather.ins) + w] if comm else held['weights'][w]
                r, q = Unit(RB, WIDE * (last - first), WIDE).at(u[1] - first)
                slot = rest(u[1], 2)
                out.append(pltpu.make_async_copy(full.at[:, :, :, :, r, q], ext[3].at[slot], ext[4].at[slot]))
        return out[0]

    def weight(u, ext):
        return ext[3][rest(u, 2)].reshape(d, WIDE)

    def gain(row):
        return (lnsum.refs[1] if comm else held['lns'])[pl.ds(row, 1)]

    def start_body(i, ins, outs, ext):
        load((qs, qs), ext).start()
        load((qs, qs + 1), ext).start()

    def ln1_body(i, ins, outs, ext):
        (xr, *more), (ht,), (_, h, *_) = ins, outs, ext
        if more:
            held.update(weights=more[1:], lns=more[0])
        xhat, _ = norm_parts(xr[:].astype(F32))
        h1 = (xhat * gain(0)).astype(BF16)
        h[band(i, ts)] = h1
        ht[:] = h1.T

    def qkv_body(i, ins, outs, ext):
        (o,), (qkv, h, *_) = outs, ext
        load((qs, i), ext).wait()
        r = dot(h[:], weight(i, ext)).astype(BF16)
        for j in range(wide):
            head = r[:, j * hd:(j + 1) * hd]
            qkv[i * wide + j] = head
            o[j] = head
        pl.when(i + 2 < os)(lambda: load((qs, i + 2), ext).start())
        pl.when(i + 2 >= os)(lambda: load((os, i + 2), ext).start())

    def attn_body(i, ins, outs, ext):
        (sl,), (o, l), (qkv, _, a, *_) = ins, outs, ext
        attn_fwd(qkv.at[i], qkv.at[heads + i], qkv.at[2 * heads + i], o, l.at[0], sl[i], scale, tq)
        a[:, pl.ds(pl.multiple_of(i * hd, hd), hd)] = o[:]

    def out_body(i, ins, outs, ext):
        (xs,), (o, ht), (_, h, a, *_) = ins, outs, ext

        @pl.when(i == 0)
        def _():
            for u in range(os, us):
                load((os, u), ext).wait()

        ar = a[band(i, ts)]
        r = jnp.concatenate([dot(ar, weight(u, ext)) for u in range(os, us)], axis=1)
        x1 = (xs[:].astype(F32) + r).astype(BF16)
        o[:] = x1
        xhat, _ = norm_parts(x1.astype(F32))
        h2 = (xhat * gain(1)).astype(BF16)
        h[band(i, ts)] = h2
        ht[:] = h2.T

        @pl.when(i == ns - 1)
        def _():
            for u in range(us, us + 2):
                load((us, u), ext).start()

    def up_body(i, ins, outs, ext):
        (dyr,), (go, gpo, gd), h = ins, outs, ext[1]
        load((us, us + i), ext).wait()
        u = dot(h[:], weight(us + i, ext))
        cdf = 0.5 * (1.0 + lax.erf(u * math.sqrt(0.5)))
        g = (u * cdf).astype(BF16)
        go[:] = g
        gpo[:] = cdf + u * (jnp.exp(-0.5 * u * u) * math.sqrt(0.5 / math.pi))
        gd[:] = t_dot(g, dyr[:]).astype(BF16)
        pl.when(us + i + 2 < ds)(lambda: load((us, us + i + 2), ext).start())

    wide = WIDE // hd
    more = [] if comm else [(lns, pltpu.VMEM, None)] + [(blocks(w), HBM, None) for w in (wq, wo, wu)]
    pa = [Phase(ns, 1, [rows_of(x, ts), *more], [cols_of(b16(d, seq), ts)], ln1_body, 5),
          Phase(1, 0, [], [], start_body, 4),
          Phase(nq // WIDE, 3, [], [heads_of(b16(3 * heads, seq, hd), wide)], qkv_body, 5 + ns),
          Phase(heads, 2.7, [slopes], [cols_of(act, hd), heads_of(f32(heads, seq, 1), 1)], attn_body, 5 + ns + nq // WIDE),
          Phase(ns, 2, [rows_of(x, ts)], [rows_of(act, ts), cols_of(b16(d, seq), ts)], out_body, 5 + ns + nq // WIDE + heads),
          Phase(ff // WIDE, 6, [whole(dy)], [cols_of(wide_act, WIDE), cols_of(f32(seq, ff), WIDE), rows_of(b16(ff, d), WIDE)], up_body, 5 + 2 * ns + nq // WIDE + heads)]
    shared = [vm16(3 * heads, seq, hd), vm16(seq, d), vm16(seq, d), vm16(2, *CHIPS, 2, RB, WIDE), pltpu.SemaphoreType.DMA((2,))]
    t_qkv, t_attn, t_out, t_up = (p.at for p in pa[2:])
    fires = [*range(6), t_qkv - 4, t_qkv, t_qkv + 2, t_qkv + 4, t_attn - 1, *range(t_attn, t_up, 4), *range(t_up, t_up + ff // WIDE + 3)]
    got = host('forward', pa, [gather, lnsum] if comm else [], shared=shared, fires=fires if comm else None)
    h1t, qkv, attn, lse, x1, h2t, g, gp, g_down, *full = got
    fq, fo, fu, fd = wq, wo, wu, wd
    if comm:
        fq, fo, fu, fd = (f.reshape(-1, f.shape[-1]) for f in full[:4])
        lns = full[4]

    def dup_body(i, ins, outs, ext):
        (dyr, w, gr, gpr, ht), (duo, gu), (acc,) = ins, outs, ext
        du = (dot_t(dyr[:], w[:]) * gpr[:]).astype(BF16)
        duo[:] = du
        gu[:] = dot(ht[:], du).astype(BF16)
        put(acc, i, lambda: dot(gr[:], w[:]))

    def y_body(i, ins, outs, ext):
        (xr,), (o,), (acc,) = ins, outs, ext
        o[:] = (xr[:].astype(F32) + acc[band(i)]).astype(BF16)

    pd = [Phase(nf, 6, [whole(dy), rows_of(fd, ft), cols_of(g, ft), cols_of(gp, ft), whole(h2t)], [cols_of(wide_act, ft), cols_of(b16(d, ff), ft)], dup_body),
          Phase(nm, 1, [rows_of(x1, tm)], [rows_of(act, tm)], y_body)]
    n_down = Unit(ff // 32, d).count
    d_up, g_up, y, *r1 = host('down', pd, S([(g_down, n_down)], [n_down - CARRY]), shared=[vm32(seq, d)])

    def dh2_body(i, ins, outs, ext):
        (du, w), acc = ins, ext[0]
        put(acc, i, lambda: dot_t(du[:], w[:]))

    def ln2b_body(i, ins, outs, ext):
        (xr, dyr, lw), (dmo, dmbo, gwo), (acc, dmb, *_) = ins, outs, ext
        dx, gw = norm_back(acc[band(i)], xr[:].astype(F32), lw[pl.ds(1, 1)])
        dm = dyr[:].astype(F32) + dx
        dmo[:] = dm
        dmb[band(i)] = dmbo[:] = dm.astype(BF16)
        put(gwo, i, lambda: gw)

    def dattn_body(i, ins, outs, ext):
        (w,), (acc, dmb, *_) = ins, ext
        acc[:, pl.ds(pl.multiple_of(i * ft, ft), ft)] = dot_t(dmb[:], w[:])

    def battn_body(i, ins, outs, ext):
        (qkv, a, l, sl), (o,), (acc, _, dk, dv) = ins, outs, ext
        da = acc.at[:, pl.ds(pl.multiple_of(i * hd, hd), hd)]
        attn_bwd(*(qkv.at[j, 0] for j in range(3)), a, da, l.at[0], *(o.at[j, 0] for j in range(3)), dk, dv, sl[i], scale, tq)

    triple = lambda a: (a, (3, 1, seq, hd), lambda i: (0, i, 0, 0))
    pe = [Phase(nf, 2.4, [cols_of(d_up, ft), cols_of(fu, ft)], [], dh2_body),
          Phase(nm, 2, [rows_of(x1, tm), rows_of(dy, tm), whole(lns)], [rows_of(f32(seq, d), tm), rows_of(act, tm), one_vec], ln2b_body),
          Phase(d // ft, 1.9, [rows_of(fo, ft)], [], dattn_body),
          Phase(heads, 3.5, [triple(qkv.reshape(3, heads, seq, hd)), cols_of(attn, hd), heads_of(lse, 1), slopes],
                [triple(b16(3, heads, seq, hd))], battn_body)]
    d_mid, d_mid_bf, g_ln2, d_qkv, *r2 = host('back', pe, S([(g_up, n_down)], [CARRY, n_down - CARRY], carry=r1[1:]),
                                          shared=[vm32(seq, d), vm16(seq, d), vm32(seq, hd), vm32(seq, hd)])
    d_qkv = d_qkv.reshape(3 * heads, seq, hd)

    no = d // SUB
    scat = S([*zip(packs, (no, nu))], [CARRY, no, -nu], carry=r2[2:], last=True)

    def tile_copy(i, ext):
        r, q = Unit(RB, nq).at(i)
        return pltpu.make_async_copy(ext[1].at[rest(i, 2)], scat[0].written(-1).at[:, :, :, :, r, q], ext[2].at[rest(i, 2)])

    def slab_copy(i, ext):
        return pltpu.make_async_copy(ext[3].at[rest(i, 2)], scat[0].written(-2).at[i], ext[2].at[2 + rest(i, 2)])

    def gout_body(i, ins, outs, ext):
        a, dm = ins
        r = t_dot(a[:], dm[:]).astype(BF16)
        if comm:
            pl.when(i > 1)(lambda: slab_copy(i - 2, ext).wait())
            ext[3][rest(i, 2)] = r.reshape(*CHIPS[1:], 2, RB, d)
            slab_copy(i, ext).start()
        else:
            outs[0][:] = r

    def ship_out_body(i, ins, outs, ext):
        for j in (2, 3):
            slab_copy(j, ext).wait()
        for u in range(no):
            scat[0].ship(u)

    def macro_body(i, ins, outs, ext):
        (ht, dq, w), acc = ins, ext[0]
        tile = side_by_side(dq, per)
        r = dot(ht[:], tile).astype(BF16)
        if comm:
            ext[1][rest(i, 2)] = r.reshape(*CHIPS, 2, RB, SUB)
            tile_copy(i, ext).start()
        else:
            outs[0][:] = r
        put(acc, i, lambda: dot_t(tile, w[:]))

    def ship_body(i, ins, outs, ext):
        tile_copy(i, ext).wait()
        scat[0].ship(no + i)

    def ln1b_body(i, ins, outs, ext):
        (xr, dm, lw), (o, gwo) = ins, outs
        dx, gw = norm_back(ext[0][band(i)], xr[:].astype(F32), lw[pl.ds(0, 1)])
        o[:] = (dm[:] + dx).astype(BF16)
        put(gwo, i, lambda: gw)

    firsts = ([], []) if comm else ([rows_of(b16(d, d), slab)], [cols_of(b16(d, nq), SUB)])
    pf = [Phase(4, 2, [cols_of(attn, slab), whole(d_mid_bf)], firsts[0], gout_body),
          Phase(nu, 3.9, [whole(h1t), heads_of(d_qkv, per), cols_of(fq, SUB)], firsts[1], macro_body),
          Phase(nm, 2, [rows_of(x, tm), rows_of(d_mid, tm), whole(lns)], [rows_of(act, tm), one_vec], ln1b_body)]
    if comm:
        pf += [Phase(1, 0, [], [], ship_out_body, 4), Phase(nu, 0, [], [], ship_body, 5)]
        scat.append(SmallSum(g_ln2, 4 + nu + nm, 1))
    shared = [vm32(seq, d), vm16(2, *CHIPS, 2, RB, SUB), pltpu.SemaphoreType.DMA((4,)), vm16(2, *CHIPS[1:], 2, RB, d)]
    got = host('last', pf, scat, shared=shared, fires=range(5, 5 + no + nu + 3 * LAG) if comm else None)
    if not comm:
        g_out, g_qkv, dx, g_ln1 = got
        return y, dx, g_ln1, g_qkv, g_out, g_ln2, g_up, g_down
    dx, _, up_b, g_out, g_qkv, _, _, sums = got
    down_a, (down_b, up_a) = r1[0], r2[:2]
    g_down = jnp.concatenate([down_a, down_b], axis=1).reshape(RB, -1, d).transpose(1, 0, 2).reshape(-1, d)
    return y, dx, sums, g_qkv, g_out, None, jnp.concatenate([up_a, up_b], axis=1), g_down


def solution(mesh):
    row_spec = P('fsdp')

    def step(x_in, ln1_w, w_qkv, w_out, ln2_w, w_up, w_down, dy_out):
        rows, _, heads, hd = w_qkv.shape
        d = x_in.shape[-1]
        lns = jnp.pad(jnp.stack([ln1_w, ln2_w]), ((0, 6), (0, d - rows)))
        wq = w_qkv.transpose(1, 2, 0, 3).reshape(-1, rows, hd)
        y, dx, sums, g_qkv, g_out, _, g_up, g_down = local_step(x_in[0], lns, wq, w_out, w_up, w_down, dy_out[0])
        g_qkv = g_qkv.reshape(3, heads, rows, hd).transpose(2, 0, 1, 3)
        return y[None], dx[None], sums[1, :rows], g_qkv, g_out, sums[0, :rows], g_up, g_down

    return jax.shard_map(step, mesh=mesh, in_specs=(row_spec,) * 8, out_specs=(row_spec,) * 8, check_vma=False)
```

```python
import functools
import math

import jax
import jax.numpy as jnp
from jax import lax
from jax.experimental import pallas as pl
from jax.experimental.pallas import tpu as pltpu
from jax.sharding import PartitionSpec as P

EPS = 1e-5
LOG2E = math.log2(math.e)
SUB = 512
WIDE = 768
NARROW = 256
HALF = SUB // 2
LAG = 2
GLAG = 1
CARRY = 2 * LAG
LEAD = 3
FRONT = 0.92
SIDE = -4
RB = 48
F32, BF16 = jnp.float32, jnp.bfloat16
VMEM_LIMIT = 67_000_000
MESH = pl.DeviceIdType.MESH
HBM = pltpu.MemorySpace.HBM
CHIPS = (4, 2, 2)


def sds(shape, dtype):
    return jax.ShapeDtypeStruct(shape, dtype)


def dot(a, b, ca=1, cb=0):
    return lax.dot_general(a, b, (((ca,), (cb,)), ((), ())), preferred_element_type=F32)


def dot_t(a, b):
    return dot(a, b, 1, 1)


def t_dot(a, b):
    return dot(a, b, 0, 0)


def over_rows(f):
    return functools.partial(f, axis=-1, keepdims=True)


row_sum, row_max, row_mean = map(over_rows, (jnp.sum, jnp.max, jnp.mean))


def clip(t, n):
    return jnp.minimum(jnp.maximum(t, 0), n - 1)


class Phase:
    def __init__(self, n, cost, ins, outs, body, at=None):
        self.n, self.cost, self.ins, self.outs, self.body, self.at = n, cost, ins, outs, body, at

    def on(self, t):
        return (t >= self.at) & (t < self.at + self.n)

    def index(self, f):
        return lambda t: f(clip(t - self.at, self.n))


def quot(a, b):
    return a // b if isinstance(a, int) else lax.div(a, b)


def rest(a, b):
    return a % b if isinstance(a, int) else lax.rem(a, b)


HERE = {}


def locate():
    me = lax.axis_index('fsdp')
    left, place = me, []
    for n in (2, *reversed(CHIPS)):
        place.append(rest(left, n))
        left = quot(left, n)
    c, x, y, z = place
    n, step, ways = CHIPS[0], 8, (1, 2, 3)
    cp, xp, yp = (me + s - 2 * s * b for s, b in zip((1, 2, 4), place))
    HERE.update(coords=(me, z, y, x, c), peers=([rest(me + step * d, step * n) for d in ways], yp, xp, cp), zs=[rest(z + d, n) for d in ways])


def coords():
    return HERE['coords']


def peers():
    return HERE['peers']


def remote(src, dst, ssem, rsem, dev):
    return pltpu.make_async_remote_copy(src_ref=src, dst_ref=dst, send_sem=ssem, recv_sem=rsem, device_id=(dev,), device_id_type=MESH)


class Unit:
    def __init__(self, rows, cols, wide=SUB, high=RB):
        self.wide, self.high, self.nr = wide, high, rows // high
        self.count = cols // wide * self.nr

    def at(self, u, half=None):
        lanes, col = self.wide, quot(u, self.nr) * self.wide
        if half is not None:
            lanes //= 2
            col = col + half * lanes
        rows = slice(None) if self.nr == 1 else pl.ds(pl.multiple_of(rest(u, self.nr) * self.high, 16), self.high)
        return rows, pl.ds(pl.multiple_of(col, 128), lanes)


class Moves:
    tail, k, alias = 0, 1, ()


class Gather(Moves):
    def __init__(self, weights):
        self.w, self.ins, self.outs, n = [], [], [], 0
        for shard, size in weights:
            heads, rows = shard.shape[:2] if shard.ndim == 3 else (0, shard.shape[0])
            shape = (rows, shard.size // rows)
            unit = Unit(*shape, *size)
            self.w.append((SIDE if heads else len(self.ins), unit, n, n + unit.count))
            n += unit.count
            if heads:
                self.heads, side = (len(self.ins), heads), pltpu.VMEM(shape, BF16)
            self.ins.append((shard, pl.BlockSpec(memory_space=pltpu.VMEM)))
            self.outs.append((sds(CHIPS + (2,) + shape, BF16), pl.BlockSpec(memory_space=HBM)))
        self.n, self.k1 = n, n + 2 * GLAG
        self.k = self.k1 + 1
        self.scratch = [side, pltpu.SemaphoreType.DMA((n, 8)), pltpu.SemaphoreType.DMA((n, 8)), pltpu.SemaphoreType.DMA((len(weights),))]

    def copies(self, stage, w, u, refs):
        i, unit, first, _ = self.w[w]
        shard, full = refs[i], refs[len(self.ins) + w]
        sems = lambda i: (refs[-3].at[u, i], refs[-2].at[u, i])
        me, z, y, x, c = coords()
        zs, yp, xp, cp = peers()
        r, q = unit.at(u - first)
        if stage == 0:
            return [remote(shard.at[r, q], full.at[z, y, x, c, r, q], *sems(d), zs[d]) for d in range(3)]
        if stage == 3:
            v = full.at[:, :, :, c, r, q]
            return [remote(v, v, *sems(7), cp)]
        out = []
        for half in range(2):
            r, q = unit.at(u - first, half)
            j = 2 * stage + 1 + half
            if stage == 1:
                v = full.at[:, y, x, c, r, q]
            else:
                v = full.at[:, y, :, c, r, q] if half else full.at[:, :, x, c, r, q]
            out.append(remote(v, v, *sems(j), xp if half == stage % 2 else yp))
        return out

    def each(self, lo, hi, u, fn):
        for w, (_, _, first, last) in enumerate(self.w):
            a, b = max(lo, first), min(hi, last)
            if a < b:
                if u is None:
                    pl.loop(a, b)(functools.partial(fn, w))
                else:
                    pl.when((u >= a) & (u < b))(functools.partial(fn, w, u))

    def go(self, stage, w, u, refs):
        for cp in self.copies(stage, w, u, refs):
            cp.start()

    def arrive(self, stage, w, u, refs):
        for cp in self.copies(stage, w, u, refs):
            cp.wait_recv()

    def left(self, stage, w, u, refs):
        for cp in self.copies(stage, w, u, refs):
            cp.wait_send()

    def step(self, k, fire, begin, refs):
        me, z, y, x, c = coords()
        n, k1 = self.n, self.k1

        @pl.when(begin)
        def _():
            i, heads = self.heads
            for h in range(heads):
                refs[SIDE][:, h * 128:(h + 1) * 128] = refs[i][h]
            own = [pltpu.make_async_copy(refs[i], refs[len(self.ins) + w].at[z, y, x, c], refs[-1].at[w]) for w, (i, *_) in enumerate(self.w)]
            for cp in own:
                cp.start()
            self.each(0, LEAD, None, lambda w, u: self.go(0, w, u, refs))
            for cp in own:
                cp.wait()

        @pl.when(fire & (k < k1))
        def _():
            self.each(0, n, k + LEAD, lambda w, u: self.go(0, w, u, refs))
            for stage in (1, 2, 3):
                u = k + GLAG * (1 - stage)
                self.each(0, n, u, lambda w, u: self.arrive(stage - 1, w, u, refs))
                self.each(0, n, u, lambda w, u: self.go(stage, w, u, refs))
            self.each(0, n, k - 3 * GLAG, lambda w, u: self.arrive(3, w, u, refs))

        @pl.when(fire & (k == k1))
        def _():
            self.each(k1 - 3 * GLAG, n, None, lambda w, u: self.arrive(3, w, u, refs))
            for stage in range(4):
                self.each(0, n, None, lambda w, u: self.left(stage, w, u, refs))


class Scatter(Moves):
    def __init__(self, grads, layout, carry=None, last=False):
        self.last, self.carried = last, carry is not None
        self.parts, self.ins, n = [], [], 0
        self.late = []
        for g, u0, m in grads:
            self.parts.append((n, n + m, u0, Unit(*g.shape[-2:])))
            if isinstance(g, jax.ShapeDtypeStruct):
                self.late.append(g)
            else:
                self.ins.append((g, pl.BlockSpec(memory_space=HBM)))
            n += m
        self.known = sum(m for g, _, m in grads if not isinstance(g, jax.ShapeDtypeStruct))
        self.n = n
        self.first = 0 if self.carried else CARRY
        self.end = n + CARRY
        self.done = self.end if last else n
        self.k = n + (3 * LAG if last else 1)
        if last:
            self.tail = 3 * LAG - 1
        self.two_shape, self.three_shape = (2, 4, 2, RB, HALF), (4, RB, SUB)
        if self.carried:
            self.ins += [(a, pl.BlockSpec(memory_space=pltpu.VMEM)) for a in carry]
        self.scratch = [
            pltpu.VMEM((n, *CHIPS, RB, SUB), BF16),
            pltpu.VMEM((2, *CHIPS, RB, SUB), BF16),
            pltpu.VMEM((self.end, *self.two_shape), BF16),
            pltpu.VMEM((self.end, *self.three_shape), BF16),
            pltpu.VMEM((self.end, 3, RB, SUB), BF16),
            pltpu.SemaphoreType.DMA((self.end, 8)), pltpu.SemaphoreType.DMA((self.end, 8)), pltpu.SemaphoreType.DMA((2,))]
        self.layout = layout
        outs = [sds((nr * RB, m // nr * SUB) if nr else (m * SUB // 128, RB, 128), F32) for nr, m in layout]
        if not last:
            outs += [sds((LAG, *shape), BF16) for shape in (self.two_shape, self.three_shape)]
        self.outs = [(o, pl.BlockSpec(memory_space=pltpu.VMEM)) for o in outs]
        self.outs += [(g, pl.BlockSpec(memory_space=HBM)) for g in self.late]
        self.alias = []

    def source(self, j, refs, fn):
        for i, (a, b, u0, unit) in enumerate(self.parts):
            ref = self.written(i - len(self.parts)) if self.late and a >= self.known else refs[i]
            u = j - CARRY
            if len(self.parts) == 1:
                fn(ref, *unit.at(u0 + u))
            else:
                pl.when((u >= a) & (u < b))(functools.partial(lambda ref, unit, u: fn(ref, *unit.at(u)), ref, unit, u0 + u - a))

    def written(self, i):
        return self.refs[len(self.ins) + len(self.outs) + i]

    def ship(self, u):
        self.swap(CARRY + self.known + u, self.refs, lambda cp: cp.start())

    def bufs(self, refs):
        return refs[len(self.ins) + len(self.outs):]

    def local(self, j, refs, act):
        me, z, y, x, c = coords()
        own, ls = self.bufs(refs)[1], self.bufs(refs)[-1]
        slot = rest(j, 2)
        self.source(j, refs, lambda g, r, q: act(pltpu.make_async_copy(g.at[:, :, :, c, r, q], own.at[slot], ls.at[slot])))

    def swap(self, j, refs, act):
        me, z, y, x, c = coords()
        got, ss, rs = self.bufs(refs)[0], *self.bufs(refs)[-3:-1]
        cp = peers()[-1]
        self.source(j, refs, lambda g, r, q: act(remote(g.at[:, :, :, 1 - c, r, q], got.at[j - CARRY], ss.at[j, 0], rs.at[j, 0], cp)))

    def copies(self, stage, j, refs):
        got, own, two, three, four, ss, rs, ls = self.bufs(refs)
        me, z, y, x, c = coords()
        zs, yp, xp, cp = peers()
        a, b = pl.ds(0, HALF), pl.ds(HALF, HALF)
        if stage == 1:
            pairs = [(got.at[j - CARRY, :, 1 - y, :, :, a], two.at[j, 0], yp), (got.at[j - CARRY, :, :, 1 - x, :, b], two.at[j, 1], xp)]
        elif stage == 2:
            pairs = [(two.at[j, 0, :, 1 - x], three.at[j, :, :, a], xp), (two.at[j, 1, :, 1 - y], three.at[j, :, :, b], yp)]
        else:
            pairs = [(three.at[j, HERE['zs'][d]], four.at[j, d], zs[d]) for d in range(3)]
        return [remote(src, dst, ss.at[j, 2 * stage + i - 1], rs.at[j, 2 * stage + i - 1], dev) for i, (src, dst, dev) in enumerate(pairs)]

    def add(self, stage, j, refs):
        got, own, two, three, four, ss, rs, ls = self.bufs(refs)
        me, z, y, x, c = coords()
        a, b = pl.ds(0, HALF), pl.ds(HALF, HALF)
        slot = rest(j, 2)
        if stage == 1:
            @pl.loop(0, 4)
            def _(zz):
                for yy in range(2):
                    for xx in range(2):
                        got[j - CARRY, zz, yy, xx] += own[slot, zz, yy, xx]
        elif stage == 2:
            @pl.loop(0, 4)
            def _(zz):
                for i in range(2):
                    two[j, 0, zz, i] += got[j - CARRY, zz, y, i, :, a]
                    two[j, 1, zz, i] += got[j - CARRY, zz, i, x, :, b]
        elif stage == 3:
            for zz in range(4):
                three[j, zz, :, a] += two[j, 0, zz, x]
                three[j, zz, :, b] += two[j, 1, zz, y]
        else:
            total = three[j, z].astype(F32)
            for d in range(3):
                total += four[j, d].astype(F32)
            a = self.first
            for i, (nr, m) in enumerate(self.layout):
                b, out = a + m, refs[len(self.ins) + i]

                @pl.when((j >= a) & (j < b))
                def _(out=out, nr=nr, u=j - a):
                    if nr:
                        rows, cols = pl.ds(pl.multiple_of(rest(u, nr) * RB, RB), RB), pl.ds(pl.multiple_of(quot(u, nr) * SUB, SUB), SUB)
                        out[rows, cols] = total
                    else:
                        lane = out.shape[-1]
                        for h in range(SUB // lane):
                            out[u * (SUB // lane) + h] = total[:, h * lane:(h + 1) * lane]

                a = b

    def step(self, k, fire, begin, refs):
        n, end, last = self.n, self.end, self.last
        got, own, two, three, four, ss, rs, ls = self.bufs(refs)
        start = lambda cp: cp.start()

        def go(stage, j):
            for cp in self.copies(stage, j, refs):
                cp.start()

        def take(stage, j):
            for cp in self.copies(stage - 1, j, refs):
                cp.wait_recv()
            self.add(stage, j, refs)

        @pl.when(begin)
        def _():
            if self.known:
                pl.loop(CARRY, CARRY + self.known)(lambda j: self.swap(j, refs, start))
                self.local(CARRY, refs, start)
            if self.carried:
                for i in range(LAG):
                    two[LAG + i] = refs[len(self.ins) - 2][i]
                    three[i] = refs[len(self.ins) - 1][i]
                    go(2, LAG + i)
                    go(3, i)

        @pl.when(fire & (k < n))
        def _():
            j = k + CARRY
            late = CARRY + self.known
            pl.when(j == late)(lambda: self.local(j, refs, start))
            pl.when((j + 1 < end) & (j + 1 != late))(lambda: self.local(j + 1, refs, start))
            self.swap(j, refs, lambda cp: cp.wait_recv())
            self.local(j, refs, lambda cp: cp.wait())
            self.add(1, j, refs)
            go(1, j)

        lows = [CARRY, LAG, 0] if self.carried else [CARRY] * 3
        for stage, low in zip((2, 3, 4), lows):
            j = k + (3 - stage) * LAG

            @pl.when(fire & (j >= low) & (j < end) & ((k < n) | last))
            def _(stage=stage, j=j):
                take(stage, j)
                if stage < 4:
                    go(stage, j)

        @pl.when(fire & (k == self.k - 1))
        def _():
            for stage, low in zip((2, 3, 4), lows):
                a = n + (3 - stage) * LAG
                if not last:
                    pl.loop(max(a, low), a + LAG)(functools.partial(take, stage))

                @pl.loop(CARRY if stage == 2 else low, end if last else a + LAG)
                def _(j):
                    for cp in self.copies(stage - 1, j, refs):
                        cp.wait_send()

            @pl.loop(CARRY, end)
            def _(j):
                self.swap(j, refs, lambda cp: cp.wait_send())

            if not last:
                for i in range(LAG):
                    refs[len(self.ins) + len(self.layout)][i] = two[n + LAG + i]
                    refs[len(self.ins) + len(self.layout) + 1][i] = three[n + i]


class SmallSum(Moves):
    def __init__(self, rows, t0, at=None):
        d = rows.shape[1]
        self.at, self.t0 = at, t0
        self.ins = [(rows, pl.BlockSpec(memory_space=pltpu.VMEM))]
        self.outs = [(sds((8, d if at is None else 128), F32), pl.BlockSpec(memory_space=pltpu.VMEM))]
        self.alias = []
        self.scratch = [pltpu.VMEM((4, 8, d), F32), pltpu.VMEM((6, 8, d), F32), pltpu.SemaphoreType.DMA((6,)), pltpu.SemaphoreType.DMA((6,))]

    def run(self, t, outs):
        rows, out, acc, got, ss, rs = self.refs
        me = coords()[0]
        zs, yp, xp, cp = peers()
        near = (cp, xp, yp, *zs)
        n = len(near) - len(zs)
        copies = [remote(acc.at[min(i, n)], got.at[i], ss.at[i], rs.at[i], dev) for i, dev in enumerate(near)]

        for i in range(n + 2):
            @pl.when(t == self.t0 + i)
            def _(i=i):
                if not i:
                    if self.at is None:
                        acc[i] = pltpu.roll(rows[:], RB * me, 1)
                    else:
                        acc[i] = jnp.zeros_like(acc[i])
                        acc[i, pl.ds(0, 1)] = rows[:]
                        acc[i, pl.ds(self.at, 1)] = outs[self.at][:]
                elif i <= n:
                    copies[i - 1].wait_recv()
                    acc[i] = acc[i - 1] + got[i - 1]
                else:
                    total = acc[n]
                    for j in range(n, len(near)):
                        copies[j].wait_recv()
                        total += got[j]
                    out[:] = total if self.at is None else pltpu.roll(total, total.shape[1] - RB * me, 1)[:, :128]
                    for copy in copies:
                        copy.wait_send()
                for copy in copies[i:i + 1] if i < n else copies[n:] if i == n else ():
                    copy.start()


KERNELS = ['forward', 'down', 'back', 'last']


def host(name, phases, comms=(), shared=(), fires=None):
    k_all = max([c.k for c in comms], default=1)
    at = 0
    for p in phases:
        if p.at is None:
            p.at = at
        at = max(at, p.at + p.n)
    small = [c for c in comms if isinstance(c, SmallSum)]
    tail = max([c.tail for c in comms], default=0)
    if fires is None:
        spread, clock, fires = k_all - 1 - tail, [0.0], [0]
        for t in range(at):
            clock.append(clock[-1] + sum(p.cost for p in phases if p.at <= t < p.at + p.n))
        for k in range(1, k_all):
            t = at if k >= spread else min(t for t in range(at + 1) if clock[t] * spread >= FRONT * clock[at] * k)
            fires.append(max(t, fires[-1] + 1))
    assert len(fires) == k_all
    total = max([at, fires[-1] + 1] + [c.t0 + 5 for c in small])
    ins, in_specs, outs, out_specs, scratch, alias, resident = [], [], [], [], [], {}, []
    for p in phases:
        for arr, block, index in p.ins:
            if isinstance(block, pltpu.MemorySpace):
                in_specs.append(pl.BlockSpec(memory_space=block))
            elif index is None:
                resident.append((len(ins), p.at))
                in_specs.append(pl.BlockSpec(memory_space=HBM))
            else:
                in_specs.append(pl.BlockSpec(block, p.index(index)))
            ins.append(arr)
        for shape, block, index in p.outs:
            outs.append(shape)
            out_specs.append(pl.BlockSpec(block, p.index(index)))
    for c in comms:
        alias.update({len(ins) + i: len(outs) + o for i, o in c.alias})
        for arr, spec in c.ins:
            ins.append(arr)
            in_specs.append(spec)
        for shape, spec in c.outs:
            outs.append(shape)
            out_specs.append(spec)
        scratch += c.scratch
    scratch += [pltpu.VMEM(ins[i].shape, ins[i].dtype) for i, _ in resident] + [pltpu.SemaphoreType.DMA((max(len(resident), 1),))]
    scratch += list(shared)

    def kernel(*refs):
        refs = list(refs)
        rin, rout, rscr = refs[:len(ins)], refs[len(ins):len(ins) + len(outs)], refs[len(ins) + len(outs):]
        t = pl.program_id(0)
        if comms:
            locate()

            @pl.when(t == 0)
            def _():
                zs, yp, xp, cp = peers()
                near = (*zs, yp, xp, cp)
                bar = pltpu.get_barrier_semaphore()
                for dev in near:
                    pl.semaphore_signal(bar, inc=1, device_id=(dev,), device_id_type=MESH)
                pl.semaphore_wait(bar, len(near))
        i, o, s = sum(len(p.ins) for p in phases), sum(len(p.outs) for p in phases), 0
        k = sum([(t >= f).astype(jnp.int32) for f in fires[1:]], 0 * t)
        fire = functools.reduce(jnp.logical_or, [t == f for f in fires])
        for c in comms:
            ni, no, ns = len(c.ins), len(c.outs), len(c.scratch)
            crefs = rin[i:i + ni] + rout[o:o + no] + rscr[s:s + ns]
            c.refs = crefs
            if c not in small:
                c.step(k, fire, t == 0, crefs)
            elif c.at is None:
                c.run(t, rout)
            i, o, s = i + ni, o + no, s + ns
        held, rsem, extra = rscr[s:s + len(resident)], rscr[s + len(resident)], rscr[s + len(resident) + 1:]
        loads = [(pltpu.make_async_copy(rin[i], h, rsem.at[n]), at) for n, ((i, at), h) in enumerate(zip(resident, held))]
        if loads:
            @pl.when(t == 0)
            def _():
                for cp, _ in loads:
                    cp.start()
        for cp, at in loads:
            pl.when(t == at)(cp.wait)
        for (i, _), h in zip(resident, held):
            rin[i] = h
        i = o = 0
        for p in phases:
            pi, po = rin[i:i + len(p.ins)], rout[o:o + len(p.outs)]
            i, o = i + len(p.ins), o + len(p.outs)

            @pl.when(p.on(t))
            def _(p=p, pi=pi, po=po):
                p.body(t - p.at, pi, po, extra)

        for c in small:
            if c.at is not None:
                c.run(t, rout)

    params = dict(dimension_semantics=("arbitrary",), vmem_limit_bytes=VMEM_LIMIT)
    if comms:
        params.update(collective_id=KERNELS.index(name), has_side_effects=True)
    got = pl.pallas_call(kernel, grid=(total,), in_specs=in_specs, out_specs=out_specs, out_shape=outs, scratch_shapes=scratch,
                         input_output_aliases=alias, compiler_params=pltpu.CompilerParams(**params), name=name,
                         cost_estimate=pl.CostEstimate(flops=2 ** 34, bytes_accessed=2 ** 25, transcendentals=0))(*ins)
    return list(got)


def norm_parts(t):
    mean = row_mean(t)
    cen = t - mean
    rstd = lax.rsqrt(row_mean(cen * cen) + EPS)
    return cen * rstd, rstd


def norm_back(d, t, w):
    xhat, rstd = norm_parts(t)
    dh = d * w
    m1 = row_mean(dh)
    m2 = row_mean(dh * xhat)
    return rstd * (dh - m1 - xhat * m2), jnp.sum(d * xhat, axis=0, keepdims=True)


def alibi_slopes(n_heads):
    padded = 2 ** math.ceil(math.log2(n_heads))
    base = [2.0 ** (-8.0 * (k + 1) / padded) for k in range(padded)]
    ordered = base if padded == n_heads else base[1::2] + base[0::2]
    return jnp.array(ordered[:n_heads], dtype=F32)


def bias(i, tq, slope):
    def ahead(n, first):
        return lax.broadcasted_iota(jnp.int32, (1, n), 1).astype(F32) * slope + slope * first

    row, col = (lax.broadcasted_iota(jnp.int32, (tq, tq), a) for a in range(2))
    return ahead(tq, 0.0), ahead(i * tq, -float(i * tq)) if i else None, row >= col


def attn_fwd(q_ref, k_ref, v_ref, o_ref, l_ref, slope, scale, tq):
    slope, scale = slope * LOG2E, scale * LOG2E
    for i in range(q_ref.shape[0] // tq):
        rows, before = pl.ds(i * tq, tq), pl.ds(0, i * tq)
        q = q_ref[rows]
        near, far, keep = bias(i, tq, slope)
        sd = jnp.where(keep, dot_t(q, k_ref[rows]) * scale + near, -jnp.inf)
        m = row_max(sd)
        if i:
            sp = dot_t(q, k_ref[before]) * scale + far
            m = jnp.maximum(m, row_max(sp))
            ep = jnp.exp2(sp - m)
        ed = jnp.exp2(sd - m)
        l = row_sum(ed)
        if i:
            l = l + row_sum(ep)
        inv = 1 / l
        o = dot((ed * inv).astype(BF16), v_ref[rows])
        if i:
            o = o + dot((ep * inv).astype(BF16), v_ref[before])
        o_ref[rows] = o.astype(BF16)
        l_ref[rows] = m + jnp.log2(l)


def attn_bwd(q_ref, k_ref, v_ref, a_ref, da_ref, l_ref, dq_ref, dk_ref, dv_ref, dk_s, dv_s, slope, scale, tq):
    slope2, scale2 = slope * LOG2E, scale * LOG2E
    dk_s[:] = jnp.zeros_like(dk_s)
    dv_s[:] = jnp.zeros_like(dv_s)
    for i in range(q_ref.shape[0] // tq):
        rows, before = pl.ds(i * tq, tq), pl.ds(0, i * tq)
        q, da = q_ref[rows], da_ref[rows].astype(BF16)
        lse = l_ref[rows]
        delta = row_sum(da.astype(F32) * a_ref[rows].astype(F32))
        near, far, keep = bias(i, tq, slope2)
        dq = None
        for keys, ahead in ((rows, near), (before, far))[:2 if i else 1]:
            kk, vv = k_ref[keys], v_ref[keys]
            p = jnp.exp2(dot_t(q, kk) * scale2 + ahead - lse)
            if keys is rows:
                p = jnp.where(keep, p, 0)
            ds = (p * (dot_t(da, vv) - delta)).astype(BF16)
            dv_s[keys] += t_dot(p.astype(BF16), da)
            dk_s[keys] += t_dot(ds, q)
            part = dot(ds, kk)
            dq = part if dq is None else dq + part
        dq_ref[rows] = (dq * scale).astype(BF16)
    dk_ref[:] = (dk_s[:] * scale).astype(BF16)
    dv_ref[:] = dv_s[:].astype(BF16)


def row_map(i):
    return i, 0


def col_map(i):
    return 0, i


def rows_of(a, n):
    return a, (n, a.shape[1]), row_map


def cols_of(a, n):
    return a, (a.shape[0], n), col_map


def heads_of(a, n):
    return a, (n,) + a.shape[1:], lambda i: (i, 0, 0)


def whole(a):
    return a, a.shape, None


def put(ref, i, part):
    @pl.when(i == 0)
    def _():
        ref[:] = jnp.zeros_like(ref)

    ref[:] += part()


def side_by_side(ref, n):
    return jnp.concatenate([ref[j] for j in range(n)], axis=1)


def local_step(x, lns, wq, wo, wu, wd, dy, comm=True):
    seq, d = x.shape
    heads, hd, ft = 12, 128, 512
    ff, nq, per, slab = wu.shape[1], 3 * d, SUB // hd, d // 4
    scale = 1 / math.sqrt(hd)
    tq = min(256, seq)
    tm = tq
    nm, nf = seq // tm, ff // ft
    slopes = (alibi_slopes(heads), pltpu.SMEM, None)
    b16 = lambda *shape: sds(shape, BF16)
    f32 = lambda *shape: sds(shape, F32)
    vm16 = lambda *shape: pltpu.VMEM(shape, BF16)
    vm32 = lambda *shape: pltpu.VMEM(shape, F32)
    act, wide_act, vec = b16(seq, d), b16(seq, ff), f32(1, d)
    one_vec = (vec, vec.shape, lambda i: (0, 0))
    band = lambda i, n=tm: pl.ds(pl.multiple_of(i * n, n), n)
    ts = tm // 2
    ns = seq // ts
    qs, os, us, ds = (n // WIDE for n in (0, nq, nq + d, nq + d + ff))
    nu = nq // SUB
    packs = [sds((*CHIPS, 2, RB, n), BF16) for n in (d, nq)]

    def S(parts, *args, **kw):
        return [Scatter([(a.reshape(*CHIPS, 2, -1, a.shape[-1]) if isinstance(a, jax.Array) else a, u0, n) for a, u0, n in parts], *args, **kw)] if comm else []

    blocks = lambda w: w.reshape(*CHIPS, 2, -1, w.shape[-1])
    if comm:
        gather = Gather([(w, (WIDE,)) for w in (wq, wo, wu)] + [(wd, (NARROW, wd.shape[0]))])
        lnsum = SmallSum(lns, 0)
    held = {}

    def load(u, ext):
        out = []
        for w, (first, last) in enumerate(((qs, os), (os, us), (us, ds))):
            if first <= u[0] < last:
                full = gather.refs[len(gather.ins) + w] if comm else held['weights'][w]
                r, q = Unit(RB, WIDE * (last - first), WIDE).at(u[1] - first)
                slot = rest(u[1], 2)
                out.append(pltpu.make_async_copy(full.at[:, :, :, :, r, q], ext[3].at[slot], ext[4].at[slot]))
        return out[0]

    def load_down(i, ext):
        full = gather.refs[len(gather.ins) + 3] if comm else held['weights'][3]
        return pltpu.make_async_copy(full.at[:, :, :, :, :, pl.ds(pl.multiple_of(i * NARROW, NARROW), NARROW)], ext[5], ext[4].at[0])

    def weight(u, ext):
        return ext[3][rest(u, 2)].reshape(d, WIDE)

    def gain(row):
        return (lnsum.refs[1] if comm else held['lns'])[pl.ds(row, 1)]

    def start_body(i, ins, outs, ext):
        load((qs, qs), ext).start()
        load((qs, qs + 1), ext).start()

    def ln1_body(i, ins, outs, ext):
        (xr, *more), (ht,), (_, h, *_) = ins, outs, ext
        if more:
            held.update(weights=more[1:], lns=more[0])
        xhat, _ = norm_parts(xr[:].astype(F32))
        h1 = (xhat * gain(0)).astype(BF16)
        h[band(i, ts)] = h1
        ht[:] = h1.T

    def head_of(qkv, h):
        return qkv.at[:, pl.ds(pl.multiple_of(h * hd, hd), hd)]

    def qkv_body(i, ins, outs, ext):
        (o,), (qkv, h, *_) = outs, ext
        load((qs, i), ext).wait()
        r = dot(h[:], weight(i, ext)).astype(BF16)
        for j in range(wide):
            head = r[:, j * hd:(j + 1) * hd]
            head_of(qkv, i * wide + j)[:] = head
            o[j] = head
        pl.when(i + 2 < os)(lambda: load((qs, i + 2), ext).start())
        pl.when(i + 2 >= os)(lambda: load((os, i + 2), ext).start())

    def attn_body(i, ins, outs, ext):
        (sl,), (o, l), (qkv, _, a, *_) = ins, outs, ext
        attn_fwd(*(head_of(qkv, j * heads + i) for j in range(3)), o, l.at[0], sl[i], scale, tq)
        a[:, pl.ds(pl.multiple_of(i * hd, hd), hd)] = o[:]

    def out_body(i, ins, outs, ext):
        (xs,), (o, ht), (_, h, a, *_) = ins, outs, ext

        @pl.when(i == 0)
        def _():
            for u in range(os, us):
                load((os, u), ext).wait()

        ar = a[band(i, ts)]
        r = jnp.concatenate([dot(ar, weight(u, ext)) for u in range(os, us)], axis=1)
        x1 = (xs[:].astype(F32) + r).astype(BF16)
        o[:] = x1
        a[band(i, ts)] = x1
        xhat, _ = norm_parts(x1.astype(F32))
        h2 = (xhat * gain(1)).astype(BF16)
        h[band(i, ts)] = h2
        ht[:] = h2.T

        @pl.when(i == ns - 1)
        def _():
            for u in range(us, us + 2):
                load((us, u), ext).start()

    def up_body(i, ins, outs, ext):
        (dyr,), (gpo, gd), (go, h, *_) = ins, outs, ext
        load((us, us + i), ext).wait()
        u = dot(h[:], weight(us + i, ext))
        cdf = 0.5 * (1.0 + lax.erf(u * math.sqrt(0.5)))
        g = (u * cdf).astype(BF16)
        go[:, pl.ds(pl.multiple_of(i * WIDE, WIDE), WIDE)] = g
        gpo[:] = cdf + u * (jnp.exp(-0.5 * u * u) * math.sqrt(0.5 / math.pi))
        gd[:] = t_dot(g, dyr[:]).astype(BF16)
        pl.when(us + i + 2 < ds)(lambda: load((us, us + i + 2), ext).start())

    def y_body(i, ins, outs, ext):
        (o,), (gr, _, x1r, *_) = outs, ext
        load_down(i, ext).start()
        load_down(i, ext).wait()
        cols = pl.ds(pl.multiple_of(i * NARROW, NARROW), NARROW)
        o[:] = (x1r[:, cols].astype(F32) + dot(gr[:], ext[5][:].reshape(ff, NARROW))).astype(BF16)

    wide = WIDE // hd
    more = [] if comm else [(lns, pltpu.VMEM, None)] + [(blocks(w), HBM, None) for w in (wq, wo, wu, wd)]
    pa = [Phase(ns, 1, [rows_of(x, ts), *more], [cols_of(b16(d, seq), ts)], ln1_body, 5),
          Phase(1, 0, [], [], start_body, 4),
          Phase(nq // WIDE, 3, [], [heads_of(b16(3 * heads, seq, hd), wide)], qkv_body, 5 + ns),
          Phase(heads, 2.7, [slopes], [cols_of(act, hd), heads_of(f32(heads, seq, 1), 1)], attn_body, 5 + ns + nq // WIDE),
          Phase(ns, 2, [rows_of(x, ts)], [rows_of(act, ts), cols_of(b16(d, seq), ts)], out_body, 5 + ns + nq // WIDE + heads),
          Phase(ff // WIDE, 6, [whole(dy)], [cols_of(f32(seq, ff), WIDE), rows_of(b16(ff, d), WIDE)], up_body, 5 + 2 * ns + nq // WIDE + heads),
          Phase(d // NARROW, 4, [], [cols_of(act, NARROW)], y_body, 4 + 2 * ns + nq // WIDE + heads + ff // WIDE)]
    shared = [vm16(seq, ff), vm16(seq, d), vm16(seq, d), vm16(2, *CHIPS, 2, RB, WIDE), pltpu.SemaphoreType.DMA((2,)), vm16(*CHIPS, 2, ff // 32, NARROW)]
    t_qkv, t_attn, t_out, t_up, t_y = (p.at for p in pa[2:])
    fires = [*range(6), t_qkv - 4, t_qkv, t_qkv + 2, t_qkv + 4, t_attn - 1, *range(t_attn, t_up, 4), *range(t_up, t_y, 2), *range(t_y + 1, t_y + d // NARROW)]
    got = host('forward', pa, [gather, lnsum] if comm else [], shared=shared, fires=fires if comm else None)
    h1t, qkv, attn, lse, x1, h2t, gp, g_down, y, *full = got
    fq, fo, fu, fd = wq, wo, wu, wd
    if comm:
        fq, fo, fu, fd = (f.reshape(-1, f.shape[-1]) for f in full[:4])
        lns = full[4]

    def dup_body(i, ins, outs, ext):
        (dyr, w, gpr, ht), (duo, gu) = ins, outs
        du = (dot_t(dyr[:], w[:]) * gpr[:]).astype(BF16)
        duo[:] = du
        gu[:] = dot(ht[:], du).astype(BF16)

    pd = [Phase(nf, 4.6, [whole(dy), rows_of(fd, ft), cols_of(gp, ft), whole(h2t)], [cols_of(wide_act, ft), cols_of(b16(d, ff), ft)], dup_body)]
    n_down = Unit(ff // 32, d).count
    d_up, g_up, *r1 = host('down', pd, S([(g_down, 0, n_down)], [(4, n_down - CARRY)]))

    def dh2_body(i, ins, outs, ext):
        (du, w), acc = ins, ext[0]
        put(acc, i, lambda: dot_t(du[:], w[:]))

    def ln2b_body(i, ins, outs, ext):
        (xr, dyr, lw), (dmo, dmbo, gwo), (acc, dmb, *_) = ins, outs, ext
        dx, gw = norm_back(acc[band(i)], xr[:].astype(F32), lw[pl.ds(1, 1)])
        dm = dyr[:].astype(F32) + dx
        dmo[:] = dm
        dmb[band(i)] = dmbo[:] = dm.astype(BF16)
        put(gwo, i, lambda: gw)

    def dattn_body(i, ins, outs, ext):
        (w,), (acc, dmb, *_) = ins, ext
        acc[:, pl.ds(pl.multiple_of(i * ft, ft), ft)] = dot_t(dmb[:], w[:])

    def battn_body(i, ins, outs, ext):
        (qkv, a, l, sl), (o,), (acc, _, dk, dv) = ins, outs, ext

        @pl.loop(0, pair)
        def _(j):
            h = i * pair + j
            own, here = (pl.ds(pl.multiple_of(n * hd, hd), hd) for n in (h, j))
            attn_bwd(*(qkv.at[n, j] for n in range(3)), a.at[:, here], acc.at[:, own], l.at[j], *(o.at[n, j] for n in range(3)),
                     dk, dv, sl[h], scale, tq)

    pair = 2
    triple = lambda a: (a, (3, pair, seq, hd), lambda i: (0, i, 0, 0))
    pe = [Phase(nf, 2.4, [cols_of(d_up, ft), cols_of(fu, ft)], [], dh2_body),
          Phase(nm, 2, [rows_of(x1, tm), rows_of(dy, tm), whole(lns)], [rows_of(f32(seq, d), tm), rows_of(act, tm), one_vec], ln2b_body),
          Phase(d // ft, 1.9, [rows_of(fo, ft)], [], dattn_body),
          Phase(heads // pair, 6, [triple(qkv.reshape(3, heads, seq, hd)), cols_of(attn, pair * hd), heads_of(lse, pair), slopes],
                [triple(b16(3, heads, seq, hd))], battn_body)]
    early = n_down - 2
    d_mid, d_mid_bf, g_ln2, d_qkv, *r2 = host('back', pe, S([(g_up, 0, early)], [(4, CARRY), (1, early - CARRY)], carry=r1[1:]),
                                          shared=[vm32(seq, d), vm16(seq, d), vm32(seq, hd), vm32(seq, hd)])
    d_qkv = d_qkv.reshape(3 * heads, seq, hd)

    no = d // SUB
    scat = S([(g_up, early, 2), (packs[0], 0, no), (packs[1], 0, nu)], [(1, CARRY + 2), (1, no), (0, nu)], carry=r2[2:], last=True)

    def tile_copy(i, ext):
        r, q = Unit(RB, nq).at(i)
        return pltpu.make_async_copy(ext[1].at[rest(i, 2)], scat[0].written(-1).at[:, :, :, :, r, q], ext[2].at[rest(i, 2)])

    def slab_copy(i, ext):
        return pltpu.make_async_copy(ext[3].at[rest(i, 2)], scat[0].written(-2).at[i], ext[2].at[2 + rest(i, 2)])

    def gout_body(i, ins, outs, ext):
        a, dm = ins
        r = t_dot(a[:], dm[:]).astype(BF16)
        if comm:
            pl.when(i > 1)(lambda: slab_copy(i - 2, ext).wait())
            ext[3][rest(i, 2)] = r.reshape(*CHIPS[1:], 2, RB, d)
            slab_copy(i, ext).start()
        else:
            outs[0][:] = r

    def ship_out_body(i, ins, outs, ext):
        for j in (2, 3):
            slab_copy(j, ext).wait()
        for u in range(no):
            scat[0].ship(u)

    def macro_body(i, ins, outs, ext):
        (ht, dq, w), acc = ins, ext[0]
        tile = side_by_side(dq, per)
        r = dot(ht[:], tile).astype(BF16)
        if comm:
            ext[1][rest(i, 2)] = r.reshape(*CHIPS, 2, RB, SUB)
            tile_copy(i, ext).start()
        else:
            outs[0][:] = r
        put(acc, i, lambda: dot_t(tile, w[:]))

    def ship_body(i, ins, outs, ext):
        tile_copy(i, ext).wait()
        scat[0].ship(no + i)

    def ln1b_body(i, ins, outs, ext):
        (xr, dm, lw), (o, gwo) = ins, outs
        dx, gw = norm_back(ext[0][band(i)], xr[:].astype(F32), lw[pl.ds(0, 1)])
        o[:] = (dm[:] + dx).astype(BF16)
        put(gwo, i, lambda: gw)

    firsts = ([], []) if comm else ([rows_of(b16(d, d), slab)], [cols_of(b16(d, nq), SUB)])
    pf = [Phase(4, 2, [cols_of(attn, slab), whole(d_mid_bf)], firsts[0], gout_body),
          Phase(nu, 3.9, [whole(h1t), heads_of(d_qkv, per), cols_of(fq, SUB)], firsts[1], macro_body),
          Phase(nm, 2, [rows_of(x, tm), rows_of(d_mid, tm), whole(lns)], [rows_of(act, tm), one_vec], ln1b_body)]
    if comm:
        pf += [Phase(1, 0, [], [], ship_out_body, 4), Phase(nu, 0, [], [], ship_body, 5)]
        scat.append(SmallSum(g_ln2, 4 + nu + nm, 1))
    shared = [vm32(seq, d), vm16(2, *CHIPS, 2, RB, SUB), pltpu.SemaphoreType.DMA((4,)), vm16(2, *CHIPS[1:], 2, RB, d)]
    got = host('last', pf, scat, shared=shared, fires=[0, 2, *range(5, 5 + no + nu + 3 * LAG)] if comm else None)
    if not comm:
        g_out, g_qkv, dx, g_ln1 = got
        return y, dx, g_ln1, g_qkv, g_out, g_ln2, g_up, g_down
    dx, _, up_b, g_out, g_qkv, _, _, sums = got
    down_a, (down_b, up_a) = r1[0], r2[:2]
    g_up, g_down = (jnp.concatenate(p, axis=1) for p in ((up_a, up_b), (down_a, down_b)))
    return y, dx, sums, g_qkv, g_out, g_up, g_down


def solution(mesh):
    row_spec = P('fsdp')

    def step(x_in, ln1_w, w_qkv, w_out, ln2_w, w_up, w_down, dy_out):
        rows, _, heads, hd = w_qkv.shape
        d = x_in.shape[-1]
        lns = jnp.pad(jnp.stack([ln1_w, ln2_w]), ((0, 6), (0, d - rows)))
        wq = w_qkv.transpose(1, 2, 0, 3).reshape(-1, rows, hd)
        y, dx, sums, g_qkv, g_out, g_up, g_down = local_step(x_in[0], lns, wq, w_out, w_up, w_down, dy_out[0])
        g_qkv = g_qkv.reshape(3, heads, rows, hd).transpose(2, 0, 1, 3)
        return y[None], dx[None], sums[1, :rows], g_qkv, g_out, sums[0, :rows], g_up, g_down

    return jax.shard_map(step, mesh=mesh, in_specs=(row_spec,) * 8, out_specs=(row_spec,) * 8, check_vma=False)
```

```python
import functools
import math

import jax
import jax.numpy as jnp
from jax import lax
from jax.experimental import pallas as pl
from jax.experimental.pallas import tpu as pltpu
from jax.sharding import PartitionSpec as P

EPS = 1e-5
LOG2E = math.log2(math.e)
SUB = 512
WIDE = 768
HALF = SUB // 2
LAG = 2
GLAG = 1
CARRY = 2 * LAG
LEAD = 3
SIDE = -4
RB = 48
F32, BF16 = jnp.float32, jnp.bfloat16
VMEM_LIMIT = 67_000_000
MESH = pl.DeviceIdType.MESH
HBM = pltpu.MemorySpace.HBM
CHIPS = (4, 2, 2)


def sds(shape, dtype):
    return jax.ShapeDtypeStruct(shape, dtype)


def dot(a, b, ca=1, cb=0):
    return lax.dot_general(a, b, (((ca,), (cb,)), ((), ())), preferred_element_type=F32)


def dot_t(a, b):
    return dot(a, b, 1, 1)


def t_dot(a, b):
    return dot(a, b, 0, 0)


def over_rows(f):
    return functools.partial(f, axis=-1, keepdims=True)


row_sum, row_max, row_mean = map(over_rows, (jnp.sum, jnp.max, jnp.mean))


def clip(t, n):
    return jnp.minimum(jnp.maximum(t, 0), n - 1)


class Phase:
    def __init__(self, n, cost, ins, outs, body, at=None):
        self.n, self.cost, self.ins, self.outs, self.body, self.at = n, cost, ins, outs, body, at

    def on(self, t):
        return (t >= self.at) & (t < self.at + self.n)

    def index(self, f):
        return lambda t: f(clip(t - self.at, self.n))


def quot(a, b):
    return a // b if isinstance(a, int) else lax.div(a, b)


def rest(a, b):
    return a % b if isinstance(a, int) else lax.rem(a, b)


HERE = {}


def locate():
    me = lax.axis_index('fsdp')
    left, place = me, []
    for n in (2, *reversed(CHIPS)):
        place.append(rest(left, n))
        left = quot(left, n)
    c, x, y, z = place
    n, step, ways = CHIPS[0], 8, (1, 2, 3)
    cp, xp, yp = (me + s - 2 * s * b for s, b in zip((1, 2, 4), place))
    HERE.update(coords=(me, z, y, x, c), peers=([rest(me + step * d, step * n) for d in ways], yp, xp, cp), zs=[rest(z + d, n) for d in ways])


def coords():
    return HERE['coords']


def peers():
    return HERE['peers']


def remote(src, dst, ssem, rsem, dev):
    return pltpu.make_async_remote_copy(src_ref=src, dst_ref=dst, send_sem=ssem, recv_sem=rsem, device_id=(dev,), device_id_type=MESH)


class Unit:
    def __init__(self, rows, cols, width=SUB):
        self.width, self.nc, self.nr = width, cols // width, rows // RB
        self.count = self.nc * self.nr

    def at(self, u, half=None):
        lanes, col = self.width, rest(u, self.nc) * self.width
        if half is not None:
            lanes //= 2
            col = col + half * lanes
        rows = slice(None) if self.nr == 1 else pl.ds(pl.multiple_of(quot(u, self.nc) * RB, 16), RB)
        return rows, pl.ds(pl.multiple_of(col, 128), lanes)


class Gather:
    def __init__(self, weights, k0, k1):
        self.k0, self.k1 = k0, k1
        self.k, self.tail = k1 - k0 + 1, 0
        self.z0 = k0 + LEAD if k0 else 0
        self.z1 = k1 + LEAD
        self.w, self.ins, self.outs, self.alias = [], [], [], []
        for shard, full, first, wide in weights:
            heads, rows = shard.shape[:2] if shard.ndim == 3 else (0, shard.shape[0])
            shape = (rows, shard.size // rows)
            unit = Unit(*shape, wide)
            self.w.append((SIDE if heads else len(self.ins), unit, first, first + unit.count, full is None))
            self.ins.append((shard, pl.BlockSpec(memory_space=pltpu.VMEM)))
            if heads:
                self.heads, side = (len(self.ins) - 1, heads), pltpu.VMEM(shape, BF16)
            if full is not None:
                self.alias.append((len(self.ins), len(self.outs)))
                self.ins.append((full, pl.BlockSpec(memory_space=HBM)))
            self.outs.append((sds(CHIPS + (2,) + shape, BF16), pl.BlockSpec(memory_space=HBM)))
        self.base = max(k0 - 2 * GLAG, 0)
        n = self.z1 - self.base
        self.scratch = [side, pltpu.SemaphoreType.DMA((n, 8)), pltpu.SemaphoreType.DMA((n, 8)), pltpu.SemaphoreType.DMA((len(weights),))]

    def copies(self, stage, w, u, refs):
        i, unit, first, _, _ = self.w[w]
        shard, full = refs[i], refs[len(self.ins) + w]
        sems = lambda i: (refs[-3].at[u - self.base, i], refs[-2].at[u - self.base, i])
        me, z, y, x, c = coords()
        zs, yp, xp, cp = peers()
        r, q = unit.at(u - first)
        if stage == 0:
            return [remote(shard.at[r, q], full.at[z, y, x, c, r, q], *sems(d), zs[d]) for d in range(3)]
        if stage == 3:
            v = full.at[:, :, :, c, r, q]
            return [remote(v, v, *sems(7), cp)]
        out = []
        for half in range(2):
            r, q = unit.at(u - first, half)
            j = 2 * stage + 1 + half
            if stage == 1:
                v = full.at[:, y, x, c, r, q]
            else:
                v = full.at[:, y, :, c, r, q] if half else full.at[:, :, x, c, r, q]
            out.append(remote(v, v, *sems(j), xp if half == stage % 2 else yp))
        return out

    def each(self, lo, hi, u, fn):
        for w, (_, _, first, last, _) in enumerate(self.w):
            a, b = max(lo, first), min(hi, last)
            if a < b:
                if u is None:
                    pl.loop(a, b)(functools.partial(fn, w))
                else:
                    pl.when((u >= a) & (u < b))(functools.partial(fn, w, u))

    def go(self, stage, w, u, refs):
        for cp in self.copies(stage, w, u, refs):
            cp.start()

    def arrive(self, stage, w, u, refs):
        for cp in self.copies(stage, w, u, refs):
            cp.wait_recv()

    def left(self, stage, w, u, refs):
        for cp in self.copies(stage, w, u, refs):
            cp.wait_send()

    def step(self, k, fire, begin, refs):
        me, z, y, x, c = coords()
        k0, k1, k = self.k0, self.k1, k + self.k0
        span = [(self.z0, self.z1)] + [(max(k0 - i * GLAG, 0), k1 - i * GLAG) for i in range(3)]

        @pl.when(fire & (k == k0))
        def _():
            i, heads = self.heads
            for h in range(heads):
                refs[SIDE][:, h * 128:(h + 1) * 128] = refs[i][h]
            own = [pltpu.make_async_copy(refs[i], refs[len(self.ins) + w].at[z, y, x, c], refs[-1].at[w])
                   for w, (i, _, _, _, fresh) in enumerate(self.w) if fresh]
            for cp in own:
                cp.start()
            if k0 == 0:
                self.each(0, LEAD, None, lambda w, u: self.go(0, w, u, refs))
            for cp in own:
                cp.wait()

        @pl.when(fire & (k < k1))
        def _():
            self.each(*span[0], k + LEAD, lambda w, u: self.go(0, w, u, refs))
            for stage in (1, 2, 3):
                u = k + GLAG * (1 - stage)
                lo, hi = span[stage - 1]
                self.each(lo, hi, u, lambda w, u: self.arrive(stage - 1, w, u, refs))
                self.each(*span[stage], u, lambda w, u: self.go(stage, w, u, refs))
            self.each(*span[3], k - 3 * GLAG, lambda w, u: self.arrive(3, w, u, refs))

        @pl.when(fire & (k == k1))
        def _():
            for stage in range(4):
                lo, hi = span[stage]
                self.each(max(lo, k1 - stage * GLAG), hi, None, lambda w, u: self.arrive(stage, w, u, refs))
                self.each(lo, hi, None, lambda w, u: self.left(stage, w, u, refs))


class Scatter:
    def __init__(self, grads, layout, carry=None, last=False):
        self.last, self.carried = last, carry is not None
        self.parts, self.ins, n = [], [], 0
        self.late = []
        for g, u0, m in grads:
            self.parts.append((n, n + m, u0, Unit(*g.shape[-2:])))
            if isinstance(g, jax.ShapeDtypeStruct):
                self.late.append(g)
            else:
                self.ins.append((g, pl.BlockSpec(memory_space=HBM)))
            n += m
        self.known = sum(m for g, _, m in grads if not isinstance(g, jax.ShapeDtypeStruct))
        self.n = n
        self.first = 0 if self.carried else CARRY
        self.end = n + CARRY
        self.done = self.end if last else n
        self.k = n + (3 * LAG if last else 1)
        self.tail = 3 * LAG - 1 if last else 0
        self.two_shape, self.three_shape = (2, 4, 2, RB, HALF), (4, RB, SUB)
        if self.carried:
            self.ins += [(a, pl.BlockSpec(memory_space=pltpu.VMEM)) for a in carry]
        self.scratch = [
            pltpu.VMEM((n, *CHIPS, RB, SUB), BF16),
            pltpu.VMEM((2, *CHIPS, RB, SUB), BF16),
            pltpu.VMEM((self.end, *self.two_shape), BF16),
            pltpu.VMEM((self.end, *self.three_shape), BF16),
            pltpu.VMEM((self.end, 3, RB, SUB), BF16),
            pltpu.SemaphoreType.DMA((self.end, 8)), pltpu.SemaphoreType.DMA((self.end, 8)), pltpu.SemaphoreType.DMA((2,))]
        self.layout = layout
        outs = [sds((RB, n * SUB) if n > 0 else (-n * SUB // 128, RB, 128), F32) for n in layout]
        if not last:
            outs += [sds((LAG, *shape), BF16) for shape in (self.two_shape, self.three_shape)]
        self.outs = [(o, pl.BlockSpec(memory_space=pltpu.VMEM)) for o in outs]
        self.outs += [(g, pl.BlockSpec(memory_space=HBM)) for g in self.late]
        self.alias = []

    def source(self, j, refs, fn):
        for i, (a, b, u0, unit) in enumerate(self.parts):
            ref = self.written(i - len(self.parts)) if self.late and a >= self.known else refs[i]
            u = j - CARRY
            if len(self.parts) == 1:
                fn(ref, *unit.at(u0 + u))
            else:
                pl.when((u >= a) & (u < b))(functools.partial(lambda ref, unit, u: fn(ref, *unit.at(u)), ref, unit, u0 + u - a))

    def written(self, i):
        return self.refs[len(self.ins) + len(self.outs) + i]

    def ship(self, u):
        self.swap(CARRY + u, self.refs, lambda cp: cp.start())

    def bufs(self, refs):
        return refs[len(self.ins) + len(self.outs):]

    def local(self, j, refs, act):
        me, z, y, x, c = coords()
        own, ls = self.bufs(refs)[1], self.bufs(refs)[-1]
        slot = rest(j, 2)
        self.source(j, refs, lambda g, r, q: act(pltpu.make_async_copy(g.at[:, :, :, c, r, q], own.at[slot], ls.at[slot])))

    def swap(self, j, refs, act):
        me, z, y, x, c = coords()
        got, ss, rs = self.bufs(refs)[0], *self.bufs(refs)[-3:-1]
        cp = peers()[-1]
        self.source(j, refs, lambda g, r, q: act(remote(g.at[:, :, :, 1 - c, r, q], got.at[j - CARRY], ss.at[j, 0], rs.at[j, 0], cp)))

    def copies(self, stage, j, refs):
        got, own, two, three, four, ss, rs, ls = self.bufs(refs)
        me, z, y, x, c = coords()
        zs, yp, xp, cp = peers()
        a, b = pl.ds(0, HALF), pl.ds(HALF, HALF)
        if stage == 1:
            pairs = [(got.at[j - CARRY, :, 1 - y, :, :, a], two.at[j, 0], yp), (got.at[j - CARRY, :, :, 1 - x, :, b], two.at[j, 1], xp)]
        elif stage == 2:
            pairs = [(two.at[j, 0, :, 1 - x], three.at[j, :, :, a], xp), (two.at[j, 1, :, 1 - y], three.at[j, :, :, b], yp)]
        else:
            pairs = [(three.at[j, HERE['zs'][d]], four.at[j, d], zs[d]) for d in range(3)]
        return [remote(src, dst, ss.at[j, 2 * stage + i - 1], rs.at[j, 2 * stage + i - 1], dev) for i, (src, dst, dev) in enumerate(pairs)]

    def add(self, stage, j, refs):
        got, own, two, three, four, ss, rs, ls = self.bufs(refs)
        me, z, y, x, c = coords()
        a, b = pl.ds(0, HALF), pl.ds(HALF, HALF)
        slot = rest(j, 2)
        if stage == 1:
            @pl.loop(0, 4)
            def _(zz):
                for yy in range(2):
                    for xx in range(2):
                        got[j - CARRY, zz, yy, xx] += own[slot, zz, yy, xx]
        elif stage == 2:
            @pl.loop(0, 4)
            def _(zz):
                for i in range(2):
                    two[j, 0, zz, i] += got[j - CARRY, zz, y, i, :, a]
                    two[j, 1, zz, i] += got[j - CARRY, zz, i, x, :, b]
        elif stage == 3:
            for zz in range(4):
                three[j, zz, :, a] += two[j, 0, zz, x]
                three[j, zz, :, b] += two[j, 1, zz, y]
        else:
            total = three[j, z].astype(F32)
            for d in range(3):
                total += four[j, d].astype(F32)
            a = self.first
            for i, n in enumerate(self.layout):
                b, out = a + abs(n), refs[len(self.ins) + i]

                @pl.when((j >= a) & (j < b))
                def _(out=out, a=a, n=n):
                    if n > 0:
                        out[:, pl.ds(pl.multiple_of((j - a) * SUB, SUB), SUB)] = total
                    else:
                        for h in range(SUB // 128):
                            out[(j - a) * (SUB // 128) + h] = total[:, h * 128:(h + 1) * 128]

                a = b

    def step(self, k, fire, begin, refs):
        n, end, last = self.n, self.end, self.last
        got, own, two, three, four, ss, rs, ls = self.bufs(refs)
        start = lambda cp: cp.start()

        def go(stage, j):
            for cp in self.copies(stage, j, refs):
                cp.start()

        def take(stage, j):
            for cp in self.copies(stage - 1, j, refs):
                cp.wait_recv()
            self.add(stage, j, refs)

        @pl.when(begin)
        def _():
            if self.known:
                pl.loop(CARRY, CARRY + self.known)(lambda j: self.swap(j, refs, start))
                self.local(CARRY, refs, start)
            if self.carried:
                for i in range(LAG):
                    two[LAG + i] = refs[len(self.ins) - 2][i]
                    three[i] = refs[len(self.ins) - 1][i]
                    go(2, LAG + i)
                    go(3, i)

        @pl.when(fire & (k < n))
        def _():
            j = k + CARRY
            if not self.known:
                pl.when(j == CARRY)(lambda: self.local(j, refs, start))
            pl.when(j + 1 < end)(lambda: self.local(j + 1, refs, start))
            self.swap(j, refs, lambda cp: cp.wait_recv())
            self.local(j, refs, lambda cp: cp.wait())
            self.add(1, j, refs)
            go(1, j)

        lows = [CARRY, LAG, 0] if self.carried else [CARRY] * 3
        for stage, low in zip((2, 3, 4), lows):
            j = k + (3 - stage) * LAG

            @pl.when(fire & (j >= low) & (j < end) & ((k < n) | last))
            def _(stage=stage, j=j):
                take(stage, j)
                if stage < 4:
                    go(stage, j)

        @pl.when(fire & (k == self.k - 1))
        def _():
            for stage, low in zip((2, 3, 4), lows):
                a = n + (3 - stage) * LAG
                if not last:
                    pl.loop(max(a, low), a + LAG)(functools.partial(take, stage))

                @pl.loop(CARRY if stage == 2 else low, end if last else a + LAG)
                def _(j):
                    for cp in self.copies(stage - 1, j, refs):
                        cp.wait_send()

            @pl.loop(CARRY, end)
            def _(j):
                self.swap(j, refs, lambda cp: cp.wait_send())

            if not last:
                for i in range(LAG):
                    refs[len(self.ins) + len(self.layout)][i] = two[n + LAG + i]
                    refs[len(self.ins) + len(self.layout) + 1][i] = three[n + i]


class SmallSum:
    def __init__(self, rows, t0, at=None):
        d = rows.shape[1]
        self.at, self.t0, self.k, self.tail = at, t0, 1, 0
        self.ins = [(rows, pl.BlockSpec(memory_space=pltpu.VMEM))]
        self.outs = [(sds((8, d if at is None else 128), F32), pl.BlockSpec(memory_space=pltpu.VMEM))]
        self.alias = []
        self.scratch = [pltpu.VMEM((4, 8, d), F32), pltpu.VMEM((6, 8, d), F32), pltpu.SemaphoreType.DMA((6,)), pltpu.SemaphoreType.DMA((6,))]

    def run(self, t, outs):
        rows, out, acc, got, ss, rs = self.refs
        me = coords()[0]
        zs, yp, xp, cp = peers()
        near = (cp, xp, yp, *zs)
        n = len(near) - len(zs)
        copies = [remote(acc.at[min(i, n)], got.at[i], ss.at[i], rs.at[i], dev) for i, dev in enumerate(near)]

        for i in range(n + 2):
            @pl.when(t == self.t0 + i)
            def _(i=i):
                if not i:
                    if self.at is None:
                        acc[i] = pltpu.roll(rows[:], RB * me, 1)
                    else:
                        acc[i] = jnp.zeros_like(acc[i])
                        acc[i, pl.ds(0, 1)] = rows[:]
                        acc[i, pl.ds(self.at, 1)] = outs[self.at][:]
                elif i <= n:
                    copies[i - 1].wait_recv()
                    acc[i] = acc[i - 1] + got[i - 1]
                else:
                    total = acc[n]
                    for j in range(n, len(near)):
                        copies[j].wait_recv()
                        total += got[j]
                    out[:] = total if self.at is None else pltpu.roll(total, total.shape[1] - RB * me, 1)[:, :128]
                    for copy in copies:
                        copy.wait_send()
                for copy in copies[i:i + 1] if i < n else copies[n:] if i == n else ():
                    copy.start()


KERNELS = ['forward', 'down', 'back', 'last']


def host(name, phases, comms=(), shared=(), fires=None):
    k_all = max([c.k for c in comms], default=1)
    at = 0
    for p in phases:
        if p.at is None:
            p.at = at
        at = max(at, p.at + p.n)
    small = [c for c in comms if isinstance(c, SmallSum)]
    tail = max([c.tail for c in comms], default=0)
    if fires is None:
        spread, clock, fires = k_all - 1 - tail, [0.0], [0]
        for t in range(at):
            clock.append(clock[-1] + sum(p.cost for p in phases if p.at <= t < p.at + p.n))
        for k in range(1, k_all):
            t = at if k >= spread else min(t for t in range(at + 1) if clock[t] * spread >= clock[at] * k)
            fires.append(max(t, fires[-1] + 1))
    total = max([at, fires[-1] + 1] + [c.t0 + 5 for c in small])
    ins, in_specs, outs, out_specs, scratch, alias, resident = [], [], [], [], [], {}, []
    for p in phases:
        for arr, block, index in p.ins:
            if isinstance(block, pltpu.MemorySpace):
                in_specs.append(pl.BlockSpec(memory_space=block))
            elif index is None:
                resident.append((len(ins), p.at))
                in_specs.append(pl.BlockSpec(memory_space=HBM))
            else:
                in_specs.append(pl.BlockSpec(block, p.index(index)))
            ins.append(arr)
        for shape, block, index in p.outs:
            outs.append(shape)
            out_specs.append(pl.BlockSpec(block, p.index(index)))
    for c in comms:
        alias.update({len(ins) + i: len(outs) + o for i, o in c.alias})
        for arr, spec in c.ins:
            ins.append(arr)
            in_specs.append(spec)
        for shape, spec in c.outs:
            outs.append(shape)
            out_specs.append(spec)
        scratch += c.scratch
    scratch += [pltpu.VMEM(ins[i].shape, ins[i].dtype) for i, _ in resident] + [pltpu.SemaphoreType.DMA((max(len(resident), 1),))]
    scratch += list(shared)

    def kernel(*refs):
        refs = list(refs)
        rin, rout, rscr = refs[:len(ins)], refs[len(ins):len(ins) + len(outs)], refs[len(ins) + len(outs):]
        t = pl.program_id(0)
        if comms:
            locate()

            @pl.when(t == 0)
            def _():
                zs, yp, xp, cp = peers()
                near = (*zs, yp, xp, cp)
                bar = pltpu.get_barrier_semaphore()
                for dev in near:
                    pl.semaphore_signal(bar, inc=1, device_id=(dev,), device_id_type=MESH)
                pl.semaphore_wait(bar, len(near))
        i, o, s = sum(len(p.ins) for p in phases), sum(len(p.outs) for p in phases), 0
        k = sum([(t >= f).astype(jnp.int32) for f in fires[1:]], 0 * t)
        fire = functools.reduce(jnp.logical_or, [t == f for f in fires])
        for c in comms:
            ni, no, ns = len(c.ins), len(c.outs), len(c.scratch)
            crefs = rin[i:i + ni] + rout[o:o + no] + rscr[s:s + ns]
            c.refs = crefs
            if c not in small:
                c.step(k, fire, t == 0, crefs)
            elif c.at is None:
                c.run(t, rout)
            i, o, s = i + ni, o + no, s + ns
        held, rsem, extra = rscr[s:s + len(resident)], rscr[s + len(resident)], rscr[s + len(resident) + 1:]
        loads = [(pltpu.make_async_copy(rin[i], h, rsem.at[n]), at) for n, ((i, at), h) in enumerate(zip(resident, held))]
        if loads:
            @pl.when(t == 0)
            def _():
                for cp, _ in loads:
                    cp.start()
        for cp, at in loads:
            pl.when(t == at)(cp.wait)
        for (i, _), h in zip(resident, held):
            rin[i] = h
        i = o = 0
        for p in phases:
            pi, po = rin[i:i + len(p.ins)], rout[o:o + len(p.outs)]
            i, o = i + len(p.ins), o + len(p.outs)

            @pl.when(p.on(t))
            def _(p=p, pi=pi, po=po):
                p.body(t - p.at, pi, po, extra)

        for c in small:
            if c.at is not None:
                c.run(t, rout)

    params = dict(dimension_semantics=("arbitrary",), vmem_limit_bytes=VMEM_LIMIT)
    if comms:
        params.update(collective_id=KERNELS.index(name), has_side_effects=True)
    got = pl.pallas_call(kernel, grid=(total,), in_specs=in_specs, out_specs=out_specs, out_shape=outs, scratch_shapes=scratch,
                         input_output_aliases=alias, compiler_params=pltpu.CompilerParams(**params), name=name,
                         cost_estimate=pl.CostEstimate(flops=2 ** 34, bytes_accessed=2 ** 25, transcendentals=0))(*ins)
    return list(got)


def norm_parts(t):
    mean = row_mean(t)
    cen = t - mean
    rstd = lax.rsqrt(row_mean(cen * cen) + EPS)
    return cen * rstd, rstd


def norm_back(d, t, w):
    xhat, rstd = norm_parts(t)
    dh = d * w
    m1 = row_mean(dh)
    m2 = row_mean(dh * xhat)
    return rstd * (dh - m1 - xhat * m2), jnp.sum(d * xhat, axis=0, keepdims=True)


def alibi_slopes(n_heads):
    padded = 2 ** math.ceil(math.log2(n_heads))
    base = [2.0 ** (-8.0 * (k + 1) / padded) for k in range(padded)]
    ordered = base if padded == n_heads else base[1::2] + base[0::2]
    return jnp.array(ordered[:n_heads], dtype=F32)


def bias(i, tq, slope):
    def ahead(n, first):
        return lax.broadcasted_iota(jnp.int32, (1, n), 1).astype(F32) * slope + slope * first

    row, col = (lax.broadcasted_iota(jnp.int32, (tq, tq), a) for a in range(2))
    return ahead(tq, 0.0), ahead(i * tq, -float(i * tq)) if i else None, row >= col


def attn_fwd(q_ref, k_ref, v_ref, o_ref, l_ref, slope, scale, tq):
    slope, scale = slope * LOG2E, scale * LOG2E
    for i in range(q_ref.shape[0] // tq):
        rows, before = pl.ds(i * tq, tq), pl.ds(0, i * tq)
        q = q_ref[rows]
        near, far, keep = bias(i, tq, slope)
        sd = jnp.where(keep, dot_t(q, k_ref[rows]) * scale + near, -jnp.inf)
        m = row_max(sd)
        if i:
            sp = dot_t(q, k_ref[before]) * scale + far
            m = jnp.maximum(m, row_max(sp))
            ep = jnp.exp2(sp - m)
        ed = jnp.exp2(sd - m)
        l = row_sum(ed)
        if i:
            l = l + row_sum(ep)
        inv = 1 / l
        o = dot((ed * inv).astype(BF16), v_ref[rows])
        if i:
            o = o + dot((ep * inv).astype(BF16), v_ref[before])
        o_ref[rows] = o.astype(BF16)
        l_ref[rows] = m + jnp.log2(l)


def attn_bwd(q_ref, k_ref, v_ref, a_ref, da_ref, l_ref, dq_ref, dk_ref, dv_ref, dk_s, dv_s, slope, scale, tq):
    slope2, scale2 = slope * LOG2E, scale * LOG2E
    dk_s[:] = jnp.zeros_like(dk_s)
    dv_s[:] = jnp.zeros_like(dv_s)
    for i in range(q_ref.shape[0] // tq):
        rows, before = pl.ds(i * tq, tq), pl.ds(0, i * tq)
        q, da = q_ref[rows], da_ref[rows].astype(BF16)
        lse = l_ref[rows]
        delta = row_sum(da.astype(F32) * a_ref[rows].astype(F32))
        near, far, keep = bias(i, tq, slope2)
        dq = None
        for keys, ahead in ((rows, near), (before, far))[:2 if i else 1]:
            kk, vv = k_ref[keys], v_ref[keys]
            p = jnp.exp2(dot_t(q, kk) * scale2 + ahead - lse)
            if keys is rows:
                p = jnp.where(keep, p, 0)
            ds = (p * (dot_t(da, vv) - delta)).astype(BF16)
            dv_s[keys] += t_dot(p.astype(BF16), da)
            dk_s[keys] += t_dot(ds, q)
            part = dot(ds, kk)
            dq = part if dq is None else dq + part
        dq_ref[rows] = (dq * scale).astype(BF16)
    dk_ref[:] = (dk_s[:] * scale).astype(BF16)
    dv_ref[:] = dv_s[:].astype(BF16)


def row_map(i):
    return i, 0


def col_map(i):
    return 0, i


def rows_of(a, n):
    return a, (n, a.shape[1]), row_map


def cols_of(a, n):
    return a, (a.shape[0], n), col_map


def heads_of(a, n):
    return a, (n,) + a.shape[1:], lambda i: (i, 0, 0)


def whole(a):
    return a, a.shape, None


def put(ref, i, part):
    @pl.when(i == 0)
    def _():
        ref[:] = jnp.zeros_like(ref)

    ref[:] += part()


def side_by_side(ref, n):
    return jnp.concatenate([ref[j] for j in range(n)], axis=1)


def local_step(x, lns, wq, wo, wu, wd, dy, comm=True):
    seq, d = x.shape
    heads, hd, ft = 12, 128, 512
    ff, nq, per, slab = wu.shape[1], 3 * d, SUB // hd, 3 * hd
    scale = 1 / math.sqrt(hd)
    tq = min(256, seq)
    tm = tq
    nm, nf = seq // tm, ff // ft
    slopes = (alibi_slopes(heads), pltpu.SMEM, None)
    b16 = lambda *shape: sds(shape, BF16)
    f32 = lambda *shape: sds(shape, F32)
    vm16 = lambda *shape: pltpu.VMEM(shape, BF16)
    vm32 = lambda *shape: pltpu.VMEM(shape, F32)
    act, wide_act, vec = b16(seq, d), b16(seq, ff), f32(1, d)
    one_vec = (vec, vec.shape, lambda i: (0, 0))
    band = lambda i, n=tm: pl.ds(pl.multiple_of(i * n, n), n)
    ts = tm // 2
    ns = seq // ts
    qs, os, us, ds = (n // WIDE for n in (0, nq, nq + d, nq + d + ff))
    nu = nq // SUB
    pack = sds((*CHIPS, 2, RB, nq), BF16)

    def S(parts, *args, **kw):
        return [Scatter([(a.reshape(*CHIPS, 2, -1, a.shape[-1]) if isinstance(a, jax.Array) else a, 0, n) for a, n in parts], *args, **kw)] if comm else []

    blocks = lambda w: w.reshape(*CHIPS, 2, -1, w.shape[-1])
    if comm:
        half = (ds - us) // 2
        gather = Gather([(wq, None, qs, WIDE), (wo, None, os, WIDE), (wu, None, us, d), (wd, None, us + half, d)], qs, ds + 2 * GLAG)
        lnsum = SmallSum(lns, 0)
    held = {}

    def load(u, ext):
        out = []
        for w, (first, last) in enumerate(((qs, os), (os, us), (us, ds))):
            if first <= u[0] < last:
                full = gather.refs[len(gather.ins) + w] if comm else held['weights'][w]
                r, q = Unit(RB, WIDE * (last - first), WIDE).at(u[1] - first)
                slot = rest(u[1], 2)
                out.append(pltpu.make_async_copy(full.at[:, :, :, :, r, q], ext[3].at[slot], ext[4].at[slot]))
        return out[0]

    def weight(u, ext):
        return ext[3][rest(u, 2)].reshape(d, WIDE)

    def gain(row):
        return (lnsum.refs[1] if comm else held['lns'])[pl.ds(row, 1)]

    def start_body(i, ins, outs, ext):
        load((qs, qs), ext).start()
        load((qs, qs + 1), ext).start()

    def ln1_body(i, ins, outs, ext):
        (xr, *more), (ht,), (_, h, *_) = ins, outs, ext
        if more:
            held.update(weights=more[1:], lns=more[0])
        xhat, _ = norm_parts(xr[:].astype(F32))
        h1 = (xhat * gain(0)).astype(BF16)
        h[band(i, ts)] = h1
        ht[:] = h1.T

    def qkv_body(i, ins, outs, ext):
        (o,), (qkv, h, *_) = outs, ext
        load((qs, i), ext).wait()
        r = dot(h[:], weight(i, ext)).astype(BF16)
        for j in range(wide):
            head = r[:, j * hd:(j + 1) * hd]
            qkv[i * wide + j] = head
            o[j] = head
        pl.when(i + 2 < os)(lambda: load((qs, i + 2), ext).start())

    def attn_body(i, ins, outs, ext):
        (sl,), (o, l), (qkv, _, a, *_) = ins, outs, ext
        attn_fwd(qkv.at[i], qkv.at[heads + i], qkv.at[2 * heads + i], o, l.at[0], sl[i], scale, tq)
        a[:, pl.ds(pl.multiple_of(i * hd, hd), hd)] = o[:]

        @pl.when(i == heads // 2)
        def _():
            for u in range(os, us):
                load((os, u), ext).start()

    def out_body(i, ins, outs, ext):
        (xs,), (o, ht), (_, h, a, *_) = ins, outs, ext

        @pl.when(i == 0)
        def _():
            for u in range(os, us):
                load((os, u), ext).wait()

        ar = a[band(i, ts)]
        r = jnp.concatenate([dot(ar, weight(u, ext)) for u in range(os, us)], axis=1)
        x1 = (xs[:].astype(F32) + r).astype(BF16)
        o[:] = x1
        xhat, _ = norm_parts(x1.astype(F32))
        h2 = (xhat * gain(1)).astype(BF16)
        h[band(i, ts)] = h2
        ht[:] = h2.T

        @pl.when(i == ns - 1)
        def _():
            for u in range(us, us + 2):
                load((us, u), ext).start()

    def up_body(i, ins, outs, ext):
        (dyr,), (go, gpo, gd), h = ins, outs, ext[1]
        load((us, us + i), ext).wait()
        u = dot(h[:], weight(us + i, ext))
        cdf = 0.5 * (1.0 + lax.erf(u * math.sqrt(0.5)))
        g = (u * cdf).astype(BF16)
        go[:] = g
        gpo[:] = cdf + u * (jnp.exp(-0.5 * u * u) * math.sqrt(0.5 / math.pi))
        gd[:] = t_dot(g, dyr[:]).astype(BF16)
        pl.when(us + i + 2 < ds)(lambda: load((us, us + i + 2), ext).start())

    wide = WIDE // hd
    more = [] if comm else [(lns, pltpu.VMEM, None)] + [(blocks(w), HBM, None) for w in (wq, wo, wu)]
    pa = [Phase(ns, 1, [rows_of(x, ts), *more], [cols_of(b16(d, seq), ts)], ln1_body, 5),
          Phase(1, 0, [], [], start_body, 4),
          Phase(nq // WIDE, 3, [], [heads_of(b16(3 * heads, seq, hd), wide)], qkv_body, 5 + ns),
          Phase(heads, 2.7, [slopes], [cols_of(act, hd), heads_of(f32(heads, seq, 1), 1)], attn_body, 5 + ns + nq // WIDE),
          Phase(ns, 2, [rows_of(x, ts)], [rows_of(act, ts), cols_of(b16(d, seq), ts)], out_body, 5 + ns + nq // WIDE + heads),
          Phase(ff // WIDE, 6, [whole(dy)], [cols_of(wide_act, WIDE), cols_of(f32(seq, ff), WIDE), rows_of(b16(ff, d), WIDE)], up_body, 5 + 2 * ns + nq // WIDE + heads)]
    shared = [vm16(3 * heads, seq, hd), vm16(seq, d), vm16(seq, d), vm16(2, *CHIPS, 2, RB, WIDE), pltpu.SemaphoreType.DMA((2,))]
    t_qkv, t_attn, t_out, t_up = (p.at for p in pa[2:])
    fires = [*range(6), t_qkv - 4, t_qkv, t_qkv + 2, t_attn, t_attn + heads // 2, t_out, *range(t_up, t_up + ff // WIDE, 2)]
    fires += [fires[-1] + i for i in (2, 3, 4)]
    got = host('forward', pa, [gather, lnsum] if comm else [], shared=shared, fires=fires if comm else None)
    h1t, qkv, attn, lse, x1, h2t, g, gp, g_down, *full = got
    fq, fo, fu, fd = wq, wo, wu, wd
    if comm:
        fq, fo, fu, fd = (f.reshape(-1, f.shape[-1]) for f in full[:4])
        lns = full[4]

    def dup_body(i, ins, outs, ext):
        (dyr, w, gr, gpr, ht), (duo, gu), (acc,) = ins, outs, ext
        du = (dot_t(dyr[:], w[:]) * gpr[:]).astype(BF16)
        duo[:] = du
        gu[:] = dot(ht[:], du).astype(BF16)
        put(acc, i, lambda: dot(gr[:], w[:]))

    def y_body(i, ins, outs, ext):
        (xr,), (o,), (acc,) = ins, outs, ext
        o[:] = (xr[:].astype(F32) + acc[band(i)]).astype(BF16)

    pd = [Phase(nf, 6, [whole(dy), rows_of(fd, ft), cols_of(g, ft), cols_of(gp, ft), whole(h2t)], [cols_of(wide_act, ft), cols_of(b16(d, ff), ft)], dup_body),
          Phase(nm, 1, [rows_of(x1, tm)], [rows_of(act, tm)], y_body)]
    n_down = Unit(ff // 32, d).count
    d_up, g_up, y, *r1 = host('down', pd, S([(g_down, n_down)], [n_down - CARRY]), shared=[vm32(seq, d)])

    def dh2_body(i, ins, outs, ext):
        (du, w), acc = ins, ext[0]
        put(acc, i, lambda: dot_t(du[:], w[:]))

    def ln2b_body(i, ins, outs, ext):
        (xr, dyr, lw), (dmo, gwo), (acc, dmb, *_) = ins, outs, ext
        dx, gw = norm_back(acc[band(i)], xr[:].astype(F32), lw[pl.ds(1, 1)])
        dm = dyr[:].astype(F32) + dx
        dmo[:] = dm
        dmb[band(i)] = dm.astype(BF16)
        put(gwo, i, lambda: gw)

    def dattn_body(i, ins, outs, ext):
        (w,), (acc, dmb, *_) = ins, ext
        acc[:, pl.ds(pl.multiple_of(i * slab, slab), slab)] = dot_t(dmb[:], w[:])

    def battn_body(i, ins, outs, ext):
        (qkv, a, l, sl), (o,), (acc, _, dk, dv) = ins, outs, ext

        @pl.loop(0, pair)
        def _(j):
            h = i * pair + j
            own, here = (pl.ds(pl.multiple_of(n * hd, hd), hd) for n in (h, j))
            attn_bwd(*(qkv.at[n, j] for n in range(3)), a.at[:, here], acc.at[:, own], l.at[j], *(o.at[n, j] for n in range(3)),
                     dk, dv, sl[h], scale, tq)

    def gout_body(i, ins, outs, ext):
        (a,), (o,), (_, dmb, *_) = ins, outs, ext
        o[:] = t_dot(a[:], dmb[:]).astype(BF16)

    pair = 2
    triple = lambda a: (a, (3, pair, seq, hd), lambda i: (0, i, 0, 0))
    pe = [Phase(nf, 2.4, [cols_of(d_up, ft), cols_of(fu, ft)], [], dh2_body),
          Phase(nm, 2, [rows_of(x1, tm), rows_of(dy, tm), whole(lns)], [rows_of(f32(seq, d), tm), one_vec], ln2b_body),
          Phase(d // slab, 1.9, [rows_of(fo, slab)], [], dattn_body),
          Phase(heads // pair, 6, [triple(qkv.reshape(3, heads, seq, hd)), cols_of(attn, pair * hd), heads_of(lse, pair), slopes],
                [triple(b16(3, heads, seq, hd))], battn_body),
          Phase(d // slab, 2, [cols_of(attn, slab)], [rows_of(b16(d, d), slab)], gout_body)]
    d_mid, g_ln2, d_qkv, g_out, *r2 = host('back', pe, S([(g_up, n_down)], [CARRY, n_down - CARRY], carry=r1[1:]),
                                          shared=[vm32(seq, d), vm16(seq, d), vm32(seq, hd), vm32(seq, hd)])
    d_qkv = d_qkv.reshape(3 * heads, seq, hd)

    no = d // SUB
    scat = S([(g_out, no), (pack, nu)], [CARRY, no, -nu], carry=r2[2:], last=True)

    def tile_copy(i, ext):
        r, q = Unit(RB, nq).at(i)
        return pltpu.make_async_copy(ext[1].at[rest(i, 2)], scat[0].written(-1).at[:, :, :, :, r, q], ext[2].at[rest(i, 2)])

    def macro_body(i, ins, outs, ext):
        (ht, dq, w), acc = ins, ext[0]
        tile = side_by_side(dq, per)
        r = dot(ht[:], tile).astype(BF16)
        if comm:
            ext[1][rest(i, 2)] = r.reshape(*CHIPS, 2, RB, SUB)
            tile_copy(i, ext).start()
        else:
            outs[0][:] = r
        put(acc, i, lambda: dot_t(tile, w[:]))

    def ship_body(i, ins, outs, ext):
        tile_copy(i, ext).wait()
        scat[0].ship(no + i)

    def ln1b_body(i, ins, outs, ext):
        (xr, dm, lw), (o, gwo) = ins, outs
        dx, gw = norm_back(ext[0][band(i)], xr[:].astype(F32), lw[pl.ds(0, 1)])
        o[:] = (dm[:] + dx).astype(BF16)
        put(gwo, i, lambda: gw)

    first = [] if comm else [cols_of(b16(d, nq), SUB)]
    pf = [Phase(nu, 3.9, [whole(h1t), heads_of(d_qkv, per), cols_of(fq, SUB)], first, macro_body),
          Phase(nm, 2, [rows_of(x, tm), rows_of(d_mid, tm), whole(lns)], [rows_of(act, tm), one_vec], ln1b_body)]
    if comm:
        pf.append(Phase(nu, 0, [], [], ship_body, 1))
        scat.append(SmallSum(g_ln2, nu + nm, 1))
    shared = [vm32(seq, d), vm16(2, *CHIPS, 2, RB, SUB), pltpu.SemaphoreType.DMA((2,))]
    got = host('last', pf, scat, shared=shared, fires=range(no + nu + 3 * LAG) if comm else None)
    if not comm:
        g_qkv, dx, g_ln1 = got
        return y, dx, g_ln1, g_qkv, g_out, g_ln2, g_up, g_down
    dx, _, up_b, g_out, g_qkv, _, sums = got
    down_a, (down_b, up_a) = r1[0], r2[:2]
    g_down = jnp.concatenate([down_a, down_b], axis=1).reshape(RB, -1, d).transpose(1, 0, 2).reshape(-1, d)
    return y, dx, sums, g_qkv, g_out, None, jnp.concatenate([up_a, up_b], axis=1), g_down


def solution(mesh):
    row_spec = P('fsdp')

    def step(x_in, ln1_w, w_qkv, w_out, ln2_w, w_up, w_down, dy_out):
        rows, _, heads, hd = w_qkv.shape
        d = x_in.shape[-1]
        lns = jnp.pad(jnp.stack([ln1_w, ln2_w]), ((0, 6), (0, d - rows)))
        wq = w_qkv.transpose(1, 2, 0, 3).reshape(-1, rows, hd)
        y, dx, sums, g_qkv, g_out, _, g_up, g_down = local_step(x_in[0], lns, wq, w_out, w_up, w_down, dy_out[0])
        g_qkv = g_qkv.reshape(3, heads, rows, hd).transpose(2, 0, 1, 3)
        return y[None], dx[None], sums[1, :rows], g_qkv, g_out, sums[0, :rows], g_up, g_down

    return jax.shard_map(step, mesh=mesh, in_specs=(row_spec,) * 8, out_specs=(row_spec,) * 8, check_vma=False)
```

```python
import functools
import math

import jax
import jax.numpy as jnp
from jax import lax
from jax.experimental import pallas as pl
from jax.experimental.pallas import tpu as pltpu
from jax.sharding import PartitionSpec as P

EPS = 1e-5
LOG2E = math.log2(math.e)
SUB = 512
WIDE = 768
HALF = SUB // 2
LAG = 2
GLAG = 1
CARRY = 2 * LAG
LEAD = 3
SIDE = -4
RB = 48
F32, BF16 = jnp.float32, jnp.bfloat16
VMEM_LIMIT = 67_000_000
MESH = pl.DeviceIdType.MESH
HBM = pltpu.MemorySpace.HBM
CHIPS = (4, 2, 2)


def sds(shape, dtype):
    return jax.ShapeDtypeStruct(shape, dtype)


def dot(a, b, ca=1, cb=0):
    return lax.dot_general(a, b, (((ca,), (cb,)), ((), ())), preferred_element_type=F32)


def dot_t(a, b):
    return dot(a, b, 1, 1)


def t_dot(a, b):
    return dot(a, b, 0, 0)


def over_rows(f):
    return functools.partial(f, axis=-1, keepdims=True)


row_sum, row_max, row_mean = map(over_rows, (jnp.sum, jnp.max, jnp.mean))


def clip(t, n):
    return jnp.minimum(jnp.maximum(t, 0), n - 1)


class Phase:
    def __init__(self, n, cost, ins, outs, body, at=None):
        self.n, self.cost, self.ins, self.outs, self.body, self.at = n, cost, ins, outs, body, at

    def on(self, t):
        return (t >= self.at) & (t < self.at + self.n)

    def index(self, f):
        return lambda t: f(clip(t - self.at, self.n))


def quot(a, b):
    return a // b if isinstance(a, int) else lax.div(a, b)


def rest(a, b):
    return a % b if isinstance(a, int) else lax.rem(a, b)


HERE = {}


def locate():
    me = lax.axis_index('fsdp')
    left, place = me, []
    for n in (2, *reversed(CHIPS)):
        place.append(rest(left, n))
        left = quot(left, n)
    c, x, y, z = place
    n, step, ways = CHIPS[0], 8, (1, 2, 3)
    cp, xp, yp = (me + s - 2 * s * b for s, b in zip((1, 2, 4), place))
    HERE.update(coords=(me, z, y, x, c), peers=([rest(me + step * d, step * n) for d in ways], yp, xp, cp), zs=[rest(z + d, n) for d in ways])


def coords():
    return HERE['coords']


def peers():
    return HERE['peers']


def remote(src, dst, ssem, rsem, dev):
    return pltpu.make_async_remote_copy(src_ref=src, dst_ref=dst, send_sem=ssem, recv_sem=rsem, device_id=(dev,), device_id_type=MESH)


class Unit:
    def __init__(self, rows, cols, width=SUB):
        self.width, self.nc, self.nr = width, cols // width, rows // RB
        self.count = self.nc * self.nr

    def at(self, u, half=None):
        lanes, col = self.width, rest(u, self.nc) * self.width
        if half is not None:
            lanes //= 2
            col = col + half * lanes
        rows = slice(None) if self.nr == 1 else pl.ds(pl.multiple_of(quot(u, self.nc) * RB, 16), RB)
        return rows, pl.ds(pl.multiple_of(col, 128), lanes)


class Gather:
    def __init__(self, weights, k0, k1):
        self.k0, self.k1 = k0, k1
        self.k, self.tail = k1 - k0 + 1, 0
        self.z0 = k0 + LEAD if k0 else 0
        self.z1 = k1 + LEAD
        self.w, self.ins, self.outs, self.alias = [], [], [], []
        for shard, full, first, wide in weights:
            heads, rows = shard.shape[:2] if shard.ndim == 3 else (0, shard.shape[0])
            shape = (rows, shard.size // rows)
            unit = Unit(*shape, wide)
            self.w.append((SIDE if heads else len(self.ins), unit, first, first + unit.count, full is None))
            self.ins.append((shard, pl.BlockSpec(memory_space=pltpu.VMEM)))
            if heads:
                self.heads, side = (len(self.ins) - 1, heads), pltpu.VMEM(shape, BF16)
            if full is not None:
                self.alias.append((len(self.ins), len(self.outs)))
                self.ins.append((full, pl.BlockSpec(memory_space=HBM)))
            self.outs.append((sds(CHIPS + (2,) + shape, BF16), pl.BlockSpec(memory_space=HBM)))
        self.base = max(k0 - 2 * GLAG, 0)
        n = self.z1 - self.base
        self.scratch = [side, pltpu.SemaphoreType.DMA((n, 8)), pltpu.SemaphoreType.DMA((n, 8)), pltpu.SemaphoreType.DMA((len(weights),))]

    def copies(self, stage, w, u, refs):
        i, unit, first, _, _ = self.w[w]
        shard, full = refs[i], refs[len(self.ins) + w]
        sems = lambda i: (refs[-3].at[u - self.base, i], refs[-2].at[u - self.base, i])
        me, z, y, x, c = coords()
        zs, yp, xp, cp = peers()
        r, q = unit.at(u - first)
        if stage == 0:
            return [remote(shard.at[r, q], full.at[z, y, x, c, r, q], *sems(d), zs[d]) for d in range(3)]
        if stage == 3:
            v = full.at[:, :, :, c, r, q]
            return [remote(v, v, *sems(7), cp)]
        out = []
        for half in range(2):
            r, q = unit.at(u - first, half)
            j = 2 * stage + 1 + half
            if stage == 1:
                v = full.at[:, y, x, c, r, q]
            else:
                v = full.at[:, y, :, c, r, q] if half else full.at[:, :, x, c, r, q]
            out.append(remote(v, v, *sems(j), xp if half == stage % 2 else yp))
        return out

    def each(self, lo, hi, u, fn):
        for w, (_, _, first, last, _) in enumerate(self.w):
            a, b = max(lo, first), min(hi, last)
            if a < b:
                if u is None:
                    pl.loop(a, b)(functools.partial(fn, w))
                else:
                    pl.when((u >= a) & (u < b))(functools.partial(fn, w, u))

    def go(self, stage, w, u, refs):
        for cp in self.copies(stage, w, u, refs):
            cp.start()

    def arrive(self, stage, w, u, refs):
        for cp in self.copies(stage, w, u, refs):
            cp.wait_recv()

    def left(self, stage, w, u, refs):
        for cp in self.copies(stage, w, u, refs):
            cp.wait_send()

    def step(self, k, fire, begin, refs):
        me, z, y, x, c = coords()
        k0, k1, k = self.k0, self.k1, k + self.k0
        span = [(self.z0, self.z1)] + [(max(k0 - i * GLAG, 0), k1 - i * GLAG) for i in range(3)]

        @pl.when(fire & (k == k0))
        def _():
            i, heads = self.heads
            for h in range(heads):
                refs[SIDE][:, h * 128:(h + 1) * 128] = refs[i][h]
            own = [pltpu.make_async_copy(refs[i], refs[len(self.ins) + w].at[z, y, x, c], refs[-1].at[w])
                   for w, (i, _, _, _, fresh) in enumerate(self.w) if fresh]
            for cp in own:
                cp.start()
            if k0 == 0:
                self.each(0, LEAD, None, lambda w, u: self.go(0, w, u, refs))
            for cp in own:
                cp.wait()

        @pl.when(fire & (k < k1))
        def _():
            self.each(*span[0], k + LEAD, lambda w, u: self.go(0, w, u, refs))
            for stage in (1, 2, 3):
                u = k + GLAG * (1 - stage)
                lo, hi = span[stage - 1]
                self.each(lo, hi, u, lambda w, u: self.arrive(stage - 1, w, u, refs))
                self.each(*span[stage], u, lambda w, u: self.go(stage, w, u, refs))
            self.each(*span[3], k - 3 * GLAG, lambda w, u: self.arrive(3, w, u, refs))

        @pl.when(fire & (k == k1))
        def _():
            for stage in range(4):
                lo, hi = span[stage]
                self.each(max(lo, k1 - stage * GLAG), hi, None, lambda w, u: self.arrive(stage, w, u, refs))
                self.each(lo, hi, None, lambda w, u: self.left(stage, w, u, refs))


class Scatter:
    def __init__(self, grads, layout, carry=None, last=False):
        self.last, self.carried = last, carry is not None
        self.parts, self.ins, n = [], [], 0
        self.late = []
        for g, u0, m in grads:
            self.parts.append((n, n + m, u0, Unit(*g.shape[-2:])))
            if isinstance(g, jax.ShapeDtypeStruct):
                self.late.append(g)
            else:
                self.ins.append((g, pl.BlockSpec(memory_space=HBM)))
            n += m
        self.known = sum(m for g, _, m in grads if not isinstance(g, jax.ShapeDtypeStruct))
        self.n = n
        self.first = 0 if self.carried else CARRY
        self.end = n + CARRY
        self.done = self.end if last else n
        self.k = n + (3 * LAG if last else 1)
        self.tail = 3 * LAG - 1 if last else 0
        self.two_shape, self.three_shape = (2, 4, 2, RB, HALF), (4, RB, SUB)
        if self.carried:
            self.ins += [(a, pl.BlockSpec(memory_space=pltpu.VMEM)) for a in carry]
        self.scratch = [
            pltpu.VMEM((n, *CHIPS, RB, SUB), BF16),
            pltpu.VMEM((2, *CHIPS, RB, SUB), BF16),
            pltpu.VMEM((self.end, *self.two_shape), BF16),
            pltpu.VMEM((self.end, *self.three_shape), BF16),
            pltpu.VMEM((self.end, 3, RB, SUB), BF16),
            pltpu.SemaphoreType.DMA((self.end, 8)), pltpu.SemaphoreType.DMA((self.end, 8)), pltpu.SemaphoreType.DMA((2,))]
        self.layout = layout
        outs = [sds((RB, n * SUB) if n > 0 else (-n * SUB // 128, RB, 128), F32) for n in layout]
        if not last:
            outs += [sds((LAG, *shape), BF16) for shape in (self.two_shape, self.three_shape)]
        self.outs = [(o, pl.BlockSpec(memory_space=pltpu.VMEM)) for o in outs]
        self.outs += [(g, pl.BlockSpec(memory_space=HBM)) for g in self.late]
        self.alias = []

    def source(self, j, refs, fn):
        for i, (a, b, u0, unit) in enumerate(self.parts):
            ref = self.written(i - len(self.parts)) if self.late and a >= self.known else refs[i]
            u = j - CARRY
            if len(self.parts) == 1:
                fn(ref, *unit.at(u0 + u))
            else:
                pl.when((u >= a) & (u < b))(functools.partial(lambda ref, unit, u: fn(ref, *unit.at(u)), ref, unit, u0 + u - a))

    def written(self, i):
        return self.refs[len(self.ins) + len(self.outs) + i]

    def ship(self, u):
        self.swap(CARRY + u, self.refs, lambda cp: cp.start())

    def bufs(self, refs):
        return refs[len(self.ins) + len(self.outs):]

    def local(self, j, refs, act):
        me, z, y, x, c = coords()
        own, ls = self.bufs(refs)[1], self.bufs(refs)[-1]
        slot = rest(j, 2)
        self.source(j, refs, lambda g, r, q: act(pltpu.make_async_copy(g.at[:, :, :, c, r, q], own.at[slot], ls.at[slot])))

    def swap(self, j, refs, act):
        me, z, y, x, c = coords()
        got, ss, rs = self.bufs(refs)[0], *self.bufs(refs)[-3:-1]
        cp = peers()[-1]
        self.source(j, refs, lambda g, r, q: act(remote(g.at[:, :, :, 1 - c, r, q], got.at[j - CARRY], ss.at[j, 0], rs.at[j, 0], cp)))

    def copies(self, stage, j, refs):
        got, own, two, three, four, ss, rs, ls = self.bufs(refs)
        me, z, y, x, c = coords()
        zs, yp, xp, cp = peers()
        a, b = pl.ds(0, HALF), pl.ds(HALF, HALF)
        if stage == 1:
            pairs = [(got.at[j - CARRY, :, 1 - y, :, :, a], two.at[j, 0], yp), (got.at[j - CARRY, :, :, 1 - x, :, b], two.at[j, 1], xp)]
        elif stage == 2:
            pairs = [(two.at[j, 0, :, 1 - x], three.at[j, :, :, a], xp), (two.at[j, 1, :, 1 - y], three.at[j, :, :, b], yp)]
        else:
            pairs = [(three.at[j, HERE['zs'][d]], four.at[j, d], zs[d]) for d in range(3)]
        return [remote(src, dst, ss.at[j, 2 * stage + i - 1], rs.at[j, 2 * stage + i - 1], dev) for i, (src, dst, dev) in enumerate(pairs)]

    def add(self, stage, j, refs):
        got, own, two, three, four, ss, rs, ls = self.bufs(refs)
        me, z, y, x, c = coords()
        a, b = pl.ds(0, HALF), pl.ds(HALF, HALF)
        slot = rest(j, 2)
        if stage == 1:
            @pl.loop(0, 4)
            def _(zz):
                for yy in range(2):
                    for xx in range(2):
                        got[j - CARRY, zz, yy, xx] += own[slot, zz, yy, xx]
        elif stage == 2:
            @pl.loop(0, 4)
            def _(zz):
                for i in range(2):
                    two[j, 0, zz, i] += got[j - CARRY, zz, y, i, :, a]
                    two[j, 1, zz, i] += got[j - CARRY, zz, i, x, :, b]
        elif stage == 3:
            for zz in range(4):
                three[j, zz, :, a] += two[j, 0, zz, x]
                three[j, zz, :, b] += two[j, 1, zz, y]
        else:
            total = three[j, z].astype(F32)
            for d in range(3):
                total += four[j, d].astype(F32)
            a = self.first
            for i, n in enumerate(self.layout):
                b, out = a + abs(n), refs[len(self.ins) + i]

                @pl.when((j >= a) & (j < b))
                def _(out=out, a=a, n=n):
                    if n > 0:
                        out[:, pl.ds(pl.multiple_of((j - a) * SUB, SUB), SUB)] = total
                    else:
                        for h in range(SUB // 128):
                            out[(j - a) * (SUB // 128) + h] = total[:, h * 128:(h + 1) * 128]

                a = b

    def step(self, k, fire, begin, refs):
        n, end, last = self.n, self.end, self.last
        got, own, two, three, four, ss, rs, ls = self.bufs(refs)
        start = lambda cp: cp.start()

        def go(stage, j):
            for cp in self.copies(stage, j, refs):
                cp.start()

        def take(stage, j):
            for cp in self.copies(stage - 1, j, refs):
                cp.wait_recv()
            self.add(stage, j, refs)

        @pl.when(begin)
        def _():
            if self.known:
                pl.loop(CARRY, CARRY + self.known)(lambda j: self.swap(j, refs, start))
                self.local(CARRY, refs, start)
            if self.carried:
                for i in range(LAG):
                    two[LAG + i] = refs[len(self.ins) - 2][i]
                    three[i] = refs[len(self.ins) - 1][i]
                    go(2, LAG + i)
                    go(3, i)

        @pl.when(fire & (k < n))
        def _():
            j = k + CARRY
            if not self.known:
                pl.when(j == CARRY)(lambda: self.local(j, refs, start))
            pl.when(j + 1 < end)(lambda: self.local(j + 1, refs, start))
            self.swap(j, refs, lambda cp: cp.wait_recv())
            self.local(j, refs, lambda cp: cp.wait())
            self.add(1, j, refs)
            go(1, j)

        lows = [CARRY, LAG, 0] if self.carried else [CARRY] * 3
        for stage, low in zip((2, 3, 4), lows):
            j = k + (3 - stage) * LAG

            @pl.when(fire & (j >= low) & (j < end) & ((k < n) | last))
            def _(stage=stage, j=j):
                take(stage, j)
                if stage < 4:
                    go(stage, j)

        @pl.when(fire & (k == self.k - 1))
        def _():
            for stage, low in zip((2, 3, 4), lows):
                a = n + (3 - stage) * LAG
                if not last:
                    pl.loop(max(a, low), a + LAG)(functools.partial(take, stage))

                @pl.loop(CARRY if stage == 2 else low, end if last else a + LAG)
                def _(j):
                    for cp in self.copies(stage - 1, j, refs):
                        cp.wait_send()

            @pl.loop(CARRY, end)
            def _(j):
                self.swap(j, refs, lambda cp: cp.wait_send())

            if not last:
                for i in range(LAG):
                    refs[len(self.ins) + len(self.layout)][i] = two[n + LAG + i]
                    refs[len(self.ins) + len(self.layout) + 1][i] = three[n + i]


class SmallSum:
    def __init__(self, rows, t0, at=None):
        d = rows.shape[1]
        self.at, self.t0, self.k, self.tail = at, t0, 1, 0
        self.ins = [(rows, pl.BlockSpec(memory_space=pltpu.VMEM))]
        self.outs = [(sds((8, d if at is None else 128), F32), pl.BlockSpec(memory_space=pltpu.VMEM))]
        self.alias = []
        self.scratch = [pltpu.VMEM((4, 8, d), F32), pltpu.VMEM((6, 8, d), F32), pltpu.SemaphoreType.DMA((6,)), pltpu.SemaphoreType.DMA((6,))]

    def run(self, t, outs):
        rows, out, acc, got, ss, rs = self.refs
        me = coords()[0]
        zs, yp, xp, cp = peers()
        near = (cp, xp, yp, *zs)
        n = len(near) - len(zs)
        copies = [remote(acc.at[min(i, n)], got.at[i], ss.at[i], rs.at[i], dev) for i, dev in enumerate(near)]

        for i in range(n + 2):
            @pl.when(t == self.t0 + i)
            def _(i=i):
                if not i:
                    if self.at is None:
                        acc[i] = pltpu.roll(rows[:], RB * me, 1)
                    else:
                        acc[i] = jnp.zeros_like(acc[i])
                        acc[i, pl.ds(0, 1)] = rows[:]
                        acc[i, pl.ds(self.at, 1)] = outs[self.at][:]
                elif i <= n:
                    copies[i - 1].wait_recv()
                    acc[i] = acc[i - 1] + got[i - 1]
                else:
                    total = acc[n]
                    for j in range(n, len(near)):
                        copies[j].wait_recv()
                        total += got[j]
                    out[:] = total if self.at is None else pltpu.roll(total, total.shape[1] - RB * me, 1)[:, :128]
                    for copy in copies:
                        copy.wait_send()
                for copy in copies[i:i + 1] if i < n else copies[n:] if i == n else ():
                    copy.start()


KERNELS = ['forward', 'down', 'back', 'last']


def host(name, phases, comms=(), shared=(), fires=None):
    k_all = max([c.k for c in comms], default=1)
    at = 0
    for p in phases:
        if p.at is None:
            p.at = at
        at = max(at, p.at + p.n)
    small = [c for c in comms if isinstance(c, SmallSum)]
    tail = max([c.tail for c in comms], default=0)
    if fires is None:
        spread, clock, fires = k_all - 1 - tail, [0.0], [0]
        for t in range(at):
            clock.append(clock[-1] + sum(p.cost for p in phases if p.at <= t < p.at + p.n))
        for k in range(1, k_all):
            t = at if k >= spread else min(t for t in range(at + 1) if clock[t] * spread >= clock[at] * k)
            fires.append(max(t, fires[-1] + 1))
    total = max([at, fires[-1] + 1] + [c.t0 + 5 for c in small])
    ins, in_specs, outs, out_specs, scratch, alias, resident = [], [], [], [], [], {}, []
    for p in phases:
        for arr, block, index in p.ins:
            if isinstance(block, pltpu.MemorySpace):
                in_specs.append(pl.BlockSpec(memory_space=block))
            elif index is None:
                resident.append((len(ins), p.at))
                in_specs.append(pl.BlockSpec(memory_space=HBM))
            else:
                in_specs.append(pl.BlockSpec(block, p.index(index)))
            ins.append(arr)
        for shape, block, index in p.outs:
            outs.append(shape)
            out_specs.append(pl.BlockSpec(block, p.index(index)))
    for c in comms:
        alias.update({len(ins) + i: len(outs) + o for i, o in c.alias})
        for arr, spec in c.ins:
            ins.append(arr)
            in_specs.append(spec)
        for shape, spec in c.outs:
            outs.append(shape)
            out_specs.append(spec)
        scratch += c.scratch
    scratch += [pltpu.VMEM(ins[i].shape, ins[i].dtype) for i, _ in resident] + [pltpu.SemaphoreType.DMA((max(len(resident), 1),))]
    scratch += list(shared)

    def kernel(*refs):
        refs = list(refs)
        rin, rout, rscr = refs[:len(ins)], refs[len(ins):len(ins) + len(outs)], refs[len(ins) + len(outs):]
        t = pl.program_id(0)
        if comms:
            locate()

            @pl.when(t == 0)
            def _():
                zs, yp, xp, cp = peers()
                near = (*zs, yp, xp, cp)
                bar = pltpu.get_barrier_semaphore()
                for dev in near:
                    pl.semaphore_signal(bar, inc=1, device_id=(dev,), device_id_type=MESH)
                pl.semaphore_wait(bar, len(near))
        i, o, s = sum(len(p.ins) for p in phases), sum(len(p.outs) for p in phases), 0
        k = sum([(t >= f).astype(jnp.int32) for f in fires[1:]], 0 * t)
        fire = functools.reduce(jnp.logical_or, [t == f for f in fires])
        for c in comms:
            ni, no, ns = len(c.ins), len(c.outs), len(c.scratch)
            crefs = rin[i:i + ni] + rout[o:o + no] + rscr[s:s + ns]
            c.refs = crefs
            if c not in small:
                c.step(k, fire, t == 0, crefs)
            elif c.at is None:
                c.run(t, rout)
            i, o, s = i + ni, o + no, s + ns
        held, rsem, extra = rscr[s:s + len(resident)], rscr[s + len(resident)], rscr[s + len(resident) + 1:]
        loads = [(pltpu.make_async_copy(rin[i], h, rsem.at[n]), at) for n, ((i, at), h) in enumerate(zip(resident, held))]
        if loads:
            @pl.when(t == 0)
            def _():
                for cp, _ in loads:
                    cp.start()
        for cp, at in loads:
            pl.when(t == at)(cp.wait)
        for (i, _), h in zip(resident, held):
            rin[i] = h
        i = o = 0
        for p in phases:
            pi, po = rin[i:i + len(p.ins)], rout[o:o + len(p.outs)]
            i, o = i + len(p.ins), o + len(p.outs)

            @pl.when(p.on(t))
            def _(p=p, pi=pi, po=po):
                p.body(t - p.at, pi, po, extra)

        for c in small:
            if c.at is not None:
                c.run(t, rout)

    params = dict(dimension_semantics=("arbitrary",), vmem_limit_bytes=VMEM_LIMIT)
    if comms:
        params.update(collective_id=KERNELS.index(name), has_side_effects=True)
    got = pl.pallas_call(kernel, grid=(total,), in_specs=in_specs, out_specs=out_specs, out_shape=outs, scratch_shapes=scratch,
                         input_output_aliases=alias, compiler_params=pltpu.CompilerParams(**params), name=name,
                         cost_estimate=pl.CostEstimate(flops=2 ** 34, bytes_accessed=2 ** 25, transcendentals=0))(*ins)
    return list(got)


def norm_parts(t):
    mean = row_mean(t)
    cen = t - mean
    rstd = lax.rsqrt(row_mean(cen * cen) + EPS)
    return cen * rstd, rstd


def norm_back(d, t, w):
    xhat, rstd = norm_parts(t)
    dh = d * w
    m1 = row_mean(dh)
    m2 = row_mean(dh * xhat)
    return rstd * (dh - m1 - xhat * m2), jnp.sum(d * xhat, axis=0, keepdims=True)


def alibi_slopes(n_heads):
    padded = 2 ** math.ceil(math.log2(n_heads))
    base = [2.0 ** (-8.0 * (k + 1) / padded) for k in range(padded)]
    ordered = base if padded == n_heads else base[1::2] + base[0::2]
    return jnp.array(ordered[:n_heads], dtype=F32)


def bias(i, tq, slope):
    def ahead(n, first):
        return lax.broadcasted_iota(jnp.int32, (1, n), 1).astype(F32) * slope + slope * first

    row, col = (lax.broadcasted_iota(jnp.int32, (tq, tq), a) for a in range(2))
    return ahead(tq, 0.0), ahead(i * tq, -float(i * tq)) if i else None, row >= col


def attn_fwd(q_ref, k_ref, v_ref, o_ref, l_ref, slope, scale, tq):
    slope, scale = slope * LOG2E, scale * LOG2E
    for i in range(q_ref.shape[0] // tq):
        rows, before = pl.ds(i * tq, tq), pl.ds(0, i * tq)
        q = q_ref[rows]
        near, far, keep = bias(i, tq, slope)
        sd = jnp.where(keep, dot_t(q, k_ref[rows]) * scale + near, -jnp.inf)
        m = row_max(sd)
        if i:
            sp = dot_t(q, k_ref[before]) * scale + far
            m = jnp.maximum(m, row_max(sp))
            ep = jnp.exp2(sp - m)
        ed = jnp.exp2(sd - m)
        l = row_sum(ed)
        if i:
            l = l + row_sum(ep)
        inv = 1 / l
        o = dot((ed * inv).astype(BF16), v_ref[rows])
        if i:
            o = o + dot((ep * inv).astype(BF16), v_ref[before])
        o_ref[rows] = o.astype(BF16)
        l_ref[rows] = m + jnp.log2(l)


def attn_bwd(q_ref, k_ref, v_ref, a_ref, da_ref, l_ref, dq_ref, dk_ref, dv_ref, dq_s, slope, scale, tq):
    slope2, scale2 = slope * LOG2E, scale * LOG2E
    seq = q_ref.shape[0]
    da_all = da_ref[:].astype(BF16)
    delta = row_sum(da_all.astype(F32) * a_ref[:].astype(F32))
    near, _, keep = bias(0, tq, slope2)
    for j in range(seq // tq):
        keys, rows = pl.ds(j * tq, tq), pl.ds(j * tq, seq - j * tq)
        kk, q, da = k_ref[keys], q_ref[rows], da_all[j * tq:]
        l = jnp.concatenate([l_ref[pl.ds(i * tq, tq)] + slope2 * float((i - j) * tq) for i in range(j, seq // tq)], axis=0)
        p = jnp.exp2(dot_t(q, kk) * scale2 + near - l)
        own = jnp.where(keep, p[:tq], 0)
        p = own if j == seq // tq - 1 else jnp.concatenate([own, p[tq:]], axis=0)
        ds = (p * (dot_t(da, v_ref[keys]) - delta[j * tq:])).astype(BF16)
        dv_ref[keys] = t_dot(p.astype(BF16), da).astype(BF16)
        dk_ref[keys] = (t_dot(ds, q) * scale).astype(BF16)
        part = dot(ds, kk)
        if j:
            dq_s[rows] += part
        else:
            dq_s[:] = part
    dq_ref[:] = (dq_s[:] * scale).astype(BF16)


def row_map(i):
    return i, 0


def col_map(i):
    return 0, i


def rows_of(a, n):
    return a, (n, a.shape[1]), row_map


def cols_of(a, n):
    return a, (a.shape[0], n), col_map


def heads_of(a, n):
    return a, (n,) + a.shape[1:], lambda i: (i, 0, 0)


def whole(a):
    return a, a.shape, None


def put(ref, i, part):
    @pl.when(i == 0)
    def _():
        ref[:] = jnp.zeros_like(ref)

    ref[:] += part()


def side_by_side(ref, n):
    return jnp.concatenate([ref[j] for j in range(n)], axis=1)


def local_step(x, lns, wq, wo, wu, wd, dy, comm=True):
    seq, d = x.shape
    heads, hd, ft = 12, 128, 512
    ff, nq, per, slab = wu.shape[1], 3 * d, SUB // hd, 3 * hd
    scale = 1 / math.sqrt(hd)
    tq = min(256, seq)
    tm = tq
    nm, nf = seq // tm, ff // ft
    slopes = (alibi_slopes(heads), pltpu.SMEM, None)
    b16 = lambda *shape: sds(shape, BF16)
    f32 = lambda *shape: sds(shape, F32)
    vm16 = lambda *shape: pltpu.VMEM(shape, BF16)
    vm32 = lambda *shape: pltpu.VMEM(shape, F32)
    act, wide_act, vec = b16(seq, d), b16(seq, ff), f32(1, d)
    one_vec = (vec, vec.shape, lambda i: (0, 0))
    band = lambda i, n=tm: pl.ds(pl.multiple_of(i * n, n), n)
    ts = tm // 2
    ns = seq // ts
    qs, os, us, ds = (n // WIDE for n in (0, nq, nq + d, nq + d + ff))
    nu = nq // SUB
    pack = sds((*CHIPS, 2, RB, nq), BF16)

    def S(parts, *args, **kw):
        return [Scatter([(a.reshape(*CHIPS, 2, -1, a.shape[-1]) if isinstance(a, jax.Array) else a, 0, n) for a, n in parts], *args, **kw)] if comm else []

    blocks = lambda w: w.reshape(*CHIPS, 2, -1, w.shape[-1])
    if comm:
        half = (ds - us) // 2
        gather = Gather([(wq, None, qs, WIDE), (wo, None, os, WIDE), (wu, None, us, d), (wd, None, us + half, d)], qs, ds + 2 * GLAG)
        lnsum = SmallSum(lns, 0)
    held = {}

    def load(u, ext):
        out = []
        for w, (first, last) in enumerate(((qs, os), (os, us), (us, ds))):
            if first <= u[0] < last:
                full = gather.refs[len(gather.ins) + w] if comm else held['weights'][w]
                r, q = Unit(RB, WIDE * (last - first), WIDE).at(u[1] - first)
                slot = rest(u[1], 2)
                out.append(pltpu.make_async_copy(full.at[:, :, :, :, r, q], ext[3].at[slot], ext[4].at[slot]))
        return out[0]

    def weight(u, ext):
        return ext[3][rest(u, 2)].reshape(d, WIDE)

    def gain(row):
        return (lnsum.refs[1] if comm else held['lns'])[pl.ds(row, 1)]

    def start_body(i, ins, outs, ext):
        load((qs, qs), ext).start()
        load((qs, qs + 1), ext).start()

    def ln1_body(i, ins, outs, ext):
        (xr, *more), (ht,), (_, h, *_) = ins, outs, ext
        if more:
            held.update(weights=more[1:], lns=more[0])
        xhat, _ = norm_parts(xr[:].astype(F32))
        h1 = (xhat * gain(0)).astype(BF16)
        h[band(i, ts)] = h1
        ht[:] = h1.T

    def qkv_body(i, ins, outs, ext):
        (o,), (qkv, h, *_) = outs, ext
        load((qs, i), ext).wait()
        r = dot(h[:], weight(i, ext)).astype(BF16)
        for j in range(wide):
            head = r[:, j * hd:(j + 1) * hd]
            qkv[i * wide + j] = head
            o[j] = head
        pl.when(i + 2 < os)(lambda: load((qs, i + 2), ext).start())

    def attn_body(i, ins, outs, ext):
        (sl,), (o, l), (qkv, _, a, *_) = ins, outs, ext
        attn_fwd(qkv.at[i], qkv.at[heads + i], qkv.at[2 * heads + i], o, l.at[0], sl[i], scale, tq)
        a[:, pl.ds(pl.multiple_of(i * hd, hd), hd)] = o[:]

        @pl.when(i == heads // 2)
        def _():
            for u in range(os, us):
                load((os, u), ext).start()

    def out_body(i, ins, outs, ext):
        (xs,), (o, ht), (_, h, a, *_) = ins, outs, ext

        @pl.when(i == 0)
        def _():
            for u in range(os, us):
                load((os, u), ext).wait()

        ar = a[band(i, ts)]
        r = jnp.concatenate([dot(ar, weight(u, ext)) for u in range(os, us)], axis=1)
        x1 = (xs[:].astype(F32) + r).astype(BF16)
        o[:] = x1
        xhat, _ = norm_parts(x1.astype(F32))
        h2 = (xhat * gain(1)).astype(BF16)
        h[band(i, ts)] = h2
        ht[:] = h2.T

        @pl.when(i == ns - 1)
        def _():
            for u in range(us, us + 2):
                load((us, u), ext).start()

    def up_body(i, ins, outs, ext):
        (dyr,), (go, gpo, gd), h = ins, outs, ext[1]
        load((us, us + i), ext).wait()
        u = dot(h[:], weight(us + i, ext))
        cdf = 0.5 * (1.0 + lax.erf(u * math.sqrt(0.5)))
        g = (u * cdf).astype(BF16)
        go[:] = g
        gpo[:] = cdf + u * (jnp.exp(-0.5 * u * u) * math.sqrt(0.5 / math.pi))
        gd[:] = t_dot(g, dyr[:]).astype(BF16)
        pl.when(us + i + 2 < ds)(lambda: load((us, us + i + 2), ext).start())

    wide = WIDE // hd
    more = [] if comm else [(lns, pltpu.VMEM, None)] + [(blocks(w), HBM, None) for w in (wq, wo, wu)]
    pa = [Phase(ns, 1, [rows_of(x, ts), *more], [cols_of(b16(d, seq), ts)], ln1_body, 5),
          Phase(1, 0, [], [], start_body, 4),
          Phase(nq // WIDE, 3, [], [heads_of(b16(3 * heads, seq, hd), wide)], qkv_body, 5 + ns),
          Phase(heads, 2.7, [slopes], [cols_of(act, hd), heads_of(f32(heads, seq, 1), 1)], attn_body, 5 + ns + nq // WIDE),
          Phase(ns, 2, [rows_of(x, ts)], [rows_of(act, ts), cols_of(b16(d, seq), ts)], out_body, 5 + ns + nq // WIDE + heads),
          Phase(ff // WIDE, 6, [whole(dy)], [cols_of(wide_act, WIDE), cols_of(f32(seq, ff), WIDE), rows_of(b16(ff, d), WIDE)], up_body, 5 + 2 * ns + nq // WIDE + heads)]
    shared = [vm16(3 * heads, seq, hd), vm16(seq, d), vm16(seq, d), vm16(2, *CHIPS, 2, RB, WIDE), pltpu.SemaphoreType.DMA((2,))]
    t_qkv, t_attn, t_out, t_up = (p.at for p in pa[2:])
    fires = [*range(6), t_qkv - 4, t_qkv, t_qkv + 2, t_attn, t_attn + heads // 2, t_out, *range(t_up, t_up + ff // WIDE, 2)]
    fires += [fires[-1] + i for i in (2, 3, 4)]
    got = host('forward', pa, [gather, lnsum] if comm else [], shared=shared, fires=fires if comm else None)
    h1t, qkv, attn, lse, x1, h2t, g, gp, g_down, *full = got
    fq, fo, fu, fd = wq, wo, wu, wd
    if comm:
        fq, fo, fu, fd = (f.reshape(-1, f.shape[-1]) for f in full[:4])
        lns = full[4]

    def dup_body(i, ins, outs, ext):
        (dyr, w, gr, gpr, ht), (duo, gu), (acc,) = ins, outs, ext
        du = (dot_t(dyr[:], w[:]) * gpr[:]).astype(BF16)
        duo[:] = du
        gu[:] = dot(ht[:], du).astype(BF16)
        put(acc, i, lambda: dot(gr[:], w[:]))

    def y_body(i, ins, outs, ext):
        (xr,), (o,), (acc,) = ins, outs, ext
        o[:] = (xr[:].astype(F32) + acc[band(i)]).astype(BF16)

    pd = [Phase(nf, 6, [whole(dy), rows_of(fd, ft), cols_of(g, ft), cols_of(gp, ft), whole(h2t)], [cols_of(wide_act, ft), cols_of(b16(d, ff), ft)], dup_body),
          Phase(nm, 1, [rows_of(x1, tm)], [rows_of(act, tm)], y_body)]
    n_down = Unit(ff // 32, d).count
    d_up, g_up, y, *r1 = host('down', pd, S([(g_down, n_down)], [n_down - CARRY]), shared=[vm32(seq, d)])

    def dh2_body(i, ins, outs, ext):
        (du, w), acc = ins, ext[0]
        put(acc, i, lambda: dot_t(du[:], w[:]))

    def ln2b_body(i, ins, outs, ext):
        (xr, dyr, lw), (dmo, gwo), (acc, dmb, *_) = ins, outs, ext
        dx, gw = norm_back(acc[band(i)], xr[:].astype(F32), lw[pl.ds(1, 1)])
        dm = dyr[:].astype(F32) + dx
        dmo[:] = dm
        dmb[band(i)] = dm.astype(BF16)
        put(gwo, i, lambda: gw)

    def dattn_body(i, ins, outs, ext):
        (w,), (acc, dmb, *_) = ins, ext
        acc[:, pl.ds(pl.multiple_of(i * slab, slab), slab)] = dot_t(dmb[:], w[:])

    def battn_body(i, ins, outs, ext):
        (qkv, a, l, sl), (o,), (acc, _, dq) = ins, outs, ext

        @pl.loop(0, pair)
        def _(j):
            h = i * pair + j
            own, here = (pl.ds(pl.multiple_of(n * hd, hd), hd) for n in (h, j))
            attn_bwd(*(qkv.at[n, j] for n in range(3)), a.at[:, here], acc.at[:, own], l.at[j], *(o.at[n, j] for n in range(3)),
                     dq, sl[h], scale, tq)

    def gout_body(i, ins, outs, ext):
        (a,), (o,), (_, dmb, *_) = ins, outs, ext
        o[:] = t_dot(a[:], dmb[:]).astype(BF16)

    pair = 2
    triple = lambda a: (a, (3, pair, seq, hd), lambda i: (0, i, 0, 0))
    pe = [Phase(nf, 2.4, [cols_of(d_up, ft), cols_of(fu, ft)], [], dh2_body),
          Phase(nm, 2, [rows_of(x1, tm), rows_of(dy, tm), whole(lns)], [rows_of(f32(seq, d), tm), one_vec], ln2b_body),
          Phase(d // slab, 1.9, [rows_of(fo, slab)], [], dattn_body),
          Phase(heads // pair, 6, [triple(qkv.reshape(3, heads, seq, hd)), cols_of(attn, pair * hd), heads_of(lse, pair), slopes],
                [triple(b16(3, heads, seq, hd))], battn_body),
          Phase(d // slab, 2, [cols_of(attn, slab)], [rows_of(b16(d, d), slab)], gout_body)]
    d_mid, g_ln2, d_qkv, g_out, *r2 = host('back', pe, S([(g_up, n_down)], [CARRY, n_down - CARRY], carry=r1[1:]),
                                          shared=[vm32(seq, d), vm16(seq, d), vm32(seq, hd)])
    d_qkv = d_qkv.reshape(3 * heads, seq, hd)

    no = d // SUB
    scat = S([(g_out, no), (pack, nu)], [CARRY, no, -nu], carry=r2[2:], last=True)

    def tile_copy(i, ext):
        r, q = Unit(RB, nq).at(i)
        return pltpu.make_async_copy(ext[1].at[rest(i, 2)], scat[0].written(-1).at[:, :, :, :, r, q], ext[2].at[rest(i, 2)])

    def macro_body(i, ins, outs, ext):
        (ht, dq, w), acc = ins, ext[0]
        tile = side_by_side(dq, per)
        r = dot(ht[:], tile).astype(BF16)
        if comm:
            ext[1][rest(i, 2)] = r.reshape(*CHIPS, 2, RB, SUB)
            tile_copy(i, ext).start()
        else:
            outs[0][:] = r
        put(acc, i, lambda: dot_t(tile, w[:]))

    def ship_body(i, ins, outs, ext):
        tile_copy(i, ext).wait()
        scat[0].ship(no + i)

    def ln1b_body(i, ins, outs, ext):
        (xr, dm, lw), (o, gwo) = ins, outs
        dx, gw = norm_back(ext[0][band(i)], xr[:].astype(F32), lw[pl.ds(0, 1)])
        o[:] = (dm[:] + dx).astype(BF16)
        put(gwo, i, lambda: gw)

    first = [] if comm else [cols_of(b16(d, nq), SUB)]
    pf = [Phase(nu, 3.9, [whole(h1t), heads_of(d_qkv, per), cols_of(fq, SUB)], first, macro_body),
          Phase(nm, 2, [rows_of(x, tm), rows_of(d_mid, tm), whole(lns)], [rows_of(act, tm), one_vec], ln1b_body)]
    if comm:
        pf.append(Phase(nu, 0, [], [], ship_body, 1))
        scat.append(SmallSum(g_ln2, nu + nm, 1))
    shared = [vm32(seq, d), vm16(2, *CHIPS, 2, RB, SUB), pltpu.SemaphoreType.DMA((2,))]
    got = host('last', pf, scat, shared=shared, fires=range(no + nu + 3 * LAG) if comm else None)
    if not comm:
        g_qkv, dx, g_ln1 = got
        return y, dx, g_ln1, g_qkv, g_out, g_ln2, g_up, g_down
    dx, _, up_b, g_out, g_qkv, _, sums = got
    down_a, (down_b, up_a) = r1[0], r2[:2]
    g_down = jnp.concatenate([down_a, down_b], axis=1).reshape(RB, -1, d).transpose(1, 0, 2).reshape(-1, d)
    return y, dx, sums, g_qkv, g_out, None, jnp.concatenate([up_a, up_b], axis=1), g_down


def solution(mesh):
    row_spec = P('fsdp')

    def step(x_in, ln1_w, w_qkv, w_out, ln2_w, w_up, w_down, dy_out):
        rows, _, heads, hd = w_qkv.shape
        d = x_in.shape[-1]
        lns = jnp.pad(jnp.stack([ln1_w, ln2_w]), ((0, 6), (0, d - rows)))
        wq = w_qkv.transpose(1, 2, 0, 3).reshape(-1, rows, hd)
        y, dx, sums, g_qkv, g_out, _, g_up, g_down = local_step(x_in[0], lns, wq, w_out, w_up, w_down, dy_out[0])
        g_qkv = g_qkv.reshape(3, heads, rows, hd).transpose(2, 0, 1, 3)
        return y[None], dx[None], sums[1, :rows], g_qkv, g_out, sums[0, :rows], g_up, g_down

    return jax.shard_map(step, mesh=mesh, in_specs=(row_spec,) * 8, out_specs=(row_spec,) * 8, check_vma=False)
```

```python
import functools
import math

import jax
import jax.numpy as jnp
from jax import lax
from jax.experimental import pallas as pl
from jax.experimental.pallas import tpu as pltpu
from jax.sharding import PartitionSpec as P

EPS = 1e-5
LOG2E = math.log2(math.e)
SUB = 512
WIDE = 768
HALF = SUB // 2
LAG = 2
GLAG = 1
CARRY = 2 * LAG
LEAD = 3
SIDE = -4
RB = 48
F32, BF16 = jnp.float32, jnp.bfloat16
VMEM_LIMIT = 67_000_000
MESH = pl.DeviceIdType.MESH
HBM = pltpu.MemorySpace.HBM
CHIPS = (4, 2, 2)


def sds(shape, dtype):
    return jax.ShapeDtypeStruct(shape, dtype)


def dot(a, b, ca=1, cb=0):
    return lax.dot_general(a, b, (((ca,), (cb,)), ((), ())), preferred_element_type=F32)


def dot_t(a, b):
    return dot(a, b, 1, 1)


def t_dot(a, b):
    return dot(a, b, 0, 0)


def over_rows(f):
    return functools.partial(f, axis=-1, keepdims=True)


row_sum, row_max, row_mean = map(over_rows, (jnp.sum, jnp.max, jnp.mean))


def clip(t, n):
    return jnp.minimum(jnp.maximum(t, 0), n - 1)


class Phase:
    def __init__(self, n, cost, ins, outs, body, at=None):
        self.n, self.cost, self.ins, self.outs, self.body, self.at = n, cost, ins, outs, body, at

    def on(self, t):
        return (t >= self.at) & (t < self.at + self.n)

    def index(self, f):
        return lambda t: f(clip(t - self.at, self.n))


def quot(a, b):
    return a // b if isinstance(a, int) else lax.div(a, b)


def rest(a, b):
    return a % b if isinstance(a, int) else lax.rem(a, b)


HERE = {}


def locate():
    me = lax.axis_index('fsdp')
    left, place = me, []
    for n in (2, *reversed(CHIPS)):
        place.append(rest(left, n))
        left = quot(left, n)
    c, x, y, z = place
    n, step, ways = CHIPS[0], 8, (1, 2, 3)
    cp, xp, yp = (me + s - 2 * s * b for s, b in zip((1, 2, 4), place))
    HERE.update(coords=(me, z, y, x, c), peers=([rest(me + step * d, step * n) for d in ways], yp, xp, cp), zs=[rest(z + d, n) for d in ways])


def coords():
    return HERE['coords']


def peers():
    return HERE['peers']


def remote(src, dst, ssem, rsem, dev):
    return pltpu.make_async_remote_copy(src_ref=src, dst_ref=dst, send_sem=ssem, recv_sem=rsem, device_id=(dev,), device_id_type=MESH)


class Unit:
    def __init__(self, rows, cols, width=SUB):
        self.width, self.nc, self.nr = width, cols // width, rows // RB
        self.count = self.nc * self.nr

    def at(self, u, half=None):
        lanes, col = self.width, rest(u, self.nc) * self.width
        if half is not None:
            lanes //= 2
            col = col + half * lanes
        rows = slice(None) if self.nr == 1 else pl.ds(pl.multiple_of(quot(u, self.nc) * RB, 16), RB)
        return rows, pl.ds(pl.multiple_of(col, 128), lanes)


class Gather:
    def __init__(self, weights, k0, k1):
        self.k0, self.k1 = k0, k1
        self.k, self.tail = k1 - k0 + 1, 0
        self.z0 = k0 + LEAD if k0 else 0
        self.z1 = k1 + LEAD
        self.w, self.ins, self.outs, self.alias = [], [], [], []
        for shard, full, first, wide in weights:
            heads, rows = shard.shape[:2] if shard.ndim == 3 else (0, shard.shape[0])
            shape = (rows, shard.size // rows)
            unit = Unit(*shape, wide)
            self.w.append((SIDE if heads else len(self.ins), unit, first, first + unit.count, full is None))
            self.ins.append((shard, pl.BlockSpec(memory_space=pltpu.VMEM)))
            if heads:
                self.heads, side = (len(self.ins) - 1, heads), pltpu.VMEM(shape, BF16)
            if full is not None:
                self.alias.append((len(self.ins), len(self.outs)))
                self.ins.append((full, pl.BlockSpec(memory_space=HBM)))
            self.outs.append((sds(CHIPS + (2,) + shape, BF16), pl.BlockSpec(memory_space=HBM)))
        self.base = max(k0 - 2 * GLAG, 0)
        n = self.z1 - self.base
        self.scratch = [side, pltpu.SemaphoreType.DMA((n, 8)), pltpu.SemaphoreType.DMA((n, 8)), pltpu.SemaphoreType.DMA((len(weights),))]

    def copies(self, stage, w, u, refs):
        i, unit, first, _, _ = self.w[w]
        shard, full = refs[i], refs[len(self.ins) + w]
        sems = lambda i: (refs[-3].at[u - self.base, i], refs[-2].at[u - self.base, i])
        me, z, y, x, c = coords()
        zs, yp, xp, cp = peers()
        r, q = unit.at(u - first)
        if stage == 0:
            return [remote(shard.at[r, q], full.at[z, y, x, c, r, q], *sems(d), zs[d]) for d in range(3)]
        if stage == 3:
            v = full.at[:, :, :, c, r, q]
            return [remote(v, v, *sems(7), cp)]
        out = []
        for half in range(2):
            r, q = unit.at(u - first, half)
            j = 2 * stage + 1 + half
            if stage == 1:
                v = full.at[:, y, x, c, r, q]
            else:
                v = full.at[:, y, :, c, r, q] if half else full.at[:, :, x, c, r, q]
            out.append(remote(v, v, *sems(j), xp if half == stage % 2 else yp))
        return out

    def each(self, lo, hi, u, fn):
        for w, (_, _, first, last, _) in enumerate(self.w):
            a, b = max(lo, first), min(hi, last)
            if a < b:
                if u is None:
                    pl.loop(a, b)(functools.partial(fn, w))
                else:
                    pl.when((u >= a) & (u < b))(functools.partial(fn, w, u))

    def go(self, stage, w, u, refs):
        for cp in self.copies(stage, w, u, refs):
            cp.start()

    def arrive(self, stage, w, u, refs):
        for cp in self.copies(stage, w, u, refs):
            cp.wait_recv()

    def left(self, stage, w, u, refs):
        for cp in self.copies(stage, w, u, refs):
            cp.wait_send()

    def step(self, k, fire, begin, refs):
        me, z, y, x, c = coords()
        k0, k1, k = self.k0, self.k1, k + self.k0
        span = [(self.z0, self.z1)] + [(max(k0 - i * GLAG, 0), k1 - i * GLAG) for i in range(3)]

        @pl.when(fire & (k == k0))
        def _():
            i, heads = self.heads
            for h in range(heads):
                refs[SIDE][:, h * 128:(h + 1) * 128] = refs[i][h]
            own = [pltpu.make_async_copy(refs[i], refs[len(self.ins) + w].at[z, y, x, c], refs[-1].at[w])
                   for w, (i, _, _, _, fresh) in enumerate(self.w) if fresh]
            for cp in own:
                cp.start()
            if k0 == 0:
                self.each(0, LEAD, None, lambda w, u: self.go(0, w, u, refs))
            for cp in own:
                cp.wait()

        @pl.when(fire & (k < k1))
        def _():
            self.each(*span[0], k + LEAD, lambda w, u: self.go(0, w, u, refs))
            for stage in (1, 2, 3):
                u = k + GLAG * (1 - stage)
                lo, hi = span[stage - 1]
                self.each(lo, hi, u, lambda w, u: self.arrive(stage - 1, w, u, refs))
                self.each(*span[stage], u, lambda w, u: self.go(stage, w, u, refs))
            self.each(*span[3], k - 3 * GLAG, lambda w, u: self.arrive(3, w, u, refs))

        @pl.when(fire & (k == k1))
        def _():
            for stage in range(4):
                lo, hi = span[stage]
                self.each(max(lo, k1 - stage * GLAG), hi, None, lambda w, u: self.arrive(stage, w, u, refs))
                self.each(lo, hi, None, lambda w, u: self.left(stage, w, u, refs))


class Scatter:
    def __init__(self, grads, layout, carry=None, last=False):
        self.last, self.carried = last, carry is not None
        self.parts, self.ins, n = [], [], 0
        self.late = []
        for g, u0, m in grads:
            self.parts.append((n, n + m, u0, Unit(*g.shape[-2:])))
            if isinstance(g, jax.ShapeDtypeStruct):
                self.late.append(g)
            else:
                self.ins.append((g, pl.BlockSpec(memory_space=HBM)))
            n += m
        self.known = sum(m for g, _, m in grads if not isinstance(g, jax.ShapeDtypeStruct))
        self.n = n
        self.first = 0 if self.carried else CARRY
        self.end = n + CARRY
        self.done = self.end if last else n
        self.k = n + (3 * LAG if last else 1)
        self.tail = 3 * LAG - 1 if last else 0
        self.two_shape, self.three_shape = (2, 4, 2, RB, HALF), (4, RB, SUB)
        if self.carried:
            self.ins += [(a, pl.BlockSpec(memory_space=pltpu.VMEM)) for a in carry]
        self.scratch = [
            pltpu.VMEM((n, *CHIPS, RB, SUB), BF16),
            pltpu.VMEM((2, *CHIPS, RB, SUB), BF16),
            pltpu.VMEM((self.end, *self.two_shape), BF16),
            pltpu.VMEM((self.end, *self.three_shape), BF16),
            pltpu.VMEM((self.end, 3, RB, SUB), BF16),
            pltpu.SemaphoreType.DMA((self.end, 8)), pltpu.SemaphoreType.DMA((self.end, 8)), pltpu.SemaphoreType.DMA((2,))]
        self.layout = layout
        outs = [sds((RB, n * SUB) if n > 0 else (-n * SUB // 128, RB, 128), F32) for n in layout]
        if not last:
            outs += [sds((LAG, *shape), BF16) for shape in (self.two_shape, self.three_shape)]
        self.outs = [(o, pl.BlockSpec(memory_space=pltpu.VMEM)) for o in outs]
        self.outs += [(g, pl.BlockSpec(memory_space=HBM)) for g in self.late]
        self.alias = []

    def source(self, j, refs, fn):
        for i, (a, b, u0, unit) in enumerate(self.parts):
            ref = self.written(i - len(self.parts)) if self.late and a >= self.known else refs[i]
            u = j - CARRY
            if len(self.parts) == 1:
                fn(ref, *unit.at(u0 + u))
            else:
                pl.when((u >= a) & (u < b))(functools.partial(lambda ref, unit, u: fn(ref, *unit.at(u)), ref, unit, u0 + u - a))

    def written(self, i):
        return self.refs[len(self.ins) + len(self.outs) + i]

    def ship(self, u):
        self.swap(CARRY + u, self.refs, lambda cp: cp.start())

    def bufs(self, refs):
        return refs[len(self.ins) + len(self.outs):]

    def local(self, j, refs, act):
        me, z, y, x, c = coords()
        own, ls = self.bufs(refs)[1], self.bufs(refs)[-1]
        slot = rest(j, 2)
        self.source(j, refs, lambda g, r, q: act(pltpu.make_async_copy(g.at[:, :, :, c, r, q], own.at[slot], ls.at[slot])))

    def swap(self, j, refs, act):
        me, z, y, x, c = coords()
        got, ss, rs = self.bufs(refs)[0], *self.bufs(refs)[-3:-1]
        cp = peers()[-1]
        self.source(j, refs, lambda g, r, q: act(remote(g.at[:, :, :, 1 - c, r, q], got.at[j - CARRY], ss.at[j, 0], rs.at[j, 0], cp)))

    def copies(self, stage, j, refs):
        got, own, two, three, four, ss, rs, ls = self.bufs(refs)
        me, z, y, x, c = coords()
        zs, yp, xp, cp = peers()
        a, b = pl.ds(0, HALF), pl.ds(HALF, HALF)
        if stage == 1:
            pairs = [(got.at[j - CARRY, :, 1 - y, :, :, a], two.at[j, 0], yp), (got.at[j - CARRY, :, :, 1 - x, :, b], two.at[j, 1], xp)]
        elif stage == 2:
            pairs = [(two.at[j, 0, :, 1 - x], three.at[j, :, :, a], xp), (two.at[j, 1, :, 1 - y], three.at[j, :, :, b], yp)]
        else:
            pairs = [(three.at[j, HERE['zs'][d]], four.at[j, d], zs[d]) for d in range(3)]
        return [remote(src, dst, ss.at[j, 2 * stage + i - 1], rs.at[j, 2 * stage + i - 1], dev) for i, (src, dst, dev) in enumerate(pairs)]

    def add(self, stage, j, refs):
        got, own, two, three, four, ss, rs, ls = self.bufs(refs)
        me, z, y, x, c = coords()
        a, b = pl.ds(0, HALF), pl.ds(HALF, HALF)
        slot = rest(j, 2)
        if stage == 1:
            @pl.loop(0, 4)
            def _(zz):
                for yy in range(2):
                    for xx in range(2):
                        got[j - CARRY, zz, yy, xx] += own[slot, zz, yy, xx]
        elif stage == 2:
            @pl.loop(0, 4)
            def _(zz):
                for i in range(2):
                    two[j, 0, zz, i] += got[j - CARRY, zz, y, i, :, a]
                    two[j, 1, zz, i] += got[j - CARRY, zz, i, x, :, b]
        elif stage == 3:
            for zz in range(4):
                three[j, zz, :, a] += two[j, 0, zz, x]
                three[j, zz, :, b] += two[j, 1, zz, y]
        else:
            total = three[j, z].astype(F32)
            for d in range(3):
                total += four[j, d].astype(F32)
            a = self.first
            for i, n in enumerate(self.layout):
                b, out = a + abs(n), refs[len(self.ins) + i]

                @pl.when((j >= a) & (j < b))
                def _(out=out, a=a, n=n):
                    if n > 0:
                        out[:, pl.ds(pl.multiple_of((j - a) * SUB, SUB), SUB)] = total
                    else:
                        for h in range(SUB // 128):
                            out[(j - a) * (SUB // 128) + h] = total[:, h * 128:(h + 1) * 128]

                a = b

    def step(self, k, fire, begin, refs):
        n, end, last = self.n, self.end, self.last
        got, own, two, three, four, ss, rs, ls = self.bufs(refs)
        start = lambda cp: cp.start()

        def go(stage, j):
            for cp in self.copies(stage, j, refs):
                cp.start()

        def take(stage, j):
            for cp in self.copies(stage - 1, j, refs):
                cp.wait_recv()
            self.add(stage, j, refs)

        @pl.when(begin)
        def _():
            if self.known:
                pl.loop(CARRY, CARRY + self.known)(lambda j: self.swap(j, refs, start))
                self.local(CARRY, refs, start)
            if self.carried:
                for i in range(LAG):
                    two[LAG + i] = refs[len(self.ins) - 2][i]
                    three[i] = refs[len(self.ins) - 1][i]
                    go(2, LAG + i)
                    go(3, i)

        @pl.when(fire & (k < n))
        def _():
            j = k + CARRY
            if not self.known:
                pl.when(j == CARRY)(lambda: self.local(j, refs, start))
            pl.when(j + 1 < end)(lambda: self.local(j + 1, refs, start))
            self.swap(j, refs, lambda cp: cp.wait_recv())
            self.local(j, refs, lambda cp: cp.wait())
            self.add(1, j, refs)
            go(1, j)

        lows = [CARRY, LAG, 0] if self.carried else [CARRY] * 3
        for stage, low in zip((2, 3, 4), lows):
            j = k + (3 - stage) * LAG

            @pl.when(fire & (j >= low) & (j < end) & ((k < n) | last))
            def _(stage=stage, j=j):
                take(stage, j)
                if stage < 4:
                    go(stage, j)

        @pl.when(fire & (k == self.k - 1))
        def _():
            for stage, low in zip((2, 3, 4), lows):
                a = n + (3 - stage) * LAG
                if not last:
                    pl.loop(max(a, low), a + LAG)(functools.partial(take, stage))

                @pl.loop(CARRY if stage == 2 else low, end if last else a + LAG)
                def _(j):
                    for cp in self.copies(stage - 1, j, refs):
                        cp.wait_send()

            @pl.loop(CARRY, end)
            def _(j):
                self.swap(j, refs, lambda cp: cp.wait_send())

            if not last:
                for i in range(LAG):
                    refs[len(self.ins) + len(self.layout)][i] = two[n + LAG + i]
                    refs[len(self.ins) + len(self.layout) + 1][i] = three[n + i]


class SmallSum:
    def __init__(self, rows, d, t0, at=None):
        self.at, self.t0, self.k, self.tail = at, t0, 1, 0
        self.ins = [(row, pl.BlockSpec(memory_space=pltpu.VMEM)) for row in rows]
        self.outs = [(sds((8, d if at is None else 128), F32), pl.BlockSpec(memory_space=pltpu.VMEM))]
        self.alias = []
        self.scratch = [pltpu.VMEM((4, 8, d), F32), pltpu.VMEM((6, 8, d), F32), pltpu.SemaphoreType.DMA((6,)), pltpu.SemaphoreType.DMA((6,))]

    def run(self, t, outs):
        *rows, out, acc, got, ss, rs = self.refs
        if self.at is not None:
            rows.append(outs[self.at])
        me = coords()[0]
        zs, yp, xp, cp = peers()
        near = (cp, xp, yp, *zs)
        n = len(near) - len(zs)
        copies = [remote(acc.at[min(i, n)], got.at[i], ss.at[i], rs.at[i], dev) for i, dev in enumerate(near)]

        for i in range(n + 2):
            @pl.when(t == self.t0 + i)
            def _(i=i):
                if not i:
                    acc[i] = jnp.zeros_like(acc[i])
                    for j, row in enumerate(rows):
                        acc[i, pl.ds(j, 1), pl.ds(0, row.shape[1])] = row[:]
                    if self.at is None:
                        acc[i] = pltpu.roll(acc[i], RB * me, 1)
                elif i <= n:
                    copies[i - 1].wait_recv()
                    acc[i] = acc[i - 1] + got[i - 1]
                else:
                    total = acc[n]
                    for j in range(n, len(near)):
                        copies[j].wait_recv()
                        total += got[j]
                    out[:] = total if self.at is None else pltpu.roll(total, total.shape[1] - RB * me, 1)[:, :128]
                    for copy in copies:
                        copy.wait_send()
                for copy in copies[i:i + 1] if i < n else copies[n:] if i == n else ():
                    copy.start()


KERNELS = ['forward', 'down', 'back', 'last']


def host(name, phases, comms=(), shared=(), fires=None):
    k_all = max([c.k for c in comms], default=1)
    at = 0
    for p in phases:
        if p.at is None:
            p.at = at
        at = max(at, p.at + p.n)
    small = [c for c in comms if isinstance(c, SmallSum)]
    tail = max([c.tail for c in comms], default=0)
    if fires is None:
        spread, clock, fires = k_all - 1 - tail, [0.0], [0]
        for t in range(at):
            clock.append(clock[-1] + sum(p.cost for p in phases if p.at <= t < p.at + p.n))
        for k in range(1, k_all):
            t = at if k >= spread else min(t for t in range(at + 1) if clock[t] * spread >= clock[at] * k)
            fires.append(max(t, fires[-1] + 1))
    total = max([at, fires[-1] + 1] + [c.t0 + 5 for c in small])
    ins, in_specs, outs, out_specs, scratch, alias, resident = [], [], [], [], [], {}, []
    for p in phases:
        for arr, block, index in p.ins:
            if isinstance(block, pltpu.MemorySpace):
                in_specs.append(pl.BlockSpec(memory_space=block))
            elif index is None:
                resident.append((len(ins), p.at))
                in_specs.append(pl.BlockSpec(memory_space=HBM))
            else:
                in_specs.append(pl.BlockSpec(block, p.index(index)))
            ins.append(arr)
        for shape, block, index in p.outs:
            outs.append(shape)
            out_specs.append(pl.BlockSpec(block, p.index(index)))
    for c in comms:
        alias.update({len(ins) + i: len(outs) + o for i, o in c.alias})
        for arr, spec in c.ins:
            ins.append(arr)
            in_specs.append(spec)
        for shape, spec in c.outs:
            outs.append(shape)
            out_specs.append(spec)
        scratch += c.scratch
    scratch += [pltpu.VMEM(ins[i].shape, ins[i].dtype) for i, _ in resident] + [pltpu.SemaphoreType.DMA((max(len(resident), 1),))]
    scratch += list(shared)

    def kernel(*refs):
        refs = list(refs)
        rin, rout, rscr = refs[:len(ins)], refs[len(ins):len(ins) + len(outs)], refs[len(ins) + len(outs):]
        t = pl.program_id(0)
        if comms:
            locate()

            @pl.when(t == 0)
            def _():
                zs, yp, xp, cp = peers()
                near = (*zs, yp, xp, cp)
                bar = pltpu.get_barrier_semaphore()
                for dev in near:
                    pl.semaphore_signal(bar, inc=1, device_id=(dev,), device_id_type=MESH)
                pl.semaphore_wait(bar, len(near))
        i, o, s = sum(len(p.ins) for p in phases), sum(len(p.outs) for p in phases), 0
        k = sum([(t >= f).astype(jnp.int32) for f in fires[1:]], 0 * t)
        fire = functools.reduce(jnp.logical_or, [t == f for f in fires])
        for c in comms:
            ni, no, ns = len(c.ins), len(c.outs), len(c.scratch)
            crefs = rin[i:i + ni] + rout[o:o + no] + rscr[s:s + ns]
            c.refs = crefs
            if c not in small:
                c.step(k, fire, t == 0, crefs)
            elif c.at is None:
                c.run(t, rout)
            i, o, s = i + ni, o + no, s + ns
        held, rsem, extra = rscr[s:s + len(resident)], rscr[s + len(resident)], rscr[s + len(resident) + 1:]
        loads = [(pltpu.make_async_copy(rin[i], h, rsem.at[n]), at) for n, ((i, at), h) in enumerate(zip(resident, held))]
        if loads:
            @pl.when(t == 0)
            def _():
                for cp, _ in loads:
                    cp.start()
        for cp, at in loads:
            pl.when(t == at)(cp.wait)
        for (i, _), h in zip(resident, held):
            rin[i] = h
        i = o = 0
        for p in phases:
            pi, po = rin[i:i + len(p.ins)], rout[o:o + len(p.outs)]
            i, o = i + len(p.ins), o + len(p.outs)

            @pl.when(p.on(t))
            def _(p=p, pi=pi, po=po):
                p.body(t - p.at, pi, po, extra)

        for c in small:
            if c.at is not None:
                c.run(t, rout)

    params = dict(dimension_semantics=("arbitrary",), vmem_limit_bytes=VMEM_LIMIT)
    if comms:
        params.update(collective_id=KERNELS.index(name), has_side_effects=True)
    got = pl.pallas_call(kernel, grid=(total,), in_specs=in_specs, out_specs=out_specs, out_shape=outs, scratch_shapes=scratch,
                         input_output_aliases=alias, compiler_params=pltpu.CompilerParams(**params), name=name,
                         cost_estimate=pl.CostEstimate(flops=2 ** 34, bytes_accessed=2 ** 25, transcendentals=0))(*ins)
    return list(got)


def norm_parts(t):
    mean = row_mean(t)
    cen = t - mean
    rstd = lax.rsqrt(row_mean(cen * cen) + EPS)
    return cen * rstd, rstd


def norm_back(d, t, w):
    xhat, rstd = norm_parts(t)
    dh = d * w
    m1 = row_mean(dh)
    m2 = row_mean(dh * xhat)
    return rstd * (dh - m1 - xhat * m2), jnp.sum(d * xhat, axis=0, keepdims=True)


def alibi_slopes(n_heads):
    padded = 2 ** math.ceil(math.log2(n_heads))
    base = [2.0 ** (-8.0 * (k + 1) / padded) for k in range(padded)]
    ordered = base if padded == n_heads else base[1::2] + base[0::2]
    return jnp.array(ordered[:n_heads], dtype=F32)


def bias(i, tq, slope):
    def ahead(n, first):
        return lax.broadcasted_iota(jnp.int32, (1, n), 1).astype(F32) * slope + slope * first

    row, col = (lax.broadcasted_iota(jnp.int32, (tq, tq), a) for a in range(2))
    return ahead(tq, 0.0), ahead(i * tq, -float(i * tq)) if i else None, row >= col


def attn_fwd(q_ref, k_ref, v_ref, o_ref, l_ref, slope, scale, tq):
    slope, scale = slope * LOG2E, scale * LOG2E
    for i in range(q_ref.shape[0] // tq):
        rows, before = pl.ds(i * tq, tq), pl.ds(0, i * tq)
        q = q_ref[rows]
        near, far, keep = bias(i, tq, slope)
        sd = jnp.where(keep, dot_t(q, k_ref[rows]) * scale + near, -jnp.inf)
        m = row_max(sd)
        if i:
            sp = dot_t(q, k_ref[before]) * scale + far
            m = jnp.maximum(m, row_max(sp))
            ep = jnp.exp2(sp - m)
        ed = jnp.exp2(sd - m)
        l = row_sum(ed)
        if i:
            l = l + row_sum(ep)
        inv = 1 / l
        o = dot((ed * inv).astype(BF16), v_ref[rows])
        if i:
            o = o + dot((ep * inv).astype(BF16), v_ref[before])
        o_ref[rows] = o.astype(BF16)
        l_ref[rows] = m + jnp.log2(l)


def attn_bwd(q_ref, k_ref, v_ref, a_ref, da_ref, l_ref, dq_ref, dk_ref, dv_ref, dq_s, slope, scale, tq):
    slope2, scale2 = slope * LOG2E, scale * LOG2E
    seq = q_ref.shape[0]
    da_all = da_ref[:].astype(BF16)
    delta = row_sum(da_all.astype(F32) * a_ref[:].astype(F32))
    near, _, keep = bias(0, tq, slope2)
    for j in range(seq // tq):
        keys, rows = pl.ds(j * tq, tq), pl.ds(j * tq, seq - j * tq)
        kk, q, da = k_ref[keys], q_ref[rows], da_all[j * tq:]
        l = jnp.concatenate([l_ref[pl.ds(i * tq, tq)] + slope2 * float((i - j) * tq) for i in range(j, seq // tq)], axis=0)
        p = jnp.exp2(dot_t(q, kk) * scale2 + near - l)
        own = jnp.where(keep, p[:tq], 0)
        p = own if j == seq // tq - 1 else jnp.concatenate([own, p[tq:]], axis=0)
        ds = (p * (dot_t(da, v_ref[keys]) - delta[j * tq:])).astype(BF16)
        dv_ref[keys] = t_dot(p.astype(BF16), da).astype(BF16)
        dk_ref[keys] = (t_dot(ds, q) * scale).astype(BF16)
        part = dot(ds, kk)
        if j:
            dq_s[rows] += part
        else:
            dq_s[:] = part
    dq_ref[:] = (dq_s[:] * scale).astype(BF16)


def row_map(i):
    return i, 0


def col_map(i):
    return 0, i


def rows_of(a, n):
    return a, (n, a.shape[1]), row_map


def cols_of(a, n):
    return a, (a.shape[0], n), col_map


def heads_of(a, n):
    return a, (n,) + a.shape[1:], lambda i: (i, 0, 0)


def whole(a):
    return a, a.shape, None


def put(ref, i, part):
    @pl.when(i == 0)
    def _():
        ref[:] = jnp.zeros_like(ref)

    ref[:] += part()


def side_by_side(ref, n):
    return jnp.concatenate([ref[j] for j in range(n)], axis=1)


def local_step(x, lns, wq, wo, wu, wd, dy, comm=True):
    seq, d = x.shape
    heads, hd, ft = 12, 128, 512
    ff, nq, per, slab = wu.shape[1], 3 * d, SUB // hd, 3 * hd
    scale = 1 / math.sqrt(hd)
    tq = min(256, seq)
    tm = tq
    nm, nf = seq // tm, ff // ft
    slopes = (alibi_slopes(heads), pltpu.SMEM, None)
    b16 = lambda *shape: sds(shape, BF16)
    f32 = lambda *shape: sds(shape, F32)
    vm16 = lambda *shape: pltpu.VMEM(shape, BF16)
    vm32 = lambda *shape: pltpu.VMEM(shape, F32)
    act, wide_act, vec = b16(seq, d), b16(seq, ff), f32(1, d)
    one_vec = (vec, vec.shape, lambda i: (0, 0))
    band = lambda i, n=tm: pl.ds(pl.multiple_of(i * n, n), n)
    ts = tm // 2
    ns = seq // ts
    qs, os, us, ds = (n // WIDE for n in (0, nq, nq + d, nq + d + ff))
    nu = nq // SUB
    pack = sds((*CHIPS, 2, RB, nq), BF16)

    def S(parts, *args, **kw):
        return [Scatter([(a.reshape(*CHIPS, 2, -1, a.shape[-1]) if isinstance(a, jax.Array) else a, 0, n) for a, n in parts], *args, **kw)] if comm else []

    blocks = lambda w: w.reshape(*CHIPS, 2, -1, w.shape[-1])
    if comm:
        half = (ds - us) // 2
        gather = Gather([(wq, None, qs, WIDE), (wo, None, os, WIDE), (wu, None, us, d), (wd, None, us + half, d)], qs, ds + 2 * GLAG)
        lnsum = SmallSum(lns, d, 0)
    held = {}

    def load(u, ext):
        out = []
        for w, (first, last) in enumerate(((qs, os), (os, us), (us, ds))):
            if first <= u[0] < last:
                full = gather.refs[len(gather.ins) + w] if comm else held['weights'][w]
                r, q = Unit(RB, WIDE * (last - first), WIDE).at(u[1] - first)
                slot = rest(u[1], 2)
                out.append(pltpu.make_async_copy(full.at[:, :, :, :, r, q], ext[3].at[slot], ext[4].at[slot]))
        return out[0]

    def weight(u, ext):
        return ext[3][rest(u, 2)].reshape(d, WIDE)

    def gain(row):
        return (lnsum.refs[len(lnsum.ins)] if comm else held['lns'])[pl.ds(row, 1)]

    def start_body(i, ins, outs, ext):
        load((qs, qs), ext).start()
        load((qs, qs + 1), ext).start()

    def ln1_body(i, ins, outs, ext):
        (xr, *more), (ht,), (_, h, *_) = ins, outs, ext
        if more:
            held.update(weights=more[1:], lns=more[0])
        xhat, _ = norm_parts(xr[:].astype(F32))
        h1 = (xhat * gain(0)).astype(BF16)
        h[band(i, ts)] = h1
        ht[:] = h1.T

    def qkv_body(i, ins, outs, ext):
        (o,), (qkv, h, *_) = outs, ext
        load((qs, i), ext).wait()
        r = dot(h[:], weight(i, ext)).astype(BF16)
        for j in range(wide):
            head = r[:, j * hd:(j + 1) * hd]
            qkv[i * wide + j] = head
            o[j] = head
        pl.when(i + 2 < os)(lambda: load((qs, i + 2), ext).start())

    def attn_body(i, ins, outs, ext):
        (sl,), (o, l), (qkv, _, a, *_) = ins, outs, ext
        attn_fwd(qkv.at[i], qkv.at[heads + i], qkv.at[2 * heads + i], o, l.at[0], sl[i], scale, tq)
        a[:, pl.ds(pl.multiple_of(i * hd, hd), hd)] = o[:]

        @pl.when(i == heads // 2)
        def _():
            for u in range(os, us):
                load((os, u), ext).start()

    def out_body(i, ins, outs, ext):
        (xs,), (o, ht), (_, h, a, *_) = ins, outs, ext

        @pl.when(i == 0)
        def _():
            for u in range(os, us):
                load((os, u), ext).wait()

        ar = a[band(i, ts)]
        r = jnp.concatenate([dot(ar, weight(u, ext)) for u in range(os, us)], axis=1)
        x1 = (xs[:].astype(F32) + r).astype(BF16)
        o[:] = x1
        xhat, _ = norm_parts(x1.astype(F32))
        h2 = (xhat * gain(1)).astype(BF16)
        h[band(i, ts)] = h2
        ht[:] = h2.T

        @pl.when(i == ns - 1)
        def _():
            for u in range(us, us + 2):
                load((us, u), ext).start()

    def up_body(i, ins, outs, ext):
        (dyr,), (go, gpo, gd), h = ins, outs, ext[1]
        load((us, us + i), ext).wait()
        u = dot(h[:], weight(us + i, ext))
        cdf = 0.5 * (1.0 + lax.erf(u * math.sqrt(0.5)))
        g = (u * cdf).astype(BF16)
        go[:] = g
        gpo[:] = cdf + u * (jnp.exp(-0.5 * u * u) * math.sqrt(0.5 / math.pi))
        gd[:] = t_dot(g, dyr[:]).astype(BF16)
        pl.when(us + i + 2 < ds)(lambda: load((us, us + i + 2), ext).start())

    wide = WIDE // hd
    more = [] if comm else [(lns, pltpu.VMEM, None)] + [(blocks(w), HBM, None) for w in (wq, wo, wu)]
    pa = [Phase(ns, 1, [rows_of(x, ts), *more], [cols_of(b16(d, seq), ts)], ln1_body, 5),
          Phase(1, 0, [], [], start_body, 4),
          Phase(nq // WIDE, 3, [], [heads_of(b16(3 * heads, seq, hd), wide)], qkv_body, 5 + ns),
          Phase(heads, 2.7, [slopes], [cols_of(act, hd), heads_of(f32(heads, seq, 1), 1)], attn_body, 5 + ns + nq // WIDE),
          Phase(ns, 2, [rows_of(x, ts)], [rows_of(act, ts), cols_of(b16(d, seq), ts)], out_body, 5 + ns + nq // WIDE + heads),
          Phase(ff // WIDE, 6, [whole(dy)], [cols_of(wide_act, WIDE), cols_of(f32(seq, ff), WIDE), rows_of(b16(ff, d), WIDE)], up_body, 5 + 2 * ns + nq // WIDE + heads)]
    shared = [vm16(3 * heads, seq, hd), vm16(seq, d), vm16(seq, d), vm16(2, *CHIPS, 2, RB, WIDE), pltpu.SemaphoreType.DMA((2,))]
    t_qkv, t_attn, t_out, t_up = (p.at for p in pa[2:])
    fires = [*range(6), t_qkv - 4, t_qkv, t_qkv + 2, t_attn, t_attn + heads // 2, t_out, *range(t_up, t_up + ff // WIDE, 2)]
    fires += [fires[-1] + i for i in (2, 3, 4)]
    got = host('forward', pa, [gather, lnsum] if comm else [], shared=shared, fires=fires if comm else None)
    h1t, qkv, attn, lse, x1, h2t, g, gp, g_down, *full = got
    fq, fo, fu, fd = wq, wo, wu, wd
    if comm:
        fq, fo, fu, fd = (f.reshape(-1, f.shape[-1]) for f in full[:4])
        lns = full[4]

    def dup_body(i, ins, outs, ext):
        (dyr, w, gr, gpr, ht), (duo, gu), (acc,) = ins, outs, ext
        du = (dot_t(dyr[:], w[:]) * gpr[:]).astype(BF16)
        duo[:] = du
        gu[:] = dot(ht[:], du).astype(BF16)
        put(acc, i, lambda: dot(gr[:], w[:]))

    def y_body(i, ins, outs, ext):
        (xr,), (o,), (acc,) = ins, outs, ext
        o[:] = (xr[:].astype(F32) + acc[band(i)]).astype(BF16)

    pd = [Phase(nf, 6, [whole(dy), rows_of(fd, ft), cols_of(g, ft), cols_of(gp, ft), whole(h2t)], [cols_of(wide_act, ft), cols_of(b16(d, ff), ft)], dup_body),
          Phase(nm, 1, [rows_of(x1, tm)], [rows_of(act, tm)], y_body)]
    n_down = Unit(ff // 32, d).count
    d_up, g_up, y, *r1 = host('down', pd, S([(g_down, n_down)], [n_down - CARRY]), shared=[vm32(seq, d)])

    def dh2_body(i, ins, outs, ext):
        (du, w), acc = ins, ext[0]
        put(acc, i, lambda: dot_t(du[:], w[:]))

    def ln2b_body(i, ins, outs, ext):
        (xr, dyr, lw), (dmo, gwo), (acc, dmb, *_) = ins, outs, ext
        dx, gw = norm_back(acc[band(i)], xr[:].astype(F32), lw[pl.ds(1, 1)])
        dm = dyr[:].astype(F32) + dx
        dmo[:] = dm
        dmb[band(i)] = dm.astype(BF16)
        put(gwo, i, lambda: gw)

    def dattn_body(i, ins, outs, ext):
        (w,), (acc, dmb, *_) = ins, ext
        acc[:, pl.ds(pl.multiple_of(i * slab, slab), slab)] = dot_t(dmb[:], w[:])

    def battn_body(i, ins, outs, ext):
        (qkv, a, l, sl), (o,), (acc, _, dq) = ins, outs, ext

        @pl.loop(0, pair)
        def _(j):
            h = i * pair + j
            own, here = (pl.ds(pl.multiple_of(n * hd, hd), hd) for n in (h, j))
            attn_bwd(*(qkv.at[n, j] for n in range(3)), a.at[:, here], acc.at[:, own], l.at[j], *(o.at[n, j] for n in range(3)),
                     dq, sl[h], scale, tq)

    def gout_body(i, ins, outs, ext):
        (a,), (o,), (_, dmb, *_) = ins, outs, ext
        o[:] = t_dot(a[:], dmb[:]).astype(BF16)

    pair = 2
    triple = lambda a: (a, (3, pair, seq, hd), lambda i: (0, i, 0, 0))
    pe = [Phase(nf, 2.4, [cols_of(d_up, ft), cols_of(fu, ft)], [], dh2_body),
          Phase(nm, 2, [rows_of(x1, tm), rows_of(dy, tm), whole(lns)], [rows_of(f32(seq, d), tm), one_vec], ln2b_body),
          Phase(d // slab, 1.9, [rows_of(fo, slab)], [], dattn_body),
          Phase(heads // pair, 6, [triple(qkv.reshape(3, heads, seq, hd)), cols_of(attn, pair * hd), heads_of(lse, pair), slopes],
                [triple(b16(3, heads, seq, hd))], battn_body),
          Phase(d // slab, 2, [cols_of(attn, slab)], [rows_of(b16(d, d), slab)], gout_body)]
    d_mid, g_ln2, d_qkv, g_out, *r2 = host('back', pe, S([(g_up, n_down)], [CARRY, n_down - CARRY], carry=r1[1:]),
                                          shared=[vm32(seq, d), vm16(seq, d), vm32(seq, hd)])
    d_qkv = d_qkv.reshape(3 * heads, seq, hd)

    no = d // SUB
    scat = S([(g_out, no), (pack, nu)], [CARRY, no, -nu], carry=r2[2:], last=True)

    def tile_copy(i, ext):
        r, q = Unit(RB, nq).at(i)
        return pltpu.make_async_copy(ext[1].at[rest(i, 2)], scat[0].written(-1).at[:, :, :, :, r, q], ext[2].at[rest(i, 2)])

    def macro_body(i, ins, outs, ext):
        (ht, dq, w), acc = ins, ext[0]
        tile = side_by_side(dq, per)
        r = dot(ht[:], tile).astype(BF16)
        if comm:
            ext[1][rest(i, 2)] = r.reshape(*CHIPS, 2, RB, SUB)
            tile_copy(i, ext).start()
        else:
            outs[0][:] = r
        put(acc, i, lambda: dot_t(tile, w[:]))

    def ship_body(i, ins, outs, ext):
        tile_copy(i, ext).wait()
        scat[0].ship(no + i)

    def ln1b_body(i, ins, outs, ext):
        (xr, dm, lw), (o, gwo) = ins, outs
        dx, gw = norm_back(ext[0][band(i)], xr[:].astype(F32), lw[pl.ds(0, 1)])
        o[:] = (dm[:] + dx).astype(BF16)
        put(gwo, i, lambda: gw)

    def join_body(i, ins, outs, ext):
        (low, high, up), (down_o, up_o) = ins, outs
        wide = up.shape[1]
        up_o[:, :wide] = up[:]
        up_o[:, wide:] = scat[0].refs[len(scat[0].ins)][:]
        for u in range(n_down):
            part, v = (low, u) if u * SUB < wide else (high, u - wide // SUB)
            down_o[pl.ds(u // no * RB, RB), pl.ds(u % no * SUB, SUB)] = part[:, pl.ds(v * SUB, SUB)]

    first = [] if comm else [cols_of(b16(d, nq), SUB)]
    pf = [Phase(nu, 3.9, [whole(h1t), heads_of(d_qkv, per), cols_of(fq, SUB)], first, macro_body),
          Phase(nm, 2, [rows_of(x, tm), rows_of(d_mid, tm), whole(lns)], [rows_of(act, tm), one_vec], ln1b_body)]
    if comm:
        pieces = r1[0], *r2[:2]
        pf.append(Phase(nu, 0, [], [], ship_body, 1))
        pf.append(Phase(1, 0, [(p, pltpu.VMEM, None) for p in pieces], [(o, o.shape, lambda i: (0, 0)) for o in (f32(ff // 32, d), f32(RB, ff))],
                        join_body, nu + nm))
        scat.append(SmallSum([g_ln2], d, nu + nm, 1))
    shared = [vm32(seq, d), vm16(2, *CHIPS, 2, RB, SUB), pltpu.SemaphoreType.DMA((2,))]
    got = host('last', pf, scat, shared=shared, fires=range(no + nu + 3 * LAG) if comm else None)
    if not comm:
        g_qkv, dx, g_ln1 = got
        return y, dx, g_ln1, g_qkv, g_out, g_ln2, g_up, g_down
    dx, _, g_down, g_up, _, g_out, g_qkv, _, sums = got
    return y, dx, sums, g_qkv, g_out, g_up, g_down


def solution(mesh):
    row_spec = P('fsdp')

    def step(x_in, ln1_w, w_qkv, w_out, ln2_w, w_up, w_down, dy_out):
        rows, _, heads, hd = w_qkv.shape
        d = x_in.shape[-1]
        lns = [w.reshape(1, rows) for w in (ln1_w, ln2_w)]
        wq = w_qkv.transpose(1, 2, 0, 3).reshape(-1, rows, hd)
        y, dx, sums, g_qkv, g_out, g_up, g_down = local_step(x_in[0], lns, wq, w_out, w_up, w_down, dy_out[0])
        g_qkv = g_qkv.reshape(3, heads, rows, hd).transpose(2, 0, 1, 3)
        return y[None], dx[None], sums[1, :rows], g_qkv, g_out, sums[0, :rows], g_up, g_down

    return jax.shard_map(step, mesh=mesh, in_specs=(row_spec,) * 8, out_specs=(row_spec,) * 8, check_vma=False)
```

```python
import functools
import math

import jax
import jax.numpy as jnp
from jax import lax
from jax.experimental import pallas as pl
from jax.experimental.pallas import tpu as pltpu
from jax.sharding import PartitionSpec as P

EPS = 1e-5
LOG2E = math.log2(math.e)
SUB = 512
WIDE = 768
HALF = SUB // 2
LAG = 2
GLAG = 1
CARRY = 2 * LAG
LEAD = 3
FRONT = 0.92
SIDE = -4
RB = 48
F32, BF16 = jnp.float32, jnp.bfloat16
VMEM_LIMIT = 67_000_000
MESH = pl.DeviceIdType.MESH
HBM = pltpu.MemorySpace.HBM
CHIPS = (4, 2, 2)


def sds(shape, dtype):
    return jax.ShapeDtypeStruct(shape, dtype)


def dot(a, b, ca=1, cb=0):
    return lax.dot_general(a, b, (((ca,), (cb,)), ((), ())), preferred_element_type=F32)


def dot_t(a, b):
    return dot(a, b, 1, 1)


def t_dot(a, b):
    return dot(a, b, 0, 0)


def over_rows(f):
    return functools.partial(f, axis=-1, keepdims=True)


row_sum, row_max, row_mean = map(over_rows, (jnp.sum, jnp.max, jnp.mean))


def clip(t, n):
    return jnp.minimum(jnp.maximum(t, 0), n - 1)


class Phase:
    def __init__(self, n, cost, ins, outs, body, at=None):
        self.n, self.cost, self.ins, self.outs, self.body, self.at = n, cost, ins, outs, body, at

    def on(self, t):
        return (t >= self.at) & (t < self.at + self.n)

    def index(self, f):
        return lambda t: f(clip(t - self.at, self.n))


def quot(a, b):
    return a // b if isinstance(a, int) else lax.div(a, b)


def rest(a, b):
    return a % b if isinstance(a, int) else lax.rem(a, b)


HERE = {}


def locate():
    me = lax.axis_index('fsdp')
    left, place = me, []
    for n in (2, *reversed(CHIPS)):
        place.append(rest(left, n))
        left = quot(left, n)
    c, x, y, z = place
    n, step, ways = CHIPS[0], 8, (1, 2, 3)
    cp, xp, yp = (me + s - 2 * s * b for s, b in zip((1, 2, 4), place))
    HERE.update(coords=(me, z, y, x, c), peers=([rest(me + step * d, step * n) for d in ways], yp, xp, cp), zs=[rest(z + d, n) for d in ways])


def coords():
    return HERE['coords']


def peers():
    return HERE['peers']


def remote(src, dst, ssem, rsem, dev):
    return pltpu.make_async_remote_copy(src_ref=src, dst_ref=dst, send_sem=ssem, recv_sem=rsem, device_id=(dev,), device_id_type=MESH)


class Unit:
    def __init__(self, rows, cols, width=SUB):
        self.width, self.nc, self.nr = width, cols // width, rows // RB
        self.count = self.nc * self.nr

    def at(self, u, half=None):
        lanes, col = self.width, rest(u, self.nc) * self.width
        if half is not None:
            lanes //= 2
            col = col + half * lanes
        rows = slice(None) if self.nr == 1 else pl.ds(pl.multiple_of(quot(u, self.nc) * RB, 16), RB)
        return rows, pl.ds(pl.multiple_of(col, 128), lanes)


class Gather:
    def __init__(self, weights, k0, k1):
        self.k0, self.k1 = k0, k1
        self.k, self.tail = k1 - k0 + 1, 0
        self.z0 = k0 + LEAD if k0 else 0
        self.z1 = k1 + LEAD
        self.w, self.ins, self.outs, self.alias = [], [], [], []
        for shard, full, first, wide in weights:
            heads, rows = shard.shape[:2] if shard.ndim == 3 else (0, shard.shape[0])
            shape = (rows, shard.size // rows)
            unit = Unit(*shape, wide)
            self.w.append((SIDE if heads else len(self.ins), unit, first, first + unit.count, full is None))
            self.ins.append((shard, pl.BlockSpec(memory_space=pltpu.VMEM)))
            if heads:
                self.heads, side = (len(self.ins) - 1, heads), pltpu.VMEM(shape, BF16)
            if full is not None:
                self.alias.append((len(self.ins), len(self.outs)))
                self.ins.append((full, pl.BlockSpec(memory_space=HBM)))
            self.outs.append((sds(CHIPS + (2,) + shape, BF16), pl.BlockSpec(memory_space=HBM)))
        self.base = max(k0 - 2 * GLAG, 0)
        n = self.z1 - self.base
        self.scratch = [side, pltpu.SemaphoreType.DMA((n, 8)), pltpu.SemaphoreType.DMA((n, 8)), pltpu.SemaphoreType.DMA((len(weights),))]

    def copies(self, stage, w, u, refs):
        i, unit, first, _, _ = self.w[w]
        shard, full = refs[i], refs[len(self.ins) + w]
        sems = lambda i: (refs[-3].at[u - self.base, i], refs[-2].at[u - self.base, i])
        me, z, y, x, c = coords()
        zs, yp, xp, cp = peers()
        r, q = unit.at(u - first)
        if stage == 0:
            return [remote(shard.at[r, q], full.at[z, y, x, c, r, q], *sems(d), zs[d]) for d in range(3)]
        if stage == 3:
            v = full.at[:, :, :, c, r, q]
            return [remote(v, v, *sems(7), cp)]
        out = []
        for half in range(2):
            r, q = unit.at(u - first, half)
            j = 2 * stage + 1 + half
            if stage == 1:
                v = full.at[:, y, x, c, r, q]
            else:
                v = full.at[:, y, :, c, r, q] if half else full.at[:, :, x, c, r, q]
            out.append(remote(v, v, *sems(j), xp if half == stage % 2 else yp))
        return out

    def each(self, lo, hi, u, fn):
        for w, (_, _, first, last, _) in enumerate(self.w):
            a, b = max(lo, first), min(hi, last)
            if a < b:
                if u is None:
                    pl.loop(a, b)(functools.partial(fn, w))
                else:
                    pl.when((u >= a) & (u < b))(functools.partial(fn, w, u))

    def go(self, stage, w, u, refs):
        for cp in self.copies(stage, w, u, refs):
            cp.start()

    def arrive(self, stage, w, u, refs):
        for cp in self.copies(stage, w, u, refs):
            cp.wait_recv()

    def left(self, stage, w, u, refs):
        for cp in self.copies(stage, w, u, refs):
            cp.wait_send()

    def step(self, k, fire, begin, refs):
        me, z, y, x, c = coords()
        k0, k1, k = self.k0, self.k1, k + self.k0
        span = [(self.z0, self.z1)] + [(max(k0 - i * GLAG, 0), k1 - i * GLAG) for i in range(3)]

        @pl.when(fire & (k == k0))
        def _():
            i, heads = self.heads
            for h in range(heads):
                refs[SIDE][:, h * 128:(h + 1) * 128] = refs[i][h]
            own = [pltpu.make_async_copy(refs[i], refs[len(self.ins) + w].at[z, y, x, c], refs[-1].at[w])
                   for w, (i, _, _, _, fresh) in enumerate(self.w) if fresh]
            for cp in own:
                cp.start()
            if k0 == 0:
                self.each(0, LEAD, None, lambda w, u: self.go(0, w, u, refs))
            for cp in own:
                cp.wait()

        @pl.when(fire & (k < k1))
        def _():
            self.each(*span[0], k + LEAD, lambda w, u: self.go(0, w, u, refs))
            for stage in (1, 2, 3):
                u = k + GLAG * (1 - stage)
                lo, hi = span[stage - 1]
                self.each(lo, hi, u, lambda w, u: self.arrive(stage - 1, w, u, refs))
                self.each(*span[stage], u, lambda w, u: self.go(stage, w, u, refs))
            self.each(*span[3], k - 3 * GLAG, lambda w, u: self.arrive(3, w, u, refs))

        @pl.when(fire & (k == k1))
        def _():
            for stage in range(4):
                lo, hi = span[stage]
                self.each(max(lo, k1 - stage * GLAG), hi, None, lambda w, u: self.arrive(stage, w, u, refs))
                self.each(lo, hi, None, lambda w, u: self.left(stage, w, u, refs))


class Scatter:
    def __init__(self, grads, layout, carry=None, last=False):
        self.last, self.carried = last, carry is not None
        self.parts, self.ins, n = [], [], 0
        self.late = []
        for g, u0, m in grads:
            self.parts.append((n, n + m, u0, Unit(*g.shape[-2:])))
            if isinstance(g, jax.ShapeDtypeStruct):
                self.late.append(g)
            else:
                self.ins.append((g, pl.BlockSpec(memory_space=HBM)))
            n += m
        self.known = sum(m for g, _, m in grads if not isinstance(g, jax.ShapeDtypeStruct))
        self.n = n
        self.first = 0 if self.carried else CARRY
        self.end = n + CARRY
        self.done = self.end if last else n
        self.k = n + (3 * LAG if last else 1)
        self.tail = 3 * LAG - 1 if last else 0
        self.two_shape, self.three_shape = (2, 4, 2, RB, HALF), (4, RB, SUB)
        if self.carried:
            self.ins += [(a, pl.BlockSpec(memory_space=pltpu.VMEM)) for a in carry]
        self.scratch = [
            pltpu.VMEM((n, *CHIPS, RB, SUB), BF16),
            pltpu.VMEM((2, *CHIPS, RB, SUB), BF16),
            pltpu.VMEM((self.end, *self.two_shape), BF16),
            pltpu.VMEM((self.end, *self.three_shape), BF16),
            pltpu.VMEM((self.end, 3, RB, SUB), BF16),
            pltpu.SemaphoreType.DMA((self.end, 8)), pltpu.SemaphoreType.DMA((self.end, 8)), pltpu.SemaphoreType.DMA((2,))]
        self.layout = layout
        outs = [sds((RB, n * SUB) if n > 0 else (-n * SUB // 128, RB, 128), F32) for n in layout]
        if not last:
            outs += [sds((LAG, *shape), BF16) for shape in (self.two_shape, self.three_shape)]
        self.outs = [(o, pl.BlockSpec(memory_space=pltpu.VMEM)) for o in outs]
        self.outs += [(g, pl.BlockSpec(memory_space=HBM)) for g in self.late]
        self.alias = []

    def source(self, j, refs, fn):
        for i, (a, b, u0, unit) in enumerate(self.parts):
            ref = self.written(i - len(self.parts)) if self.late and a >= self.known else refs[i]
            u = j - CARRY
            if len(self.parts) == 1:
                fn(ref, *unit.at(u0 + u))
            else:
                pl.when((u >= a) & (u < b))(functools.partial(lambda ref, unit, u: fn(ref, *unit.at(u)), ref, unit, u0 + u - a))

    def written(self, i):
        return self.refs[len(self.ins) + len(self.outs) + i]

    def ship(self, u):
        self.swap(CARRY + u, self.refs, lambda cp: cp.start())

    def bufs(self, refs):
        return refs[len(self.ins) + len(self.outs):]

    def local(self, j, refs, act):
        me, z, y, x, c = coords()
        own, ls = self.bufs(refs)[1], self.bufs(refs)[-1]
        slot = rest(j, 2)
        self.source(j, refs, lambda g, r, q: act(pltpu.make_async_copy(g.at[:, :, :, c, r, q], own.at[slot], ls.at[slot])))

    def swap(self, j, refs, act):
        me, z, y, x, c = coords()
        got, ss, rs = self.bufs(refs)[0], *self.bufs(refs)[-3:-1]
        cp = peers()[-1]
        self.source(j, refs, lambda g, r, q: act(remote(g.at[:, :, :, 1 - c, r, q], got.at[j - CARRY], ss.at[j, 0], rs.at[j, 0], cp)))

    def copies(self, stage, j, refs):
        got, own, two, three, four, ss, rs, ls = self.bufs(refs)
        me, z, y, x, c = coords()
        zs, yp, xp, cp = peers()
        a, b = pl.ds(0, HALF), pl.ds(HALF, HALF)
        if stage == 1:
            pairs = [(got.at[j - CARRY, :, 1 - y, :, :, a], two.at[j, 0], yp), (got.at[j - CARRY, :, :, 1 - x, :, b], two.at[j, 1], xp)]
        elif stage == 2:
            pairs = [(two.at[j, 0, :, 1 - x], three.at[j, :, :, a], xp), (two.at[j, 1, :, 1 - y], three.at[j, :, :, b], yp)]
        else:
            pairs = [(three.at[j, HERE['zs'][d]], four.at[j, d], zs[d]) for d in range(3)]
        return [remote(src, dst, ss.at[j, 2 * stage + i - 1], rs.at[j, 2 * stage + i - 1], dev) for i, (src, dst, dev) in enumerate(pairs)]

    def add(self, stage, j, refs):
        got, own, two, three, four, ss, rs, ls = self.bufs(refs)
        me, z, y, x, c = coords()
        a, b = pl.ds(0, HALF), pl.ds(HALF, HALF)
        slot = rest(j, 2)
        if stage == 1:
            @pl.loop(0, 4)
            def _(zz):
                for yy in range(2):
                    for xx in range(2):
                        got[j - CARRY, zz, yy, xx] += own[slot, zz, yy, xx]
        elif stage == 2:
            @pl.loop(0, 4)
            def _(zz):
                for i in range(2):
                    two[j, 0, zz, i] += got[j - CARRY, zz, y, i, :, a]
                    two[j, 1, zz, i] += got[j - CARRY, zz, i, x, :, b]
        elif stage == 3:
            for zz in range(4):
                three[j, zz, :, a] += two[j, 0, zz, x]
                three[j, zz, :, b] += two[j, 1, zz, y]
        else:
            total = three[j, z].astype(F32)
            for d in range(3):
                total += four[j, d].astype(F32)
            a = self.first
            for i, n in enumerate(self.layout):
                b, out = a + abs(n), refs[len(self.ins) + i]

                @pl.when((j >= a) & (j < b))
                def _(out=out, a=a, n=n):
                    if n > 0:
                        out[:, pl.ds(pl.multiple_of((j - a) * SUB, SUB), SUB)] = total
                    else:
                        for h in range(SUB // 128):
                            out[(j - a) * (SUB // 128) + h] = total[:, h * 128:(h + 1) * 128]

                a = b

    def step(self, k, fire, begin, refs):
        n, end, last = self.n, self.end, self.last
        got, own, two, three, four, ss, rs, ls = self.bufs(refs)
        start = lambda cp: cp.start()

        def go(stage, j):
            for cp in self.copies(stage, j, refs):
                cp.start()

        def take(stage, j):
            for cp in self.copies(stage - 1, j, refs):
                cp.wait_recv()
            self.add(stage, j, refs)

        @pl.when(begin)
        def _():
            if self.known:
                pl.loop(CARRY, CARRY + self.known)(lambda j: self.swap(j, refs, start))
                self.local(CARRY, refs, start)
            if self.carried:
                for i in range(LAG):
                    two[LAG + i] = refs[len(self.ins) - 2][i]
                    three[i] = refs[len(self.ins) - 1][i]
                    go(2, LAG + i)
                    go(3, i)

        @pl.when(fire & (k < n))
        def _():
            j = k + CARRY
            if not self.known:
                pl.when(j == CARRY)(lambda: self.local(j, refs, start))
            pl.when(j + 1 < end)(lambda: self.local(j + 1, refs, start))
            self.swap(j, refs, lambda cp: cp.wait_recv())
            self.local(j, refs, lambda cp: cp.wait())
            self.add(1, j, refs)
            go(1, j)

        lows = [CARRY, LAG, 0] if self.carried else [CARRY] * 3
        for stage, low in zip((2, 3, 4), lows):
            j = k + (3 - stage) * LAG

            @pl.when(fire & (j >= low) & (j < end) & ((k < n) | last))
            def _(stage=stage, j=j):
                take(stage, j)
                if stage < 4:
                    go(stage, j)

        @pl.when(fire & (k == self.k - 1))
        def _():
            for stage, low in zip((2, 3, 4), lows):
                a = n + (3 - stage) * LAG
                if not last:
                    pl.loop(max(a, low), a + LAG)(functools.partial(take, stage))

                @pl.loop(CARRY if stage == 2 else low, end if last else a + LAG)
                def _(j):
                    for cp in self.copies(stage - 1, j, refs):
                        cp.wait_send()

            @pl.loop(CARRY, end)
            def _(j):
                self.swap(j, refs, lambda cp: cp.wait_send())

            if not last:
                for i in range(LAG):
                    refs[len(self.ins) + len(self.layout)][i] = two[n + LAG + i]
                    refs[len(self.ins) + len(self.layout) + 1][i] = three[n + i]


class SmallSum:
    def __init__(self, rows, d, t0, at=None):
        self.at, self.t0, self.k, self.tail = at, t0, 1, 0
        self.ins = [(row, pl.BlockSpec(memory_space=pltpu.VMEM)) for row in rows]
        self.outs = [(sds((8, d if at is None else 128), F32), pl.BlockSpec(memory_space=pltpu.VMEM))]
        self.alias = []
        self.scratch = [pltpu.VMEM((4, 8, d), F32), pltpu.VMEM((6, 8, d), F32), pltpu.SemaphoreType.DMA((6,)), pltpu.SemaphoreType.DMA((6,))]

    def run(self, t, outs):
        *rows, out, acc, got, ss, rs = self.refs
        if self.at is not None:
            rows.append(outs[self.at])
        me = coords()[0]
        zs, yp, xp, cp = peers()
        near = (cp, xp, yp, *zs)
        n = len(near) - len(zs)
        copies = [remote(acc.at[min(i, n)], got.at[i], ss.at[i], rs.at[i], dev) for i, dev in enumerate(near)]

        for i in range(n + 2):
            @pl.when(t == self.t0 + i)
            def _(i=i):
                if not i:
                    acc[i] = jnp.zeros_like(acc[i])
                    for j, row in enumerate(rows):
                        acc[i, pl.ds(j, 1), pl.ds(0, row.shape[1])] = row[:]
                    if self.at is None:
                        acc[i] = pltpu.roll(acc[i], RB * me, 1)
                elif i <= n:
                    copies[i - 1].wait_recv()
                    acc[i] = acc[i - 1] + got[i - 1]
                else:
                    total = acc[n]
                    for j in range(n, len(near)):
                        copies[j].wait_recv()
                        total += got[j]
                    out[:] = total if self.at is None else pltpu.roll(total, total.shape[1] - RB * me, 1)[:, :128]
                    for copy in copies:
                        copy.wait_send()
                for copy in copies[i:i + 1] if i < n else copies[n:] if i == n else ():
                    copy.start()


KERNELS = ['forward', 'down', 'back', 'last']


def host(name, phases, comms=(), shared=(), fires=None):
    k_all = max([c.k for c in comms], default=1)
    at = 0
    for p in phases:
        if p.at is None:
            p.at = at
        at = max(at, p.at + p.n)
    small = [c for c in comms if isinstance(c, SmallSum)]
    tail = max([c.tail for c in comms], default=0)
    if fires is None:
        spread, clock, fires = k_all - 1 - tail, [0.0], [0]
        for t in range(at):
            clock.append(clock[-1] + sum(p.cost for p in phases if p.at <= t < p.at + p.n))
        for k in range(1, k_all):
            t = at if k >= spread else min(t for t in range(at + 1) if clock[t] * spread >= FRONT * clock[at] * k)
            fires.append(max(t, fires[-1] + 1))
    total = max([at, fires[-1] + 1] + [c.t0 + 5 for c in small])
    ins, in_specs, outs, out_specs, scratch, alias, resident = [], [], [], [], [], {}, []
    for p in phases:
        for arr, block, index in p.ins:
            if isinstance(block, pltpu.MemorySpace):
                in_specs.append(pl.BlockSpec(memory_space=block))
            elif index is None:
                resident.append((len(ins), p.at))
                in_specs.append(pl.BlockSpec(memory_space=HBM))
            else:
                in_specs.append(pl.BlockSpec(block, p.index(index)))
            ins.append(arr)
        for shape, block, index in p.outs:
            outs.append(shape)
            out_specs.append(pl.BlockSpec(block, p.index(index)))
    for c in comms:
        alias.update({len(ins) + i: len(outs) + o for i, o in c.alias})
        for arr, spec in c.ins:
            ins.append(arr)
            in_specs.append(spec)
        for shape, spec in c.outs:
            outs.append(shape)
            out_specs.append(spec)
        scratch += c.scratch
    scratch += [pltpu.VMEM(ins[i].shape, ins[i].dtype) for i, _ in resident] + [pltpu.SemaphoreType.DMA((max(len(resident), 1),))]
    scratch += list(shared)

    def kernel(*refs):
        refs = list(refs)
        rin, rout, rscr = refs[:len(ins)], refs[len(ins):len(ins) + len(outs)], refs[len(ins) + len(outs):]
        t = pl.program_id(0)
        if comms:
            locate()

            @pl.when(t == 0)
            def _():
                zs, yp, xp, cp = peers()
                near = (*zs, yp, xp, cp)
                bar = pltpu.get_barrier_semaphore()
                for dev in near:
                    pl.semaphore_signal(bar, inc=1, device_id=(dev,), device_id_type=MESH)
                pl.semaphore_wait(bar, len(near))
        i, o, s = sum(len(p.ins) for p in phases), sum(len(p.outs) for p in phases), 0
        k = sum([(t >= f).astype(jnp.int32) for f in fires[1:]], 0 * t)
        fire = functools.reduce(jnp.logical_or, [t == f for f in fires])
        for c in comms:
            ni, no, ns = len(c.ins), len(c.outs), len(c.scratch)
            crefs = rin[i:i + ni] + rout[o:o + no] + rscr[s:s + ns]
            c.refs = crefs
            if c not in small:
                c.step(k, fire, t == 0, crefs)
            elif c.at is None:
                c.run(t, rout)
            i, o, s = i + ni, o + no, s + ns
        held, rsem, extra = rscr[s:s + len(resident)], rscr[s + len(resident)], rscr[s + len(resident) + 1:]
        loads = [(pltpu.make_async_copy(rin[i], h, rsem.at[n]), at) for n, ((i, at), h) in enumerate(zip(resident, held))]
        if loads:
            @pl.when(t == 0)
            def _():
                for cp, _ in loads:
                    cp.start()
        for cp, at in loads:
            pl.when(t == at)(cp.wait)
        for (i, _), h in zip(resident, held):
            rin[i] = h
        i = o = 0
        for p in phases:
            pi, po = rin[i:i + len(p.ins)], rout[o:o + len(p.outs)]
            i, o = i + len(p.ins), o + len(p.outs)

            @pl.when(p.on(t))
            def _(p=p, pi=pi, po=po):
                p.body(t - p.at, pi, po, extra)

        for c in small:
            if c.at is not None:
                c.run(t, rout)

    params = dict(dimension_semantics=("arbitrary",), vmem_limit_bytes=VMEM_LIMIT)
    if comms:
        params.update(collective_id=KERNELS.index(name), has_side_effects=True)
    got = pl.pallas_call(kernel, grid=(total,), in_specs=in_specs, out_specs=out_specs, out_shape=outs, scratch_shapes=scratch,
                         input_output_aliases=alias, compiler_params=pltpu.CompilerParams(**params), name=name,
                         cost_estimate=pl.CostEstimate(flops=2 ** 34, bytes_accessed=2 ** 25, transcendentals=0))(*ins)
    return list(got)


def norm_parts(t):
    mean = row_mean(t)
    cen = t - mean
    rstd = lax.rsqrt(row_mean(cen * cen) + EPS)
    return cen * rstd, rstd


def norm_back(d, t, w):
    xhat, rstd = norm_parts(t)
    dh = d * w
    m1 = row_mean(dh)
    m2 = row_mean(dh * xhat)
    return rstd * (dh - m1 - xhat * m2), jnp.sum(d * xhat, axis=0, keepdims=True)


def alibi_slopes(n_heads):
    padded = 2 ** math.ceil(math.log2(n_heads))
    base = [2.0 ** (-8.0 * (k + 1) / padded) for k in range(padded)]
    ordered = base if padded == n_heads else base[1::2] + base[0::2]
    return jnp.array(ordered[:n_heads], dtype=F32)


def bias(i, tq, slope):
    def ahead(n, first):
        return lax.broadcasted_iota(jnp.int32, (1, n), 1).astype(F32) * slope + slope * first

    row, col = (lax.broadcasted_iota(jnp.int32, (tq, tq), a) for a in range(2))
    return ahead(tq, 0.0), ahead(i * tq, -float(i * tq)) if i else None, row >= col


def attn_fwd(q_ref, k_ref, v_ref, o_ref, l_ref, slope, scale, tq):
    slope, scale = slope * LOG2E, scale * LOG2E
    for i in range(q_ref.shape[0] // tq):
        rows, before = pl.ds(i * tq, tq), pl.ds(0, i * tq)
        q = q_ref[rows]
        near, far, keep = bias(i, tq, slope)
        sd = jnp.where(keep, dot_t(q, k_ref[rows]) * scale + near, -jnp.inf)
        m = row_max(sd)
        if i:
            sp = dot_t(q, k_ref[before]) * scale + far
            m = jnp.maximum(m, row_max(sp))
            ep = jnp.exp2(sp - m)
        ed = jnp.exp2(sd - m)
        l = row_sum(ed)
        if i:
            l = l + row_sum(ep)
        inv = 1 / l
        o = dot((ed * inv).astype(BF16), v_ref[rows])
        if i:
            o = o + dot((ep * inv).astype(BF16), v_ref[before])
        o_ref[rows] = o.astype(BF16)
        l_ref[rows] = m + jnp.log2(l)


def attn_bwd(q_ref, k_ref, v_ref, a_ref, da_ref, l_ref, dq_ref, dk_ref, dv_ref, dq_s, slope, scale, tq):
    slope2, scale2 = slope * LOG2E, scale * LOG2E
    seq = q_ref.shape[0]
    da_all = da_ref[:].astype(BF16)
    delta = row_sum(da_all.astype(F32) * a_ref[:].astype(F32))
    near, _, keep = bias(0, tq, slope2)
    for j in range(seq // tq):
        keys, rows = pl.ds(j * tq, tq), pl.ds(j * tq, seq - j * tq)
        kk, q, da = k_ref[keys], q_ref[rows], da_all[j * tq:]
        l = jnp.concatenate([l_ref[pl.ds(i * tq, tq)] + slope2 * float((i - j) * tq) for i in range(j, seq // tq)], axis=0)
        p = jnp.exp2(dot_t(q, kk) * scale2 + near - l)
        own = jnp.where(keep, p[:tq], 0)
        p = own if j == seq // tq - 1 else jnp.concatenate([own, p[tq:]], axis=0)
        ds = (p * (dot_t(da, v_ref[keys]) - delta[j * tq:])).astype(BF16)
        dv_ref[keys] = t_dot(p.astype(BF16), da).astype(BF16)
        dk_ref[keys] = (t_dot(ds, q) * scale).astype(BF16)
        part = dot(ds, kk)
        if j:
            dq_s[rows] += part
        else:
            dq_s[:] = part
    dq_ref[:] = (dq_s[:] * scale).astype(BF16)


def row_map(i):
    return i, 0


def col_map(i):
    return 0, i


def rows_of(a, n):
    return a, (n, a.shape[1]), row_map


def cols_of(a, n):
    return a, (a.shape[0], n), col_map


def heads_of(a, n):
    return a, (n,) + a.shape[1:], lambda i: (i, 0, 0)


def whole(a):
    return a, a.shape, None


def put(ref, i, part):
    @pl.when(i == 0)
    def _():
        ref[:] = jnp.zeros_like(ref)

    ref[:] += part()


def side_by_side(ref, n):
    return jnp.concatenate([ref[j] for j in range(n)], axis=1)


def local_step(x, lns, wq, wo, wu, wd, dy, comm=True):
    seq, d = x.shape
    heads, hd, ft = 12, 128, 512
    ff, nq, per, slab = wu.shape[1], 3 * d, SUB // hd, 3 * hd
    scale = 1 / math.sqrt(hd)
    tq = min(256, seq)
    tm = tq
    nm, nf = seq // tm, ff // ft
    slopes = (alibi_slopes(heads), pltpu.SMEM, None)
    b16 = lambda *shape: sds(shape, BF16)
    f32 = lambda *shape: sds(shape, F32)
    vm16 = lambda *shape: pltpu.VMEM(shape, BF16)
    vm32 = lambda *shape: pltpu.VMEM(shape, F32)
    act, wide_act, vec = b16(seq, d), b16(seq, ff), f32(1, d)
    one_vec = (vec, vec.shape, lambda i: (0, 0))
    band = lambda i, n=tm: pl.ds(pl.multiple_of(i * n, n), n)
    ts = tm // 2
    ns = seq // ts
    qs, os, us, ds = (n // WIDE for n in (0, nq, nq + d, nq + d + ff))
    nu = nq // SUB
    pack = sds((*CHIPS, 2, RB, nq), BF16)

    def S(parts, *args, **kw):
        return [Scatter([(a.reshape(*CHIPS, 2, -1, a.shape[-1]) if isinstance(a, jax.Array) else a, 0, n) for a, n in parts], *args, **kw)] if comm else []

    blocks = lambda w: w.reshape(*CHIPS, 2, -1, w.shape[-1])
    if comm:
        half = (ds - us) // 2
        gather = Gather([(wq, None, qs, WIDE), (wo, None, os, WIDE), (wu, None, us, d), (wd, None, us + half, d)], qs, ds + 2 * GLAG)
        lnsum = SmallSum(lns, d, 0)
    held = {}

    def load(u, ext):
        out = []
        for w, (first, last) in enumerate(((qs, os), (os, us), (us, ds))):
            if first <= u[0] < last:
                full = gather.refs[len(gather.ins) + w] if comm else held['weights'][w]
                r, q = Unit(RB, WIDE * (last - first), WIDE).at(u[1] - first)
                slot = rest(u[1], 2)
                out.append(pltpu.make_async_copy(full.at[:, :, :, :, r, q], ext[3].at[slot], ext[4].at[slot]))
        return out[0]

    def weight(u, ext):
        return ext[3][rest(u, 2)].reshape(d, WIDE)

    def gain(row):
        return (lnsum.refs[len(lnsum.ins)] if comm else held['lns'])[pl.ds(row, 1)]

    def start_body(i, ins, outs, ext):
        load((qs, qs), ext).start()
        load((qs, qs + 1), ext).start()

    def ln1_body(i, ins, outs, ext):
        (xr, *more), (ht,), (_, h, *_) = ins, outs, ext
        if more:
            held.update(weights=more[1:], lns=more[0])
        xhat, _ = norm_parts(xr[:].astype(F32))
        h1 = (xhat * gain(0)).astype(BF16)
        h[band(i, ts)] = h1
        ht[:] = h1.T

    def qkv_body(i, ins, outs, ext):
        (o,), (qkv, h, *_) = outs, ext
        load((qs, i), ext).wait()
        r = dot(h[:], weight(i, ext)).astype(BF16)
        for j in range(wide):
            head = r[:, j * hd:(j + 1) * hd]
            qkv[i * wide + j] = head
            o[j] = head
        pl.when(i + 2 < os)(lambda: load((qs, i + 2), ext).start())

    def attn_body(i, ins, outs, ext):
        (sl,), (o, l), (qkv, _, a, *_) = ins, outs, ext
        attn_fwd(qkv.at[i], qkv.at[heads + i], qkv.at[2 * heads + i], o, l.at[0], sl[i], scale, tq)
        a[:, pl.ds(pl.multiple_of(i * hd, hd), hd)] = o[:]

        @pl.when(i == heads // 2)
        def _():
            for u in range(os, us):
                load((os, u), ext).start()

    def out_body(i, ins, outs, ext):
        (xs,), (o, ht), (_, h, a, *_) = ins, outs, ext

        @pl.when(i == 0)
        def _():
            for u in range(os, us):
                load((os, u), ext).wait()

        ar = a[band(i, ts)]
        r = jnp.concatenate([dot(ar, weight(u, ext)) for u in range(os, us)], axis=1)
        x1 = (xs[:].astype(F32) + r).astype(BF16)
        o[:] = x1
        xhat, _ = norm_parts(x1.astype(F32))
        h2 = (xhat * gain(1)).astype(BF16)
        h[band(i, ts)] = h2
        ht[:] = h2.T

        @pl.when(i == ns - 1)
        def _():
            for u in range(us, us + 2):
                load((us, u), ext).start()

    def up_body(i, ins, outs, ext):
        (dyr,), (go, gpo, gd), h = ins, outs, ext[1]
        load((us, us + i), ext).wait()
        u = dot(h[:], weight(us + i, ext))
        cdf = 0.5 * (1.0 + lax.erf(u * math.sqrt(0.5)))
        g = (u * cdf).astype(BF16)
        go[:] = g
        gpo[:] = cdf + u * (jnp.exp(-0.5 * u * u) * math.sqrt(0.5 / math.pi))
        gd[:] = t_dot(g, dyr[:]).astype(BF16)
        pl.when(us + i + 2 < ds)(lambda: load((us, us + i + 2), ext).start())

    wide = WIDE // hd
    more = [] if comm else [(lns, pltpu.VMEM, None)] + [(blocks(w), HBM, None) for w in (wq, wo, wu)]
    pa = [Phase(ns, 1, [rows_of(x, ts), *more], [cols_of(b16(d, seq), ts)], ln1_body, 5),
          Phase(1, 0, [], [], start_body, 4),
          Phase(nq // WIDE, 3, [], [heads_of(b16(3 * heads, seq, hd), wide)], qkv_body, 5 + ns),
          Phase(heads, 2.7, [slopes], [cols_of(act, hd), heads_of(f32(heads, seq, 1), 1)], attn_body, 5 + ns + nq // WIDE),
          Phase(ns, 2, [rows_of(x, ts)], [rows_of(act, ts), cols_of(b16(d, seq), ts)], out_body, 5 + ns + nq // WIDE + heads),
          Phase(ff // WIDE, 6, [whole(dy)], [cols_of(wide_act, WIDE), cols_of(f32(seq, ff), WIDE), rows_of(b16(ff, d), WIDE)], up_body, 5 + 2 * ns + nq // WIDE + heads)]
    shared = [vm16(3 * heads, seq, hd), vm16(seq, d), vm16(seq, d), vm16(2, *CHIPS, 2, RB, WIDE), pltpu.SemaphoreType.DMA((2,))]
    t_qkv, t_attn, t_out, t_up = (p.at for p in pa[2:])
    fires = [*range(6), t_qkv - 4, t_qkv, t_qkv + 2, t_attn, t_attn + heads // 2, t_out, *range(t_up, t_up + ff // WIDE, 2)]
    fires += [fires[-1] + i for i in (2, 3, 4)]
    got = host('forward', pa, [gather, lnsum] if comm else [], shared=shared, fires=fires if comm else None)
    h1t, qkv, attn, lse, x1, h2t, g, gp, g_down, *full = got
    fq, fo, fu, fd = wq, wo, wu, wd
    if comm:
        fq, fo, fu, fd = (f.reshape(-1, f.shape[-1]) for f in full[:4])
        lns = full[4]

    def dup_body(i, ins, outs, ext):
        (dyr, w, gr, gpr, ht), (duo, gu), (acc,) = ins, outs, ext
        du = (dot_t(dyr[:], w[:]) * gpr[:]).astype(BF16)
        duo[:] = du
        gu[:] = dot(ht[:], du).astype(BF16)
        put(acc, i, lambda: dot(gr[:], w[:]))

    def y_body(i, ins, outs, ext):
        (xr,), (o,), (acc,) = ins, outs, ext
        o[:] = (xr[:].astype(F32) + acc[band(i)]).astype(BF16)

    pd = [Phase(nf, 6, [whole(dy), rows_of(fd, ft), cols_of(g, ft), cols_of(gp, ft), whole(h2t)], [cols_of(wide_act, ft), cols_of(b16(d, ff), ft)], dup_body),
          Phase(nm, 1, [rows_of(x1, tm)], [rows_of(act, tm)], y_body)]
    n_down = Unit(ff // 32, d).count
    d_up, g_up, y, *r1 = host('down', pd, S([(g_down, n_down)], [n_down - CARRY]), shared=[vm32(seq, d)])

    def dh2_body(i, ins, outs, ext):
        (du, w), acc = ins, ext[0]
        put(acc, i, lambda: dot_t(du[:], w[:]))

    def ln2b_body(i, ins, outs, ext):
        (xr, dyr, lw), (dmo, gwo), (acc, dmb, *_) = ins, outs, ext
        dx, gw = norm_back(acc[band(i)], xr[:].astype(F32), lw[pl.ds(1, 1)])
        dm = dyr[:].astype(F32) + dx
        dmo[:] = dm
        dmb[band(i)] = dm.astype(BF16)
        put(gwo, i, lambda: gw)

    def dattn_body(i, ins, outs, ext):
        (w,), (acc, dmb, *_) = ins, ext
        acc[:, pl.ds(pl.multiple_of(i * slab, slab), slab)] = dot_t(dmb[:], w[:])

    def battn_body(i, ins, outs, ext):
        (qkv, a, l, sl), (o,), (acc, _, dq) = ins, outs, ext

        @pl.loop(0, pair)
        def _(j):
            h = i * pair + j
            own, here = (pl.ds(pl.multiple_of(n * hd, hd), hd) for n in (h, j))
            attn_bwd(*(qkv.at[n, j] for n in range(3)), a.at[:, here], acc.at[:, own], l.at[j], *(o.at[n, j] for n in range(3)),
                     dq, sl[h], scale, tq)

    def gout_body(i, ins, outs, ext):
        (a,), (o,), (_, dmb, *_) = ins, outs, ext
        o[:] = t_dot(a[:], dmb[:]).astype(BF16)

    pair = 2
    triple = lambda a: (a, (3, pair, seq, hd), lambda i: (0, i, 0, 0))
    pe = [Phase(nf, 2.4, [cols_of(d_up, ft), cols_of(fu, ft)], [], dh2_body),
          Phase(nm, 2, [rows_of(x1, tm), rows_of(dy, tm), whole(lns)], [rows_of(f32(seq, d), tm), one_vec], ln2b_body),
          Phase(d // slab, 1.9, [rows_of(fo, slab)], [], dattn_body),
          Phase(heads // pair, 6, [triple(qkv.reshape(3, heads, seq, hd)), cols_of(attn, pair * hd), heads_of(lse, pair), slopes],
                [triple(b16(3, heads, seq, hd))], battn_body),
          Phase(d // slab, 2, [cols_of(attn, slab)], [rows_of(b16(d, d), slab)], gout_body)]
    d_mid, g_ln2, d_qkv, g_out, *r2 = host('back', pe, S([(g_up, n_down)], [CARRY, n_down - CARRY], carry=r1[1:]),
                                          shared=[vm32(seq, d), vm16(seq, d), vm32(seq, hd)])
    d_qkv = d_qkv.reshape(3 * heads, seq, hd)

    no = d // SUB
    scat = S([(g_out, no), (pack, nu)], [CARRY, no, -nu], carry=r2[2:], last=True)

    def tile_copy(i, ext):
        r, q = Unit(RB, nq).at(i)
        return pltpu.make_async_copy(ext[1].at[rest(i, 2)], scat[0].written(-1).at[:, :, :, :, r, q], ext[2].at[rest(i, 2)])

    def macro_body(i, ins, outs, ext):
        (ht, dq, w), acc = ins, ext[0]
        tile = side_by_side(dq, per)
        r = dot(ht[:], tile).astype(BF16)
        if comm:
            ext[1][rest(i, 2)] = r.reshape(*CHIPS, 2, RB, SUB)
            tile_copy(i, ext).start()
        else:
            outs[0][:] = r
        put(acc, i, lambda: dot_t(tile, w[:]))

    def ship_body(i, ins, outs, ext):
        tile_copy(i, ext).wait()
        scat[0].ship(no + i)

    def ln1b_body(i, ins, outs, ext):
        (xr, dm, lw), (o, gwo) = ins, outs
        dx, gw = norm_back(ext[0][band(i)], xr[:].astype(F32), lw[pl.ds(0, 1)])
        o[:] = (dm[:] + dx).astype(BF16)
        put(gwo, i, lambda: gw)

    def join_body(i, ins, outs, ext):
        (low, high, up), (down_o, up_o) = ins, outs
        wide = up.shape[1]
        up_o[:, :wide] = up[:]
        up_o[:, wide:] = scat[0].refs[len(scat[0].ins)][:]
        for u in range(n_down):
            part, v = (low, u) if u * SUB < wide else (high, u - wide // SUB)
            down_o[pl.ds(u // no * RB, RB), pl.ds(u % no * SUB, SUB)] = part[:, pl.ds(v * SUB, SUB)]

    first = [] if comm else [cols_of(b16(d, nq), SUB)]
    pf = [Phase(nu, 3.9, [whole(h1t), heads_of(d_qkv, per), cols_of(fq, SUB)], first, macro_body),
          Phase(nm, 2, [rows_of(x, tm), rows_of(d_mid, tm), whole(lns)], [rows_of(act, tm), one_vec], ln1b_body)]
    if comm:
        pieces = r1[0], *r2[:2]
        pf.append(Phase(nu, 0, [], [], ship_body, 1))
        pf.append(Phase(1, 0, [(p, pltpu.VMEM, None) for p in pieces], [(o, o.shape, lambda i: (0, 0)) for o in (f32(ff // 32, d), f32(RB, ff))],
                        join_body, nu + nm))
        scat.append(SmallSum([g_ln2], d, nu + nm, 1))
    shared = [vm32(seq, d), vm16(2, *CHIPS, 2, RB, SUB), pltpu.SemaphoreType.DMA((2,))]
    got = host('last', pf, scat, shared=shared, fires=range(no + nu + 3 * LAG) if comm else None)
    if not comm:
        g_qkv, dx, g_ln1 = got
        return y, dx, g_ln1, g_qkv, g_out, g_ln2, g_up, g_down
    dx, _, g_down, g_up, _, g_out, g_qkv, _, sums = got
    return y, dx, sums, g_qkv, g_out, g_up, g_down


def solution(mesh):
    row_spec = P('fsdp')

    def step(x_in, ln1_w, w_qkv, w_out, ln2_w, w_up, w_down, dy_out):
        rows, _, heads, hd = w_qkv.shape
        d = x_in.shape[-1]
        lns = [w.reshape(1, rows) for w in (ln1_w, ln2_w)]
        wq = w_qkv.transpose(1, 2, 0, 3).reshape(-1, rows, hd)
        y, dx, sums, g_qkv, g_out, g_up, g_down = local_step(x_in[0], lns, wq, w_out, w_up, w_down, dy_out[0])
        g_qkv = g_qkv.reshape(3, heads, rows, hd).transpose(2, 0, 1, 3)
        return y[None], dx[None], sums[1, :rows], g_qkv, g_out, sums[0, :rows], g_up, g_down

    return jax.shard_map(step, mesh=mesh, in_specs=(row_spec,) * 8, out_specs=(row_spec,) * 8, check_vma=False)
```
